128 devices in a mesh: sub: 16 (over z, y), fsdp: 8 (over x, core).
Axes of the slice: x: 4, y: 4, z: 4, core: 2. Of those that a mesh axis runs over, the one named last changes fastest.
Arguments:
- x_in: bfloat16 [128, 192, 1536], P(('sub', 'fsdp'))
- w_q: bfloat16 [2, 1536, 12, 128], P(None, ('sub', 'fsdp'))
- w_k: bfloat16 [2, 1536, 2, 128], P(None, ('sub', 'fsdp'))
- w_v: bfloat16 [2, 1536, 2, 128], P(None, ('sub', 'fsdp'))
- w_o: bfloat16 [2, 1536, 12, 128], P(None, ('sub', 'fsdp'))
- w_up: bfloat16 [2, 1536, 8960], P(None, ('sub', 'fsdp'))
- w_down: bfloat16 [2, 8960, 1536], P(None, ('sub', 'fsdp'))
- grad_out: bfloat16 [128, 192, 1536], P(('sub', 'fsdp'))
Outputs:
- output 1: bfloat16 [128, 192, 1536], P(('sub', 'fsdp'))
- output 2: bfloat16 [128, 192, 1536], P(('sub', 'fsdp'))
- output 3: float32 [2, 1536, 12, 128], P(None, ('sub', 'fsdp'))
- output 4: float32 [2, 1536, 2, 128], P(None, ('sub', 'fsdp'))
- output 5: float32 [2, 1536, 2, 128], P(None, ('sub', 'fsdp'))
- output 6: float32 [2, 1536, 12, 128], P(None, ('sub', 'fsdp'))
- output 7: float32 [2, 1536, 8960], P(None, ('sub', 'fsdp'))
- output 8: float32 [2, 8960, 1536], P(None, ('sub', 'fsdp'))
All inputs are finite; a program needn't handle non-finite values.
Results may differ from the reference program's by a relative error of at most 0.02.
Values are sent between devices in bfloat16 or wider.
A program may use at most 1 GiB of HBM per device.

```python
import jax
import jax.numpy as jnp
from jax import lax

D = 1536
FF = 8960
HEADS = 12
KV_HEADS = 2
HEAD = 128
SEQ = 192
SEQS_DEV = 1
BLOCKS = 128
PAIRS = 2
EPS = 1e-6
MASK_FILL = -1e30

SEQS = BLOCKS * SEQS_DEV
ROWS = SEQS_DEV * SEQ
Q_PER_KV = HEADS // KV_HEADS
Q_WIDTH = HEADS * HEAD
KV_WIDTH = KV_HEADS * HEAD
SCALE = HEAD ** -0.5


def setup_inputs(seed: int = 0) -> dict:
    key_list = jax.random.split(jax.random.key(seed), 8)
    x_in = jax.random.normal(key_list[0], (SEQS, SEQ, D), jnp.float32)
    w_q = jax.random.normal(key_list[1], (PAIRS, D, HEADS, HEAD), jnp.float32) * D ** -0.5
    w_k = jax.random.normal(key_list[2], (PAIRS, D, KV_HEADS, HEAD), jnp.float32) * D ** -0.5
    w_v = jax.random.normal(key_list[3], (PAIRS, D, KV_HEADS, HEAD), jnp.float32) * D ** -0.5
    w_o = jax.random.normal(key_list[4], (PAIRS, D, HEADS, HEAD), jnp.float32) * (2.0 * (Q_WIDTH * PAIRS) ** -0.5)
    w_up = jax.random.normal(key_list[5], (PAIRS, D, FF), jnp.float32) * D ** -0.5
    w_down = jax.random.normal(key_list[6], (PAIRS, FF, D), jnp.float32) * (1.5 * (FF * PAIRS) ** -0.5)
    grad_out = jax.random.normal(key_list[7], (SEQS, SEQ, D), jnp.float32)
    arrays = {"x_in": x_in, "w_q": w_q, "w_k": w_k, "w_v": w_v, "w_o": w_o, "w_up": w_up, "w_down": w_down, "grad_out": grad_out}
    return {name: value.astype(jnp.bfloat16) for name, value in arrays.items()}


def rms_norm(values):
    return values * lax.rsqrt(jnp.mean(values * values, axis=-1, keepdims=True) + EPS)


def norm_bf16(x_blk):
    return rms_norm(x_blk.astype(jnp.float32)).astype(jnp.bfloat16)


def norm_back(x_blk, grad_norm):
    _, pull_back = jax.vjp(rms_norm, x_blk.astype(jnp.float32))
    return pull_back(grad_norm)[0]


def matmul(left, right):
    return jnp.dot(left, right, preferred_element_type=jnp.float32)


def attn_inner(x_blk, q_weight, k_weight, v_weight):
    normed = norm_bf16(x_blk)
    q_act = matmul(normed, q_weight.reshape(D, Q_WIDTH)).astype(jnp.bfloat16)
    k_act = matmul(normed, k_weight.reshape(D, KV_WIDTH)).astype(jnp.bfloat16)
    v_act = matmul(normed, v_weight.reshape(D, KV_WIDTH)).astype(jnp.bfloat16)
    q_grid = q_act.reshape(SEQS_DEV, SEQ, KV_HEADS, Q_PER_KV, HEAD).astype(jnp.float32)
    k_grid = k_act.reshape(SEQS_DEV, SEQ, KV_HEADS, HEAD).astype(jnp.float32)
    v_grid = v_act.reshape(SEQS_DEV, SEQ, KV_HEADS, HEAD).astype(jnp.float32)
    scores = jnp.einsum("bskge,btke->bkgst", q_grid, k_grid) * SCALE
    positions = jnp.arange(SEQ)
    causal = positions[:, None] >= positions[None, :]
    p_float = jax.nn.softmax(jnp.where(causal, scores, MASK_FILL), axis=-1)
    p_bf16 = p_float.astype(jnp.bfloat16)
    o_act = jnp.einsum("bkgst,btke->bskge", p_bf16.astype(jnp.float32), v_grid).astype(jnp.bfloat16)
    return normed, q_grid, k_grid, v_grid, p_float, p_bf16, o_act.reshape(ROWS, Q_WIDTH)


def attn_forward(x_blk, q_weight, k_weight, v_weight, o_weight):
    o_act = attn_inner(x_blk, q_weight, k_weight, v_weight)[6]
    proj = matmul(o_act, o_weight.reshape(D, Q_WIDTH).T)
    return (x_blk.astype(jnp.float32) + proj).astype(jnp.bfloat16)


def attn_backward(x_blk, q_weight, k_weight, v_weight, o_weight, grad_y):
    normed, q_grid, k_grid, v_grid, p_float, p_bf16, o_act = attn_inner(x_blk, q_weight, k_weight, v_weight)
    q_mat = q_weight.reshape(D, Q_WIDTH)
    k_mat = k_weight.reshape(D, KV_WIDTH)
    v_mat = v_weight.reshape(D, KV_WIDTH)
    d_o_w = matmul(grad_y.T, o_act)
    d_o = matmul(grad_y, o_weight.reshape(D, Q_WIDTH)).astype(jnp.bfloat16)
    d_o_grid = d_o.reshape(SEQS_DEV, SEQ, KV_HEADS, Q_PER_KV, HEAD).astype(jnp.float32)
    d_p = jnp.einsum("bskge,btke->bkgst", d_o_grid, v_grid)
    d_v = jnp.einsum("bkgst,bskge->btke", p_bf16.astype(jnp.float32), d_o_grid).astype(jnp.bfloat16)
    d_s = p_float * (d_p - jnp.sum(p_float * d_p, axis=-1, keepdims=True))
    ds_bf16 = (d_s * SCALE).astype(jnp.bfloat16).astype(jnp.float32)
    d_q = jnp.einsum("bkgst,btke->bskge", ds_bf16, k_grid).astype(jnp.bfloat16).reshape(ROWS, Q_WIDTH)
    d_k = jnp.einsum("bkgst,bskge->btke", ds_bf16, q_grid).astype(jnp.bfloat16).reshape(ROWS, KV_WIDTH)
    d_v = d_v.reshape(ROWS, KV_WIDTH)
    d_q_w = matmul(normed.T, d_q)
    d_k_w = matmul(normed.T, d_k)
    d_v_w = matmul(normed.T, d_v)
    d_norm = matmul(d_q, q_mat.T) + matmul(d_k, k_mat.T) + matmul(d_v, v_mat.T)
    grad_x = (grad_y.astype(jnp.float32) + norm_back(x_blk, d_norm)).astype(jnp.bfloat16)
    return (grad_x, d_q_w.reshape(D, HEADS, HEAD), d_k_w.reshape(D, KV_HEADS, HEAD),
            d_v_w.reshape(D, KV_HEADS, HEAD), d_o_w.reshape(D, HEADS, HEAD))


def mlp_forward(x_blk, up_weight, down_weight):
    normed = norm_bf16(x_blk)
    gelu_act = jax.nn.gelu(matmul(normed, up_weight)).astype(jnp.bfloat16)
    return (x_blk.astype(jnp.float32) + matmul(gelu_act, down_weight)).astype(jnp.bfloat16)


def mlp_backward(x_blk, up_weight, down_weight, grad_y):
    normed = norm_bf16(x_blk)
    gelu_f32, gelu_pull = jax.vjp(jax.nn.gelu, matmul(normed, up_weight))
    gelu_act = gelu_f32.astype(jnp.bfloat16)
    d_down = matmul(gelu_act.T, grad_y)
    d_hid = gelu_pull(matmul(grad_y, down_weight.T))[0].astype(jnp.bfloat16)
    d_up = matmul(normed.T, d_hid)
    d_norm = matmul(d_hid, up_weight.T)
    grad_x = (grad_y.astype(jnp.float32) + norm_back(x_blk, d_norm)).astype(jnp.bfloat16)
    return grad_x, d_up, d_down


def block_pass(x_blk, g_blk, weights):
    def fwd_step(carry_x, layer_w):
        q_weight, k_weight, v_weight, o_weight, up_weight, down_weight = layer_w
        mid_act = attn_forward(carry_x, q_weight, k_weight, v_weight, o_weight)
        out_act = mlp_forward(mid_act, up_weight, down_weight)
        return out_act, (carry_x, mid_act)

    y_blk, (attn_in, mlp_in) = lax.scan(fwd_step, x_blk, weights)

    def bwd_step(grad_act, packed):
        q_weight, k_weight, v_weight, o_weight, up_weight, down_weight, attn_x, mlp_x = packed
        grad_mid, d_up, d_down = mlp_backward(mlp_x, up_weight, down_weight, grad_act)
        grad_in, d_q, d_k, d_v, d_o = attn_backward(attn_x, q_weight, k_weight, v_weight, o_weight, grad_mid)
        return grad_in, (d_q, d_k, d_v, d_o, d_up, d_down)

    dx_blk, grads = lax.scan(bwd_step, g_blk, weights + (attn_in, mlp_in), reverse=True)
    return y_blk, dx_blk, grads


def reference(x_in, w_q, w_k, w_v, w_o, w_up, w_down, grad_out):
    weights = (w_q, w_k, w_v, w_o, w_up, w_down)
    x_blocks = x_in.reshape(BLOCKS, ROWS, D)
    g_blocks = grad_out.reshape(BLOCKS, ROWS, D)
    zero_grads = tuple(jnp.zeros(weight.shape, jnp.float32) for weight in weights)

    def block_step(acc_grads, pair_blk):
        y_blk, dx_blk, grads = block_pass(pair_blk[0], pair_blk[1], weights)
        acc_grads = tuple(prev_sum + block_grad for prev_sum, block_grad in zip(acc_grads, grads))
        return acc_grads, (y_blk, dx_blk)

    totals, (y_all, dx_all) = lax.scan(block_step, zero_grads, (x_blocks, g_blocks))
    return (y_all.reshape(SEQS, SEQ, D), dx_all.reshape(SEQS, SEQ, D),
            totals[0], totals[1], totals[2], totals[3], totals[4], totals[5])
```

```python
import jax
import jax.numpy as jnp
from jax import lax
from jax.sharding import Mesh, PartitionSpec as P

CHIP_AXES = ("z", "y", "x")
ALL_AXES = ("z", "y", "x", "c")
EPS = 1e-6
MASK_FILL = -1e30
BLOCK = 72


def rms_norm(values):
    return values * lax.rsqrt(jnp.mean(values * values, axis=-1, keepdims=True) + EPS)


def norm_bf16(x_loc):
    return rms_norm(x_loc.astype(jnp.float32)).astype(jnp.bfloat16)


def norm_back(x_loc, grad_norm):
    _, pull_back = jax.vjp(rms_norm, x_loc.astype(jnp.float32))
    return pull_back(grad_norm)[0]


def mixed(form, left, right):
    return jnp.einsum(form, left, right, preferred_element_type=jnp.float32)


def attn_inner(x_loc, halves, kv_heads, heads, head_dim):
    seq = x_loc.shape[0]
    q_width, kv_width = heads * head_dim, kv_heads * head_dim
    normed = norm_bf16(x_loc)
    qk = mixed("sd,dw->sw", normed, halves[0]).astype(jnp.bfloat16)
    v_act = mixed("sd,dw->sw", normed, halves[1][:, :kv_width]).astype(jnp.bfloat16)
    q_act = qk[:, :q_width].reshape(seq, kv_heads, heads // kv_heads, head_dim)
    k_act = qk[:, q_width:].reshape(seq, kv_heads, head_dim)
    v_act = v_act.reshape(seq, kv_heads, head_dim)
    scores = mixed("skge,tke->kgst", q_act, k_act) * (head_dim ** -0.5)
    positions = jnp.arange(seq)
    causal = positions[:, None] >= positions[None, :]
    p_float = jax.nn.softmax(jnp.where(causal, scores, MASK_FILL), axis=-1)
    p_bf16 = p_float.astype(jnp.bfloat16)
    o_act = mixed("kgst,tke->skge", p_bf16, v_act).astype(jnp.bfloat16)
    return normed, q_act, k_act, v_act, p_float, p_bf16, o_act.reshape(seq, q_width)


def attn_forward(x_loc, halves, dims):
    o_act = attn_inner(x_loc, halves, *dims)[6]
    proj = mixed("sw,dw->sd", o_act, halves[1][:, dims[0] * dims[2]:])
    return (x_loc.astype(jnp.float32) + proj).astype(jnp.bfloat16)


def attn_backward(x_loc, halves, dims, grad_y):
    kv_heads, heads, head_dim = dims
    seq = x_loc.shape[0]
    q_width, kv_width = heads * head_dim, kv_heads * head_dim
    normed, q_act, k_act, v_act, p_float, p_bf16, o_act = attn_inner(x_loc, halves, *dims)
    d_o_w = mixed("sd,sw->dw", grad_y, o_act)
    d_o = mixed("sd,dw->sw", grad_y, halves[1][:, kv_width:]).astype(jnp.bfloat16)
    d_o = d_o.reshape(seq, kv_heads, heads // kv_heads, head_dim)
    d_p = mixed("skge,tke->kgst", d_o, v_act)
    d_v = mixed("kgst,skge->tke", p_bf16, d_o).astype(jnp.bfloat16)
    d_s = p_float * (d_p - jnp.sum(p_float * d_p, axis=-1, keepdims=True))
    ds_bf16 = (d_s * (head_dim ** -0.5)).astype(jnp.bfloat16)
    d_q = mixed("kgst,tke->skge", ds_bf16, k_act).astype(jnp.bfloat16)
    d_k = mixed("kgst,skge->tke", ds_bf16, q_act).astype(jnp.bfloat16)
    d_qk = jnp.concatenate([d_q.reshape(seq, q_width), d_k.reshape(seq, kv_width)], axis=1)
    d_v = d_v.reshape(seq, kv_width)
    d_qk_w = mixed("sd,sw->dw", normed, d_qk)
    d_v_w = mixed("sd,sw->dw", normed, d_v)
    d_norm = mixed("sw,dw->sd", d_qk, halves[0]) + mixed("sw,dw->sd", d_v, halves[1][:, :kv_width])
    grad_x = (grad_y.astype(jnp.float32) + norm_back(x_loc, d_norm)).astype(jnp.bfloat16)
    grads = jnp.stack([d_qk_w.astype(jnp.bfloat16),
                       jnp.concatenate([d_v_w.astype(jnp.bfloat16), d_o_w.astype(jnp.bfloat16)], axis=1)])
    return grad_x, grads


def mlp_hidden(normed, up_halves):
    return jnp.concatenate([mixed("sd,df->sf", normed, up_halves[0]),
                            mixed("sd,df->sf", normed, up_halves[1])], axis=1)


def core_scatter(grad_halves):
    return lax.psum_scatter(grad_halves, "c", scatter_dimension=0, tiled=True)[0]


def solution(mesh):
    mesh4 = Mesh(mesh.devices.reshape(4, 4, 4, 2), ALL_AXES)
    row_spec = P(ALL_AXES)
    weight_spec = P(None, ALL_AXES)

    def body(x_in, w_q, w_k, w_v, w_o, w_up, w_down, grad_out):
        pairs, rows, heads, head_dim = w_q.shape
        kv_heads = w_k.shape[2]
        dims = (kv_heads, heads, head_dim)
        q_width, kv_width = heads * head_dim, kv_heads * head_dim
        half_w = q_width + kv_width
        ff_rows = w_down.shape[1]
        ff = w_up.shape[2]
        blocks = ff // ff_rows
        half_f = blocks * BLOCK // 2
        core = lax.axis_index("c")
        x_loc, g_loc = x_in[0], grad_out[0]

        attn_sh = jnp.concatenate([w_q.reshape(pairs, rows, q_width), w_k.reshape(pairs, rows, kv_width),
                                   w_v.reshape(pairs, rows, kv_width), w_o.reshape(pairs, rows, q_width)], axis=2)
        up_sh = jnp.pad(w_up.reshape(pairs, rows, blocks, ff_rows),
                        ((0, 0), (0, 0), (0, 0), (0, BLOCK - ff_rows))).reshape(pairs, rows, 2 * half_f)
        both = jnp.concatenate([attn_sh[:, :, :half_w], up_sh[:, :, :half_f],
                                attn_sh[:, :, half_w:], up_sh[:, :, half_f:]], axis=2)
        both = lax.all_gather(both, "c", axis=1, tiled=True)
        mine = lax.dynamic_slice_in_dim(both, core * (half_w + half_f), half_w + half_f, axis=2)
        attn_half, up_half = mine[:, :, :half_w], mine[:, :, half_w:]
        down_sh = jnp.pad(w_down, ((0, 0), (0, BLOCK - ff_rows), (0, 0)))

        def gather_halves(part):
            chip = lax.all_gather(part, CHIP_AXES, axis=0, tiled=True)
            return lax.all_gather(chip[None], "c", axis=0, tiled=True)

        def gather_down(part):
            return lax.all_gather(part, ALL_AXES, axis=0, tiled=True)

        def after(value, *deps):
            return lax.optimization_barrier((value,) + deps)[0]

        carry = x_loc
        inputs = []
        kept = []
        up_gate, down_gate = None, None
        for layer in range(pairs):
            attn_w = gather_halves(attn_half[layer])
            up_part = up_half[layer] if up_gate is None else after(up_half[layer], up_gate)
            up_w = gather_halves(up_part)
            down_part = after(down_sh[layer], up_w) if down_gate is None else after(down_sh[layer], up_w, down_gate)
            down_w = gather_down(down_part)
            inputs.append(carry)
            carry = attn_forward(carry, attn_w, dims)
            inputs.append(carry)
            normed = norm_bf16(carry)
            gelu_act = jax.nn.gelu(mlp_hidden(normed, up_w)).astype(jnp.bfloat16)
            up_gate = gelu_act
            proj = mixed("sf,fd->sd", gelu_act, down_w)
            carry = (carry.astype(jnp.float32) + proj).astype(jnp.bfloat16)
            down_gate = carry
            kept.append((attn_w, up_w, down_w))
        y_loc = carry

        grad_x = g_loc
        attn_out, up_out, down_out = [], [], []
        gate = None
        for layer in reversed(range(pairs)):
            if layer == pairs - 1:
                attn_w, up_w, down_w = kept[layer]
            else:
                down_w = gather_down(after(down_sh[layer], gate))
                up_w = gather_halves(after(up_half[layer], gate))
                attn_w = gather_halves(after(attn_half[layer], gate))
            mlp_x = inputs[2 * layer + 1]
            normed = norm_bf16(mlp_x)
            gelu_f32, gelu_pull = jax.vjp(jax.nn.gelu, mlp_hidden(normed, up_w))
            gelu_act = gelu_f32.astype(jnp.bfloat16)
            d_down = mixed("sf,sd->fd", gelu_act, grad_x).astype(jnp.bfloat16)
            d_hid = gelu_pull(mixed("sd,fd->sf", grad_x, down_w))[0].astype(jnp.bfloat16)
            d_up = jnp.stack([mixed("sd,sf->df", normed, d_hid[:, :half_f]).astype(jnp.bfloat16),
                              mixed("sd,sf->df", normed, d_hid[:, half_f:]).astype(jnp.bfloat16)])
            d_norm = mixed("sf,df->sd", d_hid[:, :half_f], up_w[0]) + mixed("sf,df->sd", d_hid[:, half_f:], up_w[1])
            grad_x = (grad_x.astype(jnp.float32) + norm_back(mlp_x, d_norm)).astype(jnp.bfloat16)
            gate = grad_x
            down_out.append(lax.psum_scatter(d_down, ALL_AXES, scatter_dimension=0, tiled=True))
            up_out.append(lax.psum_scatter(core_scatter(d_up), CHIP_AXES, scatter_dimension=0, tiled=True))
            grad_x, d_attn = attn_backward(inputs[2 * layer], attn_w, dims, grad_x)
            attn_out.append(lax.psum_scatter(core_scatter(d_attn), CHIP_AXES, scatter_dimension=0, tiled=True))

        down_grad = jnp.stack(down_out[::-1])[:, :ff_rows].astype(jnp.float32)
        merged = jnp.concatenate([jnp.stack(attn_out[::-1]), jnp.stack(up_out[::-1])], axis=2)
        merged = lax.all_gather(merged[:, :, None], "c", axis=2, tiled=True)
        merged = lax.dynamic_slice_in_dim(merged, core * rows, rows, axis=1).astype(jnp.float32)
        attn_grad = jnp.concatenate([merged[:, :, 0, :half_w], merged[:, :, 1, :half_w]], axis=2)
        up_grad = jnp.concatenate([merged[:, :, 0, half_w:], merged[:, :, 1, half_w:]], axis=2)
        up_grad = up_grad.reshape(pairs, rows, blocks, BLOCK)[:, :, :, :ff_rows].reshape(pairs, rows, ff)
        splits = [q_width, q_width + kv_width, q_width + 2 * kv_width]
        d_q, d_k, d_v, d_o = jnp.split(attn_grad, splits, axis=2)
        return (y_loc[None], grad_x[None],
                d_q.reshape(w_q.shape), d_k.reshape(w_k.shape), d_v.reshape(w_v.shape), d_o.reshape(w_o.shape),
                up_grad, down_grad)

    return jax.shard_map(body, mesh=mesh4, in_specs=(row_spec,) + (weight_spec,) * 6 + (row_spec,),
                         out_specs=(row_spec, row_spec) + (weight_spec,) * 6, check_vma=False)
```

```python
import functools

import jax
import jax.numpy as jnp
from jax import lax
from jax.experimental import pallas as pl
from jax.experimental.pallas import tpu as pltpu
from jax.sharding import Mesh, PartitionSpec as P

MESH = pl.DeviceIdType.MESH
ALL_AXES = ("z", "y", "x", "c")
CORE_MAJOR = ("c", "z", "y", "x")
EPS = 1e-6
MASK_FILL = -1e30


DIMS = ("z", "y", "x")
ORDERS = (("x", "y", "z"), ("y", "z", "x"), ("z", "x", "y"))
COLS = 256
ROWS = 24
LAG = 2


def _block(color, stage, position):
    dims = tuple(dim for dim in DIMS if dim not in ORDERS[color][:stage])
    return tuple(position if dim == ORDERS[color][stage] else slice(None) for dim in dims)


def grad_kernel(segments, n_chunks, n_in, *refs):
    arrays, out_ref = refs[:n_in], refs[n_in]
    (lhs, rhs, outgo, peer, sum0, sum1, sum2, sa0, ra0, sb0, rb0, sa1, ra1, sb1, rb1, sa2, ra2, sb2, rb2,
     load_sem, pair_send, pair_recv, ring_send, ring_recv, credit) = refs[n_in + 1:]
    sums = (sum0, sum1, sum2)
    half_bufs = ((sa0, ra0), (sa1, ra1), (sa2, ra2))
    full_bufs = ((sb0, rb0), (sb1, rb1), (sb2, rb2))
    core = lax.axis_index("c")
    place = {dim: lax.axis_index(dim) for dim in DIMS}
    nxt = {dim: lax.rem(place[dim] + 1, 4) for dim in DIMS}
    prv = {dim: lax.rem(place[dim] + 3, 4) for dim in DIMS}
    opp = {dim: lax.rem(place[dim] + 2, 4) for dim in DIMS}
    sibling = {"c": 1 - core}
    partners = [({dim: (nxt, prv)[way][dim]}, 2 * d + 1 - way, 2 * d + way)
                for d, dim in enumerate(DIMS) for way in range(2)]
    partners.append((sibling, 6, 6))

    barrier = pltpu.get_barrier_semaphore()
    for device, _, _ in partners:
        pl.semaphore_signal(barrier, inc=1, device_id=device, device_id_type=MESH)
    pl.semaphore_wait(barrier, len(partners))

    depth = 1 + 8 * LAG
    n_ticks = n_chunks + depth

    def load(lhs_ref, rhs_ref, slot, role):
        return (pltpu.make_async_copy(lhs_ref, lhs.at[slot, role], load_sem.at[slot, role, 0]),
                pltpu.make_async_copy(rhs_ref, rhs.at[slot, role], load_sem.at[slot, role, 1]))

    def fetch(chunk):
        slot = lax.rem(chunk, 4)
        for half in range(2):
            role = jnp.where(core == half, 0, 1)
            first = 0
            for count, lhs_name, lhs_start, rhs_name, rhs_start in segments[half]:
                @pl.when((chunk >= first) & (chunk < first + count))
                def _(first=first, lhs_name=lhs_name, lhs_start=lhs_start, rhs_name=rhs_name, rhs_start=rhs_start):
                    start = pl.multiple_of(rhs_start + (chunk - first) * COLS, COLS)
                    width = lhs.shape[-1]
                    for copy in load(arrays[lhs_name].at[:, lhs_start:lhs_start + width],
                                     arrays[rhs_name].at[:, pl.ds(start, COLS)], slot, role):
                        copy.start()
                first += count

    def pair_copy(slot):
        return pltpu.make_async_remote_copy(
            src_ref=outgo.at[slot], dst_ref=peer.at[slot], send_sem=pair_send.at[slot],
            recv_sem=pair_recv.at[slot], device_id=sibling, device_id_type=MESH)

    def multiply(chunk):
        slot = lax.rem(chunk, 4)
        for role in range(2):
            for copy in load(lhs.at[slot, role], rhs.at[slot, role], slot, role):
                copy.wait()
        quarter = lhs.shape[-1] // 4
        for role in (1, 0):
            for z in range(4):
                part = lax.dot_general(lhs[slot, role, :, quarter * z:quarter * z + quarter], rhs[slot, role],
                                       (((0,), (0,)), ((), ())), preferred_element_type=jnp.float32)
                if role == 0:
                    sum0[lax.rem(chunk, 8), z] = part.reshape(4, 4, ROWS, COLS)
                else:
                    outgo[slot, z] = part.astype(jnp.bfloat16).reshape(4, 4, ROWS, COLS)
        pair_copy(slot).start()

    def merge_pair(chunk):
        slot, lead = lax.rem(chunk, 4), lax.rem(chunk, 8)
        pair_copy(slot).wait_send()
        pair_copy(slot).wait_recv()
        for z in range(4):
            for y in range(4):
                sum0[lead, z, y] = sum0[lead, z, y] + peer[slot, z, y].astype(jnp.float32)

    def ring_copy(stage, part, slot, color, way):
        send, recv = (half_bufs, full_bufs)[part][stage]
        dim = ORDERS[color][stage]
        return pltpu.make_async_remote_copy(
            src_ref=send.at[slot, color, way], dst_ref=recv.at[slot, color, way],
            send_sem=ring_send.at[2 * stage + part, slot], recv_sem=ring_recv.at[2 * stage + part, slot],
            device_id={dim: (nxt, prv)[way][dim]}, device_id_type=MESH)

    def ring_wait(stage, part, slot):
        send, recv = (half_bufs, full_bufs)[part][stage]
        whole = pltpu.make_async_remote_copy(
            src_ref=send.at[slot], dst_ref=recv.at[slot],
            send_sem=ring_send.at[2 * stage + part, slot], recv_sem=ring_recv.at[2 * stage + part, slot],
            device_id=sibling, device_id_type=MESH)
        whole.wait_send()
        whole.wait_recv()

    def source(stage, chunk, color, position, cols):
        lead = lax.rem(chunk, 8)
        if stage == 0:
            return sum0[(lead,) + _block(color, 0, position) + (slice(8 * color, 8 * color + 8), cols)]
        return sums[stage][(lead, color) + _block(color, stage, position) + (slice(None), cols)]

    left, right, every = slice(0, COLS // 2), slice(COLS // 2, COLS), slice(0, COLS)

    def store_halves(stage, chunk):
        slot = lax.rem(chunk, 4)
        send = half_bufs[stage][0]
        for color in range(3):
            far = opp[ORDERS[color][stage]]
            send[slot, color, 0] = source(stage, chunk, color, far, left).astype(jnp.bfloat16)
            send[slot, color, 1] = source(stage, chunk, color, far, right).astype(jnp.bfloat16)

    def store_fulls(stage, chunk):
        slot = lax.rem(chunk, 4)
        ring_wait(stage, 0, slot)
        recv = half_bufs[stage][1]
        send = full_bufs[stage][0]
        lead = (slice(None),) * (len(send.shape) - 4)
        for color in range(3):
            dim = ORDERS[color][stage]
            for way, near, summed, plain in ((0, nxt, left, right), (1, prv, right, left)):
                send[(slot, color, way) + lead + (summed,)] = (
                    source(stage, chunk, color, near[dim], summed)
                    + recv[slot, color, way].astype(jnp.float32)).astype(jnp.bfloat16)
                send[(slot, color, way) + lead + (plain,)] = source(
                    stage, chunk, color, near[dim], plain).astype(jnp.bfloat16)

    def close_stage(stage, chunk):
        slot = lax.rem(chunk, 4)
        ring_wait(stage, 1, slot)
        recv = full_bufs[stage][1]
        for color in range(3):
            dim = ORDERS[color][stage]
            total = (source(stage, chunk, color, place[dim], every)
                     + recv[slot, color, 0].astype(jnp.float32)
                     + recv[slot, color, 1].astype(jnp.float32))
            if stage < 2:
                sums[stage + 1][lax.rem(chunk, 8), color] = total
            else:
                out_ref[chunk, 8 * color:8 * color + 8, :] = total

    def send_all(stage, part, chunk):
        slot = lax.rem(chunk, 4)
        for color in range(3):
            for way in range(2):
                ring_copy(stage, part, slot, color, way).start()

    def open_first(chunk):
        merge_pair(chunk)
        store_halves(0, chunk)
        send_all(0, 0, chunk)

    def middle(stage, chunk):
        store_fulls(stage, chunk)
        send_all(stage, 1, chunk)

    def turn(stage, chunk):
        close_stage(stage, chunk)
        if stage < 2:
            store_halves(stage + 1, chunk)
            send_all(stage + 1, 0, chunk)

    steps = [(0, fetch), (1 + 2 * LAG, functools.partial(middle, 0)), (1 + LAG, open_first),
             (1 + 3 * LAG, functools.partial(turn, 0)), (1 + 4 * LAG, functools.partial(middle, 1)),
             (1 + 5 * LAG, functools.partial(turn, 1)), (1 + 6 * LAG, functools.partial(middle, 2)),
             (1 + 7 * LAG, functools.partial(turn, 2)), (1, multiply)]

    def tick(now, carry):
        @pl.when(now >= 2)
        def _():
            for _, _, mine in partners:
                pl.semaphore_wait(credit.at[mine], 1)

        for lag, step in steps:
            @pl.when((now >= lag) & (now < lag + n_chunks))
            def _(lag=lag, step=step):
                step(now - lag)

        @pl.when(now < n_ticks - 2)
        def _():
            for device, theirs, _ in partners:
                pl.semaphore_signal(credit.at[theirs], inc=1, device_id=device, device_id_type=MESH)
        return carry

    lax.fori_loop(0, n_ticks, tick, 0)


def grad_scatter(arrays, segments):
    n_chunks = sum(segment[0] for segment in segments[0])
    seq = arrays[0].shape[0]
    width = 64 * ROWS
    bf16, f32 = jnp.bfloat16, jnp.float32
    half = COLS // 2
    scratch = [pltpu.VMEM((4, 2, seq, width), bf16), pltpu.VMEM((4, 2, seq, COLS), bf16),
               pltpu.VMEM((4, 4, 4, 4, ROWS, COLS), bf16), pltpu.VMEM((4, 4, 4, 4, ROWS, COLS), bf16),
               pltpu.VMEM((8, 4, 4, 4, ROWS, COLS), f32), pltpu.VMEM((8, 3, 4, 4, 8, COLS), f32),
               pltpu.VMEM((8, 3, 4, 8, COLS), f32)]
    for size in ((4, 4), (4,), ()):
        scratch += [pltpu.VMEM((4, 3, 2) + size + (8, half), bf16)] * 2
        scratch += [pltpu.VMEM((4, 3, 2) + size + (8, COLS), bf16)] * 2
    scratch += [pltpu.SemaphoreType.DMA((4, 2, 2)), pltpu.SemaphoreType.DMA((4,)), pltpu.SemaphoreType.DMA((4,)),
                pltpu.SemaphoreType.DMA((6, 4)), pltpu.SemaphoreType.DMA((6, 4)), pltpu.SemaphoreType.REGULAR((7,))]
    return pl.pallas_call(
        functools.partial(grad_kernel, segments, n_chunks, len(arrays)),
        name="grad_scatter",
        out_shape=jax.ShapeDtypeStruct((n_chunks, ROWS, COLS), f32),
        in_specs=[pl.BlockSpec(memory_space=pl.ANY)] * len(arrays),
        out_specs=pl.BlockSpec(memory_space=pltpu.VMEM),
        scratch_shapes=scratch,
        compiler_params=pltpu.CompilerParams(collective_id=0, has_side_effects=True,
                                             vmem_limit_bytes=60 * 1024 * 1024),
    )(*arrays)


def rms_norm(values):
    return values * lax.rsqrt(jnp.mean(values * values, axis=-1, keepdims=True) + EPS)


def norm_bf16(x_loc):
    return rms_norm(x_loc.astype(jnp.float32)).astype(jnp.bfloat16)


def norm_back(x_loc, grad_norm):
    _, pull_back = jax.vjp(rms_norm, x_loc.astype(jnp.float32))
    return pull_back(grad_norm)[0]


def mixed(form, left, right):
    return jnp.einsum(form, left, right, preferred_element_type=jnp.float32)


def attn_inner(x_loc, w_qk, w_v, kv_heads, heads, head_dim):
    seq = x_loc.shape[0]
    q_width = heads * head_dim
    normed = norm_bf16(x_loc)
    qk = mixed("sd,dw->sw", normed, w_qk).astype(jnp.bfloat16)
    v_act = mixed("sd,dw->sw", normed, w_v).astype(jnp.bfloat16)
    q_act = qk[:, :q_width].reshape(seq, kv_heads, heads // kv_heads, head_dim)
    k_act = qk[:, q_width:].reshape(seq, kv_heads, head_dim)
    v_act = v_act.reshape(seq, kv_heads, head_dim)
    scores = mixed("skge,tke->kgst", q_act, k_act) * (head_dim ** -0.5)
    positions = jnp.arange(seq)
    causal = positions[:, None] >= positions[None, :]
    p_float = jax.nn.softmax(jnp.where(causal, scores, MASK_FILL), axis=-1)
    p_bf16 = p_float.astype(jnp.bfloat16)
    o_act = mixed("kgst,tke->skge", p_bf16, v_act).astype(jnp.bfloat16)
    return normed, q_act, k_act, v_act, p_float, p_bf16, o_act.reshape(seq, q_width)


def attn_forward(x_loc, w_qk, w_v, w_o, dims):
    o_act = attn_inner(x_loc, w_qk, w_v, *dims)[6]
    proj = mixed("sw,dw->sd", o_act, w_o)
    return (x_loc.astype(jnp.float32) + proj).astype(jnp.bfloat16)


def attn_backward(x_loc, w_qk, w_v, w_o, dims, grad_y):
    kv_heads, heads, head_dim = dims
    seq = x_loc.shape[0]
    q_width, kv_width = heads * head_dim, kv_heads * head_dim
    normed, q_act, k_act, v_act, p_float, p_bf16, o_act = attn_inner(x_loc, w_qk, w_v, *dims)
    d_o = mixed("sd,dw->sw", grad_y, w_o).astype(jnp.bfloat16)
    d_o = d_o.reshape(seq, kv_heads, heads // kv_heads, head_dim)
    d_p = mixed("skge,tke->kgst", d_o, v_act)
    d_v = mixed("kgst,skge->tke", p_bf16, d_o).astype(jnp.bfloat16)
    d_s = p_float * (d_p - jnp.sum(p_float * d_p, axis=-1, keepdims=True))
    ds_bf16 = (d_s * (head_dim ** -0.5)).astype(jnp.bfloat16)
    d_q = mixed("kgst,tke->skge", ds_bf16, k_act).astype(jnp.bfloat16)
    d_k = mixed("kgst,skge->tke", ds_bf16, q_act).astype(jnp.bfloat16)
    d_qk = jnp.concatenate([d_q.reshape(seq, q_width), d_k.reshape(seq, kv_width)], axis=1)
    d_v = d_v.reshape(seq, kv_width)
    d_norm = mixed("sw,dw->sd", d_qk, w_qk) + mixed("sw,dw->sd", d_v, w_v)
    grad_x = (grad_y.astype(jnp.float32) + norm_back(x_loc, d_norm)).astype(jnp.bfloat16)
    return grad_x, [normed, d_qk, d_v, grad_y, o_act]


def solution(mesh):
    mesh4 = Mesh(mesh.devices.reshape(4, 4, 4, 2), ALL_AXES)
    row_spec = P(ALL_AXES)
    weight_spec = P(None, ALL_AXES)

    def body(x_in, w_q, w_k, w_v, w_o, w_up, w_down, grad_out):
        pairs, rows, heads, head_dim = w_q.shape
        kv_heads = w_k.shape[2]
        dims = (kv_heads, heads, head_dim)
        q_width, kv_width = heads * head_dim, kv_heads * head_dim
        half_w = q_width + kv_width
        ff_rows = w_down.shape[1]
        ff, width = w_up.shape[2], w_down.shape[2]
        chips = ff // ff_rows // 2
        ff_pad = 3 * ROWS
        half_f = chips * ff_pad
        core = lax.axis_index("c")
        x_loc, g_loc = x_in[0], grad_out[0]

        attn_sh = jnp.concatenate([w_q.reshape(pairs, rows, q_width), w_k.reshape(pairs, rows, kv_width),
                                   w_v.reshape(pairs, rows, kv_width), w_o.reshape(pairs, rows, q_width)], axis=2)
        up_sh = jnp.pad(w_up.reshape(pairs, rows, chips, 2, ff_rows),
                        ((0, 0), (0, 0), (0, 0), (0, 0), (0, ff_pad - ff_rows)))
        up_sh = up_sh.reshape(pairs, rows, chips, 2, 3, ROWS).transpose(0, 1, 3, 4, 2, 5)
        up_sh = up_sh.reshape(pairs, rows, 2 * half_f)
        both = jnp.concatenate([attn_sh[:, :, :half_w], up_sh[:, :, :half_f],
                                attn_sh[:, :, half_w:], up_sh[:, :, half_f:]], axis=2)
        both = lax.all_gather(both, "c", axis=1, tiled=True)
        mine = lax.dynamic_slice_in_dim(both, core * (half_w + half_f), half_w + half_f, axis=2)
        down_sh = jnp.pad(w_down, ((0, 0), (0, ff_pad - ff_rows), (0, 0)))
        down_sh = jnp.concatenate([down_sh[:, ROWS * part:ROWS * part + ROWS] for part in range(3)], axis=2)

        def gather(part):
            full = lax.all_gather(part, CORE_MAJOR, axis=0, tiled=True)
            return full.reshape(2, full.shape[0] // 2, full.shape[1])

        def after(value, *deps):
            return lax.optimization_barrier((value,) + deps)[0]

        def attn_weights(front):
            return front[0, :, :half_w], front[1, :, :kv_width], front[1, :, kv_width:half_w]

        def hidden(normed, front):
            return [mixed("sd,df->sf", normed, front[half, :, half_w:]) for half in range(2)]

        carry = x_loc
        inputs = []
        kept = []
        front_gate, down_gate = None, None
        for layer in range(pairs):
            front = gather(mine[layer] if front_gate is None else after(mine[layer], front_gate))
            down = gather(after(down_sh[layer], front) if down_gate is None
                          else after(down_sh[layer], front, down_gate))
            inputs.append(carry)
            carry = attn_forward(carry, *attn_weights(front), dims)
            inputs.append(carry)
            acts = [jax.nn.gelu(h).astype(jnp.bfloat16) for h in hidden(norm_bf16(carry), front)]
            front_gate = acts[1]
            proj = sum(mixed("sf,fd->sd", acts[half][:, width * part:width * part + width],
                             down[half, :, width * part:width * part + width])
                       for half in range(2) for part in range(3))
            carry = (carry.astype(jnp.float32) + proj).astype(jnp.bfloat16)
            down_gate = carry
            kept.append((front, down))
        y_loc = carry

        grad_x = g_loc
        outputs = []
        front_gate, down_gate = None, None
        for layer in reversed(range(pairs)):
            if layer == pairs - 1:
                front, down = kept[layer]
            else:
                down = gather(after(down_sh[layer], down_gate))
                front = gather(after(mine[layer], front_gate))
            mlp_x = inputs[2 * layer + 1]
            normed = norm_bf16(mlp_x)
            grad_y = grad_x
            acts, d_hids = [], []
            for half, h in enumerate(hidden(normed, front)):
                gelu_f32, gelu_pull = jax.vjp(jax.nn.gelu, h)
                acts.append(gelu_f32.astype(jnp.bfloat16))
                d_act = jnp.concatenate([mixed("sd,fd->sf", grad_y, down[half, :, width * part:width * part + width])
                                         for part in range(3)], axis=1)
                d_hids.append(gelu_pull(d_act)[0].astype(jnp.bfloat16))
            down_gate = d_hids[1]
            d_norm = sum(mixed("sf,df->sd", d_hids[half], front[half, :, half_w:]) for half in range(2))
            grad_x = (grad_y.astype(jnp.float32) + norm_back(mlp_x, d_norm)).astype(jnp.bfloat16)
            grad_x, attn_parts = attn_backward(inputs[2 * layer], *attn_weights(front), dims, grad_x)
            front_gate = grad_x
            outputs.append(attn_parts + [normed] + d_hids + acts + [grad_y])

        arrays, segments = [], [[], []]
        for parts in outputs[::-1]:
            base = len(arrays)
            arrays += parts
            n_at, dqk, dv, g_at, o_at, n_mlp, dh0, dh1, a0, a1, g_mlp = range(base, base + 11)
            segments[0] += [(half_w // COLS, n_at, 0, dqk, 0), (half_f // COLS, n_mlp, 0, dh0, 0)]
            segments[1] += [(kv_width // COLS, n_at, 0, dv, 0), (q_width // COLS, g_at, 0, o_at, 0),
                            (half_f // COLS, n_mlp, 0, dh1, 0)]
            for half, act in enumerate((a0, a1)):
                segments[half] += [(width // COLS, act, width * part, g_mlp, 0) for part in range(3)]
        summed = grad_scatter(arrays, segments)

        per_layer = summed.shape[0] // pairs
        wide = summed.reshape(pairs, per_layer, ROWS, COLS).transpose(0, 2, 1, 3).reshape(pairs, ROWS, -1)
        split = half_w + half_f
        down_grad = wide[:, :, split:].reshape(pairs, ROWS, 3, width).transpose(0, 2, 1, 3)
        down_grad = down_grad.reshape(pairs, ff_pad, width)[:, :ff_rows]
        merged = lax.all_gather(wide[:, :, None, :split], "c", axis=2, tiled=True)
        merged = lax.dynamic_slice_in_dim(merged, core * rows, rows, axis=1)
        attn_grad = jnp.concatenate([merged[:, :, 0, :half_w], merged[:, :, 1, :half_w]], axis=2)
        up_grad = merged[:, :, :, half_w:].reshape(pairs, rows, 2, 3, chips, ROWS).transpose(0, 1, 4, 2, 3, 5)
        up_grad = up_grad.reshape(pairs, rows, chips * 2, ff_pad)[:, :, :, :ff_rows].reshape(pairs, rows, ff)
        splits = [q_width, q_width + kv_width, q_width + 2 * kv_width]
        d_q, d_k, d_v, d_o = jnp.split(attn_grad, splits, axis=2)
        return (y_loc[None], grad_x[None],
                d_q.reshape(w_q.shape), d_k.reshape(w_k.shape), d_v.reshape(w_v.shape), d_o.reshape(w_o.shape),
                up_grad, down_grad)

    return jax.shard_map(body, mesh=mesh4, in_specs=(row_spec,) + (weight_spec,) * 6 + (row_spec,),
                         out_specs=(row_spec, row_spec) + (weight_spec,) * 6, check_vma=False)
```

```python
import functools

import jax
import jax.numpy as jnp
from jax import lax
from jax.experimental import pallas as pl
from jax.experimental.pallas import tpu as pltpu
from jax.sharding import Mesh, PartitionSpec as P

MESH = pl.DeviceIdType.MESH
ALL_AXES = ("z", "y", "x", "c")
CORE_MAJOR = ("c", "z", "y", "x")
EPS = 1e-6
MASK_FILL = -1e30


DIMS = ("z", "y", "x")
ORDERS = (("x", "y", "z"), ("y", "z", "x"), ("z", "x", "y"))
COLS = 256
ROWS = 24
LAG = 2


def _block(color, stage, position):
    dims = tuple(dim for dim in DIMS if dim not in ORDERS[color][:stage])
    return tuple(position if dim == ORDERS[color][stage] else slice(None) for dim in dims)


def grad_kernel(segments, n_chunks, n_in, *refs):
    arrays, out_ref = refs[:n_in], refs[n_in]
    (lhs, rhs, outgo, peer, sum0, sum1, sum2, sa0, ra0, sb0, rb0, sa1, ra1, sb1, rb1, sa2, ra2, sb2, rb2,
     load_sem, pair_send, pair_recv, ring_send, ring_recv, credit) = refs[n_in + 1:]
    sums = (sum0, sum1, sum2)
    half_bufs = ((sa0, ra0), (sa1, ra1), (sa2, ra2))
    full_bufs = ((sb0, rb0), (sb1, rb1), (sb2, rb2))
    core = lax.axis_index("c")
    place = {dim: lax.axis_index(dim) for dim in DIMS}
    nxt = {dim: lax.rem(place[dim] + 1, 4) for dim in DIMS}
    prv = {dim: lax.rem(place[dim] + 3, 4) for dim in DIMS}
    opp = {dim: lax.rem(place[dim] + 2, 4) for dim in DIMS}
    sibling = {"c": 1 - core}
    partners = [({dim: (nxt, prv)[way][dim]}, 2 * d + 1 - way, 2 * d + way)
                for d, dim in enumerate(DIMS) for way in range(2)]
    partners.append((sibling, 6, 6))

    barrier = pltpu.get_barrier_semaphore()
    for device, _, _ in partners:
        pl.semaphore_signal(barrier, inc=1, device_id=device, device_id_type=MESH)
    pl.semaphore_wait(barrier, len(partners))

    depth = 1 + 8 * LAG
    n_ticks = n_chunks + depth

    def load(lhs_ref, rhs_ref, slot, role):
        return (pltpu.make_async_copy(lhs_ref, lhs.at[slot, role], load_sem.at[slot, role, 0]),
                pltpu.make_async_copy(rhs_ref, rhs.at[slot, role], load_sem.at[slot, role, 1]))

    def fetch(chunk):
        slot = lax.rem(chunk, 4)
        for half in range(2):
            role = jnp.where(core == half, 0, 1)
            first = 0
            for count, lhs_name, lhs_start, rhs_name, rhs_start in segments[half]:
                @pl.when((chunk >= first) & (chunk < first + count))
                def _(first=first, lhs_name=lhs_name, lhs_start=lhs_start, rhs_name=rhs_name, rhs_start=rhs_start):
                    start = pl.multiple_of(rhs_start + (chunk - first) * COLS, COLS)
                    width = lhs.shape[-1]
                    for copy in load(arrays[lhs_name].at[:, lhs_start:lhs_start + width],
                                     arrays[rhs_name].at[:, pl.ds(start, COLS)], slot, role):
                        copy.start()
                first += count

    def pair_copy(slot):
        return pltpu.make_async_remote_copy(
            src_ref=outgo.at[slot], dst_ref=peer.at[slot], send_sem=pair_send.at[slot],
            recv_sem=pair_recv.at[slot], device_id=sibling, device_id_type=MESH)

    def multiply(chunk):
        slot = lax.rem(chunk, 4)
        for role in range(2):
            for copy in load(lhs.at[slot, role], rhs.at[slot, role], slot, role):
                copy.wait()
        quarter = lhs.shape[-1] // 4
        for role in (1, 0):
            for z in range(4):
                part = lax.dot_general(lhs[slot, role, :, quarter * z:quarter * z + quarter], rhs[slot, role],
                                       (((0,), (0,)), ((), ())), preferred_element_type=jnp.float32)
                if role == 0:
                    sum0[lax.rem(chunk, 8), z] = part.reshape(4, 4, ROWS, COLS)
                else:
                    outgo[slot, z] = part.astype(jnp.bfloat16).reshape(4, 4, ROWS, COLS)
        pair_copy(slot).start()

    def merge_pair(chunk):
        slot, lead = lax.rem(chunk, 4), lax.rem(chunk, 8)
        pair_copy(slot).wait_send()
        pair_copy(slot).wait_recv()
        for z in range(4):
            for y in range(4):
                sum0[lead, z, y] = sum0[lead, z, y] + peer[slot, z, y].astype(jnp.float32)

    def ring_copy(stage, part, slot, color, way):
        send, recv = (half_bufs, full_bufs)[part][stage]
        dim = ORDERS[color][stage]
        return pltpu.make_async_remote_copy(
            src_ref=send.at[slot, color, way], dst_ref=recv.at[slot, color, way],
            send_sem=ring_send.at[2 * stage + part, slot], recv_sem=ring_recv.at[2 * stage + part, slot],
            device_id={dim: (nxt, prv)[way][dim]}, device_id_type=MESH)

    def ring_wait(stage, part, slot):
        send, recv = (half_bufs, full_bufs)[part][stage]
        whole = pltpu.make_async_remote_copy(
            src_ref=send.at[slot], dst_ref=recv.at[slot],
            send_sem=ring_send.at[2 * stage + part, slot], recv_sem=ring_recv.at[2 * stage + part, slot],
            device_id=sibling, device_id_type=MESH)
        whole.wait_send()
        whole.wait_recv()

    def source(stage, chunk, color, position, cols):
        lead = lax.rem(chunk, 8)
        if stage == 0:
            return sum0[(lead,) + _block(color, 0, position) + (slice(8 * color, 8 * color + 8), cols)]
        return sums[stage][(lead, color) + _block(color, stage, position) + (slice(None), cols)]

    left, right, every = slice(0, COLS // 2), slice(COLS // 2, COLS), slice(0, COLS)

    def store_halves(stage, chunk):
        slot = lax.rem(chunk, 4)
        send = half_bufs[stage][0]
        for color in range(3):
            far = opp[ORDERS[color][stage]]
            send[slot, color, 0] = source(stage, chunk, color, far, left).astype(jnp.bfloat16)
            send[slot, color, 1] = source(stage, chunk, color, far, right).astype(jnp.bfloat16)

    def store_fulls(stage, chunk):
        slot = lax.rem(chunk, 4)
        ring_wait(stage, 0, slot)
        recv = half_bufs[stage][1]
        send = full_bufs[stage][0]
        lead = (slice(None),) * (len(send.shape) - 4)
        for color in range(3):
            dim = ORDERS[color][stage]
            for way, near, summed, plain in ((0, nxt, left, right), (1, prv, right, left)):
                send[(slot, color, way) + lead + (summed,)] = (
                    source(stage, chunk, color, near[dim], summed)
                    + recv[slot, color, way].astype(jnp.float32)).astype(jnp.bfloat16)
                send[(slot, color, way) + lead + (plain,)] = source(
                    stage, chunk, color, near[dim], plain).astype(jnp.bfloat16)

    def close_stage(stage, chunk):
        slot = lax.rem(chunk, 4)
        ring_wait(stage, 1, slot)
        recv = full_bufs[stage][1]
        for color in range(3):
            dim = ORDERS[color][stage]
            total = (source(stage, chunk, color, place[dim], every)
                     + recv[slot, color, 0].astype(jnp.float32)
                     + recv[slot, color, 1].astype(jnp.float32))
            if stage < 2:
                sums[stage + 1][lax.rem(chunk, 8), color] = total
            else:
                out_ref[chunk, 8 * color:8 * color + 8, :] = total

    def send_all(stage, part, chunk):
        slot = lax.rem(chunk, 4)
        for color in range(3):
            for way in range(2):
                ring_copy(stage, part, slot, color, way).start()

    def open_first(chunk):
        merge_pair(chunk)
        store_halves(0, chunk)
        send_all(0, 0, chunk)

    def middle(stage, chunk):
        store_fulls(stage, chunk)
        send_all(stage, 1, chunk)

    def turn(stage, chunk):
        close_stage(stage, chunk)
        if stage < 2:
            store_halves(stage + 1, chunk)
            send_all(stage + 1, 0, chunk)

    steps = [(0, fetch), (1 + 2 * LAG, functools.partial(middle, 0)), (1 + LAG, open_first),
             (1 + 3 * LAG, functools.partial(turn, 0)), (1 + 4 * LAG, functools.partial(middle, 1)),
             (1 + 5 * LAG, functools.partial(turn, 1)), (1 + 6 * LAG, functools.partial(middle, 2)),
             (1 + 7 * LAG, functools.partial(turn, 2)), (1, multiply)]

    def tick(now, carry):
        @pl.when(now >= 2)
        def _():
            for _, _, mine in partners:
                pl.semaphore_wait(credit.at[mine], 1)

        for lag, step in steps:
            @pl.when((now >= lag) & (now < lag + n_chunks))
            def _(lag=lag, step=step):
                step(now - lag)

        @pl.when(now < n_ticks - 2)
        def _():
            for device, theirs, _ in partners:
                pl.semaphore_signal(credit.at[theirs], inc=1, device_id=device, device_id_type=MESH)
        return carry

    lax.fori_loop(0, n_ticks, tick, 0)


def grad_scatter(arrays, segments):
    n_chunks = sum(segment[0] for segment in segments[0])
    seq = arrays[0].shape[0]
    width = 64 * ROWS
    bf16, f32 = jnp.bfloat16, jnp.float32
    half = COLS // 2
    scratch = [pltpu.VMEM((4, 2, seq, width), bf16), pltpu.VMEM((4, 2, seq, COLS), bf16),
               pltpu.VMEM((4, 4, 4, 4, ROWS, COLS), bf16), pltpu.VMEM((4, 4, 4, 4, ROWS, COLS), bf16),
               pltpu.VMEM((8, 4, 4, 4, ROWS, COLS), f32), pltpu.VMEM((8, 3, 4, 4, 8, COLS), f32),
               pltpu.VMEM((8, 3, 4, 8, COLS), f32)]
    for size in ((4, 4), (4,), ()):
        scratch += [pltpu.VMEM((4, 3, 2) + size + (8, half), bf16)] * 2
        scratch += [pltpu.VMEM((4, 3, 2) + size + (8, COLS), bf16)] * 2
    scratch += [pltpu.SemaphoreType.DMA((4, 2, 2)), pltpu.SemaphoreType.DMA((4,)), pltpu.SemaphoreType.DMA((4,)),
                pltpu.SemaphoreType.DMA((6, 4)), pltpu.SemaphoreType.DMA((6, 4)), pltpu.SemaphoreType.REGULAR((7,))]
    return pl.pallas_call(
        functools.partial(grad_kernel, segments, n_chunks, len(arrays)),
        name="grad_scatter",
        out_shape=jax.ShapeDtypeStruct((n_chunks, ROWS, COLS), f32),
        in_specs=[pl.BlockSpec(memory_space=pl.ANY)] * len(arrays),
        out_specs=pl.BlockSpec(memory_space=pltpu.VMEM),
        scratch_shapes=scratch,
        compiler_params=pltpu.CompilerParams(collective_id=0, has_side_effects=True,
                                             vmem_limit_bytes=60 * 1024 * 1024),
    )(*arrays)


PER_HALF = 43
HEAD = 128


def forward_kernel(n_layers, x_ref, shard, acts, w_out, wbuf, peer, state, normed, q_buf, k_buf, v_buf, gelu_buf, acc,
                   ring_send, ring_recv, pair_send, pair_recv, keep_sem, credit):
    core = lax.axis_index("c")
    place = {dim: lax.axis_index(dim) for dim in DIMS}
    nxt = {dim: lax.rem(place[dim] + 1, 4) for dim in DIMS}
    prv = {dim: lax.rem(place[dim] + 3, 4) for dim in DIMS}
    sibling = {"c": 1 - core}
    partners = [({dim: (nxt, prv)[way][dim]}, 2 * d + 1 - way, 2 * d + way)
                for d, dim in enumerate(DIMS) for way in range(2)]
    partners.append((sibling, 6, 6))
    slots = wbuf.shape[0]
    n_chunks = n_layers * PER_HALF
    ready = 6 * LAG
    last_lag = ready + 2
    n_ticks = n_chunks + last_lag
    seq, width = x_ref.shape
    third = 64 * ROWS

    barrier = pltpu.get_barrier_semaphore()
    for device, _, _ in partners:
        pl.semaphore_signal(barrier, inc=1, device_id=device, device_id_type=MESH)
    pl.semaphore_wait(barrier, len(partners))
    state[...] = x_ref[...]

    def columns(chunk):
        return pl.ds(pl.multiple_of(lax.rem(chunk, PER_HALF) * COLS, COLS), COLS)

    def spot(slot, color, stage, position, cols):
        order = ORDERS[color]
        index = []
        for dim in DIMS:
            if dim in order[:stage]:
                index.append(slice(None))
            else:
                index.append(position if dim == order[stage] else place[dim])
        return wbuf.at[(slot,) + tuple(index) + (slice(8 * color, 8 * color + 8), cols)]

    halves = (slice(0, COLS // 2), slice(COLS // 2, COLS))

    def send_own(stage, chunk):
        slot, sem = lax.rem(chunk, slots), lax.rem(chunk, 4)
        for color in range(3):
            dim = ORDERS[color][stage]
            here = spot(slot, color, stage, place[dim], slice(0, COLS))
            for way in range(2):
                source = here
                if stage == 0:
                    source = shard.at[chunk // PER_HALF, slice(8 * color, 8 * color + 8), columns(chunk)]
                pltpu.make_async_remote_copy(
                    src_ref=source, dst_ref=here, send_sem=ring_send.at[2 * stage, sem],
                    recv_sem=ring_recv.at[2 * stage, sem],
                    device_id={dim: (nxt, prv)[way][dim]}, device_id_type=MESH).start()

    def send_far(stage, chunk):
        slot, sem = lax.rem(chunk, slots), lax.rem(chunk, 4)
        for color in range(3):
            dim = ORDERS[color][stage]
            for way in range(2):
                block = spot(slot, color, stage, (prv, nxt)[way][dim], halves[way])
                pltpu.make_async_remote_copy(
                    src_ref=block, dst_ref=block, send_sem=ring_send.at[2 * stage + 1, sem],
                    recv_sem=ring_recv.at[2 * stage + 1, sem],
                    device_id={dim: (nxt, prv)[way][dim]}, device_id_type=MESH).start()

    def arrived(part, chunk):
        slot, sem = lax.rem(chunk, slots), lax.rem(chunk, 4)
        block = (wbuf.at[slot, 0, 0, 0:2], wbuf.at[slot, 0, 0, 0], wbuf.at[slot, 0, 0:2], wbuf.at[slot, 0, 0],
                 wbuf.at[slot, 0:2], wbuf.at[slot, 0])[part]
        whole = pltpu.make_async_remote_copy(src_ref=block, dst_ref=block, send_sem=ring_send.at[part, sem],
                                             recv_sem=ring_recv.at[part, sem], device_id=sibling,
                                             device_id_type=MESH)
        whole.wait_send()
        whole.wait_recv()

    def enter(chunk):
        wbuf[lax.rem(chunk, slots), place["z"], place["y"], place["x"]] = shard[chunk // PER_HALF, :, columns(chunk)]
        send_own(0, chunk)

    def pair_copy(chunk):
        slot = lax.rem(chunk, 4)
        return pltpu.make_async_remote_copy(
            src_ref=wbuf.at[lax.rem(chunk, slots)], dst_ref=peer.at[slot], send_sem=pair_send.at[slot],
            recv_sem=pair_recv.at[slot], device_id=sibling, device_id_type=MESH)

    def keep_copies(chunk):
        slot = lax.rem(chunk, 4)
        return (pltpu.make_async_copy(wbuf.at[lax.rem(chunk, slots)], w_out.at[core, :, :, :, :, columns(chunk)],
                                      keep_sem.at[0, slot]),
                pltpu.make_async_copy(peer.at[slot], w_out.at[1 - core, :, :, :, :, columns(chunk)],
                                      keep_sem.at[1, slot]))

    def exchange(chunk):
        arrived(5, chunk)
        pair_copy(chunk).start()

    def rms(values):
        wide = values.astype(jnp.float32)
        return (wide * lax.rsqrt(jnp.mean(wide * wide, axis=-1, keepdims=True) + EPS)).astype(jnp.bfloat16)

    def dot(left, right):
        return jnp.dot(left, right, preferred_element_type=jnp.float32)

    def dot_t(left, right):
        return lax.dot_general(left, right, (((1,), (1,)), ((), ())), preferred_element_type=jnp.float32)

    def compute(chunk):
        layer, index = chunk // PER_HALF, lax.rem(chunk, PER_HALF)
        pair = pair_copy(chunk)
        pair.wait_send()
        pair.wait_recv()
        keeping = chunk >= n_chunks - PER_HALF

        @pl.when(keeping)
        def _():
            for copy in keep_copies(chunk):
                copy.start()

        def weights(role):
            block = wbuf[lax.rem(chunk, slots)] if role == 0 else peer[lax.rem(chunk, 4)]
            return block.reshape(third, COLS)

        sides = ((0, core), (1, 1 - core))

        @pl.when(index == 0)
        def _():
            normed[...] = rms(state[...])

        @pl.when(index < 3)
        def _():
            for role, half in sides:
                start = pl.multiple_of(3 * COLS * half + COLS * index, COLS)
                q_buf[:, pl.ds(start, COLS)] = dot(normed[...], weights(role)).astype(jnp.bfloat16)

        @pl.when(index == 3)
        def _():
            for role, half in sides:
                both = dot(normed[...], weights(role)).astype(jnp.bfloat16)
                start = pl.multiple_of(HEAD * half, HEAD)
                k_buf[:, pl.ds(start, HEAD)] = both[:, :HEAD]
                v_buf[:, pl.ds(start, HEAD)] = both[:, HEAD:]

        @pl.when((index >= 4) & (index < 7))
        def _():
            rows = lax.broadcasted_iota(jnp.int32, (seq, seq), 0)
            cols = lax.broadcasted_iota(jnp.int32, (seq, seq), 1)
            for role, half in sides:
                start = pl.multiple_of(HEAD * half, HEAD)
                key, value = k_buf[:, pl.ds(start, HEAD)], v_buf[:, pl.ds(start, HEAD)]
                outs = []
                for head in range(2):
                    at = pl.multiple_of(3 * COLS * half + COLS * (index - 4) + HEAD * head, HEAD)
                    scores = dot_t(q_buf[:, pl.ds(at, HEAD)], key) * (HEAD ** -0.5)
                    scores = jnp.where(rows >= cols, scores, MASK_FILL)
                    weight = jnp.exp(scores - jnp.max(scores, axis=-1, keepdims=True))
                    prob = weight / jnp.sum(weight, axis=-1, keepdims=True)
                    outs.append(dot(prob.astype(jnp.bfloat16), value).astype(jnp.bfloat16))
                part = dot_t(jnp.concatenate(outs, axis=1), weights(role))
                if role == 0:
                    @pl.when(index == 4)
                    def _(part=part):
                        acc[...] = part

                    @pl.when(index > 4)
                    def _(part=part):
                        acc[...] += part
                else:
                    acc[...] += part

        @pl.when(index == 6)
        def _():
            middle = (state[...].astype(jnp.float32) + acc[...]).astype(jnp.bfloat16)
            state[...] = middle
            acts[2 * layer] = middle
            normed[...] = rms(middle)

        @pl.when((index >= 7) & (index < 25))
        def _():
            for role, half in sides:
                hidden = dot(normed[...], weights(role))
                start = pl.multiple_of(COLS * (index - 7), COLS)
                gelu_buf[half, :, pl.ds(start, COLS)] = jax.nn.gelu(hidden).astype(jnp.bfloat16)

        @pl.when(index >= 25)
        def _():
            part, block = (index - 25) // 6, lax.rem(index - 25, 6)
            start, at = pl.multiple_of(third * part, third), pl.multiple_of(COLS * block, COLS)
            total = sum(dot(gelu_buf[half, :, pl.ds(start, third)], weights(role)) for role, half in sides)

            @pl.when(part == 0)
            def _():
                acc[:, pl.ds(at, COLS)] = total

            @pl.when(part > 0)
            def _():
                acc[:, pl.ds(at, COLS)] += total

        @pl.when(index == PER_HALF - 1)
        def _():
            result = (state[...].astype(jnp.float32) + acc[...]).astype(jnp.bfloat16)
            state[...] = result
            acts[2 * layer + 1] = result

        @pl.when(keeping)
        def _():
            for copy in keep_copies(chunk):
                copy.wait()

    def forward(part, chunk):
        arrived(part, chunk)
        if part % 2 == 0:
            send_far(part // 2, chunk)
        else:
            send_own(part // 2 + 1, chunk)

    steps = [(0, enter)] + [((part + 1) * LAG, functools.partial(forward, part)) for part in range(5)]
    steps += [(ready, exchange), (last_lag, compute)]

    def tick(now, carry):
        @pl.when(now >= 2)
        def _():
            for _, _, mine in partners:
                pl.semaphore_wait(credit.at[mine], 1)

        for lag, step in steps:
            @pl.when((now >= lag) & (now < lag + n_chunks))
            def _(lag=lag, step=step):
                step(now - lag)

        @pl.when(now < n_ticks - 2)
        def _():
            for device, theirs, _ in partners:
                pl.semaphore_signal(credit.at[theirs], inc=1, device_id=device, device_id_type=MESH)
        return carry

    lax.fori_loop(0, n_ticks, tick, 0)


def forward_stack(x_loc, shards):
    n_layers = shards.shape[0]
    seq, width = x_loc.shape
    bf16, f32 = jnp.bfloat16, jnp.float32
    slots = 6 * LAG + 4
    chunk = (4, 4, 4, ROWS, COLS)
    return pl.pallas_call(
        functools.partial(forward_kernel, n_layers),
        name="forward_stack",
        out_shape=(jax.ShapeDtypeStruct((2 * n_layers, seq, width), bf16),
                   jax.ShapeDtypeStruct((2, 4, 4, 4, ROWS, PER_HALF * COLS), bf16)),
        in_specs=[pl.BlockSpec(memory_space=pltpu.VMEM)] * 2,
        out_specs=(pl.BlockSpec(memory_space=pltpu.VMEM), pl.BlockSpec(memory_space=pl.ANY)),
        scratch_shapes=[
            pltpu.VMEM((slots,) + chunk, bf16), pltpu.VMEM((4,) + chunk, bf16),
            pltpu.VMEM((seq, width), bf16), pltpu.VMEM((seq, width), bf16),
            pltpu.VMEM((seq, 6 * COLS), bf16), pltpu.VMEM((seq, 2 * HEAD), bf16), pltpu.VMEM((seq, 2 * HEAD), bf16),
            pltpu.VMEM((2, seq, 18 * COLS), bf16), pltpu.VMEM((seq, width), f32),
            pltpu.SemaphoreType.DMA((6, 4)), pltpu.SemaphoreType.DMA((6, 4)), pltpu.SemaphoreType.DMA((4,)),
            pltpu.SemaphoreType.DMA((4,)), pltpu.SemaphoreType.DMA((2, 4)), pltpu.SemaphoreType.REGULAR((7,))],
        compiler_params=pltpu.CompilerParams(collective_id=1, has_side_effects=True,
                                             vmem_limit_bytes=60 * 1024 * 1024),
    )(x_loc, shards)


def rms_norm(values):
    return values * lax.rsqrt(jnp.mean(values * values, axis=-1, keepdims=True) + EPS)


def norm_bf16(x_loc):
    return rms_norm(x_loc.astype(jnp.float32)).astype(jnp.bfloat16)


def norm_back(x_loc, grad_norm):
    _, pull_back = jax.vjp(rms_norm, x_loc.astype(jnp.float32))
    return pull_back(grad_norm)[0]


def mixed(form, left, right):
    return jnp.einsum(form, left, right, preferred_element_type=jnp.float32)


def attn_inner(x_loc, halves, heads, head_dim):
    seq = x_loc.shape[0]
    group = heads // 2 * head_dim
    normed = norm_bf16(x_loc)
    qkv = [mixed("sd,dw->sw", normed, half[:, :group + 2 * head_dim]).astype(jnp.bfloat16) for half in halves]
    q_act = jnp.stack([part[:, :group] for part in qkv], axis=1).reshape(seq, 2, heads // 2, head_dim)
    k_act = jnp.stack([part[:, group:group + head_dim] for part in qkv], axis=1)
    v_act = jnp.stack([part[:, group + head_dim:] for part in qkv], axis=1)
    scores = mixed("skge,tke->kgst", q_act, k_act) * (head_dim ** -0.5)
    positions = jnp.arange(seq)
    causal = positions[:, None] >= positions[None, :]
    p_float = jax.nn.softmax(jnp.where(causal, scores, MASK_FILL), axis=-1)
    p_bf16 = p_float.astype(jnp.bfloat16)
    o_act = mixed("kgst,tke->skge", p_bf16, v_act).astype(jnp.bfloat16)
    return normed, q_act, k_act, v_act, p_float, p_bf16, o_act.reshape(seq, heads * head_dim)


def attn_backward(x_loc, halves, heads, head_dim, grad_y):
    seq = x_loc.shape[0]
    group = heads // 2 * head_dim
    inner = group + 2 * head_dim
    normed, q_act, k_act, v_act, p_float, p_bf16, o_act = attn_inner(x_loc, halves, heads, head_dim)
    d_o = jnp.stack([mixed("sd,dw->sw", grad_y, half[:, inner:inner + group]).astype(jnp.bfloat16)
                     for half in halves], axis=1)
    d_o = d_o.reshape(seq, 2, heads // 2, head_dim)
    d_p = mixed("skge,tke->kgst", d_o, v_act)
    d_v = mixed("kgst,skge->tke", p_bf16, d_o).astype(jnp.bfloat16)
    d_s = p_float * (d_p - jnp.sum(p_float * d_p, axis=-1, keepdims=True))
    ds_bf16 = (d_s * (head_dim ** -0.5)).astype(jnp.bfloat16)
    d_q = mixed("kgst,tke->skge", ds_bf16, k_act).astype(jnp.bfloat16)
    d_k = mixed("kgst,skge->tke", ds_bf16, q_act).astype(jnp.bfloat16)
    d_qkv = [jnp.concatenate([d_q[:, kv].reshape(seq, group), d_k[:, kv], d_v[:, kv]], axis=1) for kv in range(2)]
    d_norm = sum(mixed("sw,dw->sd", d_qkv[kv], halves[kv][:, :inner]) for kv in range(2))
    grad_x = (grad_y.astype(jnp.float32) + norm_back(x_loc, d_norm)).astype(jnp.bfloat16)
    return grad_x, [normed] + d_qkv + [grad_y, o_act]


def solution(mesh):
    mesh4 = Mesh(mesh.devices.reshape(4, 4, 4, 2), ALL_AXES)
    row_spec = P(ALL_AXES)
    weight_spec = P(None, ALL_AXES)

    def body(x_in, w_q, w_k, w_v, w_o, w_up, w_down, grad_out):
        pairs, rows, heads, head_dim = w_q.shape
        kv_heads = w_k.shape[2]
        q_width, kv_width = heads * head_dim, kv_heads * head_dim
        half_w = q_width + kv_width
        ff_rows = w_down.shape[1]
        ff, width = w_up.shape[2], w_down.shape[2]
        chips = ff // ff_rows // 2
        ff_pad = 3 * ROWS
        half_f = chips * ff_pad
        core = lax.axis_index("c")
        x_loc, g_loc = x_in[0], grad_out[0]

        group = q_width // 2
        attn_sh = jnp.concatenate([w_q.reshape(pairs, rows, 2, group), w_k.reshape(pairs, rows, 2, head_dim),
                                   w_v.reshape(pairs, rows, 2, head_dim), w_o.reshape(pairs, rows, 2, group)], axis=3)
        up_sh = jnp.pad(w_up.reshape(pairs, rows, chips, 2, ff_rows),
                        ((0, 0), (0, 0), (0, 0), (0, 0), (0, ff_pad - ff_rows)))
        up_sh = up_sh.reshape(pairs, rows, chips, 2, 3, ROWS).transpose(0, 1, 3, 4, 2, 5)
        up_sh = up_sh.reshape(pairs, rows, 2, half_f)
        both = jnp.concatenate([attn_sh, up_sh], axis=3).reshape(pairs, rows, 2 * (half_w + half_f))
        both = lax.all_gather(both, "c", axis=1, tiled=True)
        mine = lax.dynamic_slice_in_dim(both, core * (half_w + half_f), half_w + half_f, axis=2)
        down_sh = jnp.pad(w_down, ((0, 0), (0, ff_pad - ff_rows), (0, 0)))
        down_sh = jnp.concatenate([down_sh[:, ROWS * part:ROWS * part + ROWS] for part in range(3)], axis=2)

        def gather(part):
            full = lax.all_gather(part, CORE_MAJOR, axis=0, tiled=True)
            return full.reshape(2, full.shape[0] // 2, full.shape[1])

        def after(value, *deps):
            return lax.optimization_barrier((value,) + deps)[0]

        def hidden(normed, ups):
            return [mixed("sd,df->sf", normed, ups[half]) for half in range(2)]

        acts_out, kept = forward_stack(x_loc, jnp.concatenate([mine, down_sh], axis=2))
        y_loc = acts_out[-1]
        inputs = [x_loc] + [acts_out[index] for index in range(2 * pairs - 1)]
        kept = kept.reshape(2, chips * ROWS, PER_HALF * COLS)

        grad_x = g_loc
        outputs = []
        front_gate, down_gate = None, None
        for layer in reversed(range(pairs)):
            if layer == pairs - 1:
                attns = [kept[half, :, :half_w] for half in range(2)]
                ups = [kept[half, :, half_w:half_w + half_f] for half in range(2)]
                downs = [kept[half, :, half_w + half_f:] for half in range(2)]
            else:
                down = gather(after(down_sh[layer], down_gate))
                front = gather(after(mine[layer], front_gate))
                attns = [front[half, :, :half_w] for half in range(2)]
                ups = [front[half, :, half_w:] for half in range(2)]
                downs = [down[half] for half in range(2)]
            mlp_x = inputs[2 * layer + 1]
            normed = norm_bf16(mlp_x)
            grad_y = grad_x
            acts, d_hids = [], []
            for half, h in enumerate(hidden(normed, ups)):
                gelu_f32, gelu_pull = jax.vjp(jax.nn.gelu, h)
                acts.append(gelu_f32.astype(jnp.bfloat16))
                d_act = jnp.concatenate([mixed("sd,fd->sf", grad_y, downs[half][:, width * part:width * part + width])
                                         for part in range(3)], axis=1)
                d_hids.append(gelu_pull(d_act)[0].astype(jnp.bfloat16))
            down_gate = d_hids[1]
            d_norm = sum(mixed("sf,df->sd", d_hids[half], ups[half]) for half in range(2))
            grad_x = (grad_y.astype(jnp.float32) + norm_back(mlp_x, d_norm)).astype(jnp.bfloat16)
            grad_x, attn_parts = attn_backward(inputs[2 * layer], attns, heads, head_dim, grad_x)
            front_gate = grad_x
            outputs.append(attn_parts + [normed] + d_hids + acts + [grad_y])

        arrays, segments = [], [[], []]
        for parts in outputs[::-1]:
            base = len(arrays)
            arrays += parts
            n_at, dqkv0, dqkv1, g_at, o_at, n_mlp, dh0, dh1, a0, a1, g_mlp = range(base, base + 11)
            for half, (dqkv, d_hid, act) in enumerate(((dqkv0, dh0, a0), (dqkv1, dh1, a1))):
                segments[half] += [((group + 2 * head_dim) // COLS, n_at, 0, dqkv, 0),
                                   (group // COLS, g_at, 0, o_at, group * half),
                                   (half_f // COLS, n_mlp, 0, d_hid, 0)]
                segments[half] += [(width // COLS, act, width * part, g_mlp, 0) for part in range(3)]
        summed = grad_scatter(arrays, segments)

        per_layer = summed.shape[0] // pairs
        wide = summed.reshape(pairs, per_layer, ROWS, COLS).transpose(0, 2, 1, 3).reshape(pairs, ROWS, -1)
        split = half_w + half_f
        down_grad = wide[:, :, split:].reshape(pairs, ROWS, 3, width).transpose(0, 2, 1, 3)
        down_grad = down_grad.reshape(pairs, ff_pad, width)[:, :ff_rows]
        merged = lax.all_gather(wide[:, :, None, :split], "c", axis=2, tiled=True)
        merged = lax.dynamic_slice_in_dim(merged, core * rows, rows, axis=1)
        up_grad = merged[:, :, :, half_w:].reshape(pairs, rows, 2, 3, chips, ROWS).transpose(0, 1, 4, 2, 3, 5)
        up_grad = up_grad.reshape(pairs, rows, chips * 2, ff_pad)[:, :, :, :ff_rows].reshape(pairs, rows, ff)
        cuts = [group, group + head_dim, group + 2 * head_dim]
        d_q, d_k, d_v, d_o = jnp.split(merged[:, :, :, :half_w], cuts, axis=3)
        return (y_loc[None], grad_x[None],
                d_q.reshape(w_q.shape), d_k.reshape(w_k.shape), d_v.reshape(w_v.shape), d_o.reshape(w_o.shape),
                up_grad, down_grad)

    return jax.shard_map(body, mesh=mesh4, in_specs=(row_spec,) + (weight_spec,) * 6 + (row_spec,),
                         out_specs=(row_spec, row_spec) + (weight_spec,) * 6, check_vma=False)
```

```python
import functools

import jax
import jax.numpy as jnp
from jax import lax
from jax.experimental import pallas as pl
from jax.experimental.pallas import tpu as pltpu
from jax.sharding import Mesh, PartitionSpec as P

MESH = pl.DeviceIdType.MESH
ALL_AXES = ("z", "y", "x", "c")
EPS = 1e-6
MASK_FILL = -1e30
DIMS = ("z", "y", "x")
ORDERS = (("x", "y", "z"), ("y", "z", "x"), ("z", "x", "y"))
COLS = 256
ROWS = 24
LAG = 2
HEAD = 128
PER_HALF = 43
UP_BLOCKS = 25
UP_END = UP_BLOCKS * COLS
RING = 4
CUBE = (RING, RING, RING)
SLOTS = 3
TILE = 8
COLORS = range(3)
TWO = range(2)
SIX = range(6)
ALL = Ellipsis
EVERY = slice(None)
QKV, ATTN, FF = 4, 7, 18
DOWN_DONE, UP_DONE, O_DONE = 18, 36, 39
G_AT, DH_AT, O_AT, QKV_AT = 0, 6, 42, 48
NORM_MLP, GRAD, NORM_ATTN = 6, 7, 8
VMEM_LIMIT = 67043328


FIFTH = UP_END // 5


def _rows(color):
    return slice(TILE * color, TILE * color + TILE)


def _rem(value, by):
    return lax.rem(value, by)


def _block(color, stage, position):
    dims = tuple(dim for dim in DIMS if dim not in ORDERS[color][:stage])
    return tuple(position if dim == ORDERS[color][stage] else EVERY for dim in dims)


def _dot(left, right):
    return jnp.dot(left, right, preferred_element_type=jnp.float32)


def _dot_rhs_t(left, right):
    return lax.dot_general(left, right, (((1,), (1,)), ((), ())), preferred_element_type=jnp.float32)


def _dot_lhs_t(left, right):
    return lax.dot_general(left, right, (((0,), (0,)), ((), ())), preferred_element_type=jnp.float32)


def _at(start, size):
    return pl.ds(pl.multiple_of(start, size), size)


def _causal(seq):
    return (lax.broadcasted_iota(jnp.int32, (seq, seq), 0) >= lax.broadcasted_iota(jnp.int32, (seq, seq), 1))


def _probs(query, key, causal):
    scores = jnp.where(causal, _dot_rhs_t(query, key) * (HEAD ** -0.5), MASK_FILL)
    weight = jnp.exp(scores - jnp.max(scores, axis=-1, keepdims=True))
    return weight / jnp.sum(weight, axis=-1, keepdims=True)


def _rms(values):
    wide = values.astype(jnp.float32)
    return (wide * lax.rsqrt(jnp.mean(wide * wide, axis=-1, keepdims=True) + EPS)).astype(jnp.bfloat16)


def _rms_back(values, grad):
    wide = values.astype(jnp.float32)
    scale = lax.rsqrt(jnp.mean(wide * wide, axis=-1, keepdims=True) + EPS)
    return scale * grad - wide * (scale * scale * scale) * jnp.mean(wide * grad, axis=-1, keepdims=True)


class Torus:
    def __init__(self, credit):
        self.core = lax.axis_index("c")
        self.place = {dim: lax.axis_index(dim) for dim in DIMS}
        self.near = tuple({dim: _rem(self.place[dim] + step, 4) for dim in DIMS} for step in (1, 3))
        self.far = {dim: _rem(self.place[dim] + 2, 4) for dim in DIMS}
        self.sibling = {"c": 1 - self.core}
        self.sides = ((0, self.core), (1, 1 - self.core))
        self.credit = credit
        self.partners = [({dim: self.near[way][dim]}, 2 * d + 1 - way, 2 * d + way)
                         for d, dim in enumerate(DIMS) for way in TWO]
        self.partners.append((self.sibling, 6, 6))

    def meet(self):
        barrier = pltpu.get_barrier_semaphore()
        for device, _, _ in self.partners:
            pl.semaphore_signal(barrier, inc=1, device_id=device, device_id_type=MESH)
        pl.semaphore_wait(barrier, len(self.partners))

    def remote(self, source, target, send_sem, recv_sem, device):
        return pltpu.make_async_remote_copy(src_ref=source, dst_ref=target, send_sem=send_sem, recv_sem=recv_sem,
                                            device_id=device, device_id_type=MESH)

    def run(self, steps, n_chunks, n_ticks):
        def tick(now, carry):
            @pl.when(now >= 2)
            def _():
                for _, _, mine in self.partners:
                    pl.semaphore_wait(self.credit.at[mine], 1)

            for lag, step in steps:
                @pl.when((now >= lag) & (now < lag + n_chunks))
                def _(lag=lag, step=step):
                    step(now - lag)

            @pl.when(now < n_ticks - 2)
            def _():
                for device, theirs, _ in self.partners:
                    pl.semaphore_signal(self.credit.at[theirs], inc=1, device_id=device, device_id_type=MESH)
            return carry

        lax.fori_loop(0, n_ticks, tick, 0)


def forward_kernel(n_layers, x_ref, rows_ref, down_ref, acts, w_out, hid_out, gelu_out, norm_out, q_out, k_out, v_out,
                   o_out, wbuf, peer, shard, twin, state, normed, q_buf, k_buf, v_buf, o_buf, gelu_buf, hid_buf, acc,
                   ring_send, ring_recv, pair_send, pair_recv, keep_sem, save_sem, hid_sem, twin_sem, credit):
    torus = Torus(credit)
    core, place, near = torus.core, torus.place, torus.near
    slots = wbuf.shape[0]
    n_chunks = n_layers * PER_HALF
    ready = 6 * LAG
    last_lag = ready + 2
    seq = x_ref.shape[0]
    third = 64 * ROWS
    torus.meet()
    swap = torus.remote(rows_ref.at[1 - core], twin, twin_sem.at[0], twin_sem.at[1], torus.sibling)
    swap.start()
    state[ALL] = x_ref[ALL]
    swap.wait_send()
    swap.wait_recv()
    for layer in range(n_layers):
        shard[layer, :, UP_END:] = down_ref[layer]
        for part in range(5):
            cols = slice(FIFTH * part, FIFTH * part + FIFTH)
            mine = rows_ref[core, layer, :, cols].astype(jnp.float32)
            other = twin[layer, :, cols].astype(jnp.float32)
            first = core == 0
            shard[layer, :, cols] = jnp.concatenate(
                [jnp.where(first, mine, other), jnp.where(first, other, mine)], axis=0).astype(jnp.bfloat16)

    def columns(chunk):
        return _at(_rem(chunk, PER_HALF) * COLS, COLS)

    def spot(slot, color, stage, position, cols):
        order = ORDERS[color]
        index = tuple(EVERY if dim in order[:stage] else position if dim == order[stage] else place[dim]
                      for dim in DIMS)
        return wbuf.at[(slot,) + index + (_rows(color), cols)]

    halves = (slice(0, COLS // 2), slice(COLS // 2, COLS))

    def send_own(stage, chunk):
        slot, sem = _rem(chunk, slots), _rem(chunk, RING)
        for color in COLORS:
            dim = ORDERS[color][stage]
            here = spot(slot, color, stage, place[dim], slice(0, COLS))
            source = here
            if stage == 0:
                source = shard.at[chunk // PER_HALF, _rows(color), columns(chunk)]
            for way in TWO:
                torus.remote(source, here, ring_send.at[2 * stage, sem], ring_recv.at[2 * stage, sem],
                             {dim: near[way][dim]}).start()

    def send_far(stage, chunk):
        slot, sem = _rem(chunk, slots), _rem(chunk, RING)
        for color in COLORS:
            dim = ORDERS[color][stage]
            for way in TWO:
                block = spot(slot, color, stage, near[1 - way][dim], halves[way])
                torus.remote(block, block, ring_send.at[2 * stage + 1, sem], ring_recv.at[2 * stage + 1, sem],
                             {dim: near[way][dim]}).start()

    def arrived(part, chunk):
        slot, sem = _rem(chunk, slots), _rem(chunk, RING)
        block = (wbuf.at[slot, 0, 0, 0:2], wbuf.at[slot, 0, 0, 0], wbuf.at[slot, 0, 0:2], wbuf.at[slot, 0, 0],
                 wbuf.at[slot, 0:2], wbuf.at[slot, 0])[part]
        whole = torus.remote(block, block, ring_send.at[part, sem], ring_recv.at[part, sem], torus.sibling)
        whole.wait_send()
        whole.wait_recv()

    def enter(chunk):
        wbuf[_rem(chunk, slots), place["z"], place["y"], place["x"]] = shard[chunk // PER_HALF, :, columns(chunk)]
        send_own(0, chunk)

    def pass_on(part, chunk):
        arrived(part, chunk)
        if part % 2 == 0:
            send_far(part // 2, chunk)
        else:
            send_own(part // 2 + 1, chunk)

    def pair_copy(chunk):
        slot = _rem(chunk, RING)
        return torus.remote(wbuf.at[_rem(chunk, slots)], peer.at[slot], pair_send.at[slot], pair_recv.at[slot],
                            torus.sibling)

    def exchange(chunk):
        arrived(5, chunk)
        pair_copy(chunk).start()

    def keep_copy(chunk):
        return pltpu.make_async_copy(wbuf.at[_rem(chunk, slots)],
                                     w_out.at[chunk // PER_HALF, :, :, :, :, columns(chunk)],
                                     keep_sem.at[_rem(chunk, RING)])

    def save_copies(layer, names):
        parts = {"n0": (normed, norm_out.at[layer, 0], 0), "n1": (normed, norm_out.at[layer, 1], 1),
                 "q": (q_buf, q_out.at[layer], 2), "k": (k_buf, k_out.at[layer], 3), "v": (v_buf, v_out.at[layer], 4),
                 "o": (o_buf, o_out.at[layer], 5)}
        for half in TWO:
            for part in COLORS:
                parts[f"a{half}{part}"] = (gelu_buf.at[half, :, slice(third * part, third * (part + 1))],
                                           gelu_out.at[layer, 3 * half + part], 6 + 3 * half + part)
        return [pltpu.make_async_copy(parts[name][0], parts[name][1], save_sem.at[parts[name][2]]) for name in names]

    gelu_names = [f"a{half}{part}" for half in TWO for part in COLORS]

    def hidden_copies(layer, order):
        slot, part, at = _rem(order, 2), order // 6, _at(_rem(order, 6) * COLS, COLS)
        return [pltpu.make_async_copy(hid_buf.at[slot, half], hid_out.at[layer, part, half, :, at],
                                      hid_sem.at[slot, half]) for half in TWO]

    def compute(chunk):
        layer, index = chunk // PER_HALF, _rem(chunk, PER_HALF)
        pair = pair_copy(chunk)
        pair.wait_send()
        pair.wait_recv()
        keep_copy(chunk).start()

        def weights(role):
            block = wbuf[_rem(chunk, slots)] if role == 0 else peer[_rem(chunk, RING)]
            return block.reshape(third, COLS)

        @pl.when(index == 0)
        def _():
            normed[ALL] = _rms(state[ALL])
            for copy in save_copies(layer, ["n0"]):
                copy.start()

        @pl.when(index < 3)
        def _():
            for role, half in torus.sides:
                q_buf[:, _at(3 * COLS * half + COLS * index, COLS)] = _dot(
                    normed[ALL], weights(role)).astype(jnp.bfloat16)

        @pl.when(index == 3)
        def _():
            for role, half in torus.sides:
                both = _dot(normed[ALL], weights(role)).astype(jnp.bfloat16)
                k_buf[:, _at(HEAD * half, HEAD)] = both[:, :HEAD]
                v_buf[:, _at(HEAD * half, HEAD)] = both[:, HEAD:]

        @pl.when(index == QKV)
        def _():
            acc[ALL] = jnp.zeros_like(acc)
            for copy in save_copies(layer, ["q", "k", "v"]):
                copy.start()

        @pl.when((index >= QKV) & (index < ATTN))
        def _():
            causal = _causal(seq)
            for role, half in torus.sides:
                key, value = k_buf[:, _at(HEAD * half, HEAD)], v_buf[:, _at(HEAD * half, HEAD)]
                outs = []
                for head in TWO:
                    at = _at(3 * COLS * half + COLS * (index - QKV) + HEAD * head, HEAD)
                    prob = _probs(q_buf[:, at], key, causal)
                    outs.append(_dot(prob.astype(jnp.bfloat16), value).astype(jnp.bfloat16))
                block = jnp.concatenate(outs, axis=1)
                o_buf[3 * half + index - QKV] = block
                acc[ALL] += _dot_rhs_t(block, weights(role))

        @pl.when(index == 6)
        def _():
            middle = (state[ALL].astype(jnp.float32) + acc[ALL]).astype(jnp.bfloat16)
            state[ALL] = middle
            acts[2 * layer] = middle
            for copy in save_copies(layer, ["n0"]):
                copy.wait()
            normed[ALL] = _rms(middle)
            for copy in save_copies(layer, ["n1", "o"]):
                copy.start()

        @pl.when((index >= 8) & (index < 26))
        def _():
            for copy in hidden_copies(layer, index - 8):
                copy.wait()

        @pl.when((index >= ATTN) & (index < UP_BLOCKS))
        def _():
            for role, half in torus.sides:
                hidden = _dot(normed[ALL], weights(role))
                hid_buf[_rem(index - ATTN, 2), half] = hidden
                gelu_buf[half, :, _at(COLS * (index - ATTN), COLS)] = jax.nn.gelu(hidden).astype(jnp.bfloat16)
            for copy in hidden_copies(layer, index - ATTN):
                copy.start()

        @pl.when(index == UP_BLOCKS)
        def _():
            for copy in save_copies(layer, gelu_names):
                copy.start()

        @pl.when(index >= UP_BLOCKS)
        def _():
            part, at = (index - UP_BLOCKS) // 6, _at(COLS * _rem(index - UP_BLOCKS, 6), COLS)
            total = sum(_dot(gelu_buf[half, :, _at(third * part, third)], weights(role))
                        for role, half in torus.sides)

            @pl.when(part == 0)
            def _():
                acc[:, at] = total

            @pl.when(part > 0)
            def _():
                acc[:, at] += total

        @pl.when(index == PER_HALF - 1)
        def _():
            result = (state[ALL].astype(jnp.float32) + acc[ALL]).astype(jnp.bfloat16)
            state[ALL] = result
            acts[2 * layer + 1] = result
            for copy in save_copies(layer, ["n1", "q", "k", "v", "o"] + gelu_names):
                copy.wait()

        keep_copy(chunk).wait()

    steps = [(0, enter)] + [((part + 1) * LAG, functools.partial(pass_on, part)) for part in range(5)]
    torus.run(steps + [(ready, exchange), (last_lag, compute)], n_chunks, n_chunks + last_lag)


def forward_stack(x_loc, rows, down):
    n_layers = down.shape[0]
    seq, width = x_loc.shape
    bf16, f32 = jnp.bfloat16, jnp.float32
    slots = 6 * LAG + 4
    chunk = CUBE + (ROWS, COLS)
    shape = jax.ShapeDtypeStruct
    hbm = pl.BlockSpec(memory_space=pl.ANY)
    vmem = pl.BlockSpec(memory_space=pltpu.VMEM)
    dma = pltpu.SemaphoreType.DMA
    return pl.pallas_call(
        functools.partial(forward_kernel, n_layers),
        name="forward_stack",
        out_shape=(shape((2 * n_layers, seq, width), bf16),
                   shape((n_layers, 4, 4, 4, ROWS, PER_HALF * COLS), bf16),
                   shape((n_layers, 3, 2, seq, width), f32), shape((n_layers, 6, seq, width), bf16),
                   shape((n_layers, 2, seq, width), bf16), shape((n_layers, seq, width), bf16),
                   shape((n_layers, seq, 2 * HEAD), bf16), shape((n_layers, seq, 2 * HEAD), bf16),
                   shape((n_layers, 6, seq, COLS), bf16)),
        in_specs=[vmem] * 3,
        out_specs=(vmem,) + (hbm,) * 8,
        scratch_shapes=[
            pltpu.VMEM((slots,) + chunk, bf16), pltpu.VMEM((RING,) + chunk, bf16),
            pltpu.VMEM((n_layers, ROWS, PER_HALF * COLS), bf16), pltpu.VMEM(rows.shape[1:], bf16),
            pltpu.VMEM((seq, width), bf16), pltpu.VMEM((seq, width), bf16),
            pltpu.VMEM((seq, 6 * COLS), bf16), pltpu.VMEM((seq, 2 * HEAD), bf16), pltpu.VMEM((seq, 2 * HEAD), bf16),
            pltpu.VMEM((6, seq, COLS), bf16), pltpu.VMEM((2, seq, 18 * COLS), bf16),
            pltpu.VMEM((2, 2, seq, COLS), f32), pltpu.VMEM((seq, width), f32),
            dma((6, RING)), dma((6, RING)), dma((RING,)), dma((RING,)), dma((RING,)), dma((12,)), dma((2, 2)), dma((2,)),
            pltpu.SemaphoreType.REGULAR((7,))],
        compiler_params=pltpu.CompilerParams(collective_id=1, has_side_effects=True,
                                             vmem_limit_bytes=VMEM_LIMIT),
    )(x_loc, rows, down)


def backward_kernel(n_layers, *refs):
    (g_ref, x_ref, acts, w_own, hid_in, gelu_in, norm_in, q_in, k_in, v_in, o_in,
     rows_out, down_out, dx_ref,
     mine, theirs, lefts, rights, hid_buf, dact, dnorm, q_buf, k_buf, v_buf, x_mid, x_in, dk_acc, dv_acc,
     outgo, peer, out, away, sum0, sum1, sum2, sa0, ra0, sb0, rb0, sa1, ra1, sb1, rb1, sa2, ra2, sb2, rb2,
     load_sem, own_sem, push_send, push_recv, pair_send, pair_recv, ring_send, ring_recv, swap_sem, credit) = refs
    torus = Torus(credit)
    core, place, near = torus.core, torus.place, torus.near
    sums = (sum0, sum1, sum2)
    half_bufs = ((sa0, ra0), (sa1, ra1), (sa2, ra2))
    full_bufs = ((sb0, rb0), (sb1, rb1), (sb2, rb2))
    n_chunks = n_layers * PER_HALF
    seq, width = g_ref.shape
    third = 64 * ROWS
    leads = sum0.shape[0]

    def pair_of(chunk):
        return n_layers - 1 - chunk // PER_HALF

    def columns(chunk):
        index = _rem(chunk, PER_HALF)
        block = jnp.where(index < DOWN_DONE, UP_BLOCKS + index,
                          jnp.where(index < UP_DONE, index - 11, jnp.where(index < O_DONE, index - 32, index - 39)))
        return _at(block * COLS, COLS)

    def loads(pair, names):
        def source(name):
            return {"a": (gelu_in.at[pair], lefts.at[0:6], 0), "n_mlp": (norm_in.at[pair, 1], lefts.at[NORM_MLP], 1),
                    "n_attn": (norm_in.at[pair, 0], lefts.at[NORM_ATTN], 2), "o": (o_in.at[pair], rights.at[O_AT:QKV_AT], 3),
                    "q": (q_in.at[pair], q_buf, 4), "k": (k_in.at[pair], k_buf, 5), "v": (v_in.at[pair], v_buf, 6),
                    "x_mid": (acts.at[2 * pair], x_mid, 7), "h0": (hid_in.at[pair, 0], hid_buf, 8),
                    "h1": (hid_in.at[pair, 1], hid_buf, 8), "h2": (hid_in.at[pair, 2], hid_buf, 8)}[name]
        return [pltpu.make_async_copy(source(name)[0], source(name)[1], load_sem.at[source(name)[2]])
                for name in names]

    def start(pair, names):
        for copy in loads(pair, names):
            copy.start()

    def finish(pair, names):
        for copy in loads(pair, names):
            copy.wait()

    def first_input(ref):
        return pltpu.make_async_copy(ref, x_in, load_sem.at[9])

    torus.meet()
    start(n_layers - 1, ["a"])
    for block in SIX:
        rights[block] = g_ref[:, COLS * block:COLS * block + COLS]

    def own_copy(chunk):
        slot = _rem(chunk, SLOTS)
        return pltpu.make_async_copy(w_own.at[pair_of(chunk), :, :, :, :, columns(chunk)], mine.at[slot],
                                     own_sem.at[slot])

    def push_copy(chunk):
        slot = _rem(chunk, SLOTS)
        return torus.remote(w_own.at[pair_of(chunk), :, :, :, :, columns(chunk)], theirs.at[slot],
                            push_send.at[slot], push_recv.at[slot], torus.sibling)

    def fetch(chunk):
        own_copy(chunk).start()
        push_copy(chunk).start()

    def total_grad():
        return jnp.concatenate([rights[block] for block in SIX], axis=1).astype(jnp.float32)

    def consume(chunk):
        pair, index = pair_of(chunk), _rem(chunk, PER_HALF)
        slot = _rem(chunk, SLOTS)
        own_copy(chunk).wait()
        push = push_copy(chunk)
        push.wait_send()
        push.wait_recv()

        def weights(role):
            return (mine, theirs)[role][slot].reshape(third, COLS)

        @pl.when(index == 0)
        def _():
            start(pair, ["n_mlp", "n_attn", "o", "q", "k", "v", "x_mid", "h0"])

            @pl.when(pair == 0)
            def _():
                first_input(x_ref).start()

            @pl.when(pair > 0)
            def _():
                first_input(acts.at[2 * pair - 1]).start()
            finish(pair, ["a"])

        for part in (1, 2):
            @pl.when(index == 6 * part)
            def _(part=part):
                start(pair, [f"h{part}"])

        @pl.when(index < DOWN_DONE)
        def _():
            block = _rem(index, 6)
            for role, half in torus.sides:
                product = _dot_rhs_t(rights[block], weights(role))

                @pl.when(block == 0)
                def _(product=product, half=half):
                    dact[half] = product

                @pl.when(block > 0)
                def _(product=product, half=half):
                    dact[half] += product

        @pl.when((index < DOWN_DONE) & (_rem(index, 6) == 5))
        def _():
            finish(pair, ["h0"])
            for half in TWO:
                for block in SIX:
                    cols = slice(COLS * block, COLS * block + COLS)
                    hidden = hid_buf[half, :, cols]
                    bend = jnp.tanh(0.7978845608028654 * (hidden + 0.044715 * (hidden * hidden * hidden)))
                    slope = 0.5 * (1.0 + bend) + 0.5 * hidden * (1.0 - bend * bend) * (
                        0.7978845608028654 * (1.0 + 0.134145 * (hidden * hidden)))
                    rights[DH_AT + FF * half + index - 5 + block] = (dact[half, :, cols] * slope).astype(jnp.bfloat16)

        @pl.when(index == DOWN_DONE)
        def _():
            finish(pair, ["n_mlp"])
            dnorm[ALL] = jnp.zeros_like(dnorm)

            @pl.when(pair > 0)
            def _():
                start(pair - 1, ["a"])

        @pl.when((index >= DOWN_DONE) & (index < UP_DONE))
        def _():
            dnorm[ALL] += sum(_dot_rhs_t(rights[DH_AT + FF * half + index - DOWN_DONE], weights(role))
                              for role, half in torus.sides)

        @pl.when(index == UP_DONE - 1)
        def _():
            finish(pair, ["x_mid"])
            lefts[GRAD] = (total_grad() + _rms_back(x_mid[ALL], dnorm[ALL])).astype(jnp.bfloat16)

        @pl.when(index == UP_DONE)
        def _():
            finish(pair, ["o", "q", "k", "v"])
            dk_acc[ALL] = jnp.zeros_like(dk_acc)
            dv_acc[ALL] = jnp.zeros_like(dv_acc)

        @pl.when((index >= UP_DONE) & (index < O_DONE))
        def _():
            causal = _causal(seq)
            for role, half in torus.sides:
                d_o = _dot(lefts[GRAD], weights(role)).astype(jnp.bfloat16)
                key, value = k_buf[:, _at(HEAD * half, HEAD)], v_buf[:, _at(HEAD * half, HEAD)]
                d_q = []
                for head in TWO:
                    query = q_buf[:, _at(3 * COLS * half + COLS * (index - UP_DONE) + HEAD * head, HEAD)]
                    d_head = d_o[:, HEAD * head:HEAD * head + HEAD]
                    prob = _probs(query, key, causal)
                    d_prob = _dot_rhs_t(d_head, value)
                    dv_acc[half] += _dot_lhs_t(prob.astype(jnp.bfloat16), d_head)
                    d_score = prob * (d_prob - jnp.sum(prob * d_prob, axis=-1, keepdims=True))
                    d_score = (d_score * (HEAD ** -0.5)).astype(jnp.bfloat16)
                    d_q.append(_dot(d_score, key).astype(jnp.bfloat16))
                    dk_acc[half] += _dot_lhs_t(d_score, query)
                rights[QKV_AT + QKV * half + index - UP_DONE] = jnp.concatenate(d_q, axis=1)

        @pl.when(index == O_DONE - 1)
        def _():
            for half in TWO:
                rights[QKV_AT + QKV * half + QKV - 1] = jnp.concatenate([dk_acc[half], dv_acc[half]], axis=1).astype(jnp.bfloat16)

        @pl.when(index == O_DONE)
        def _():
            finish(pair, ["n_attn"])
            dnorm[ALL] = jnp.zeros_like(dnorm)

        @pl.when(index >= O_DONE)
        def _():
            dnorm[ALL] += sum(_dot_rhs_t(rights[QKV_AT + QKV * half + index - O_DONE], weights(role))
                              for role, half in torus.sides)

        @pl.when(index == PER_HALF - 1)
        def _():
            first_input(x_ref).wait()
            result = (lefts[GRAD].astype(jnp.float32) + _rms_back(x_in[ALL], dnorm[ALL])).astype(jnp.bfloat16)
            dx_ref[ALL] = result
            for block in SIX:
                rights[block] = result[:, COLS * block:COLS * block + COLS]

    def pair_copy(slot):
        return torus.remote(outgo.at[slot], peer.at[slot], pair_send.at[slot], pair_recv.at[slot], torus.sibling)

    def multiply(chunk):
        index = _rem(chunk, PER_HALF)
        slot = _rem(chunk, RING)
        quarter = third // RING
        for role, half in torus.sides[::-1]:
            left = jnp.where(index < DOWN_DONE, 3 * half + index // 6,
                             jnp.where(index < UP_DONE, NORM_MLP, jnp.where(index < O_DONE, GRAD, NORM_ATTN)))
            right = jnp.where(index < DOWN_DONE, _rem(index, 6),
                              jnp.where(index < UP_DONE, DH_AT + FF * half + index - DOWN_DONE,
                                        jnp.where(index < O_DONE, O_AT + 3 * half + index - UP_DONE, QKV_AT + QKV * half + index - O_DONE)))
            for z in range(RING):
                part = _dot_lhs_t(lefts[left, :, quarter * z:quarter * z + quarter], rights[right])
                if role == 0:
                    sum0[_rem(chunk, leads), z] = part.reshape(RING, RING, ROWS, COLS)
                else:
                    outgo[slot, z] = part.astype(jnp.bfloat16).reshape(RING, RING, ROWS, COLS)
        pair_copy(slot).start()

    def merge_pair(chunk):
        slot, lead = _rem(chunk, RING), _rem(chunk, leads)
        pair_copy(slot).wait_send()
        pair_copy(slot).wait_recv()
        for z in range(RING):
            for y in range(RING):
                sum0[lead, z, y] = sum0[lead, z, y] + peer[slot, z, y].astype(jnp.float32)

    def ring_copy(stage, part, slot, color, way):
        send, recv = (half_bufs, full_bufs)[part][stage]
        dim = ORDERS[color][stage]
        return torus.remote(send.at[slot, color, way], recv.at[slot, color, way],
                            ring_send.at[2 * stage + part, slot], ring_recv.at[2 * stage + part, slot],
                            {dim: near[way][dim]})

    def ring_wait(stage, part, slot):
        send, recv = (half_bufs, full_bufs)[part][stage]
        whole = torus.remote(send.at[slot], recv.at[slot], ring_send.at[2 * stage + part, slot],
                             ring_recv.at[2 * stage + part, slot], torus.sibling)
        whole.wait_send()
        whole.wait_recv()

    def source(stage, chunk, color, position, cols):
        lead = _rem(chunk, leads)
        if stage == 0:
            return sum0[(lead,) + _block(color, 0, position) + (_rows(color), cols)]
        return sums[stage][(lead, color) + _block(color, stage, position) + (EVERY, cols)]

    left_cols, right_cols, every = slice(0, COLS // 2), slice(COLS // 2, COLS), slice(0, COLS)

    def store_halves(stage, chunk):
        slot = _rem(chunk, RING)
        send = half_bufs[stage][0]
        for color in COLORS:
            far = torus.far[ORDERS[color][stage]]
            send[slot, color, 0] = source(stage, chunk, color, far, left_cols).astype(jnp.bfloat16)
            send[slot, color, 1] = source(stage, chunk, color, far, right_cols).astype(jnp.bfloat16)

    def store_fulls(stage, chunk):
        slot = _rem(chunk, RING)
        ring_wait(stage, 0, slot)
        recv = half_bufs[stage][1]
        send = full_bufs[stage][0]
        lead = (EVERY,) * (len(send.shape) - 4)
        for color in COLORS:
            dim = ORDERS[color][stage]
            for way, summed, plain in ((0, left_cols, right_cols), (1, right_cols, left_cols)):
                send[(slot, color, way) + lead + (summed,)] = (
                    source(stage, chunk, color, near[way][dim], summed)
                    + recv[slot, color, way].astype(jnp.float32)).astype(jnp.bfloat16)
                send[(slot, color, way) + lead + (plain,)] = source(
                    stage, chunk, color, near[way][dim], plain).astype(jnp.bfloat16)

    def close_stage(stage, chunk):
        slot = _rem(chunk, RING)
        ring_wait(stage, 1, slot)
        recv = full_bufs[stage][1]
        for color in COLORS:
            dim = ORDERS[color][stage]
            total = (source(stage, chunk, color, place[dim], every)
                     + recv[slot, color, 0].astype(jnp.float32)
                     + recv[slot, color, 1].astype(jnp.float32))
            if stage < 2:
                sums[stage + 1][_rem(chunk, leads), color] = total
            else:
                out[pair_of(chunk), _rows(color), columns(chunk)] = total

    def send_all(stage, part, chunk):
        for color in COLORS:
            for way in TWO:
                ring_copy(stage, part, _rem(chunk, RING), color, way).start()

    def open_first(chunk):
        merge_pair(chunk)
        store_halves(0, chunk)
        send_all(0, 0, chunk)

    def middle(stage, chunk):
        store_fulls(stage, chunk)
        send_all(stage, 1, chunk)

    def turn(stage, chunk):
        close_stage(stage, chunk)
        if stage < 2:
            store_halves(stage + 1, chunk)
            send_all(stage + 1, 0, chunk)

    base = 1
    steps = [(0, fetch), (base + 2 * LAG, functools.partial(middle, 0)), (base + LAG, open_first),
             (base + 3 * LAG, functools.partial(turn, 0)), (base + 4 * LAG, functools.partial(middle, 1)),
             (base + 5 * LAG, functools.partial(turn, 1)), (base + 6 * LAG, functools.partial(middle, 2)),
             (base + 7 * LAG, functools.partial(turn, 2)), (base, consume), (base, multiply)]
    torus.run(steps, n_chunks, n_chunks + base + 7 * LAG)

    half_rows = ROWS // 2
    for layer in range(n_layers):
        for part in range(5):
            cols = slice(FIFTH * part, FIFTH * part + FIFTH)
            both = out[layer, :, cols]
            low, high = both[:half_rows], both[half_rows:]
            rows_out[core, layer, :, cols] = jnp.where(core == 0, low, high)
            away[layer, :, cols] = jnp.where(core == 0, high, low)
    swap = torus.remote(away, rows_out.at[core], swap_sem.at[0], swap_sem.at[1], torus.sibling)
    down_out[ALL] = out[:, :, UP_END:]
    swap.start()
    swap.wait_send()
    swap.wait_recv()


def backward_stack(n_layers, g_loc, *saved):
    seq, width = g_loc.shape
    bf16, f32 = jnp.bfloat16, jnp.float32
    half = COLS // 2
    chunk = CUBE + (ROWS, COLS)
    leads = 7
    shape = jax.ShapeDtypeStruct
    hbm = pl.BlockSpec(memory_space=pl.ANY)
    vmem = pl.BlockSpec(memory_space=pltpu.VMEM)
    dma = pltpu.SemaphoreType.DMA
    half_rows = ROWS // 2
    scratch = [pltpu.VMEM((SLOTS,) + chunk, bf16), pltpu.VMEM((SLOTS,) + chunk, bf16),
               pltpu.VMEM((9, seq, width), bf16), pltpu.VMEM((56, seq, COLS), bf16),
               pltpu.VMEM((2, seq, width), f32), pltpu.VMEM((2, seq, width), f32), pltpu.VMEM((seq, width), f32),
               pltpu.VMEM((seq, 6 * COLS), bf16), pltpu.VMEM((seq, 2 * HEAD), bf16), pltpu.VMEM((seq, 2 * HEAD), bf16),
               pltpu.VMEM((seq, width), bf16), pltpu.VMEM((seq, width), bf16),
               pltpu.VMEM((2, seq, HEAD), f32), pltpu.VMEM((2, seq, HEAD), f32),
               pltpu.VMEM((RING,) + chunk, bf16), pltpu.VMEM((RING,) + chunk, bf16),
               pltpu.VMEM((n_layers, ROWS, PER_HALF * COLS), f32), pltpu.VMEM((n_layers, half_rows, UP_END), f32),
               pltpu.VMEM((leads,) + chunk, f32), pltpu.VMEM((leads, 3, RING, RING, TILE, COLS), f32),
               pltpu.VMEM((leads, 3, RING, TILE, COLS), f32)]
    for size in ((RING, RING), (RING,), ()):
        scratch += [pltpu.VMEM((RING, 3, 2) + size + (TILE, half), bf16)] * 2
        scratch += [pltpu.VMEM((RING, 3, 2) + size + (TILE, COLS), bf16)] * 2
    scratch += [dma((10,)), dma((SLOTS,)), dma((SLOTS,)), dma((SLOTS,)), dma((RING,)), dma((RING,)), dma((6, RING)), dma((6, RING)), dma((2,)),
                pltpu.SemaphoreType.REGULAR((7,))]
    return pl.pallas_call(
        functools.partial(backward_kernel, n_layers),
        name="backward_stack",
        out_shape=(shape((2, n_layers, half_rows, UP_END), f32),
                   shape((n_layers, ROWS, (PER_HALF - UP_BLOCKS) * COLS), f32), shape((seq, width), bf16)),
        in_specs=[vmem] + [hbm] * len(saved),
        out_specs=(vmem,) * 3,
        scratch_shapes=scratch,
        compiler_params=pltpu.CompilerParams(collective_id=0, has_side_effects=True,
                                             vmem_limit_bytes=VMEM_LIMIT),
    )(g_loc, *saved)


def solution(mesh):
    mesh4 = Mesh(mesh.devices.reshape(CUBE + (2,)), ALL_AXES)
    row_spec = P(ALL_AXES)
    weight_spec = P(None, ALL_AXES)

    def body(x_in, w_q, w_k, w_v, w_o, w_up, w_down, grad_out):
        pairs, rows, heads, head_dim = w_q.shape
        group = heads // 2 * head_dim
        half_w = 2 * group + 2 * head_dim
        ff_rows = w_down.shape[1]
        ff, width = w_up.shape[2], w_down.shape[2]
        chips = ff // ff_rows // 2
        ff_pad = 3 * ROWS
        half_f = chips * ff_pad
        x_loc, g_loc = x_in[0], grad_out[0]

        attn_sh = jnp.concatenate([w_q.reshape(pairs, rows, 2, group), w_k.reshape(pairs, rows, 2, head_dim),
                                   w_v.reshape(pairs, rows, 2, head_dim), w_o.reshape(pairs, rows, 2, group)], axis=3)
        up_sh = jnp.pad(w_up.reshape(pairs, rows, chips, 2, ff_rows),
                        ((0, 0), (0, 0), (0, 0), (0, 0), (0, ff_pad - ff_rows)))
        up_sh = up_sh.reshape(pairs, rows, chips, 2, 3, ROWS).transpose(0, 1, 3, 4, 2, 5)
        up_sh = up_sh.reshape(pairs, rows, 2, half_f)
        rows_sh = jnp.concatenate([attn_sh, up_sh], axis=3).transpose(2, 0, 1, 3)
        down_sh = jnp.pad(w_down, ((0, 0), (0, ff_pad - ff_rows), (0, 0)))
        down_sh = jnp.concatenate([down_sh[:, ROWS * part:ROWS * part + ROWS] for part in COLORS], axis=2)

        acts, *saved = forward_stack(x_loc, rows_sh, down_sh)
        row_grad, down_grad, grad_x = backward_stack(pairs, g_loc, x_loc, acts, *saved)

        down_grad = down_grad.reshape(pairs, ROWS, 3, width).transpose(0, 2, 1, 3)
        down_grad = down_grad.reshape(pairs, ff_pad, width)[:, :ff_rows]
        row_grad = row_grad.transpose(1, 2, 0, 3)
        up_grad = row_grad[:, :, :, half_w:].reshape(pairs, rows, 2, 3, chips, ROWS).transpose(0, 1, 4, 2, 3, 5)
        up_grad = up_grad.reshape(pairs, rows, chips * 2, ff_pad)[:, :, :, :ff_rows].reshape(pairs, rows, ff)
        cuts = [group, group + head_dim, group + 2 * head_dim]
        d_q, d_k, d_v, d_o = jnp.split(row_grad[:, :, :, :half_w], cuts, axis=3)
        return (acts[2 * pairs - 1][None], grad_x[None],
                d_q.reshape(w_q.shape), d_k.reshape(w_k.shape), d_v.reshape(w_v.shape), d_o.reshape(w_o.shape),
                up_grad, down_grad)

    return jax.shard_map(body, mesh=mesh4, in_specs=(row_spec,) + (weight_spec,) * 6 + (row_spec,),
                         out_specs=(row_spec, row_spec) + (weight_spec,) * 6, check_vma=False)
```

```python
import functools
import math

import jax
import jax.numpy as jnp
from jax import lax
from jax.experimental import pallas as pl
from jax.experimental.pallas import tpu as pltpu
from jax.sharding import Mesh, PartitionSpec as P

MESH = pl.DeviceIdType.MESH
ALL_AXES = ("z", "y", "x", "c")
EPS = 1e-6
MASK_FILL = -1e30
DIMS = ("z", "y", "x")
ORDERS = (("x", "y", "z"), ("y", "z", "x"), ("z", "x", "y"))
COLS = 256
ROWS = 24
LAG = 2
HEAD = 128
PER_HALF = 43
UP_BLOCKS = 25
UP_END = UP_BLOCKS * COLS
RING = 4
CUBE = (RING, RING, RING)
SLOTS = 3
TILE = 8
COLORS = range(3)
TWO = range(2)
SIX = range(6)
ALL = Ellipsis
EVERY = slice(None)
QKV, ATTN, FF = 4, 7, 18
DOWN_DONE, UP_DONE, O_DONE = 18, 36, 39
G_AT, DH_AT, O_AT, QKV_AT = 0, 6, 42, 48
NORM_MLP, GRAD, NORM_ATTN = 6, 7, 8
VMEM_LIMIT = 67043328


FIFTH = UP_END // 5


def _rows(color):
    return slice(TILE * color, TILE * color + TILE)


def _rem(value, by):
    return lax.rem(value, by)


def _block(color, stage, position):
    dims = tuple(dim for dim in DIMS if dim not in ORDERS[color][:stage])
    return tuple(position if dim == ORDERS[color][stage] else EVERY for dim in dims)


def _dot(left, right):
    return jnp.dot(left, right, preferred_element_type=jnp.float32)


def _dot_rhs_t(left, right):
    return lax.dot_general(left, right, (((1,), (1,)), ((), ())), preferred_element_type=jnp.float32)


def _dot_lhs_t(left, right):
    return lax.dot_general(left, right, (((0,), (0,)), ((), ())), preferred_element_type=jnp.float32)


def _at(start, size):
    return pl.ds(pl.multiple_of(start, size), size)


def _causal(seq):
    return (lax.broadcasted_iota(jnp.int32, (seq, seq), 0) >= lax.broadcasted_iota(jnp.int32, (seq, seq), 1))


def _probs(query, key, causal):
    scores = jnp.where(causal, _dot_rhs_t(query, key) * (HEAD ** -0.5), MASK_FILL)
    weight = jnp.exp(scores - jnp.max(scores, axis=-1, keepdims=True))
    return weight / jnp.sum(weight, axis=-1, keepdims=True)


def _rms(values):
    wide = values.astype(jnp.float32)
    return (wide * lax.rsqrt(jnp.mean(wide * wide, axis=-1, keepdims=True) + EPS)).astype(jnp.bfloat16)


def _rms_back(values, grad):
    wide = values.astype(jnp.float32)
    scale = lax.rsqrt(jnp.mean(wide * wide, axis=-1, keepdims=True) + EPS)
    return scale * grad - wide * (scale * scale * scale) * jnp.mean(wide * grad, axis=-1, keepdims=True)


class Torus:
    def __init__(self, credit):
        self.core = lax.axis_index("c")
        self.place = {dim: lax.axis_index(dim) for dim in DIMS}
        self.near = tuple({dim: _rem(self.place[dim] + step, 4) for dim in DIMS} for step in (1, 3))
        self.far = {dim: _rem(self.place[dim] + 2, 4) for dim in DIMS}
        self.sibling = {"c": 1 - self.core}
        self.sides = ((0, self.core), (1, 1 - self.core))
        self.credit = credit
        self.partners = [({dim: self.near[way][dim]}, 2 * d + 1 - way, 2 * d + way)
                         for d, dim in enumerate(DIMS) for way in TWO]
        self.partners.append((self.sibling, 6, 6))

    def meet(self):
        barrier = pltpu.get_barrier_semaphore()
        for device, _, _ in self.partners:
            pl.semaphore_signal(barrier, inc=1, device_id=device, device_id_type=MESH)
        pl.semaphore_wait(barrier, len(self.partners))

    def remote(self, source, target, send_sem, recv_sem, device):
        return pltpu.make_async_remote_copy(src_ref=source, dst_ref=target, send_sem=send_sem, recv_sem=recv_sem,
                                            device_id=device, device_id_type=MESH)

    def run(self, steps, n_chunks, n_ticks):
        def tick(now, carry):
            @pl.when(now >= 2)
            def _():
                for _, _, mine in self.partners:
                    pl.semaphore_wait(self.credit.at[mine], 1)

            for lag, step in steps:
                @pl.when((now >= lag) & (now < lag + n_chunks))
                def _(lag=lag, step=step):
                    step(now - lag)

            @pl.when(now < n_ticks - 2)
            def _():
                for device, theirs, _ in self.partners:
                    pl.semaphore_signal(self.credit.at[theirs], inc=1, device_id=device, device_id_type=MESH)
            return carry

        lax.fori_loop(0, n_ticks, tick, 0)


def forward_kernel(n_layers, x_ref, rows_ref, down_ref, y_ref, acts, w_out, hid_out, gelu_out, norm_out, q_out, k_out, v_out,
                   o_out, wbuf, peer, shard, twin, state, normed, q_buf, k_buf, v_buf, o_buf, gelu_buf, hid_buf, acc,
                   ring_send, ring_recv, pair_send, pair_recv, keep_sem, save_sem, hid_sem, twin_sem, credit):
    torus = Torus(credit)
    core, place, near = torus.core, torus.place, torus.near
    slots = wbuf.shape[0]
    n_chunks = n_layers * PER_HALF
    ready = 6 * LAG
    last_lag = ready + 1
    seq = x_ref.shape[0]
    third = 64 * ROWS
    torus.meet()
    swap = torus.remote(rows_ref.at[1 - core], twin, twin_sem.at[0], twin_sem.at[1], torus.sibling)
    swap.start()
    state[ALL] = x_ref[ALL]
    swap.wait_send()
    swap.wait_recv()
    for layer in range(n_layers):
        shard[layer, :, UP_END:] = down_ref[layer]
        for part in range(5):
            cols = slice(FIFTH * part, FIFTH * part + FIFTH)
            mine = rows_ref[core, layer, :, cols].astype(jnp.float32)
            other = twin[layer, :, cols].astype(jnp.float32)
            first = core == 0
            shard[layer, :, cols] = jnp.concatenate(
                [jnp.where(first, mine, other), jnp.where(first, other, mine)], axis=0).astype(jnp.bfloat16)

    def columns(chunk):
        return _at(_rem(chunk, PER_HALF) * COLS, COLS)

    def spot(slot, color, stage, position, cols):
        order = ORDERS[color]
        index = tuple(EVERY if dim in order[:stage] else position if dim == order[stage] else place[dim]
                      for dim in DIMS)
        return wbuf.at[(slot,) + index + (_rows(color), cols)]

    halves = (slice(0, COLS // 2), slice(COLS // 2, COLS))

    def send_own(stage, chunk):
        slot, sem = _rem(chunk, slots), _rem(chunk, RING)
        for color in COLORS:
            dim = ORDERS[color][stage]
            here = spot(slot, color, stage, place[dim], slice(0, COLS))
            source = here
            if stage == 0:
                source = shard.at[chunk // PER_HALF, _rows(color), columns(chunk)]
            for way in TWO:
                torus.remote(source, here, ring_send.at[2 * stage, sem], ring_recv.at[2 * stage, sem],
                             {dim: near[way][dim]}).start()

    def send_far(stage, chunk):
        slot, sem = _rem(chunk, slots), _rem(chunk, RING)
        for color in COLORS:
            dim = ORDERS[color][stage]
            for way in TWO:
                block = spot(slot, color, stage, near[1 - way][dim], halves[way])
                torus.remote(block, block, ring_send.at[2 * stage + 1, sem], ring_recv.at[2 * stage + 1, sem],
                             {dim: near[way][dim]}).start()

    def arrived(part, chunk):
        slot, sem = _rem(chunk, slots), _rem(chunk, RING)
        block = (wbuf.at[slot, 0, 0, 0:2], wbuf.at[slot, 0, 0, 0], wbuf.at[slot, 0, 0:2], wbuf.at[slot, 0, 0],
                 wbuf.at[slot, 0:2], wbuf.at[slot, 0])[part]
        whole = torus.remote(block, block, ring_send.at[part, sem], ring_recv.at[part, sem], torus.sibling)
        whole.wait_send()
        whole.wait_recv()

    def enter(chunk):
        wbuf[_rem(chunk, slots), place["z"], place["y"], place["x"]] = shard[chunk // PER_HALF, :, columns(chunk)]
        send_own(0, chunk)

    def pass_on(part, chunk):
        arrived(part, chunk)
        if part % 2 == 0:
            send_far(part // 2, chunk)
        else:
            send_own(part // 2 + 1, chunk)

    def pair_copy(chunk):
        slot = _rem(chunk, RING)
        return torus.remote(wbuf.at[_rem(chunk, slots)], peer.at[slot], pair_send.at[slot], pair_recv.at[slot],
                            torus.sibling)

    def exchange(chunk):
        arrived(5, chunk)
        pair_copy(chunk).start()

    def keep_copy(chunk):
        return pltpu.make_async_copy(wbuf.at[_rem(chunk, slots)],
                                     w_out.at[chunk // PER_HALF, :, :, :, :, columns(chunk)],
                                     keep_sem.at[_rem(chunk, RING)])

    def save_copies(layer, names):
        parts = {"n0": (normed, norm_out.at[layer, 0], 0), "n1": (normed, norm_out.at[layer, 1], 1),
                 "q": (q_buf, q_out.at[layer], 2), "k": (k_buf, k_out.at[layer], 3), "v": (v_buf, v_out.at[layer], 4),
                 "o": (o_buf, o_out.at[layer], 5)}
        for half in TWO:
            for part in COLORS:
                parts[f"a{half}{part}"] = (gelu_buf.at[half, :, slice(third * part, third * (part + 1))],
                                           gelu_out.at[layer, 3 * half + part], 6 + 3 * half + part)
        return [pltpu.make_async_copy(parts[name][0], parts[name][1], save_sem.at[parts[name][2]]) for name in names]

    gelu_names = [f"a{half}{part}" for half in TWO for part in COLORS]

    def hidden_copies(layer, order):
        slot, part, at = _rem(order, 2), order // 6, _at(_rem(order, 6) * COLS, COLS)
        return [pltpu.make_async_copy(hid_buf.at[slot, half], hid_out.at[layer, part, half, :, at],
                                      hid_sem.at[slot, half]) for half in TWO]

    def compute(chunk):
        layer, index = chunk // PER_HALF, _rem(chunk, PER_HALF)
        pair = pair_copy(chunk)
        pair.wait_send()
        pair.wait_recv()
        keep_copy(chunk).start()

        def weights(role):
            block = wbuf[_rem(chunk, slots)] if role == 0 else peer[_rem(chunk, RING)]
            return block.reshape(third, COLS)

        @pl.when(index == 0)
        def _():
            normed[ALL] = _rms(state[ALL])
            for copy in save_copies(layer, ["n0"]):
                copy.start()

        @pl.when(index < 3)
        def _():
            for role, half in torus.sides:
                q_buf[:, _at(3 * COLS * half + COLS * index, COLS)] = _dot(
                    normed[ALL], weights(role)).astype(jnp.bfloat16)

        @pl.when(index == 3)
        def _():
            for role, half in torus.sides:
                both = _dot(normed[ALL], weights(role)).astype(jnp.bfloat16)
                k_buf[:, _at(HEAD * half, HEAD)] = both[:, :HEAD]
                v_buf[:, _at(HEAD * half, HEAD)] = both[:, HEAD:]

        @pl.when(index == QKV)
        def _():
            acc[ALL] = jnp.zeros_like(acc)
            for copy in save_copies(layer, ["q", "k", "v"]):
                copy.start()

        @pl.when((index >= QKV) & (index < ATTN))
        def _():
            causal = _causal(seq)
            for role, half in torus.sides:
                key, value = k_buf[:, _at(HEAD * half, HEAD)], v_buf[:, _at(HEAD * half, HEAD)]
                outs = []
                for head in TWO:
                    at = _at(3 * COLS * half + COLS * (index - QKV) + HEAD * head, HEAD)
                    prob = _probs(q_buf[:, at], key, causal)
                    outs.append(_dot(prob.astype(jnp.bfloat16), value).astype(jnp.bfloat16))
                block = jnp.concatenate(outs, axis=1)
                o_buf[3 * half + index - QKV] = block
                acc[ALL] += _dot_rhs_t(block, weights(role))

        @pl.when(index == 6)
        def _():
            middle = (state[ALL].astype(jnp.float32) + acc[ALL]).astype(jnp.bfloat16)
            state[ALL] = middle
            acts[2 * layer] = middle
            for copy in save_copies(layer, ["n0"]):
                copy.wait()
            normed[ALL] = _rms(middle)
            for copy in save_copies(layer, ["n1", "o"]):
                copy.start()

        @pl.when((index >= 8) & (index < 26))
        def _():
            for copy in hidden_copies(layer, index - 8):
                copy.wait()

        @pl.when((index >= ATTN) & (index < UP_BLOCKS))
        def _():
            for role, half in torus.sides:
                hidden = _dot(normed[ALL], weights(role))
                hid_buf[_rem(index - ATTN, 2), half] = hidden
                gelu_buf[half, :, _at(COLS * (index - ATTN), COLS)] = jax.nn.gelu(hidden).astype(jnp.bfloat16)
            for copy in hidden_copies(layer, index - ATTN):
                copy.start()

        @pl.when(index == UP_BLOCKS)
        def _():
            for copy in save_copies(layer, gelu_names):
                copy.start()

        @pl.when(index >= UP_BLOCKS)
        def _():
            part, at = (index - UP_BLOCKS) // 6, _at(COLS * _rem(index - UP_BLOCKS, 6), COLS)
            total = sum(_dot(gelu_buf[half, :, _at(third * part, third)], weights(role))
                        for role, half in torus.sides)

            @pl.when(part == 0)
            def _():
                acc[:, at] = total

            @pl.when(part > 0)
            def _():
                acc[:, at] += total

        @pl.when(index == PER_HALF - 1)
        def _():
            result = (state[ALL].astype(jnp.float32) + acc[ALL]).astype(jnp.bfloat16)
            state[ALL] = result

            @pl.when(layer < n_layers - 1)
            def _():
                acts[2 * layer + 1] = result

            @pl.when(layer == n_layers - 1)
            def _():
                y_ref[ALL] = result
            for copy in save_copies(layer, ["n1", "q", "k", "v", "o"] + gelu_names):
                copy.wait()

        keep_copy(chunk).wait()

    steps = [(0, enter)] + [((part + 1) * LAG, functools.partial(pass_on, part)) for part in range(5)]
    torus.run(steps + [(ready, exchange), (last_lag, compute)], n_chunks, n_chunks + last_lag)


def forward_stack(x_loc, rows, down):
    n_layers = down.shape[0]
    seq, width = x_loc.shape
    bf16, f32 = jnp.bfloat16, jnp.float32
    slots = 6 * LAG + 4
    chunk = CUBE + (ROWS, COLS)
    shape = jax.ShapeDtypeStruct
    hbm = pl.BlockSpec(memory_space=pl.ANY)
    vmem = pl.BlockSpec(memory_space=pltpu.VMEM)
    dma = pltpu.SemaphoreType.DMA
    return pl.pallas_call(
        functools.partial(forward_kernel, n_layers),
        name="forward_stack",
        out_shape=(shape((seq, width), bf16), shape((2 * n_layers - 1, seq, width), bf16),
                   shape((n_layers, 4, 4, 4, ROWS, PER_HALF * COLS), bf16),
                   shape((n_layers, 3, 2, seq, width), f32), shape((n_layers, 6, seq, width), bf16),
                   shape((n_layers, 2, seq, width), bf16), shape((n_layers, seq, width), bf16),
                   shape((n_layers, seq, 2 * HEAD), bf16), shape((n_layers, seq, 2 * HEAD), bf16),
                   shape((n_layers, 6, seq, COLS), bf16)),
        in_specs=[vmem] * 3,
        out_specs=(vmem,) * 2 + (hbm,) * 8,
        scratch_shapes=[
            pltpu.VMEM((slots,) + chunk, bf16), pltpu.VMEM((RING,) + chunk, bf16),
            pltpu.VMEM((n_layers, ROWS, PER_HALF * COLS), bf16), pltpu.VMEM(rows.shape[1:], bf16),
            pltpu.VMEM((seq, width), bf16), pltpu.VMEM((seq, width), bf16),
            pltpu.VMEM((seq, 6 * COLS), bf16), pltpu.VMEM((seq, 2 * HEAD), bf16), pltpu.VMEM((seq, 2 * HEAD), bf16),
            pltpu.VMEM((6, seq, COLS), bf16), pltpu.VMEM((2, seq, 18 * COLS), bf16),
            pltpu.VMEM((2, 2, seq, COLS), f32), pltpu.VMEM((seq, width), f32),
            dma((6, RING)), dma((6, RING)), dma((RING,)), dma((RING,)), dma((RING,)), dma((12,)), dma((2, 2)), dma((2,)),
            pltpu.SemaphoreType.REGULAR((7,))],
        compiler_params=pltpu.CompilerParams(collective_id=1, has_side_effects=True,
                                             vmem_limit_bytes=VMEM_LIMIT),
    )(x_loc, rows, down)


def backward_kernel(n_layers, *refs):
    (g_ref, x_ref, acts, w_own, hid_in, gelu_in, norm_in, q_in, k_in, v_in, o_in,
     rows_out, down_out, dx_ref,
     mine, theirs, lefts, rights, hid_buf, dact, dnorm, q_buf, k_buf, v_buf, x_mid, x_in, dk_acc, dv_acc,
     outgo, peer, out, away, sum0, sum1, sum2, sa0, ra0, sb0, rb0, sa1, ra1, sb1, rb1, sa2, ra2, sb2, rb2,
     load_sem, own_sem, push_send, push_recv, pair_send, pair_recv, ring_send, ring_recv, swap_sem, credit) = refs
    torus = Torus(credit)
    core, place, near = torus.core, torus.place, torus.near
    sums = (sum0, sum1, sum2)
    half_bufs = ((sa0, ra0), (sa1, ra1), (sa2, ra2))
    full_bufs = ((sb0, rb0), (sb1, rb1), (sb2, rb2))
    n_chunks = n_layers * PER_HALF
    seq, width = g_ref.shape
    third = 64 * ROWS
    leads = sum0.shape[0]

    def pair_of(chunk):
        return n_layers - 1 - chunk // PER_HALF

    def columns(chunk):
        index = _rem(chunk, PER_HALF)
        block = jnp.where(index < DOWN_DONE, UP_BLOCKS + index,
                          jnp.where(index < UP_DONE, index - 11, jnp.where(index < O_DONE, index - 32, index - 39)))
        return _at(block * COLS, COLS)

    def loads(pair, names):
        def source(name):
            return {"a": (gelu_in.at[pair], lefts.at[0:6], 0), "n_mlp": (norm_in.at[pair, 1], lefts.at[NORM_MLP], 1),
                    "n_attn": (norm_in.at[pair, 0], lefts.at[NORM_ATTN], 2), "o": (o_in.at[pair], rights.at[O_AT:QKV_AT], 3),
                    "q": (q_in.at[pair], q_buf, 4), "k": (k_in.at[pair], k_buf, 5), "v": (v_in.at[pair], v_buf, 6),
                    "x_mid": (acts.at[2 * pair], x_mid, 7), "h0": (hid_in.at[pair, 0], hid_buf, 8),
                    "h1": (hid_in.at[pair, 1], hid_buf, 8), "h2": (hid_in.at[pair, 2], hid_buf, 8)}[name]
        return [pltpu.make_async_copy(source(name)[0], source(name)[1], load_sem.at[source(name)[2]])
                for name in names]

    def start(pair, names):
        for copy in loads(pair, names):
            copy.start()

    def finish(pair, names):
        for copy in loads(pair, names):
            copy.wait()

    def first_input(ref):
        return pltpu.make_async_copy(ref, x_in, load_sem.at[9])

    torus.meet()
    start(n_layers - 1, ["a"])
    for block in SIX:
        rights[block] = g_ref[:, COLS * block:COLS * block + COLS]
    finish(n_layers - 1, ["a"])

    def own_copy(chunk):
        slot = _rem(chunk, SLOTS)
        return pltpu.make_async_copy(w_own.at[pair_of(chunk), :, :, :, :, columns(chunk)], mine.at[slot],
                                     own_sem.at[slot])

    def push_copy(chunk):
        slot = _rem(chunk, SLOTS)
        return torus.remote(w_own.at[pair_of(chunk), :, :, :, :, columns(chunk)], theirs.at[slot],
                            push_send.at[slot], push_recv.at[slot], torus.sibling)

    def fetch(chunk):
        own_copy(chunk).start()
        push_copy(chunk).start()

    def total_grad():
        return jnp.concatenate([rights[block] for block in SIX], axis=1).astype(jnp.float32)

    def consume(chunk):
        pair, index = pair_of(chunk), _rem(chunk, PER_HALF)
        slot = _rem(chunk, SLOTS)
        own_copy(chunk).wait()
        push = push_copy(chunk)
        push.wait_send()
        push.wait_recv()

        def weights(role):
            return (mine, theirs)[role][slot].reshape(third, COLS)

        @pl.when(index == 0)
        def _():
            start(pair, ["n_mlp", "n_attn", "o", "q", "k", "v", "x_mid", "h0"])

            @pl.when(pair == 0)
            def _():
                first_input(x_ref).start()

            @pl.when(pair > 0)
            def _():
                first_input(acts.at[2 * pair - 1]).start()

        for part in (1, 2):
            @pl.when(index == 6 * part)
            def _(part=part):
                start(pair, [f"h{part}"])

        @pl.when((index < DOWN_DONE) & (_rem(index, 6) == 0))
        def _():
            dact[ALL] = jnp.zeros_like(dact)

        @pl.when(index < DOWN_DONE)
        def _():
            for role, half in torus.sides:
                dact[half] += _dot_rhs_t(rights[_rem(index, 6)], weights(role))

        @pl.when((index < DOWN_DONE) & (_rem(index, 6) == 5))
        def _():
            finish(pair, ["h0"])
            for half in TWO:
                for block in SIX:
                    cols = slice(COLS * block, COLS * block + COLS)
                    hidden = hid_buf[half, :, cols]
                    bend = jnp.tanh(0.7978845608028654 * (hidden + 0.044715 * (hidden * hidden * hidden)))
                    slope = 0.5 * (1.0 + bend) + 0.5 * hidden * (1.0 - bend * bend) * (
                        0.7978845608028654 * (1.0 + 0.134145 * (hidden * hidden)))
                    rights[DH_AT + FF * half + index - 5 + block] = (dact[half, :, cols] * slope).astype(jnp.bfloat16)

        @pl.when(index == DOWN_DONE - 1)
        def _():
            finish(pair, ["n_mlp"])

        @pl.when(index == DOWN_DONE)
        def _():
            dnorm[ALL] = jnp.zeros_like(dnorm)

            @pl.when(pair > 0)
            def _():
                start(pair - 1, ["a"])

        @pl.when((index >= DOWN_DONE) & (index < UP_DONE))
        def _():
            dnorm[ALL] += sum(_dot_rhs_t(rights[DH_AT + FF * half + index - DOWN_DONE], weights(role))
                              for role, half in torus.sides)

        @pl.when(index == UP_DONE - 1)
        def _():
            finish(pair, ["x_mid", "o"])
            lefts[GRAD] = (total_grad() + _rms_back(x_mid[ALL], dnorm[ALL])).astype(jnp.bfloat16)

        @pl.when(index == UP_DONE)
        def _():
            finish(pair, ["q", "k", "v"])
            dk_acc[ALL] = jnp.zeros_like(dk_acc)
            dv_acc[ALL] = jnp.zeros_like(dv_acc)

        @pl.when((index >= UP_DONE) & (index < O_DONE))
        def _():
            causal = _causal(seq)
            for role, half in torus.sides:
                d_o = _dot(lefts[GRAD], weights(role)).astype(jnp.bfloat16)
                key, value = k_buf[:, _at(HEAD * half, HEAD)], v_buf[:, _at(HEAD * half, HEAD)]
                d_q = []
                for head in TWO:
                    query = q_buf[:, _at(3 * COLS * half + COLS * (index - UP_DONE) + HEAD * head, HEAD)]
                    d_head = d_o[:, HEAD * head:HEAD * head + HEAD]
                    prob = _probs(query, key, causal)
                    d_prob = _dot_rhs_t(d_head, value)
                    dv_acc[half] += _dot_lhs_t(prob.astype(jnp.bfloat16), d_head)
                    d_score = prob * (d_prob - jnp.sum(prob * d_prob, axis=-1, keepdims=True))
                    d_score = (d_score * (HEAD ** -0.5)).astype(jnp.bfloat16)
                    d_q.append(_dot(d_score, key).astype(jnp.bfloat16))
                    dk_acc[half] += _dot_lhs_t(d_score, query)
                rights[QKV_AT + QKV * half + index - UP_DONE] = jnp.concatenate(d_q, axis=1)

        @pl.when(index == O_DONE - 1)
        def _():
            finish(pair, ["n_attn"])
            for half in TWO:
                rights[QKV_AT + QKV * half + QKV - 1] = jnp.concatenate([dk_acc[half], dv_acc[half]], axis=1).astype(jnp.bfloat16)

        @pl.when(index == O_DONE)
        def _():
            dnorm[ALL] = jnp.zeros_like(dnorm)

        @pl.when(index >= O_DONE)
        def _():
            dnorm[ALL] += sum(_dot_rhs_t(rights[QKV_AT + QKV * half + index - O_DONE], weights(role))
                              for role, half in torus.sides)

        @pl.when(index == PER_HALF - 1)
        def _():
            first_input(x_ref).wait()

            @pl.when(pair > 0)
            def _():
                finish(pair - 1, ["a"])
            result = (lefts[GRAD].astype(jnp.float32) + _rms_back(x_in[ALL], dnorm[ALL])).astype(jnp.bfloat16)
            dx_ref[ALL] = result
            for block in SIX:
                rights[block] = result[:, COLS * block:COLS * block + COLS]

    def pair_copy(slot):
        return torus.remote(outgo.at[slot], peer.at[slot], pair_send.at[slot], pair_recv.at[slot], torus.sibling)

    def multiply(chunk):
        index = _rem(chunk, PER_HALF)
        slot = _rem(chunk, RING)
        quarter = third // RING
        for role, half in torus.sides[::-1]:
            left = jnp.where(index < DOWN_DONE, 3 * half + index // 6,
                             jnp.where(index < UP_DONE, NORM_MLP, jnp.where(index < O_DONE, GRAD, NORM_ATTN)))
            right = jnp.where(index < DOWN_DONE, _rem(index, 6),
                              jnp.where(index < UP_DONE, DH_AT + FF * half + index - DOWN_DONE,
                                        jnp.where(index < O_DONE, O_AT + 3 * half + index - UP_DONE, QKV_AT + QKV * half + index - O_DONE)))
            for z in range(RING):
                part = _dot_lhs_t(lefts[left, :, quarter * z:quarter * z + quarter], rights[right])
                if role == 0:
                    sum0[_rem(chunk, leads), z] = part.reshape(RING, RING, ROWS, COLS)
                else:
                    outgo[slot, z] = part.astype(jnp.bfloat16).reshape(RING, RING, ROWS, COLS)
        pair_copy(slot).start()

    def merge_pair(chunk):
        slot, lead = _rem(chunk, RING), _rem(chunk, leads)
        pair_copy(slot).wait_send()
        pair_copy(slot).wait_recv()
        for z in range(RING):
            for y in range(RING):
                sum0[lead, z, y] = sum0[lead, z, y] + peer[slot, z, y].astype(jnp.float32)

    def ring_copy(stage, part, slot, color, way):
        send, recv = (half_bufs, full_bufs)[part][stage]
        dim = ORDERS[color][stage]
        return torus.remote(send.at[slot, color, way], recv.at[slot, color, way],
                            ring_send.at[2 * stage + part, slot], ring_recv.at[2 * stage + part, slot],
                            {dim: near[way][dim]})

    def ring_wait(stage, part, slot):
        send, recv = (half_bufs, full_bufs)[part][stage]
        whole = torus.remote(send.at[slot], recv.at[slot], ring_send.at[2 * stage + part, slot],
                             ring_recv.at[2 * stage + part, slot], torus.sibling)
        whole.wait_send()
        whole.wait_recv()

    def source(stage, chunk, color, position, cols):
        lead = _rem(chunk, leads)
        if stage == 0:
            return sum0[(lead,) + _block(color, 0, position) + (_rows(color), cols)]
        return sums[stage][(lead, color) + _block(color, stage, position) + (EVERY, cols)]

    left_cols, right_cols, every = slice(0, COLS // 2), slice(COLS // 2, COLS), slice(0, COLS)

    def store_halves(stage, chunk):
        slot = _rem(chunk, RING)
        send = half_bufs[stage][0]
        for color in COLORS:
            far = torus.far[ORDERS[color][stage]]
            send[slot, color, 0] = source(stage, chunk, color, far, left_cols).astype(jnp.bfloat16)
            send[slot, color, 1] = source(stage, chunk, color, far, right_cols).astype(jnp.bfloat16)

    def store_fulls(stage, chunk):
        slot = _rem(chunk, RING)
        ring_wait(stage, 0, slot)
        recv = half_bufs[stage][1]
        send = full_bufs[stage][0]
        lead = (EVERY,) * (len(send.shape) - 4)
        for color in COLORS:
            dim = ORDERS[color][stage]
            for way, summed, plain in ((0, left_cols, right_cols), (1, right_cols, left_cols)):
                send[(slot, color, way) + lead + (summed,)] = (
                    source(stage, chunk, color, near[way][dim], summed)
                    + recv[slot, color, way].astype(jnp.float32)).astype(jnp.bfloat16)
                send[(slot, color, way) + lead + (plain,)] = source(
                    stage, chunk, color, near[way][dim], plain).astype(jnp.bfloat16)

    def close_stage(stage, chunk):
        slot = _rem(chunk, RING)
        ring_wait(stage, 1, slot)
        recv = full_bufs[stage][1]
        for color in COLORS:
            dim = ORDERS[color][stage]
            total = (source(stage, chunk, color, place[dim], every)
                     + recv[slot, color, 0].astype(jnp.float32)
                     + recv[slot, color, 1].astype(jnp.float32))
            if stage < 2:
                sums[stage + 1][_rem(chunk, leads), color] = total
            else:
                out[pair_of(chunk), _rows(color), columns(chunk)] = total

    def send_all(stage, part, chunk):
        for color in COLORS:
            for way in TWO:
                ring_copy(stage, part, _rem(chunk, RING), color, way).start()

    def open_first(chunk):
        merge_pair(chunk)
        store_halves(0, chunk)
        send_all(0, 0, chunk)

    def middle(stage, chunk):
        store_fulls(stage, chunk)
        send_all(stage, 1, chunk)

    def turn(stage, chunk):
        close_stage(stage, chunk)
        if stage < 2:
            store_halves(stage + 1, chunk)
            send_all(stage + 1, 0, chunk)

    base = 0
    steps = [(0, fetch), (base + 2 * LAG, functools.partial(middle, 0)), (base + LAG, open_first),
             (base + 3 * LAG, functools.partial(turn, 0)), (base + 4 * LAG, functools.partial(middle, 1)),
             (base + 5 * LAG, functools.partial(turn, 1)), (base + 6 * LAG, functools.partial(middle, 2)),
             (base + 7 * LAG, functools.partial(turn, 2)), (1, consume), (0, multiply)]
    torus.run(steps, n_chunks, n_chunks + base + 7 * LAG)

    half_rows = ROWS // 2
    for layer in range(n_layers):
        for part in range(5):
            cols = slice(FIFTH * part, FIFTH * part + FIFTH)
            both = out[layer, :, cols]
            low, high = both[:half_rows], both[half_rows:]
            rows_out[core, layer, :, cols] = jnp.where(core == 0, low, high)
            away[layer, :, cols] = jnp.where(core == 0, high, low)
    swap = torus.remote(away, rows_out.at[core], swap_sem.at[0], swap_sem.at[1], torus.sibling)
    down_out[ALL] = out[:, :, UP_END:]
    swap.start()
    swap.wait_send()
    swap.wait_recv()


def backward_stack(n_layers, g_loc, *saved):
    seq, width = g_loc.shape
    bf16, f32 = jnp.bfloat16, jnp.float32
    half = COLS // 2
    chunk = CUBE + (ROWS, COLS)
    leads = 7
    shape = jax.ShapeDtypeStruct
    hbm = pl.BlockSpec(memory_space=pl.ANY)
    vmem = pl.BlockSpec(memory_space=pltpu.VMEM)
    dma = pltpu.SemaphoreType.DMA
    half_rows = ROWS // 2
    scratch = [pltpu.VMEM((SLOTS,) + chunk, bf16), pltpu.VMEM((SLOTS,) + chunk, bf16),
               pltpu.VMEM((9, seq, width), bf16), pltpu.VMEM((56, seq, COLS), bf16),
               pltpu.VMEM((2, seq, width), f32), pltpu.VMEM((2, seq, width), f32), pltpu.VMEM((seq, width), f32),
               pltpu.VMEM((seq, 6 * COLS), bf16), pltpu.VMEM((seq, 2 * HEAD), bf16), pltpu.VMEM((seq, 2 * HEAD), bf16),
               pltpu.VMEM((seq, width), bf16), pltpu.VMEM((seq, width), bf16),
               pltpu.VMEM((2, seq, HEAD), f32), pltpu.VMEM((2, seq, HEAD), f32),
               pltpu.VMEM((RING,) + chunk, bf16), pltpu.VMEM((RING,) + chunk, bf16),
               pltpu.VMEM((n_layers, ROWS, PER_HALF * COLS), f32), pltpu.VMEM((n_layers, half_rows, UP_END), f32),
               pltpu.VMEM((leads,) + chunk, f32), pltpu.VMEM((leads, 3, RING, RING, TILE, COLS), f32),
               pltpu.VMEM((leads, 3, RING, TILE, COLS), f32)]
    for size in ((RING, RING), (RING,), ()):
        scratch += [pltpu.VMEM((RING, 3, 2) + size + (TILE, half), bf16)] * 2
        scratch += [pltpu.VMEM((RING, 3, 2) + size + (TILE, COLS), bf16)] * 2
    scratch += [dma((10,)), dma((SLOTS,)), dma((SLOTS,)), dma((SLOTS,)), dma((RING,)), dma((RING,)), dma((6, RING)), dma((6, RING)), dma((2,)),
                pltpu.SemaphoreType.REGULAR((7,))]
    return pl.pallas_call(
        functools.partial(backward_kernel, n_layers),
        name="backward_stack",
        out_shape=(shape((2, n_layers, half_rows, UP_END), f32),
                   shape((n_layers, ROWS, (PER_HALF - UP_BLOCKS) * COLS), f32), shape((seq, width), bf16)),
        in_specs=[vmem] + [hbm] * len(saved),
        out_specs=(vmem,) * 3,
        scratch_shapes=scratch,
        compiler_params=pltpu.CompilerParams(collective_id=0, has_side_effects=True,
                                             vmem_limit_bytes=VMEM_LIMIT),
    )(g_loc, *saved)


LANES = 128


def _pieces(moves, size):
    tiles = [[] for _ in range(size // LANES)]
    for target, source, length in moves:
        while length:
            step = min(length, LANES - target % LANES, LANES - source % LANES)
            tiles[target // LANES].append((target % LANES, source // LANES, (target - source) % LANES))
            target, source, length = target + step, source + step, length - step
    return [sorted(tile) for tile in tiles]


def _gather_tile(load, tile, lane):
    total = None
    for first, source, shift in tile:
        value = load(source)
        if shift:
            value = pltpu.roll(value, shift, axis=value.ndim - 1)
        total = value if total is None else jnp.where(lane >= first, value, total)
    return total


def pack_kernel(blocks, q_ref, k_ref, v_ref, o_ref, up_ref, down_ref, rows_out, down_out):
    layers, rows = up_ref.shape[0], up_ref.shape[1]
    group = q_ref.shape[-1] // 2
    for half in TWO:
        first = 0
        for ref, size in ((q_ref, group), (k_ref, HEAD), (v_ref, HEAD), (o_ref, group)):
            rows_out[half, :, :, first:first + size] = ref[:, :, size * half:size * half + size]
            first += size
    lane = lax.broadcasted_iota(jnp.int32, (layers, rows, LANES), 2)
    chips, block = blocks
    moves = []
    for half in TWO:
        for part in COLORS:
            for chip in range(chips):
                used = min(ROWS, block - ROWS * part)
                target = chips * ROWS * (3 * half + part) + ROWS * chip
                moves.append((target, block * (2 * chip + half) + ROWS * part, used))
    half_f = 3 * chips * ROWS
    for index, tile in enumerate(_pieces(moves, 2 * half_f)):
        value = _gather_tile(lambda source: up_ref[:, :, LANES * source:LANES * source + LANES].astype(jnp.float32),
                             tile, lane)
        last = 3 * ROWS - block
        position = lane + LANES * index % ROWS
        if LANES * index % half_f >= 2 * chips * ROWS:
            value = jnp.where(lax.rem(position, ROWS) < ROWS - last, value, 0.0)
        half, at = divmod(LANES * index, half_f)
        rows_out[half, :, :, ATTN * COLS + at:ATTN * COLS + at + LANES] = value.astype(jnp.bfloat16)
    width = down_ref.shape[-1]
    for part in COLORS:
        used = min(ROWS, block - ROWS * part)
        value = down_ref[:, ROWS * part:ROWS * part + used, :].astype(jnp.float32)
        if used < ROWS:
            value = jnp.concatenate([value, jnp.zeros((layers, ROWS - used, width), jnp.float32)], axis=1)
        down_out[:, :, width * part:width * part + width] = value.astype(jnp.bfloat16)


def pack_weights(w_q, w_k, w_v, w_o, w_up, w_down, chips):
    layers, rows = w_up.shape[:2]
    block, width = w_down.shape[1:]
    vmem = pl.BlockSpec(memory_space=pltpu.VMEM)
    shape = jax.ShapeDtypeStruct
    return pl.pallas_call(
        functools.partial(pack_kernel, (chips, block)), name="pack_weights",
        out_shape=(shape((2, layers, rows, UP_END), jnp.bfloat16), shape((layers, ROWS, 3 * width), jnp.bfloat16)),
        in_specs=[vmem] * 6, out_specs=(vmem,) * 2,
        compiler_params=pltpu.CompilerParams(vmem_limit_bytes=VMEM_LIMIT),
    )(*[weight.reshape(layers, rows, -1) for weight in (w_q, w_k, w_v, w_o, w_up)], w_down)


def unpack_kernel(blocks, rows_ref, down_ref, q_out, k_out, v_out, o_out, up_out, down_out):
    layers, rows = up_out.shape[0], up_out.shape[1]
    group = q_out.shape[-1] // 2
    for half in TWO:
        first = 0
        for ref, size in ((q_out, group), (k_out, HEAD), (v_out, HEAD), (o_out, group)):
            ref[:, :, size * half:size * half + size] = rows_ref[half, :, :, first:first + size]
            first += size
    lane = lax.broadcasted_iota(jnp.int32, (layers, rows, LANES), 2)
    chips, block = blocks
    moves = []
    for half in TWO:
        for part in COLORS:
            for chip in range(chips):
                used = min(ROWS, block - ROWS * part)
                source = chips * ROWS * (3 * half + part) + ROWS * chip
                moves.append((block * (2 * chip + half) + ROWS * part, source, used))
    half_f = 3 * chips * ROWS

    def load(source):
        half, at = divmod(LANES * source, half_f)
        return rows_ref[half, :, :, ATTN * COLS + at:ATTN * COLS + at + LANES]

    for index, tile in enumerate(_pieces(moves, 2 * chips * block)):
        up_out[:, :, LANES * index:LANES * index + LANES] = _gather_tile(load, tile, lane)
    width = down_out.shape[-1]
    for part in COLORS:
        used = min(ROWS, block - ROWS * part)
        down_out[:, ROWS * part:ROWS * part + used, :] = down_ref[:, :used, width * part:width * part + width]


def unpack_grads(row_grad, down_grad, shapes, chips):
    layers, rows = row_grad.shape[1:3]
    block, width = shapes[5][1:]
    vmem = pl.BlockSpec(memory_space=pltpu.VMEM)
    shape = jax.ShapeDtypeStruct
    flat = [shape((layers, rows, math.prod(full[2:])), jnp.float32) for full in shapes[:5]]
    outs = pl.pallas_call(
        functools.partial(unpack_kernel, (chips, block)), name="unpack_grads",
        out_shape=tuple(flat) + (shape((layers, block, width), jnp.float32),),
        in_specs=[vmem] * 2, out_specs=(vmem,) * 6,
        compiler_params=pltpu.CompilerParams(vmem_limit_bytes=VMEM_LIMIT),
    )(row_grad, down_grad)
    return tuple(out.reshape(full) for out, full in zip(outs, shapes))


def solution(mesh):
    mesh4 = Mesh(mesh.devices.reshape(CUBE + (2,)), ALL_AXES)
    row_spec = P(ALL_AXES)
    weight_spec = P(None, ALL_AXES)

    def body(x_in, w_q, w_k, w_v, w_o, w_up, w_down, grad_out):
        weights = (w_q, w_k, w_v, w_o, w_up, w_down)
        chips = w_up.shape[2] // w_down.shape[1] // 2
        rows, down = pack_weights(*weights, chips)
        y_loc, acts, *saved = forward_stack(x_in[0], rows, down)
        row_grad, down_grad, grad_x = backward_stack(w_q.shape[0], grad_out[0], x_in[0], acts, *saved)
        return (y_loc[None], grad_x[None]) + unpack_grads(row_grad, down_grad, [w.shape for w in weights], chips)

    return jax.shard_map(body, mesh=mesh4, in_specs=(row_spec,) + (weight_spec,) * 6 + (row_spec,),
                         out_specs=(row_spec, row_spec) + (weight_spec,) * 6, check_vma=False)
```

```python
import functools

import jax
import jax.numpy as jnp
from jax import lax
from jax.experimental import pallas as pl
from jax.experimental.pallas import tpu as pltpu
from jax.sharding import Mesh, PartitionSpec as P

MESH = pl.DeviceIdType.MESH
ALL_AXES = ("z", "y", "x", "c")
EPS = 1e-6
MASK_FILL = -1e30
DIMS = ("z", "y", "x")
ORDERS = (("x", "y", "z"), ("y", "z", "x"), ("z", "x", "y"))
COLS = 256
ROWS = 24
LAG = 2
HEAD = 128
PER_HALF = 43
UP_BLOCKS = 25
UP_END = UP_BLOCKS * COLS
RING = 4
CUBE = (RING, RING, RING)
SLOTS = 3
TILE = 8
COLORS = range(3)
TWO = range(2)
SIX = range(6)
ALL = Ellipsis
EVERY = slice(None)
QKV, ATTN, FF = 4, 7, 18
DOWN_DONE, UP_DONE, O_DONE = 18, 36, 39
G_AT, DH_AT, O_AT, QKV_AT = 0, 6, 42, 48
NORM_MLP, GRAD, NORM_ATTN = 6, 7, 8
VMEM_LIMIT = 67043328


FIFTH = UP_END // 5


def _rows(color):
    return slice(TILE * color, TILE * color + TILE)


def _rem(value, by):
    return lax.rem(value, by)


def _block(color, stage, position):
    dims = tuple(dim for dim in DIMS if dim not in ORDERS[color][:stage])
    return tuple(position if dim == ORDERS[color][stage] else EVERY for dim in dims)


def _dot(left, right):
    return jnp.dot(left, right, preferred_element_type=jnp.float32)


def _dot_rhs_t(left, right):
    return lax.dot_general(left, right, (((1,), (1,)), ((), ())), preferred_element_type=jnp.float32)


def _dot_lhs_t(left, right):
    return lax.dot_general(left, right, (((0,), (0,)), ((), ())), preferred_element_type=jnp.float32)


def _at(start, size):
    return pl.ds(pl.multiple_of(start, size), size)


def _causal(seq):
    return (lax.broadcasted_iota(jnp.int32, (seq, seq), 0) >= lax.broadcasted_iota(jnp.int32, (seq, seq), 1))


def _probs(query, key, causal):
    scores = jnp.where(causal, _dot_rhs_t(query, key) * (HEAD ** -0.5), MASK_FILL)
    weight = jnp.exp(scores - jnp.max(scores, axis=-1, keepdims=True))
    return weight / jnp.sum(weight, axis=-1, keepdims=True)


def _rms(values):
    wide = values.astype(jnp.float32)
    return (wide * lax.rsqrt(jnp.mean(wide * wide, axis=-1, keepdims=True) + EPS)).astype(jnp.bfloat16)


def _rms_back(values, grad):
    wide = values.astype(jnp.float32)
    scale = lax.rsqrt(jnp.mean(wide * wide, axis=-1, keepdims=True) + EPS)
    return scale * grad - wide * (scale * scale * scale) * jnp.mean(wide * grad, axis=-1, keepdims=True)


class Torus:
    def __init__(self, credit):
        self.core = lax.axis_index("c")
        self.place = {dim: lax.axis_index(dim) for dim in DIMS}
        self.near = tuple({dim: _rem(self.place[dim] + step, 4) for dim in DIMS} for step in (1, 3))
        self.far = {dim: _rem(self.place[dim] + 2, 4) for dim in DIMS}
        self.sibling = {"c": 1 - self.core}
        self.sides = ((0, self.core), (1, 1 - self.core))
        self.credit = credit
        self.partners = [({dim: self.near[way][dim]}, 2 * d + 1 - way, 2 * d + way)
                         for d, dim in enumerate(DIMS) for way in TWO]
        self.partners.append((self.sibling, 6, 6))

    def meet(self):
        barrier = pltpu.get_barrier_semaphore()
        for device, _, _ in self.partners:
            pl.semaphore_signal(barrier, inc=1, device_id=device, device_id_type=MESH)
        pl.semaphore_wait(barrier, len(self.partners))

    def remote(self, source, target, send_sem, recv_sem, device):
        return pltpu.make_async_remote_copy(src_ref=source, dst_ref=target, send_sem=send_sem, recv_sem=recv_sem,
                                            device_id=device, device_id_type=MESH)

    def run(self, steps, n_chunks, n_ticks):
        def tick(now, carry):
            @pl.when(now >= 2)
            def _():
                for _, _, mine in self.partners:
                    pl.semaphore_wait(self.credit.at[mine], 1)

            for lag, step in steps:
                @pl.when((now >= lag) & (now < lag + n_chunks))
                def _(lag=lag, step=step):
                    step(now - lag)

            @pl.when(now < n_ticks - 2)
            def _():
                for device, theirs, _ in self.partners:
                    pl.semaphore_signal(self.credit.at[theirs], inc=1, device_id=device, device_id_type=MESH)
            return carry

        lax.fori_loop(0, n_ticks, tick, 0)


def forward_kernel(n_layers, x_ref, rows_ref, down_ref, y_ref, acts, w_out, hid_out, gelu_out, norm_out, q_out, k_out, v_out,
                   o_out, wbuf, peer, shard, twin, state, normed, q_buf, k_buf, v_buf, o_buf, gelu_buf, hid_buf, acc,
                   ring_send, ring_recv, pair_send, pair_recv, keep_sem, save_sem, hid_sem, twin_sem, credit):
    torus = Torus(credit)
    core, place, near = torus.core, torus.place, torus.near
    slots = wbuf.shape[0]
    n_chunks = n_layers * PER_HALF
    ready = 6 * LAG
    last_lag = ready + 1
    seq = x_ref.shape[0]
    third = 64 * ROWS
    state[ALL] = x_ref[ALL]
    torus.meet()
    swap = torus.remote(rows_ref.at[1 - core], twin, twin_sem.at[0], twin_sem.at[1], torus.sibling)
    swap.start()
    swap.wait_send()
    swap.wait_recv()

    def assemble(chunk):
        @pl.when(chunk < 5 * n_layers)
        def _():
            layer, part = chunk // 5, _rem(chunk, 5)
            cols = _at(part * FIFTH, FIFTH)
            mine, other = [ref[layer, :, cols].astype(jnp.float32) for ref in (rows_ref.at[core], twin)]
            shard[layer, :, cols] = jnp.concatenate(
                [jnp.where(core == 0, mine, other), jnp.where(core == 0, other, mine)], axis=0).astype(jnp.bfloat16)

            @pl.when(part == 4)
            def _():
                shard[layer, :, UP_END:] = down_ref[layer]

    def columns(chunk):
        return _at(_rem(chunk, PER_HALF) * COLS, COLS)

    def spot(slot, color, stage, position, cols):
        order = ORDERS[color]
        index = tuple(EVERY if dim in order[:stage] else position if dim == order[stage] else place[dim]
                      for dim in DIMS)
        return wbuf.at[(slot,) + index + (_rows(color), cols)]

    halves = (slice(0, COLS // 2), slice(COLS // 2, COLS))

    def send_own(stage, chunk):
        slot, sem = _rem(chunk, slots), _rem(chunk, RING)
        for color in COLORS:
            dim = ORDERS[color][stage]
            here = spot(slot, color, stage, place[dim], slice(0, COLS))
            source = here
            if stage == 0:
                source = shard.at[chunk // PER_HALF, _rows(color), columns(chunk)]
            for way in TWO:
                torus.remote(source, here, ring_send.at[2 * stage, sem], ring_recv.at[2 * stage, sem],
                             {dim: near[way][dim]}).start()

    def send_far(stage, chunk):
        slot, sem = _rem(chunk, slots), _rem(chunk, RING)
        for color in COLORS:
            dim = ORDERS[color][stage]
            for way in TWO:
                block = spot(slot, color, stage, near[1 - way][dim], halves[way])
                torus.remote(block, block, ring_send.at[2 * stage + 1, sem], ring_recv.at[2 * stage + 1, sem],
                             {dim: near[way][dim]}).start()

    def arrived(part, chunk):
        slot, sem = _rem(chunk, slots), _rem(chunk, RING)
        block = (wbuf.at[slot, 0, 0, 0:2], wbuf.at[slot, 0, 0, 0], wbuf.at[slot, 0, 0:2], wbuf.at[slot, 0, 0],
                 wbuf.at[slot, 0:2], wbuf.at[slot, 0])[part]
        whole = torus.remote(block, block, ring_send.at[part, sem], ring_recv.at[part, sem], torus.sibling)
        whole.wait_send()
        whole.wait_recv()

    def enter(chunk):
        wbuf[_rem(chunk, slots), place["z"], place["y"], place["x"]] = shard[chunk // PER_HALF, :, columns(chunk)]
        send_own(0, chunk)

    def pass_on(part, chunk):
        arrived(part, chunk)
        if part % 2 == 0:
            send_far(part // 2, chunk)
        else:
            send_own(part // 2 + 1, chunk)

    def pair_copy(chunk):
        slot = _rem(chunk, RING)
        return torus.remote(wbuf.at[_rem(chunk, slots)], peer.at[slot], pair_send.at[slot], pair_recv.at[slot],
                            torus.sibling)

    def exchange(chunk):
        arrived(5, chunk)
        pair_copy(chunk).start()

    def keep_copy(chunk):
        return pltpu.make_async_copy(wbuf.at[_rem(chunk, slots)],
                                     w_out.at[chunk // PER_HALF, :, :, :, :, columns(chunk)],
                                     keep_sem.at[_rem(chunk, RING)])

    def save_copies(layer, names):
        parts = {"n0": (normed, norm_out.at[layer, 0], 0), "n1": (normed, norm_out.at[layer, 1], 1),
                 "q": (q_buf, q_out.at[layer], 2), "k": (k_buf, k_out.at[layer], 3), "v": (v_buf, v_out.at[layer], 4),
                 "o": (o_buf, o_out.at[layer], 5)}
        for half in TWO:
            for part in COLORS:
                parts[f"a{half}{part}"] = (gelu_buf.at[half, :, slice(third * part, third * (part + 1))],
                                           gelu_out.at[layer, 3 * half + part], 6 + 3 * half + part)
        return [pltpu.make_async_copy(parts[name][0], parts[name][1], save_sem.at[parts[name][2]]) for name in names]

    gelu_names = [f"a{half}{part}" for half in TWO for part in COLORS]

    def hidden_copies(layer, order):
        slot, part, at = _rem(order, 2), order // 6, _at(_rem(order, 6) * COLS, COLS)
        return [pltpu.make_async_copy(hid_buf.at[slot, half], hid_out.at[layer, part, half, :, at],
                                      hid_sem.at[slot, half]) for half in TWO]

    def compute(chunk):
        layer, index = chunk // PER_HALF, _rem(chunk, PER_HALF)
        pair = pair_copy(chunk)
        pair.wait_send()
        pair.wait_recv()
        keep_copy(chunk).start()

        def weights(role):
            block = wbuf[_rem(chunk, slots)] if role == 0 else peer[_rem(chunk, RING)]
            return block.reshape(third, COLS)

        @pl.when(index == 0)
        def _():
            normed[ALL] = _rms(state[ALL])
            for copy in save_copies(layer, ["n0"]):
                copy.start()

        @pl.when(index < 3)
        def _():
            for role, half in torus.sides:
                q_buf[:, _at(3 * COLS * half + COLS * index, COLS)] = _dot(
                    normed[ALL], weights(role)).astype(jnp.bfloat16)

        @pl.when(index == 3)
        def _():
            for role, half in torus.sides:
                both = _dot(normed[ALL], weights(role)).astype(jnp.bfloat16)
                k_buf[:, _at(HEAD * half, HEAD)] = both[:, :HEAD]
                v_buf[:, _at(HEAD * half, HEAD)] = both[:, HEAD:]

        @pl.when(index == QKV)
        def _():
            acc[ALL] = jnp.zeros_like(acc)
            for copy in save_copies(layer, ["q", "k", "v"]):
                copy.start()

        @pl.when((index >= QKV) & (index < ATTN))
        def _():
            causal = _causal(seq)
            for role, half in torus.sides:
                key, value = k_buf[:, _at(HEAD * half, HEAD)], v_buf[:, _at(HEAD * half, HEAD)]
                outs = []
                for head in TWO:
                    at = _at(3 * COLS * half + COLS * (index - QKV) + HEAD * head, HEAD)
                    prob = _probs(q_buf[:, at], key, causal)
                    outs.append(_dot(prob.astype(jnp.bfloat16), value).astype(jnp.bfloat16))
                block = jnp.concatenate(outs, axis=1)
                o_buf[3 * half + index - QKV] = block
                acc[ALL] += _dot_rhs_t(block, weights(role))

        @pl.when(index == 6)
        def _():
            middle = (state[ALL].astype(jnp.float32) + acc[ALL]).astype(jnp.bfloat16)
            state[ALL] = middle
            acts[2 * layer] = middle
            for copy in save_copies(layer, ["n0"]):
                copy.wait()
            normed[ALL] = _rms(middle)
            for copy in save_copies(layer, ["n1", "o"]):
                copy.start()

        @pl.when((index >= 8) & (index < 26))
        def _():
            for copy in hidden_copies(layer, index - 8):
                copy.wait()

        @pl.when((index >= ATTN) & (index < UP_BLOCKS))
        def _():
            for role, half in torus.sides:
                hidden = _dot(normed[ALL], weights(role))
                hid_buf[_rem(index - ATTN, 2), half] = hidden
                gelu_buf[half, :, _at(COLS * (index - ATTN), COLS)] = jax.nn.gelu(hidden).astype(jnp.bfloat16)
            for copy in hidden_copies(layer, index - ATTN):
                copy.start()

        @pl.when(index == UP_BLOCKS)
        def _():
            for copy in save_copies(layer, gelu_names):
                copy.start()

        @pl.when(index >= UP_BLOCKS)
        def _():
            part, at = (index - UP_BLOCKS) // 6, _at(COLS * _rem(index - UP_BLOCKS, 6), COLS)
            total = sum(_dot(gelu_buf[half, :, _at(third * part, third)], weights(role))
                        for role, half in torus.sides)

            @pl.when(part == 0)
            def _():
                acc[:, at] = total

            @pl.when(part > 0)
            def _():
                acc[:, at] += total

        @pl.when(index == PER_HALF - 1)
        def _():
            result = (state[ALL].astype(jnp.float32) + acc[ALL]).astype(jnp.bfloat16)
            state[ALL] = result

            @pl.when(layer < n_layers - 1)
            def _():
                acts[2 * layer + 1] = result

            @pl.when(layer == n_layers - 1)
            def _():
                y_ref[ALL] = result
            for copy in save_copies(layer, ["n1", "q", "k", "v", "o"] + gelu_names):
                copy.wait()

        keep_copy(chunk).wait()

    steps = [(0, assemble), (0, enter)] + [((part + 1) * LAG, functools.partial(pass_on, part)) for part in range(5)]
    torus.run(steps + [(ready, exchange), (last_lag, compute)], n_chunks, n_chunks + last_lag)


def forward_stack(x_loc, rows, down):
    n_layers = down.shape[0]
    seq, width = x_loc.shape
    bf16, f32 = jnp.bfloat16, jnp.float32
    slots = 6 * LAG + 4
    chunk = CUBE + (ROWS, COLS)
    shape = jax.ShapeDtypeStruct
    hbm = pl.BlockSpec(memory_space=pl.ANY)
    vmem = pl.BlockSpec(memory_space=pltpu.VMEM)
    dma = pltpu.SemaphoreType.DMA
    return pl.pallas_call(
        functools.partial(forward_kernel, n_layers),
        name="forward_stack",
        out_shape=(shape((seq, width), bf16), shape((2 * n_layers - 1, seq, width), bf16),
                   shape((n_layers, 4, 4, 4, ROWS, PER_HALF * COLS), bf16),
                   shape((n_layers, 3, 2, seq, width), f32), shape((n_layers, 6, seq, width), bf16),
                   shape((n_layers, 2, seq, width), bf16), shape((n_layers, seq, width), bf16),
                   shape((n_layers, seq, 2 * HEAD), bf16), shape((n_layers, seq, 2 * HEAD), bf16),
                   shape((n_layers, 6, seq, COLS), bf16)),
        in_specs=[vmem] * 3,
        out_specs=(vmem,) * 2 + (hbm,) * 8,
        scratch_shapes=[
            pltpu.VMEM((slots,) + chunk, bf16), pltpu.VMEM((RING,) + chunk, bf16),
            pltpu.VMEM((n_layers, ROWS, PER_HALF * COLS), bf16), pltpu.VMEM(rows.shape[1:], bf16),
            pltpu.VMEM((seq, width), bf16), pltpu.VMEM((seq, width), bf16),
            pltpu.VMEM((seq, 6 * COLS), bf16), pltpu.VMEM((seq, 2 * HEAD), bf16), pltpu.VMEM((seq, 2 * HEAD), bf16),
            pltpu.VMEM((6, seq, COLS), bf16), pltpu.VMEM((2, seq, 18 * COLS), bf16),
            pltpu.VMEM((2, 2, seq, COLS), f32), pltpu.VMEM((seq, width), f32),
            dma((6, RING)), dma((6, RING)), dma((RING,)), dma((RING,)), dma((RING,)), dma((12,)), dma((2, 2)), dma((2,)),
            pltpu.SemaphoreType.REGULAR((7,))],
        compiler_params=pltpu.CompilerParams(collective_id=1, has_side_effects=True,
                                             vmem_limit_bytes=VMEM_LIMIT),
    )(x_loc, rows, down)


def backward_kernel(n_layers, *refs):
    (g_ref, x_ref, acts, w_own, hid_in, gelu_in, norm_in, q_in, k_in, v_in, o_in,
     rows_out, down_out, dx_ref,
     mine, theirs, lefts, rights, hid_buf, dact, dnorm, q_buf, k_buf, v_buf, x_mid, x_in, dk_acc, dv_acc,
     outgo, peer, out, away, sum0, sum1, sum2, sa0, ra0, sb0, rb0, sa1, ra1, sb1, rb1, sa2, ra2, sb2, rb2,
     load_sem, own_sem, push_send, push_recv, pair_send, pair_recv, ring_send, ring_recv, swap_sem, credit) = refs
    torus = Torus(credit)
    core, place, near = torus.core, torus.place, torus.near
    sums = (sum0, sum1, sum2)
    half_bufs = ((sa0, ra0), (sa1, ra1), (sa2, ra2))
    full_bufs = ((sb0, rb0), (sb1, rb1), (sb2, rb2))
    n_chunks = n_layers * PER_HALF
    seq, width = g_ref.shape
    third = 64 * ROWS
    leads = sum0.shape[0]

    def pair_of(chunk):
        return n_layers - 1 - chunk // PER_HALF

    def columns(chunk):
        index = _rem(chunk, PER_HALF)
        block = jnp.where(index < DOWN_DONE, UP_BLOCKS + index,
                          jnp.where(index < UP_DONE, index - 11, jnp.where(index < O_DONE, index - 32, index - 39)))
        return _at(block * COLS, COLS)

    def loads(pair, names):
        def source(name):
            return {"a": (gelu_in.at[pair], lefts.at[0:6], 0), "n_mlp": (norm_in.at[pair, 1], lefts.at[NORM_MLP], 1),
                    "n_attn": (norm_in.at[pair, 0], lefts.at[NORM_ATTN], 2), "o": (o_in.at[pair], rights.at[O_AT:QKV_AT], 3),
                    "q": (q_in.at[pair], q_buf, 4), "k": (k_in.at[pair], k_buf, 5), "v": (v_in.at[pair], v_buf, 6),
                    "x_mid": (acts.at[2 * pair], x_mid, 7), "h0": (hid_in.at[pair, 0], hid_buf, 8),
                    "h1": (hid_in.at[pair, 1], hid_buf, 8), "h2": (hid_in.at[pair, 2], hid_buf, 8)}[name]
        return [pltpu.make_async_copy(source(name)[0], source(name)[1], load_sem.at[source(name)[2]])
                for name in names]

    def start(pair, names):
        for copy in loads(pair, names):
            copy.start()

    def finish(pair, names):
        for copy in loads(pair, names):
            copy.wait()

    def first_input(ref):
        return pltpu.make_async_copy(ref, x_in, load_sem.at[9])

    start(n_layers - 1, ["a"])
    for block in SIX:
        rights[block] = g_ref[:, COLS * block:COLS * block + COLS]
    torus.meet()
    finish(n_layers - 1, ["a"])

    def own_copy(chunk):
        slot = _rem(chunk, SLOTS)
        return pltpu.make_async_copy(w_own.at[pair_of(chunk), :, :, :, :, columns(chunk)], mine.at[slot],
                                     own_sem.at[slot])

    def push_copy(chunk):
        slot = _rem(chunk, SLOTS)
        return torus.remote(w_own.at[pair_of(chunk), :, :, :, :, columns(chunk)], theirs.at[slot],
                            push_send.at[slot], push_recv.at[slot], torus.sibling)

    def fetch(chunk):
        own_copy(chunk).start()
        push_copy(chunk).start()

    def total_grad():
        return jnp.concatenate([rights[block] for block in SIX], axis=1).astype(jnp.float32)

    def consume(chunk):
        pair, index = pair_of(chunk), _rem(chunk, PER_HALF)
        slot = _rem(chunk, SLOTS)
        own_copy(chunk).wait()
        push = push_copy(chunk)
        push.wait_send()
        push.wait_recv()

        def weights(role):
            return (mine, theirs)[role][slot].reshape(third, COLS)

        @pl.when(index == 0)
        def _():
            start(pair, ["n_mlp", "n_attn", "o", "q", "k", "v", "x_mid", "h0"])

            @pl.when(pair == 0)
            def _():
                first_input(x_ref).start()

            @pl.when(pair > 0)
            def _():
                first_input(acts.at[2 * pair - 1]).start()

        for part in (1, 2):
            @pl.when(index == 6 * part)
            def _(part=part):
                start(pair, [f"h{part}"])

        @pl.when((index < DOWN_DONE) & (_rem(index, 6) == 0))
        def _():
            dact[ALL] = jnp.zeros_like(dact)

        @pl.when(index < DOWN_DONE)
        def _():
            for role, half in torus.sides:
                dact[half] += _dot_rhs_t(rights[_rem(index, 6)], weights(role))

        @pl.when((index < DOWN_DONE) & (_rem(index, 6) == 5))
        def _():
            finish(pair, ["h0"])
            for half in TWO:
                for block in SIX:
                    cols = slice(COLS * block, COLS * block + COLS)
                    hidden = hid_buf[half, :, cols]
                    bend = jnp.tanh(0.7978845608028654 * (hidden + 0.044715 * (hidden * hidden * hidden)))
                    slope = 0.5 * (1.0 + bend) + 0.5 * hidden * (1.0 - bend * bend) * (
                        0.7978845608028654 * (1.0 + 0.134145 * (hidden * hidden)))
                    rights[DH_AT + FF * half + index - 5 + block] = (dact[half, :, cols] * slope).astype(jnp.bfloat16)

        @pl.when(index == DOWN_DONE - 1)
        def _():
            finish(pair, ["n_mlp"])

        @pl.when(index == DOWN_DONE)
        def _():
            dnorm[ALL] = jnp.zeros_like(dnorm)

            @pl.when(pair > 0)
            def _():
                start(pair - 1, ["a"])

        @pl.when((index >= DOWN_DONE) & (index < UP_DONE))
        def _():
            dnorm[ALL] += sum(_dot_rhs_t(rights[DH_AT + FF * half + index - DOWN_DONE], weights(role))
                              for role, half in torus.sides)

        @pl.when(index == UP_DONE - 1)
        def _():
            finish(pair, ["x_mid", "o"])
            lefts[GRAD] = (total_grad() + _rms_back(x_mid[ALL], dnorm[ALL])).astype(jnp.bfloat16)

        @pl.when(index == UP_DONE)
        def _():
            finish(pair, ["q", "k", "v"])
            dk_acc[ALL] = jnp.zeros_like(dk_acc)
            dv_acc[ALL] = jnp.zeros_like(dv_acc)

        @pl.when((index >= UP_DONE) & (index < O_DONE))
        def _():
            causal = _causal(seq)
            for role, half in torus.sides:
                d_o = _dot(lefts[GRAD], weights(role)).astype(jnp.bfloat16)
                key, value = k_buf[:, _at(HEAD * half, HEAD)], v_buf[:, _at(HEAD * half, HEAD)]
                d_q = []
                for head in TWO:
                    query = q_buf[:, _at(3 * COLS * half + COLS * (index - UP_DONE) + HEAD * head, HEAD)]
                    d_head = d_o[:, HEAD * head:HEAD * head + HEAD]
                    prob = _probs(query, key, causal)
                    d_prob = _dot_rhs_t(d_head, value)
                    dv_acc[half] += _dot_lhs_t(prob.astype(jnp.bfloat16), d_head)
                    d_score = prob * (d_prob - jnp.sum(prob * d_prob, axis=-1, keepdims=True))
                    d_score = (d_score * (HEAD ** -0.5)).astype(jnp.bfloat16)
                    d_q.append(_dot(d_score, key).astype(jnp.bfloat16))
                    dk_acc[half] += _dot_lhs_t(d_score, query)
                rights[QKV_AT + QKV * half + index - UP_DONE] = jnp.concatenate(d_q, axis=1)

        @pl.when(index == O_DONE - 1)
        def _():
            finish(pair, ["n_attn"])
            for half in TWO:
                rights[QKV_AT + QKV * half + QKV - 1] = jnp.concatenate([dk_acc[half], dv_acc[half]], axis=1).astype(jnp.bfloat16)

        @pl.when(index == O_DONE)
        def _():
            dnorm[ALL] = jnp.zeros_like(dnorm)

        @pl.when(index >= O_DONE)
        def _():
            dnorm[ALL] += sum(_dot_rhs_t(rights[QKV_AT + QKV * half + index - O_DONE], weights(role))
                              for role, half in torus.sides)

        @pl.when(index == PER_HALF - 1)
        def _():
            first_input(x_ref).wait()

            @pl.when(pair > 0)
            def _():
                finish(pair - 1, ["a"])
            result = (lefts[GRAD].astype(jnp.float32) + _rms_back(x_in[ALL], dnorm[ALL])).astype(jnp.bfloat16)
            dx_ref[ALL] = result
            for block in SIX:
                rights[block] = result[:, COLS * block:COLS * block + COLS]

    def pair_copy(slot):
        return torus.remote(outgo.at[slot], peer.at[slot], pair_send.at[slot], pair_recv.at[slot], torus.sibling)

    def multiply(chunk):
        index = _rem(chunk, PER_HALF)
        slot = _rem(chunk, RING)
        quarter = third // RING
        for role, half in torus.sides[::-1]:
            left = jnp.where(index < DOWN_DONE, 3 * half + index // 6,
                             jnp.where(index < UP_DONE, NORM_MLP, jnp.where(index < O_DONE, GRAD, NORM_ATTN)))
            right = jnp.where(index < DOWN_DONE, _rem(index, 6),
                              jnp.where(index < UP_DONE, DH_AT + FF * half + index - DOWN_DONE,
                                        jnp.where(index < O_DONE, O_AT + 3 * half + index - UP_DONE, QKV_AT + QKV * half + index - O_DONE)))
            for z in range(RING):
                part = _dot_lhs_t(lefts[left, :, quarter * z:quarter * z + quarter], rights[right])
                if role == 0:
                    sum0[_rem(chunk, leads), z] = part.reshape(RING, RING, ROWS, COLS)
                else:
                    outgo[slot, z] = part.astype(jnp.bfloat16).reshape(RING, RING, ROWS, COLS)
        pair_copy(slot).start()

    def merge_pair(chunk):
        slot, lead = _rem(chunk, RING), _rem(chunk, leads)
        pair_copy(slot).wait_send()
        pair_copy(slot).wait_recv()
        for z in range(RING):
            for y in range(RING):
                sum0[lead, z, y] = sum0[lead, z, y] + peer[slot, z, y].astype(jnp.float32)

    def ring_copy(stage, part, slot, color, way):
        send, recv = (half_bufs, full_bufs)[part][stage]
        dim = ORDERS[color][stage]
        return torus.remote(send.at[slot, color, way], recv.at[slot, color, way],
                            ring_send.at[2 * stage + part, slot], ring_recv.at[2 * stage + part, slot],
                            {dim: near[way][dim]})

    def ring_wait(stage, part, slot):
        send, recv = (half_bufs, full_bufs)[part][stage]
        whole = torus.remote(send.at[slot], recv.at[slot], ring_send.at[2 * stage + part, slot],
                             ring_recv.at[2 * stage + part, slot], torus.sibling)
        whole.wait_send()
        whole.wait_recv()

    def source(stage, chunk, color, position, cols):
        lead = _rem(chunk, leads)
        if stage == 0:
            return sum0[(lead,) + _block(color, 0, position) + (_rows(color), cols)]
        return sums[stage][(lead, color) + _block(color, stage, position) + (EVERY, cols)]

    left_cols, right_cols, every = slice(0, COLS // 2), slice(COLS // 2, COLS), slice(0, COLS)

    def store_halves(stage, chunk):
        slot = _rem(chunk, RING)
        send = half_bufs[stage][0]
        for color in COLORS:
            far = torus.far[ORDERS[color][stage]]
            send[slot, color, 0] = source(stage, chunk, color, far, left_cols).astype(jnp.bfloat16)
            send[slot, color, 1] = source(stage, chunk, color, far, right_cols).astype(jnp.bfloat16)

    def store_fulls(stage, chunk):
        slot = _rem(chunk, RING)
        ring_wait(stage, 0, slot)
        recv = half_bufs[stage][1]
        send = full_bufs[stage][0]
        lead = (EVERY,) * (len(send.shape) - 4)
        for color in COLORS:
            dim = ORDERS[color][stage]
            for way, summed, plain in ((0, left_cols, right_cols), (1, right_cols, left_cols)):
                send[(slot, color, way) + lead + (summed,)] = (
                    source(stage, chunk, color, near[way][dim], summed)
                    + recv[slot, color, way].astype(jnp.float32)).astype(jnp.bfloat16)
                send[(slot, color, way) + lead + (plain,)] = source(
                    stage, chunk, color, near[way][dim], plain).astype(jnp.bfloat16)

    def close_stage(stage, chunk):
        slot = _rem(chunk, RING)
        ring_wait(stage, 1, slot)
        recv = full_bufs[stage][1]
        for color in COLORS:
            dim = ORDERS[color][stage]
            total = (source(stage, chunk, color, place[dim], every)
                     + recv[slot, color, 0].astype(jnp.float32)
                     + recv[slot, color, 1].astype(jnp.float32))
            if stage < 2:
                sums[stage + 1][_rem(chunk, leads), color] = total
            else:
                out[pair_of(chunk), _rows(color), columns(chunk)] = total

    def send_all(stage, part, chunk):
        for color in COLORS:
            for way in TWO:
                ring_copy(stage, part, _rem(chunk, RING), color, way).start()

    def open_first(chunk):
        merge_pair(chunk)
        store_halves(0, chunk)
        send_all(0, 0, chunk)

    def middle(stage, chunk):
        store_fulls(stage, chunk)
        send_all(stage, 1, chunk)

    def turn(stage, chunk):
        close_stage(stage, chunk)
        if stage < 2:
            store_halves(stage + 1, chunk)
            send_all(stage + 1, 0, chunk)

    base = 0
    steps = [(0, fetch), (base + 2 * LAG, functools.partial(middle, 0)), (base + LAG, open_first),
             (base + 3 * LAG, functools.partial(turn, 0)), (base + 4 * LAG, functools.partial(middle, 1)),
             (base + 5 * LAG, functools.partial(turn, 1)), (base + 6 * LAG, functools.partial(middle, 2)),
             (base + 7 * LAG, functools.partial(turn, 2)), (1, consume), (0, multiply)]
    torus.run(steps, n_chunks, n_chunks + base + 7 * LAG)

    half_rows = ROWS // 2
    for layer in range(n_layers):
        for part in range(5):
            cols = slice(FIFTH * part, FIFTH * part + FIFTH)
            both = out[layer, :, cols]
            low, high = both[:half_rows], both[half_rows:]
            rows_out[core, layer, :, cols] = jnp.where(core == 0, low, high)
            away[layer, :, cols] = jnp.where(core == 0, high, low)
    swap = torus.remote(away, rows_out.at[core], swap_sem.at[0], swap_sem.at[1], torus.sibling)
    down_out[ALL] = out[:, :, UP_END:]
    swap.start()
    swap.wait_send()
    swap.wait_recv()


def backward_stack(n_layers, g_loc, *saved):
    seq, width = g_loc.shape
    bf16, f32 = jnp.bfloat16, jnp.float32
    half = COLS // 2
    chunk = CUBE + (ROWS, COLS)
    leads = 7
    shape = jax.ShapeDtypeStruct
    hbm = pl.BlockSpec(memory_space=pl.ANY)
    vmem = pl.BlockSpec(memory_space=pltpu.VMEM)
    dma = pltpu.SemaphoreType.DMA
    half_rows = ROWS // 2
    scratch = [pltpu.VMEM((SLOTS,) + chunk, bf16), pltpu.VMEM((SLOTS,) + chunk, bf16),
               pltpu.VMEM((9, seq, width), bf16), pltpu.VMEM((56, seq, COLS), bf16),
               pltpu.VMEM((2, seq, width), f32), pltpu.VMEM((2, seq, width), f32), pltpu.VMEM((seq, width), f32),
               pltpu.VMEM((seq, 6 * COLS), bf16), pltpu.VMEM((seq, 2 * HEAD), bf16), pltpu.VMEM((seq, 2 * HEAD), bf16),
               pltpu.VMEM((seq, width), bf16), pltpu.VMEM((seq, width), bf16),
               pltpu.VMEM((2, seq, HEAD), f32), pltpu.VMEM((2, seq, HEAD), f32),
               pltpu.VMEM((RING,) + chunk, bf16), pltpu.VMEM((RING,) + chunk, bf16),
               pltpu.VMEM((n_layers, ROWS, PER_HALF * COLS), f32), pltpu.VMEM((n_layers, half_rows, UP_END), f32),
               pltpu.VMEM((leads,) + chunk, f32), pltpu.VMEM((leads, 3, RING, RING, TILE, COLS), f32),
               pltpu.VMEM((leads, 3, RING, TILE, COLS), f32)]
    for size in ((RING, RING), (RING,), ()):
        scratch += [pltpu.VMEM((RING, 3, 2) + size + (TILE, half), bf16)] * 2
        scratch += [pltpu.VMEM((RING, 3, 2) + size + (TILE, COLS), bf16)] * 2
    scratch += [dma((10,)), dma((SLOTS,)), dma((SLOTS,)), dma((SLOTS,)), dma((RING,)), dma((RING,)), dma((6, RING)), dma((6, RING)), dma((2,)),
                pltpu.SemaphoreType.REGULAR((7,))]
    return pl.pallas_call(
        functools.partial(backward_kernel, n_layers),
        name="backward_stack",
        out_shape=(shape((2, n_layers, half_rows, UP_END), f32),
                   shape((n_layers, ROWS, (PER_HALF - UP_BLOCKS) * COLS), f32), shape((seq, width), bf16)),
        in_specs=[vmem] + [hbm] * len(saved),
        out_specs=(vmem,) * 3,
        scratch_shapes=scratch,
        compiler_params=pltpu.CompilerParams(collective_id=0, has_side_effects=True,
                                             vmem_limit_bytes=VMEM_LIMIT),
    )(g_loc, *saved)


LANES = 128


def _moves(chips, block, packed_first):
    moves = []
    for half in TWO:
        for part in COLORS:
            for chip in range(chips):
                packed = chips * ROWS * (3 * half + part) + ROWS * chip
                plain = block * (2 * chip + half) + ROWS * part
                pair = (packed, plain) if packed_first else (plain, packed)
                moves.append(pair + (min(ROWS, block - ROWS * part),))
    return moves


def _pieces(moves, size):
    tiles = [[] for _ in range(size // LANES)]
    for target, source, length in moves:
        while length:
            step = min(length, LANES - target % LANES, LANES - source % LANES)
            tiles[target // LANES].append((target % LANES, source // LANES, (target - source) % LANES))
            target, source, length = target + step, source + step, length - step
    return [sorted(tile) for tile in tiles]


def _gather_tile(load, tile, lane):
    total = None
    for first, source, shift in tile:
        value = load(source)
        if shift:
            value = pltpu.roll(value, shift, axis=value.ndim - 1)
        total = value if total is None else jnp.where(lane >= first, value, total)
    return total


def _span(index, size):
    return slice(size * index, size * index + size)


def pack_kernel(chips, q_ref, k_ref, v_ref, o_ref, up_ref, down_ref, rows_out, down_out, wide):
    rows, layers, cols = up_ref.shape
    block, _, width = down_ref.shape
    heads = q_ref.shape[1] // 2
    for half in TWO:
        for layer in range(layers):
            for at, ref in ((0, q_ref), (heads + 2, o_ref)):
                for head in range(heads):
                    rows_out[half, layer, :, _span(at + head, LANES)] = ref[
                        :, heads * half + head].astype(jnp.float32)[:, layer].astype(jnp.bfloat16)
            for at, ref in ((heads, k_ref), (heads + 1, v_ref)):
                rows_out[half, layer, :, _span(at, LANES)] = ref[layer].astype(
                    jnp.float32)[:, half].astype(jnp.bfloat16)
    for tile in range(cols // LANES):
        both = up_ref[:, :, _span(tile, LANES)].astype(jnp.float32)
        for layer in range(layers):
            wide[layer, :, _span(tile, LANES)] = both[:, layer]
    lane = lax.broadcasted_iota(jnp.int32, (layers, rows, LANES), 2)
    half_f = 3 * chips * ROWS
    for index, tile in enumerate(_pieces(_moves(chips, block, True), 2 * half_f)):
        value = _gather_tile(lambda source: wide[:, :, _span(source, LANES)], tile, lane)
        half, at = divmod(LANES * index, half_f)
        if at >= 2 * chips * ROWS:
            position = lax.rem(lane + LANES * index % ROWS, ROWS)
            value = jnp.where(position < block - 2 * ROWS, value, 0.0)
        start = ATTN * COLS + at
        rows_out[half, :, :, start:start + LANES] = value.astype(jnp.bfloat16)
    for part in COLORS:
        used = min(ROWS, block - ROWS * part)
        value = down_ref[ROWS * part:ROWS * part + used].astype(jnp.float32)
        for layer in range(layers):
            one = value[:, layer]
            if used < ROWS:
                one = jnp.concatenate([one, jnp.zeros((ROWS - used, width), jnp.float32)], axis=0)
            down_out[layer, :, _span(part, width)] = one.astype(jnp.bfloat16)


def pack_weights(w_q, w_k, w_v, w_o, w_up, w_down, chips):
    layers, rows = w_up.shape[:2]
    width = w_down.shape[2]
    vmem = pl.BlockSpec(memory_space=pltpu.VMEM)
    shape = jax.ShapeDtypeStruct
    return pl.pallas_call(
        functools.partial(pack_kernel, chips), name="pack_weights",
        out_shape=(shape((2, layers, rows, UP_END), jnp.bfloat16), shape((layers, ROWS, 3 * width), jnp.bfloat16)),
        in_specs=[vmem] * 6, out_specs=(vmem,) * 2,
        scratch_shapes=[pltpu.VMEM(w_up.shape, jnp.float32)],
        compiler_params=pltpu.CompilerParams(vmem_limit_bytes=VMEM_LIMIT),
    )(w_q.transpose(1, 2, 0, 3), w_k, w_v, w_o.transpose(1, 2, 0, 3), w_up.transpose(1, 0, 2),
      w_down.transpose(1, 0, 2))


def unpack_kernel(chips, rows_ref, down_ref, y_ref, dx_ref, q_out, k_out, v_out, o_out, up_out, down_out, y_out,
                  dx_out):
    rows, layers, cols = up_out.shape
    block, _, width = down_out.shape
    heads = q_out.shape[1] // 2
    for half in TWO:
        for layer in range(layers):
            for at, ref in ((0, q_out), (heads + 2, o_out)):
                for head in range(heads):
                    ref[:, heads * half + head, layer, :] = rows_ref[half, layer, :, _span(at + head, LANES)]
            for at, ref in ((heads, k_out), (heads + 1, v_out)):
                ref[layer, :, half, :] = rows_ref[half, layer, :, _span(at, LANES)]
    lane = lax.broadcasted_iota(jnp.int32, (layers, rows, LANES), 2)
    half_f = 3 * chips * ROWS

    def load(source):
        half, at = divmod(LANES * source, half_f)
        return rows_ref[half, :, :, ATTN * COLS + at:ATTN * COLS + at + LANES]

    for index, tile in enumerate(_pieces(_moves(chips, block, False), cols)):
        value = _gather_tile(load, tile, lane)
        for layer in range(layers):
            up_out[:, layer, _span(index, LANES)] = value[layer]
    for part in COLORS:
        used = min(ROWS, block - ROWS * part)
        for layer in range(layers):
            down_out[ROWS * part:ROWS * part + used, layer, :] = down_ref[layer, :used, _span(part, width)]
    y_out[ALL] = y_ref[ALL]
    dx_out[ALL] = dx_ref[ALL]


def unpack_grads(row_grad, down_grad, y_loc, grad_x, shapes, chips):
    vmem = pl.BlockSpec(memory_space=pltpu.VMEM)
    q_shape, k_shape, _, _, up_shape, down_shape = shapes
    layers, rows, heads, head_dim = q_shape
    turned = [(rows, heads, layers, head_dim), k_shape, k_shape, (rows, heads, layers, head_dim),
              (rows, layers, up_shape[2]), (down_shape[1], layers, down_shape[2])]
    shape = jax.ShapeDtypeStruct
    outs = pl.pallas_call(
        functools.partial(unpack_kernel, chips), name="unpack_grads",
        out_shape=tuple(shape(full, jnp.float32) for full in turned) + tuple(
            shape(value.shape, value.dtype) for value in (y_loc, grad_x)),
        in_specs=[vmem] * 4, out_specs=(vmem,) * 8,
        compiler_params=pltpu.CompilerParams(vmem_limit_bytes=VMEM_LIMIT),
    )(row_grad, down_grad, y_loc, grad_x)
    d_q, d_k, d_v, d_o, d_up, d_down, y_out, dx_out = outs
    return (y_out[None], dx_out[None], d_q.transpose(2, 0, 1, 3), d_k, d_v, d_o.transpose(2, 0, 1, 3),
            d_up.transpose(1, 0, 2), d_down.transpose(1, 0, 2))


def solution(mesh):
    mesh4 = Mesh(mesh.devices.reshape(CUBE + (2,)), ALL_AXES)
    row_spec = P(ALL_AXES)
    weight_spec = P(None, ALL_AXES)

    def body(x_in, w_q, w_k, w_v, w_o, w_up, w_down, grad_out):
        weights = (w_q, w_k, w_v, w_o, w_up, w_down)
        chips = w_up.shape[2] // w_down.shape[1] // 2
        rows, down = pack_weights(*weights, chips)
        y_loc, acts, *saved = forward_stack(x_in[0], rows, down)
        row_grad, down_grad, grad_x = backward_stack(w_q.shape[0], grad_out[0], x_in[0], acts, *saved)
        return unpack_grads(row_grad, down_grad, y_loc, grad_x, [weight.shape for weight in weights], chips)

    return jax.shard_map(body, mesh=mesh4, in_specs=(row_spec,) + (weight_spec,) * 6 + (row_spec,),
                         out_specs=(row_spec, row_spec) + (weight_spec,) * 6, check_vma=False)
```

```python
import functools

import jax
import jax.numpy as jnp
from jax import lax
from jax.experimental import pallas as pl
from jax.experimental.pallas import tpu as pltpu
from jax.sharding import Mesh, PartitionSpec as P

MESH = pl.DeviceIdType.MESH
ALL_AXES = ("z", "y", "x", "c")
EPS = 1e-6
MASK_FILL = -1e30
DIMS = ("z", "y", "x")
ORDERS = (("x", "y", "z"), ("y", "z", "x"), ("z", "x", "y"))
COLS = 256
ROWS = 24
LAG = 2
HEAD = 128
PER_HALF = 43
UP_BLOCKS = 25
UP_END = UP_BLOCKS * COLS
RING = 4
CUBE = (RING, RING, RING)
SLOTS = 3
EVEN, EARLY, LATE = range(3)
AHEAD = 8
MANY = 2 * AHEAD
TILE = 8
COLORS = range(3)
TWO = range(2)
SIX = range(6)
ALL = Ellipsis
EVERY = slice(None)
QKV, ATTN, FF = 4, 7, 18
DOWN_DONE, UP_DONE, O_DONE = 18, 36, 39
G_AT, DH_AT, O_AT, QKV_AT = 0, 6, 42, 48
NORM_MLP, GRAD, NORM_ATTN = 6, 7, 8
VMEM_LIMIT = 67043328


FIFTH = UP_END // 5


def _rows(color):
    return slice(TILE * color, TILE * color + TILE)


def _rem(value, by):
    return lax.rem(value, by)


def _block(color, stage, position):
    dims = tuple(dim for dim in DIMS if dim not in ORDERS[color][:stage])
    return tuple(position if dim == ORDERS[color][stage] else EVERY for dim in dims)


def _dot(left, right):
    return jnp.dot(left, right, preferred_element_type=jnp.float32)


def _dot_rhs_t(left, right):
    return lax.dot_general(left, right, (((1,), (1,)), ((), ())), preferred_element_type=jnp.float32)


def _dot_lhs_t(left, right):
    return lax.dot_general(left, right, (((0,), (0,)), ((), ())), preferred_element_type=jnp.float32)


def _at(start, size):
    return pl.ds(pl.multiple_of(start, size), size)


def _causal(seq):
    return (lax.broadcasted_iota(jnp.int32, (seq, seq), 0) >= lax.broadcasted_iota(jnp.int32, (seq, seq), 1))


def _probs(query, key, causal):
    scores = jnp.where(causal, _dot_rhs_t(query, key) * (HEAD ** -0.5), MASK_FILL)
    weight = jnp.exp(scores - jnp.max(scores, axis=-1, keepdims=True))
    return weight / jnp.sum(weight, axis=-1, keepdims=True)


def _rms(values):
    wide = values.astype(jnp.float32)
    return (wide * lax.rsqrt(jnp.mean(wide * wide, axis=-1, keepdims=True) + EPS)).astype(jnp.bfloat16)


def _rms_back(values, grad):
    wide = values.astype(jnp.float32)
    scale = lax.rsqrt(jnp.mean(wide * wide, axis=-1, keepdims=True) + EPS)
    return scale * grad - wide * (scale * scale * scale) * jnp.mean(wide * grad, axis=-1, keepdims=True)


class Torus:
    def __init__(self, credit):
        self.core = lax.axis_index("c")
        self.place = {dim: lax.axis_index(dim) for dim in DIMS}
        self.near = tuple({dim: _rem(self.place[dim] + step, 4) for dim in DIMS} for step in (1, 3))
        self.far = {dim: _rem(self.place[dim] + 2, 4) for dim in DIMS}
        self.sibling = {"c": 1 - self.core}
        self.sides = ((0, self.core), (1, 1 - self.core))
        self.credit = credit
        self.partners = [({dim: self.near[way][dim]}, 2 * d + 1 - way, 2 * d + way)
                         for d, dim in enumerate(DIMS) for way in TWO]
        self.partners.append((self.sibling, 6, 6))

    def meet(self):
        barrier = pltpu.get_barrier_semaphore()
        for device, _, _ in self.partners:
            pl.semaphore_signal(barrier, inc=1, device_id=device, device_id_type=MESH)
        pl.semaphore_wait(barrier, len(self.partners))

    def remote(self, source, target, send_sem, recv_sem, device):
        return pltpu.make_async_remote_copy(src_ref=source, dst_ref=target, send_sem=send_sem, recv_sem=recv_sem,
                                            device_id=device, device_id_type=MESH)

    def run(self, steps, n_chunks, n_ticks, after=None):
        def tick(now, carry):
            @pl.when(now >= 2)
            def _():
                for _, _, mine in self.partners:
                    pl.semaphore_wait(self.credit.at[mine], 1)

            for lag, pace, action in steps:
                beat = now - lag
                if pace == EVEN:
                    @pl.when((beat >= 0) & (beat < n_chunks))
                    def _(beat=beat, action=action):
                        action(beat)
                    continue
                if pace == EARLY:
                    double = beat < AHEAD
                    first = jnp.where(double, 2 * beat, beat + AHEAD)
                    active = (beat >= 0) & (beat < n_chunks - AHEAD)
                else:
                    double = beat >= n_chunks - AHEAD
                    first = jnp.where(double, 2 * beat - n_chunks, beat - AHEAD)
                    active = (beat >= AHEAD) & (beat < n_chunks)

                @pl.when(active)
                def _(first=first, double=double, action=action):
                    def one(order, inner):
                        action(first + order)
                        return inner
                    lax.fori_loop(0, jnp.where(double, 2, 1), one, 0)

            if after is not None:
                after(now)

            @pl.when(now < n_ticks - 2)
            def _():
                for device, theirs, _ in self.partners:
                    pl.semaphore_signal(self.credit.at[theirs], inc=1, device_id=device, device_id_type=MESH)
            return carry

        lax.fori_loop(0, n_ticks, tick, 0)


def forward_kernel(n_layers, x_ref, rows_ref, down_ref, y_ref, acts, w_out, hid_out, gelu_out, norm_out, q_out, k_out, v_out,
                   o_out, wbuf, peer, shard, twin, state, normed, q_buf, k_buf, v_buf, o_buf, gelu_buf, hid_buf, acc,
                   ring_send, ring_recv, pair_send, pair_recv, keep_sem, save_sem, hid_sem, twin_sem, credit):
    torus = Torus(credit)
    core, place, near = torus.core, torus.place, torus.near
    slots = wbuf.shape[0]
    n_chunks = n_layers * PER_HALF
    ready = 6 * LAG
    last_lag = ready + 1
    seq = x_ref.shape[0]
    third = 64 * ROWS
    state[ALL] = x_ref[ALL]
    torus.meet()
    swap = torus.remote(rows_ref.at[1 - core], twin, twin_sem.at[0], twin_sem.at[1], torus.sibling)
    swap.start()
    swap.wait_send()
    swap.wait_recv()

    def assemble(chunk):
        @pl.when(chunk < 5 * n_layers)
        def _():
            layer, part = chunk // 5, _rem(chunk, 5)
            cols = _at(part * FIFTH, FIFTH)
            mine, other = [ref[layer, :, cols].astype(jnp.float32) for ref in (rows_ref.at[core], twin)]
            shard[layer, :, cols] = jnp.concatenate(
                [jnp.where(core == 0, mine, other), jnp.where(core == 0, other, mine)], axis=0).astype(jnp.bfloat16)

            @pl.when(part == 4)
            def _():
                shard[layer, :, UP_END:] = down_ref[layer]

    def columns(chunk):
        return _at(_rem(chunk, PER_HALF) * COLS, COLS)

    def spot(slot, color, stage, position, cols):
        order = ORDERS[color]
        index = tuple(EVERY if dim in order[:stage] else position if dim == order[stage] else place[dim]
                      for dim in DIMS)
        return wbuf.at[(slot,) + index + (_rows(color), cols)]

    halves = (slice(0, COLS // 2), slice(COLS // 2, COLS))

    def send_own(stage, chunk):
        slot, sem = _rem(chunk, slots), _rem(chunk, MANY)
        for color in COLORS:
            dim = ORDERS[color][stage]
            here = spot(slot, color, stage, place[dim], slice(0, COLS))
            source = here
            if stage == 0:
                source = shard.at[chunk // PER_HALF, _rows(color), columns(chunk)]
            for way in TWO:
                torus.remote(source, here, ring_send.at[2 * stage, sem], ring_recv.at[2 * stage, sem],
                             {dim: near[way][dim]}).start()

    def send_far(stage, chunk):
        slot, sem = _rem(chunk, slots), _rem(chunk, MANY)
        for color in COLORS:
            dim = ORDERS[color][stage]
            for way in TWO:
                block = spot(slot, color, stage, near[1 - way][dim], halves[way])
                torus.remote(block, block, ring_send.at[2 * stage + 1, sem], ring_recv.at[2 * stage + 1, sem],
                             {dim: near[way][dim]}).start()

    def arrived(part, chunk):
        slot, sem = _rem(chunk, slots), _rem(chunk, MANY)
        block = (wbuf.at[slot, 0, 0, 0:2], wbuf.at[slot, 0, 0, 0], wbuf.at[slot, 0, 0:2], wbuf.at[slot, 0, 0],
                 wbuf.at[slot, 0:2], wbuf.at[slot, 0])[part]
        whole = torus.remote(block, block, ring_send.at[part, sem], ring_recv.at[part, sem], torus.sibling)
        whole.wait_send()
        whole.wait_recv()

    def enter(chunk):
        wbuf[_rem(chunk, slots), place["z"], place["y"], place["x"]] = shard[chunk // PER_HALF, :, columns(chunk)]
        send_own(0, chunk)

    def pass_on(part, chunk):
        arrived(part, chunk)
        if part % 2 == 0:
            send_far(part // 2, chunk)
        else:
            send_own(part // 2 + 1, chunk)

    def pair_copy(chunk):
        slot = _rem(chunk, RING)
        return torus.remote(wbuf.at[_rem(chunk, slots)], peer.at[slot], pair_send.at[slot], pair_recv.at[slot],
                            torus.sibling)

    def exchange(chunk):
        arrived(5, chunk)
        pair_copy(chunk).start()

    def keep_copy(chunk):
        return pltpu.make_async_copy(wbuf.at[_rem(chunk, slots)],
                                     w_out.at[chunk // PER_HALF, :, :, :, :, columns(chunk)],
                                     keep_sem.at[_rem(chunk, RING)])

    def save_copies(layer, names):
        parts = {"n0": (normed, norm_out.at[layer, 0], 0), "n1": (normed, norm_out.at[layer, 1], 1),
                 "q": (q_buf, q_out.at[layer], 2), "k": (k_buf, k_out.at[layer], 3), "v": (v_buf, v_out.at[layer], 4),
                 "o": (o_buf, o_out.at[layer], 5)}
        for half in TWO:
            for part in COLORS:
                parts[f"a{half}{part}"] = (gelu_buf.at[half, :, slice(third * part, third * (part + 1))],
                                           gelu_out.at[layer, 3 * half + part], 6 + 3 * half + part)
        return [pltpu.make_async_copy(parts[name][0], parts[name][1], save_sem.at[parts[name][2]]) for name in names]

    gelu_names = [f"a{half}{part}" for half in TWO for part in COLORS]

    def hidden_copies(layer, order):
        slot, part, at = _rem(order, 2), order // 6, _at(_rem(order, 6) * COLS, COLS)
        return [pltpu.make_async_copy(hid_buf.at[slot, half], hid_out.at[layer, part, half, :, at],
                                      hid_sem.at[slot, half]) for half in TWO]

    def compute(chunk):
        layer, index = chunk // PER_HALF, _rem(chunk, PER_HALF)
        pair = pair_copy(chunk)
        pair.wait_send()
        pair.wait_recv()
        keep_copy(chunk).start()

        def weights(role):
            block = wbuf[_rem(chunk, slots)] if role == 0 else peer[_rem(chunk, RING)]
            return block.reshape(third, COLS)

        @pl.when(index == 0)
        def _():
            normed[ALL] = _rms(state[ALL])
            for copy in save_copies(layer, ["n0"]):
                copy.start()

        @pl.when(index < 3)
        def _():
            for role, half in torus.sides:
                q_buf[:, _at(3 * COLS * half + COLS * index, COLS)] = _dot(
                    normed[ALL], weights(role)).astype(jnp.bfloat16)

        @pl.when(index == 3)
        def _():
            for role, half in torus.sides:
                both = _dot(normed[ALL], weights(role)).astype(jnp.bfloat16)
                k_buf[:, _at(HEAD * half, HEAD)] = both[:, :HEAD]
                v_buf[:, _at(HEAD * half, HEAD)] = both[:, HEAD:]

        @pl.when(index == QKV)
        def _():
            acc[ALL] = jnp.zeros_like(acc)
            for copy in save_copies(layer, ["q", "k", "v"]):
                copy.start()

        @pl.when((index >= QKV) & (index < ATTN))
        def _():
            causal = _causal(seq)
            for role, half in torus.sides:
                key, value = k_buf[:, _at(HEAD * half, HEAD)], v_buf[:, _at(HEAD * half, HEAD)]
                outs = []
                for head in TWO:
                    at = _at(3 * COLS * half + COLS * (index - QKV) + HEAD * head, HEAD)
                    prob = _probs(q_buf[:, at], key, causal)
                    outs.append(_dot(prob.astype(jnp.bfloat16), value).astype(jnp.bfloat16))
                block = jnp.concatenate(outs, axis=1)
                o_buf[3 * half + index - QKV] = block
                acc[ALL] += _dot_rhs_t(block, weights(role))

        @pl.when(index == 6)
        def _():
            middle = (state[ALL].astype(jnp.float32) + acc[ALL]).astype(jnp.bfloat16)
            state[ALL] = middle
            acts[2 * layer] = middle
            for copy in save_copies(layer, ["n0"]):
                copy.wait()
            normed[ALL] = _rms(middle)
            for copy in save_copies(layer, ["n1", "o"]):
                copy.start()

        @pl.when((index >= 8) & (index < 26))
        def _():
            for copy in hidden_copies(layer, index - 8):
                copy.wait()

        @pl.when((index >= ATTN) & (index < UP_BLOCKS))
        def _():
            for role, half in torus.sides:
                hidden = _dot(normed[ALL], weights(role))
                hid_buf[_rem(index - ATTN, 2), half] = hidden
                gelu_buf[half, :, _at(COLS * (index - ATTN), COLS)] = jax.nn.gelu(hidden).astype(jnp.bfloat16)
            for copy in hidden_copies(layer, index - ATTN):
                copy.start()

        @pl.when(index == UP_BLOCKS)
        def _():
            for copy in save_copies(layer, gelu_names):
                copy.start()

        @pl.when(index >= UP_BLOCKS)
        def _():
            part, at = (index - UP_BLOCKS) // 6, _at(COLS * _rem(index - UP_BLOCKS, 6), COLS)
            total = sum(_dot(gelu_buf[half, :, _at(third * part, third)], weights(role))
                        for role, half in torus.sides)

            @pl.when(part == 0)
            def _():
                acc[:, at] = total

            @pl.when(part > 0)
            def _():
                acc[:, at] += total

        @pl.when(index == PER_HALF - 1)
        def _():
            result = (state[ALL].astype(jnp.float32) + acc[ALL]).astype(jnp.bfloat16)
            state[ALL] = result

            @pl.when(layer < n_layers - 1)
            def _():
                acts[2 * layer + 1] = result

            @pl.when(layer == n_layers - 1)
            def _():
                y_ref[ALL] = result
            for copy in save_copies(layer, ["n1", "q", "k", "v", "o"] + gelu_names):
                copy.wait()

        keep_copy(chunk).wait()

    paces = (EARLY, EARLY, EARLY, EVEN, EVEN)
    steps = [(0, EVEN, assemble), (0, EARLY, enter)]
    steps += [((part + 1) * LAG, paces[part], functools.partial(pass_on, part)) for part in range(len(paces))]
    torus.run(steps + [(ready, EVEN, exchange), (last_lag, EVEN, compute)], n_chunks, n_chunks + last_lag)


def forward_stack(x_loc, rows, down):
    n_layers = down.shape[0]
    seq, width = x_loc.shape
    bf16, f32 = jnp.bfloat16, jnp.float32
    slots = 6 * LAG + 4 + AHEAD
    chunk = CUBE + (ROWS, COLS)
    shape = jax.ShapeDtypeStruct
    hbm = pl.BlockSpec(memory_space=pl.ANY)
    vmem = pl.BlockSpec(memory_space=pltpu.VMEM)
    dma = pltpu.SemaphoreType.DMA
    return pl.pallas_call(
        functools.partial(forward_kernel, n_layers),
        name="forward_stack",
        out_shape=(shape((seq, width), bf16), shape((2 * n_layers - 1, seq, width), bf16),
                   shape((n_layers, 4, 4, 4, ROWS, PER_HALF * COLS), bf16),
                   shape((n_layers, 3, 2, seq, width), f32), shape((n_layers, 6, seq, width), bf16),
                   shape((n_layers, 2, seq, width), bf16), shape((n_layers, seq, width), bf16),
                   shape((n_layers, seq, 2 * HEAD), bf16), shape((n_layers, seq, 2 * HEAD), bf16),
                   shape((n_layers, 6, seq, COLS), bf16)),
        in_specs=[vmem] * 3,
        out_specs=(vmem,) * 2 + (hbm,) * 8,
        scratch_shapes=[
            pltpu.VMEM((slots,) + chunk, bf16), pltpu.VMEM((RING,) + chunk, bf16),
            pltpu.VMEM((n_layers, ROWS, PER_HALF * COLS), bf16), pltpu.VMEM(rows.shape[1:], bf16),
            pltpu.VMEM((seq, width), bf16), pltpu.VMEM((seq, width), bf16),
            pltpu.VMEM((seq, 6 * COLS), bf16), pltpu.VMEM((seq, 2 * HEAD), bf16), pltpu.VMEM((seq, 2 * HEAD), bf16),
            pltpu.VMEM((6, seq, COLS), bf16), pltpu.VMEM((2, seq, 18 * COLS), bf16),
            pltpu.VMEM((2, 2, seq, COLS), f32), pltpu.VMEM((seq, width), f32),
            dma((6, MANY)), dma((6, MANY)), dma((RING,)), dma((RING,)), dma((RING,)), dma((12,)), dma((2, 2)), dma((2,)),
            pltpu.SemaphoreType.REGULAR((7,))],
        compiler_params=pltpu.CompilerParams(collective_id=1, has_side_effects=True,
                                             vmem_limit_bytes=VMEM_LIMIT),
    )(x_loc, rows, down)


def backward_kernel(n_layers, *refs):
    (g_ref, x_ref, acts, w_own, hid_in, gelu_in, norm_in, q_in, k_in, v_in, o_in,
     rows_out, down_out, dx_ref,
     mine, theirs, lefts, rights, hid_buf, dact, dnorm, q_buf, k_buf, v_buf, x_mid, x_in, dk_acc, dv_acc,
     outgo, peer, out, away, sum0, sum1, sum2, sa0, ra0, sb0, rb0, sa1, ra1, sb1, rb1, sa2, ra2, sb2, rb2,
     load_sem, own_sem, push_send, push_recv, pair_send, pair_recv, ring_send, ring_recv, swap_sem, credit) = refs
    torus = Torus(credit)
    core, place, near = torus.core, torus.place, torus.near
    sums = (sum0, sum1, sum2)
    half_bufs = ((sa0, ra0), (sa1, ra1), (sa2, ra2))
    full_bufs = ((sb0, rb0), (sb1, rb1), (sb2, rb2))
    n_chunks = n_layers * PER_HALF
    seq, width = g_ref.shape
    third = 64 * ROWS
    leads = sum0.shape[0]

    def pair_of(chunk):
        return n_layers - 1 - chunk // PER_HALF

    def columns(chunk):
        index = _rem(chunk, PER_HALF)
        block = jnp.where(index < DOWN_DONE, UP_BLOCKS + index,
                          jnp.where(index < UP_DONE, index - 11, jnp.where(index < O_DONE, index - 32, index - 39)))
        return _at(block * COLS, COLS)

    def loads(pair, names):
        def source(name):
            return {"a": (gelu_in.at[pair], lefts.at[0:6], 0), "n_mlp": (norm_in.at[pair, 1], lefts.at[NORM_MLP], 1),
                    "n_attn": (norm_in.at[pair, 0], lefts.at[NORM_ATTN], 2), "o": (o_in.at[pair], rights.at[O_AT:QKV_AT], 3),
                    "q": (q_in.at[pair], q_buf, 4), "k": (k_in.at[pair], k_buf, 5), "v": (v_in.at[pair], v_buf, 6),
                    "x_mid": (acts.at[2 * pair], x_mid, 7), "h0": (hid_in.at[pair, 0], hid_buf, 8),
                    "h1": (hid_in.at[pair, 1], hid_buf, 8), "h2": (hid_in.at[pair, 2], hid_buf, 8)}[name]
        return [pltpu.make_async_copy(source(name)[0], source(name)[1], load_sem.at[source(name)[2]])
                for name in names]

    def start(pair, names):
        for copy in loads(pair, names):
            copy.start()

    def finish(pair, names):
        for copy in loads(pair, names):
            copy.wait()

    def first_input(ref):
        return pltpu.make_async_copy(ref, x_in, load_sem.at[9])

    start(n_layers - 1, ["a"])
    for block in SIX:
        rights[block] = g_ref[:, COLS * block:COLS * block + COLS]
    torus.meet()
    finish(n_layers - 1, ["a"])

    def own_copy(chunk):
        slot = _rem(chunk, SLOTS)
        return pltpu.make_async_copy(w_own.at[pair_of(chunk), :, :, :, :, columns(chunk)], mine.at[slot],
                                     own_sem.at[slot])

    def push_copy(chunk):
        slot = _rem(chunk, SLOTS)
        return torus.remote(w_own.at[pair_of(chunk), :, :, :, :, columns(chunk)], theirs.at[slot],
                            push_send.at[slot], push_recv.at[slot], torus.sibling)

    def fetch(chunk):
        own_copy(chunk).start()
        push_copy(chunk).start()

    def total_grad():
        return jnp.concatenate([rights[block] for block in SIX], axis=1).astype(jnp.float32)

    def consume(chunk):
        pair, index = pair_of(chunk), _rem(chunk, PER_HALF)
        slot = _rem(chunk, SLOTS)
        own_copy(chunk).wait()
        push = push_copy(chunk)
        push.wait_send()
        push.wait_recv()

        def weights(role):
            return (mine, theirs)[role][slot].reshape(third, COLS)

        @pl.when(index == 0)
        def _():
            start(pair, ["n_mlp", "n_attn", "o", "q", "k", "v", "x_mid", "h0"])

            @pl.when(pair == 0)
            def _():
                first_input(x_ref).start()

            @pl.when(pair > 0)
            def _():
                first_input(acts.at[2 * pair - 1]).start()

        for part in (1, 2):
            @pl.when(index == 6 * part)
            def _(part=part):
                start(pair, [f"h{part}"])

        @pl.when((index < DOWN_DONE) & (_rem(index, 6) == 0))
        def _():
            dact[ALL] = jnp.zeros_like(dact)

        @pl.when(index < DOWN_DONE)
        def _():
            for role, half in torus.sides:
                dact[half] += _dot_rhs_t(rights[_rem(index, 6)], weights(role))

        @pl.when((index < DOWN_DONE) & (_rem(index, 6) == 5))
        def _():
            finish(pair, ["h0"])
            for half in TWO:
                for block in SIX:
                    cols = slice(COLS * block, COLS * block + COLS)
                    hidden = hid_buf[half, :, cols]
                    bend = jnp.tanh(0.7978845608028654 * (hidden + 0.044715 * (hidden * hidden * hidden)))
                    slope = 0.5 * (1.0 + bend) + 0.5 * hidden * (1.0 - bend * bend) * (
                        0.7978845608028654 * (1.0 + 0.134145 * (hidden * hidden)))
                    rights[DH_AT + FF * half + index - 5 + block] = (dact[half, :, cols] * slope).astype(jnp.bfloat16)

        @pl.when(index == DOWN_DONE - 1)
        def _():
            finish(pair, ["n_mlp"])

        @pl.when(index == DOWN_DONE)
        def _():
            dnorm[ALL] = jnp.zeros_like(dnorm)

            @pl.when(pair > 0)
            def _():
                start(pair - 1, ["a"])

        @pl.when((index >= DOWN_DONE) & (index < UP_DONE))
        def _():
            dnorm[ALL] += sum(_dot_rhs_t(rights[DH_AT + FF * half + index - DOWN_DONE], weights(role))
                              for role, half in torus.sides)

        @pl.when(index == UP_DONE - 1)
        def _():
            finish(pair, ["x_mid", "o"])
            lefts[GRAD] = (total_grad() + _rms_back(x_mid[ALL], dnorm[ALL])).astype(jnp.bfloat16)

        @pl.when(index == UP_DONE)
        def _():
            finish(pair, ["q", "k", "v"])
            dk_acc[ALL] = jnp.zeros_like(dk_acc)
            dv_acc[ALL] = jnp.zeros_like(dv_acc)

        @pl.when((index >= UP_DONE) & (index < O_DONE))
        def _():
            causal = _causal(seq)
            for role, half in torus.sides:
                d_o = _dot(lefts[GRAD], weights(role)).astype(jnp.bfloat16)
                key, value = k_buf[:, _at(HEAD * half, HEAD)], v_buf[:, _at(HEAD * half, HEAD)]
                d_q = []
                for head in TWO:
                    query = q_buf[:, _at(3 * COLS * half + COLS * (index - UP_DONE) + HEAD * head, HEAD)]
                    d_head = d_o[:, HEAD * head:HEAD * head + HEAD]
                    prob = _probs(query, key, causal)
                    d_prob = _dot_rhs_t(d_head, value)
                    dv_acc[half] += _dot_lhs_t(prob.astype(jnp.bfloat16), d_head)
                    d_score = prob * (d_prob - jnp.sum(prob * d_prob, axis=-1, keepdims=True))
                    d_score = (d_score * (HEAD ** -0.5)).astype(jnp.bfloat16)
                    d_q.append(_dot(d_score, key).astype(jnp.bfloat16))
                    dk_acc[half] += _dot_lhs_t(d_score, query)
                rights[QKV_AT + QKV * half + index - UP_DONE] = jnp.concatenate(d_q, axis=1)

        @pl.when(index == O_DONE - 1)
        def _():
            finish(pair, ["n_attn"])
            for half in TWO:
                rights[QKV_AT + QKV * half + QKV - 1] = jnp.concatenate([dk_acc[half], dv_acc[half]], axis=1).astype(jnp.bfloat16)

        @pl.when(index == O_DONE)
        def _():
            dnorm[ALL] = jnp.zeros_like(dnorm)

        @pl.when(index >= O_DONE)
        def _():
            dnorm[ALL] += sum(_dot_rhs_t(rights[QKV_AT + QKV * half + index - O_DONE], weights(role))
                              for role, half in torus.sides)

        @pl.when(index == PER_HALF - 1)
        def _():
            first_input(x_ref).wait()

            @pl.when(pair > 0)
            def _():
                finish(pair - 1, ["a"])
            result = (lefts[GRAD].astype(jnp.float32) + _rms_back(x_in[ALL], dnorm[ALL])).astype(jnp.bfloat16)
            dx_ref[ALL] = result
            for block in SIX:
                rights[block] = result[:, COLS * block:COLS * block + COLS]

    def pair_copy(slot):
        return torus.remote(outgo.at[slot], peer.at[slot], pair_send.at[slot], pair_recv.at[slot], torus.sibling)

    def multiply(chunk):
        index = _rem(chunk, PER_HALF)
        slot = _rem(chunk, RING)
        quarter = third // RING
        for role, half in torus.sides[::-1]:
            left = jnp.where(index < DOWN_DONE, 3 * half + index // 6,
                             jnp.where(index < UP_DONE, NORM_MLP, jnp.where(index < O_DONE, GRAD, NORM_ATTN)))
            right = jnp.where(index < DOWN_DONE, _rem(index, 6),
                              jnp.where(index < UP_DONE, DH_AT + FF * half + index - DOWN_DONE,
                                        jnp.where(index < O_DONE, O_AT + 3 * half + index - UP_DONE, QKV_AT + QKV * half + index - O_DONE)))
            for z in range(RING):
                part = _dot_lhs_t(lefts[left, :, quarter * z:quarter * z + quarter], rights[right])
                if role == 0:
                    sum0[_rem(chunk, leads), z] = part.reshape(RING, RING, ROWS, COLS)
                else:
                    outgo[slot, z] = part.astype(jnp.bfloat16).reshape(RING, RING, ROWS, COLS)
        pair_copy(slot).start()

    def merge_pair(chunk):
        slot, lead = _rem(chunk, RING), _rem(chunk, leads)
        pair_copy(slot).wait_send()
        pair_copy(slot).wait_recv()
        for z in range(RING):
            for y in range(RING):
                sum0[lead, z, y] = sum0[lead, z, y] + peer[slot, z, y].astype(jnp.float32)

    def ring_slot(stage, chunk):
        return _rem(chunk, RING if stage == 0 else AHEAD)

    def ring_copy(stage, part, slot, color, way):
        send, recv = (half_bufs, full_bufs)[part][stage]
        dim = ORDERS[color][stage]
        return torus.remote(send.at[slot, color, way], recv.at[slot, color, way],
                            ring_send.at[2 * stage + part, slot], ring_recv.at[2 * stage + part, slot],
                            {dim: near[way][dim]})

    def ring_wait(stage, part, slot):
        send, recv = (half_bufs, full_bufs)[part][stage]
        whole = torus.remote(send.at[slot], recv.at[slot], ring_send.at[2 * stage + part, slot],
                             ring_recv.at[2 * stage + part, slot], torus.sibling)
        whole.wait_send()
        whole.wait_recv()

    def source(stage, chunk, color, position, cols):
        lead = _rem(chunk, sums[stage].shape[0])
        if stage == 0:
            return sum0[(lead,) + _block(color, 0, position) + (_rows(color), cols)]
        return sums[stage][(lead, color) + _block(color, stage, position) + (EVERY, cols)]

    left_cols, right_cols, every = slice(0, COLS // 2), slice(COLS // 2, COLS), slice(0, COLS)

    def store_halves(stage, chunk):
        slot = ring_slot(stage, chunk)
        send = half_bufs[stage][0]
        for color in COLORS:
            far = torus.far[ORDERS[color][stage]]
            send[slot, color, 0] = source(stage, chunk, color, far, left_cols).astype(jnp.bfloat16)
            send[slot, color, 1] = source(stage, chunk, color, far, right_cols).astype(jnp.bfloat16)

    def store_fulls(stage, chunk):
        slot = ring_slot(stage, chunk)
        ring_wait(stage, 0, slot)
        recv = half_bufs[stage][1]
        send = full_bufs[stage][0]
        lead = (EVERY,) * (len(send.shape) - 4)
        for color in COLORS:
            dim = ORDERS[color][stage]
            for way, summed, plain in ((0, left_cols, right_cols), (1, right_cols, left_cols)):
                send[(slot, color, way) + lead + (summed,)] = (
                    source(stage, chunk, color, near[way][dim], summed)
                    + recv[slot, color, way].astype(jnp.float32)).astype(jnp.bfloat16)
                send[(slot, color, way) + lead + (plain,)] = source(
                    stage, chunk, color, near[way][dim], plain).astype(jnp.bfloat16)

    def close_stage(stage, chunk):
        slot = ring_slot(stage, chunk)
        ring_wait(stage, 1, slot)
        recv = full_bufs[stage][1]
        for color in COLORS:
            dim = ORDERS[color][stage]
            total = (source(stage, chunk, color, place[dim], every)
                     + recv[slot, color, 0].astype(jnp.float32)
                     + recv[slot, color, 1].astype(jnp.float32))
            if stage < 2:
                sums[stage + 1][_rem(chunk, sums[stage + 1].shape[0]), color] = total
            else:
                out[pair_of(chunk), _rows(color), columns(chunk)] = total

    def send_all(stage, part, chunk):
        for color in COLORS:
            for way in TWO:
                ring_copy(stage, part, ring_slot(stage, chunk), color, way).start()

    def open_first(chunk):
        merge_pair(chunk)
        store_halves(0, chunk)
        send_all(0, 0, chunk)

    def middle(stage, chunk):
        store_fulls(stage, chunk)
        send_all(stage, 1, chunk)

    def open_stage(stage, chunk):
        store_halves(stage, chunk)
        send_all(stage, 0, chunk)

    def turn(stage, chunk):
        close_stage(stage, chunk)
        if stage < 2:
            open_stage(stage + 1, chunk)

    half_rows = ROWS // 2

    def hand_over(layer, part):
        cols = _at(part * FIFTH, FIFTH)
        both = out[layer, :, cols]
        low, high = both[:half_rows], both[half_rows:]
        rows_out[core, layer, :, cols] = jnp.where(core == 0, low, high)
        away[layer, :, cols] = jnp.where(core == 0, high, low)
        torus.remote(away.at[layer, :, cols], rows_out.at[core, layer, :, cols], swap_sem.at[0], swap_sem.at[1],
                     torus.sibling).start()

    n_ticks = n_chunks + 7 * LAG
    tail = 2

    def hand_on(now):
        for layer in range(1, n_layers):
            begin = (n_layers - layer) * PER_HALF + AHEAD + 8 * LAG

            @pl.when((now >= begin) & (now < begin + 5))
            def _(layer=layer, begin=begin):
                hand_over(layer, now - begin)

        @pl.when(now >= n_ticks - 5 + tail)
        def _():
            hand_over(0, now - n_ticks + 5)

    steps = [(0, EVEN, fetch), (2 * LAG, EVEN, functools.partial(middle, 0)), (LAG, EVEN, open_first),
             (3 * LAG, EVEN, functools.partial(close_stage, 0)), (3 * LAG, LATE, functools.partial(open_stage, 1)),
             (4 * LAG, LATE, functools.partial(middle, 1)), (5 * LAG, LATE, functools.partial(turn, 1)),
             (6 * LAG, LATE, functools.partial(middle, 2)), (7 * LAG, LATE, functools.partial(turn, 2)),
             (1, EVEN, consume), (0, EVEN, multiply)]
    torus.run(steps, n_chunks, n_ticks, hand_on)
    for part in range(tail):
        hand_over(0, part)
    down_out[ALL] = out[:, :, UP_END:]
    swap = torus.remote(away, rows_out.at[core], swap_sem.at[0], swap_sem.at[1], torus.sibling)
    swap.wait_send()
    swap.wait_recv()


def backward_stack(n_layers, g_loc, *saved):
    seq, width = g_loc.shape
    bf16, f32 = jnp.bfloat16, jnp.float32
    half = COLS // 2
    chunk = CUBE + (ROWS, COLS)
    leads = 7
    shape = jax.ShapeDtypeStruct
    hbm = pl.BlockSpec(memory_space=pl.ANY)
    vmem = pl.BlockSpec(memory_space=pltpu.VMEM)
    dma = pltpu.SemaphoreType.DMA
    half_rows = ROWS // 2
    scratch = [pltpu.VMEM((SLOTS,) + chunk, bf16), pltpu.VMEM((SLOTS,) + chunk, bf16),
               pltpu.VMEM((9, seq, width), bf16), pltpu.VMEM((56, seq, COLS), bf16),
               pltpu.VMEM((2, seq, width), f32), pltpu.VMEM((2, seq, width), f32), pltpu.VMEM((seq, width), f32),
               pltpu.VMEM((seq, 6 * COLS), bf16), pltpu.VMEM((seq, 2 * HEAD), bf16), pltpu.VMEM((seq, 2 * HEAD), bf16),
               pltpu.VMEM((seq, width), bf16), pltpu.VMEM((seq, width), bf16),
               pltpu.VMEM((2, seq, HEAD), f32), pltpu.VMEM((2, seq, HEAD), f32),
               pltpu.VMEM((RING,) + chunk, bf16), pltpu.VMEM((RING,) + chunk, bf16),
               pltpu.VMEM((n_layers, ROWS, PER_HALF * COLS), f32), pltpu.VMEM((n_layers, half_rows, UP_END), f32),
               pltpu.VMEM((leads,) + chunk, f32), pltpu.VMEM((leads + 6, 3, RING, RING, TILE, COLS), f32),
               pltpu.VMEM((leads + 3, 3, RING, TILE, COLS), f32)]
    for slots, size in ((RING, (RING, RING)), (AHEAD, (RING,)), (AHEAD, ())):
        scratch += [pltpu.VMEM((slots, 3, 2) + size + (TILE, half), bf16)] * 2
        scratch += [pltpu.VMEM((slots, 3, 2) + size + (TILE, COLS), bf16)] * 2
    scratch += [dma((10,)), dma((SLOTS,)), dma((SLOTS,)), dma((SLOTS,)), dma((RING,)), dma((RING,)), dma((6, AHEAD)), dma((6, AHEAD)), dma((2,)),
                pltpu.SemaphoreType.REGULAR((7,))]
    return pl.pallas_call(
        functools.partial(backward_kernel, n_layers),
        name="backward_stack",
        out_shape=(shape((2, n_layers, half_rows, UP_END), f32),
                   shape((n_layers, ROWS, (PER_HALF - UP_BLOCKS) * COLS), f32), shape((seq, width), bf16)),
        in_specs=[vmem] + [hbm] * len(saved),
        out_specs=(vmem,) * 3,
        scratch_shapes=scratch,
        compiler_params=pltpu.CompilerParams(collective_id=0, has_side_effects=True,
                                             vmem_limit_bytes=VMEM_LIMIT),
    )(g_loc, *saved)


LANES = 128


def _moves(chips, block, packed_first):
    moves = []
    for half in TWO:
        for part in COLORS:
            for chip in range(chips):
                packed = chips * ROWS * (3 * half + part) + ROWS * chip
                plain = block * (2 * chip + half) + ROWS * part
                pair = (packed, plain) if packed_first else (plain, packed)
                moves.append(pair + (min(ROWS, block - ROWS * part),))
    return moves


def _pieces(moves, size):
    tiles = [[] for _ in range(size // LANES)]
    for target, source, length in moves:
        while length:
            step = min(length, LANES - target % LANES, LANES - source % LANES)
            tiles[target // LANES].append((target % LANES, source // LANES, (target - source) % LANES))
            target, source, length = target + step, source + step, length - step
    return [sorted(tile) for tile in tiles]


def _gather_tile(load, tile, lane):
    total = None
    for first, source, shift in tile:
        value = load(source)
        if shift:
            value = pltpu.roll(value, shift, axis=value.ndim - 1)
        total = value if total is None else jnp.where(lane >= first, value, total)
    return total


def _span(index, size):
    return slice(size * index, size * index + size)


def pack_kernel(chips, q_ref, k_ref, v_ref, o_ref, up_ref, down_ref, rows_out, down_out, wide):
    rows, layers, cols = up_ref.shape
    block, _, width = down_ref.shape
    heads = q_ref.shape[1] // 2
    for half in TWO:
        for layer in range(layers):
            for at, ref in ((0, q_ref), (heads + 2, o_ref)):
                for head in range(heads):
                    rows_out[half, layer, :, _span(at + head, LANES)] = ref[
                        :, heads * half + head].astype(jnp.float32)[:, layer].astype(jnp.bfloat16)
            for at, ref in ((heads, k_ref), (heads + 1, v_ref)):
                rows_out[half, layer, :, _span(at, LANES)] = ref[layer].astype(
                    jnp.float32)[:, half].astype(jnp.bfloat16)
    for tile in range(cols // LANES):
        both = up_ref[:, :, _span(tile, LANES)].astype(jnp.float32)
        for layer in range(layers):
            wide[layer, :, _span(tile, LANES)] = both[:, layer]
    lane = lax.broadcasted_iota(jnp.int32, (layers, rows, LANES), 2)
    half_f = 3 * chips * ROWS
    for index, tile in enumerate(_pieces(_moves(chips, block, True), 2 * half_f)):
        value = _gather_tile(lambda source: wide[:, :, _span(source, LANES)], tile, lane)
        half, at = divmod(LANES * index, half_f)
        if at >= 2 * chips * ROWS:
            position = lax.rem(lane + LANES * index % ROWS, ROWS)
            value = jnp.where(position < block - 2 * ROWS, value, 0.0)
        start = ATTN * COLS + at
        rows_out[half, :, :, start:start + LANES] = value.astype(jnp.bfloat16)
    for part in COLORS:
        used = min(ROWS, block - ROWS * part)
        value = down_ref[ROWS * part:ROWS * part + used].astype(jnp.float32)
        for layer in range(layers):
            one = value[:, layer]
            if used < ROWS:
                one = jnp.concatenate([one, jnp.zeros((ROWS - used, width), jnp.float32)], axis=0)
            down_out[layer, :, _span(part, width)] = one.astype(jnp.bfloat16)


def pack_weights(w_q, w_k, w_v, w_o, w_up, w_down, chips):
    layers, rows = w_up.shape[:2]
    width = w_down.shape[2]
    vmem = pl.BlockSpec(memory_space=pltpu.VMEM)
    shape = jax.ShapeDtypeStruct
    return pl.pallas_call(
        functools.partial(pack_kernel, chips), name="pack_weights",
        out_shape=(shape((2, layers, rows, UP_END), jnp.bfloat16), shape((layers, ROWS, 3 * width), jnp.bfloat16)),
        in_specs=[vmem] * 6, out_specs=(vmem,) * 2,
        scratch_shapes=[pltpu.VMEM(w_up.shape, jnp.float32)],
        compiler_params=pltpu.CompilerParams(vmem_limit_bytes=VMEM_LIMIT),
    )(w_q.transpose(1, 2, 0, 3), w_k, w_v, w_o.transpose(1, 2, 0, 3), w_up.transpose(1, 0, 2),
      w_down.transpose(1, 0, 2))


def unpack_kernel(chips, rows_ref, down_ref, y_ref, dx_ref, q_out, k_out, v_out, o_out, up_out, down_out, y_out,
                  dx_out):
    rows, layers, cols = up_out.shape
    block, _, width = down_out.shape
    heads = q_out.shape[1] // 2
    for half in TWO:
        for layer in range(layers):
            for at, ref in ((0, q_out), (heads + 2, o_out)):
                for head in range(heads):
                    ref[:, heads * half + head, layer, :] = rows_ref[half, layer, :, _span(at + head, LANES)]
            for at, ref in ((heads, k_out), (heads + 1, v_out)):
                ref[layer, :, half, :] = rows_ref[half, layer, :, _span(at, LANES)]
    lane = lax.broadcasted_iota(jnp.int32, (layers, rows, LANES), 2)
    half_f = 3 * chips * ROWS

    def load(source):
        half, at = divmod(LANES * source, half_f)
        return rows_ref[half, :, :, ATTN * COLS + at:ATTN * COLS + at + LANES]

    for index, tile in enumerate(_pieces(_moves(chips, block, False), cols)):
        value = _gather_tile(load, tile, lane)
        for layer in range(layers):
            up_out[:, layer, _span(index, LANES)] = value[layer]
    for part in COLORS:
        used = min(ROWS, block - ROWS * part)
        for layer in range(layers):
            down_out[ROWS * part:ROWS * part + used, layer, :] = down_ref[layer, :used, _span(part, width)]
    y_out[ALL] = y_ref[ALL]
    dx_out[ALL] = dx_ref[ALL]


def unpack_grads(row_grad, down_grad, y_loc, grad_x, shapes, chips):
    vmem = pl.BlockSpec(memory_space=pltpu.VMEM)
    q_shape, k_shape, _, _, up_shape, down_shape = shapes
    layers, rows, heads, head_dim = q_shape
    turned = [(rows, heads, layers, head_dim), k_shape, k_shape, (rows, heads, layers, head_dim),
              (rows, layers, up_shape[2]), (down_shape[1], layers, down_shape[2])]
    shape = jax.ShapeDtypeStruct
    outs = pl.pallas_call(
        functools.partial(unpack_kernel, chips), name="unpack_grads",
        out_shape=tuple(shape(full, jnp.float32) for full in turned) + tuple(
            shape(value.shape, value.dtype) for value in (y_loc, grad_x)),
        in_specs=[vmem] * 4, out_specs=(vmem,) * 8,
        compiler_params=pltpu.CompilerParams(vmem_limit_bytes=VMEM_LIMIT),
    )(row_grad, down_grad, y_loc, grad_x)
    d_q, d_k, d_v, d_o, d_up, d_down, y_out, dx_out = outs
    return (y_out[None], dx_out[None], d_q.transpose(2, 0, 1, 3), d_k, d_v, d_o.transpose(2, 0, 1, 3),
            d_up.transpose(1, 0, 2), d_down.transpose(1, 0, 2))


def solution(mesh):
    mesh4 = Mesh(mesh.devices.reshape(CUBE + (2,)), ALL_AXES)
    row_spec = P(ALL_AXES)
    weight_spec = P(None, ALL_AXES)

    def body(x_in, w_q, w_k, w_v, w_o, w_up, w_down, grad_out):
        weights = (w_q, w_k, w_v, w_o, w_up, w_down)
        chips = w_up.shape[2] // w_down.shape[1] // 2
        rows, down = pack_weights(*weights, chips)
        y_loc, acts, *saved = forward_stack(x_in[0], rows, down)
        row_grad, down_grad, grad_x = backward_stack(w_q.shape[0], grad_out[0], x_in[0], acts, *saved)
        return unpack_grads(row_grad, down_grad, y_loc, grad_x, [weight.shape for weight in weights], chips)

    return jax.shard_map(body, mesh=mesh4, in_specs=(row_spec,) + (weight_spec,) * 6 + (row_spec,),
                         out_specs=(row_spec, row_spec) + (weight_spec,) * 6, check_vma=False)
```

```python
import functools

import jax
import jax.numpy as jnp
from jax import lax
from jax.experimental import pallas as pl
from jax.experimental.pallas import tpu as pltpu
from jax.sharding import Mesh, PartitionSpec as P

MESH = pl.DeviceIdType.MESH
ALL_AXES = ("z", "y", "x", "c")
EPS = 1e-6
MASK_FILL = -1e30
DIMS = ("z", "y", "x")
ORDERS = (("x", "y", "z"), ("y", "z", "x"), ("z", "x", "y"))
COLS = 256
ROWS = 24
LAG = 2
HEAD = 128
PER_HALF = 43
UP_BLOCKS = 25
UP_END = UP_BLOCKS * COLS
RING = 4
CUBE = (RING, RING, RING)
SLOTS = 3
TILE = 8
COLORS = range(3)
TWO = range(2)
SIX = range(6)
ALL = Ellipsis
EVERY = slice(None)
QKV, ATTN, FF = 4, 7, 18
DOWN_DONE, UP_DONE, O_DONE = 18, 36, 39
G_AT, DH_AT, O_AT, QKV_AT = 0, 6, 42, 48
NORM_MLP, GRAD, NORM_ATTN = 6, 7, 8
VMEM_LIMIT = 67043328


FIFTH = UP_END // 5


def _rows(color):
    return slice(TILE * color, TILE * color + TILE)


def _rem(value, by):
    return lax.rem(value, by)


def _block(color, stage, position):
    dims = tuple(dim for dim in DIMS if dim not in ORDERS[color][:stage])
    return tuple(position if dim == ORDERS[color][stage] else EVERY for dim in dims)


def _dot(left, right):
    return jnp.dot(left, right, preferred_element_type=jnp.float32)


def _dot_rhs_t(left, right):
    return lax.dot_general(left, right, (((1,), (1,)), ((), ())), preferred_element_type=jnp.float32)


def _dot_lhs_t(left, right):
    return lax.dot_general(left, right, (((0,), (0,)), ((), ())), preferred_element_type=jnp.float32)


def _at(start, size):
    return pl.ds(pl.multiple_of(start, size), size)


def _causal(seq):
    return (lax.broadcasted_iota(jnp.int32, (seq, seq), 0) >= lax.broadcasted_iota(jnp.int32, (seq, seq), 1))


def _probs(query, key, causal):
    scores = jnp.where(causal, _dot_rhs_t(query, key) * (HEAD ** -0.5), MASK_FILL)
    weight = jnp.exp(scores - jnp.max(scores, axis=-1, keepdims=True))
    return weight / jnp.sum(weight, axis=-1, keepdims=True)


def _rms(values):
    wide = values.astype(jnp.float32)
    return (wide * lax.rsqrt(jnp.mean(wide * wide, axis=-1, keepdims=True) + EPS)).astype(jnp.bfloat16)


def _rms_back(values, grad):
    wide = values.astype(jnp.float32)
    scale = lax.rsqrt(jnp.mean(wide * wide, axis=-1, keepdims=True) + EPS)
    return scale * grad - wide * (scale * scale * scale) * jnp.mean(wide * grad, axis=-1, keepdims=True)


class Torus:
    def __init__(self, credit):
        self.core = lax.axis_index("c")
        self.place = {dim: lax.axis_index(dim) for dim in DIMS}
        self.near = tuple({dim: _rem(self.place[dim] + step, 4) for dim in DIMS} for step in (1, 3))
        self.far = {dim: _rem(self.place[dim] + 2, 4) for dim in DIMS}
        self.sibling = {"c": 1 - self.core}
        self.sides = ((0, self.core), (1, 1 - self.core))
        self.credit = credit
        self.partners = [({dim: self.near[way][dim]}, 2 * d + 1 - way, 2 * d + way)
                         for d, dim in enumerate(DIMS) for way in TWO]
        self.partners.append((self.sibling, 6, 6))

    def meet(self):
        barrier = pltpu.get_barrier_semaphore()
        for device, _, _ in self.partners:
            pl.semaphore_signal(barrier, inc=1, device_id=device, device_id_type=MESH)
        pl.semaphore_wait(barrier, len(self.partners))

    def remote(self, source, target, send_sem, recv_sem, device):
        return pltpu.make_async_remote_copy(src_ref=source, dst_ref=target, send_sem=send_sem, recv_sem=recv_sem,
                                            device_id=device, device_id_type=MESH)

    def run(self, steps, n_chunks, n_ticks, after):
        def tick(now, carry):
            @pl.when(now >= 2)
            def _():
                for _, _, mine in self.partners:
                    pl.semaphore_wait(self.credit.at[mine], 1)

            for lag, action in steps:
                @pl.when((now >= lag) & (now < lag + n_chunks))
                def _(lag=lag, action=action):
                    action(now - lag)
            after(now)

            @pl.when(now < n_ticks - 2)
            def _():
                for device, theirs, _ in self.partners:
                    pl.semaphore_signal(self.credit.at[theirs], inc=1, device_id=device, device_id_type=MESH)
            return carry

        lax.fori_loop(0, n_ticks, tick, 0)


def forward_steps(torus, n_layers, x_ref, rows_ref, down_ref, y_ref, saved, wbuf, peer, shard, twin, state, lefts, rights,
                  q_buf, k_buf, v_buf, hid_buf, acc, ring_send, ring_recv, pair_send, pair_recv, keep_sem, save_sem,
                  hid_sem, twin_sem):
    acts, w_out, hid_out, gelu_out, norm_out, q_out, k_out, v_out, o_out = saved
    core, place, near = torus.core, torus.place, torus.near
    slots = wbuf.shape[0]
    n_chunks = n_layers * PER_HALF
    ready = 6 * LAG
    seq = x_ref.shape[0]
    third = 64 * ROWS
    last = n_layers - 1
    swap = torus.remote(rows_ref.at[1 - core], twin, twin_sem.at[0], twin_sem.at[1], torus.sibling)
    swap.start()
    swap.wait_send()
    swap.wait_recv()

    def assemble(chunk):
        @pl.when(chunk < 5 * n_layers)
        def _():
            layer, part = chunk // 5, _rem(chunk, 5)
            cols = _at(part * FIFTH, FIFTH)
            mine, other = [ref[layer, :, cols].astype(jnp.float32) for ref in (rows_ref.at[core], twin)]
            shard[layer, :, cols] = jnp.concatenate(
                [jnp.where(core == 0, mine, other), jnp.where(core == 0, other, mine)], axis=0).astype(jnp.bfloat16)

            @pl.when(part == 4)
            def _():
                shard[layer, :, UP_END:] = down_ref[layer]

    def columns(chunk):
        return _at(_rem(chunk, PER_HALF) * COLS, COLS)

    def spot(slot, color, stage, position, cols):
        order = ORDERS[color]
        index = tuple(EVERY if dim in order[:stage] else position if dim == order[stage] else place[dim]
                      for dim in DIMS)
        return wbuf.at[(slot,) + index + (_rows(color), cols)]

    halves = (slice(0, COLS // 2), slice(COLS // 2, COLS))

    def send_own(stage, chunk):
        slot, sem = _rem(chunk, slots), _rem(chunk, RING)
        for color in COLORS:
            dim = ORDERS[color][stage]
            here = spot(slot, color, stage, place[dim], slice(0, COLS))
            source = here
            if stage == 0:
                source = shard.at[chunk // PER_HALF, _rows(color), columns(chunk)]
            for way in TWO:
                torus.remote(source, here, ring_send.at[2 * stage, sem], ring_recv.at[2 * stage, sem],
                             {dim: near[way][dim]}).start()

    def send_far(stage, chunk):
        slot, sem = _rem(chunk, slots), _rem(chunk, RING)
        for color in COLORS:
            dim = ORDERS[color][stage]
            for way in TWO:
                block = spot(slot, color, stage, near[1 - way][dim], halves[way])
                torus.remote(block, block, ring_send.at[2 * stage + 1, sem], ring_recv.at[2 * stage + 1, sem],
                             {dim: near[way][dim]}).start()

    def arrived(part, chunk):
        slot, sem = _rem(chunk, slots), _rem(chunk, RING)
        block = (wbuf.at[slot, 0, 0, 0:2], wbuf.at[slot, 0, 0, 0], wbuf.at[slot, 0, 0:2], wbuf.at[slot, 0, 0],
                 wbuf.at[slot, 0:2], wbuf.at[slot, 0])[part]
        whole = torus.remote(block, block, ring_send.at[part, sem], ring_recv.at[part, sem], torus.sibling)
        whole.wait_send()
        whole.wait_recv()

    def enter(chunk):
        wbuf[_rem(chunk, slots), place["z"], place["y"], place["x"]] = shard[chunk // PER_HALF, :, columns(chunk)]
        send_own(0, chunk)

    def pass_on(part, chunk):
        arrived(part, chunk)
        if part % 2 == 0:
            send_far(part // 2, chunk)
        else:
            send_own(part // 2 + 1, chunk)

    def pair_copy(chunk):
        slot = _rem(chunk, RING)
        return torus.remote(wbuf.at[_rem(chunk, slots)], peer.at[slot], pair_send.at[slot], pair_recv.at[slot],
                            torus.sibling)

    def exchange(chunk):
        arrived(5, chunk)
        pair_copy(chunk).start()

    def keep_copy(chunk):
        return pltpu.make_async_copy(wbuf.at[_rem(chunk, slots)],
                                     w_out.at[chunk // PER_HALF, :, :, :, :, columns(chunk)],
                                     keep_sem.at[_rem(chunk, RING)])

    def save_copies(layer, names):
        parts = {"n0": (lefts.at[NORM_ATTN], norm_out.at[layer, 0], 0), "n1": (lefts.at[NORM_MLP], norm_out.at[layer, 1], 1),
                 "q": (q_buf, q_out.at[layer], 2), "k": (k_buf, k_out.at[layer], 3), "v": (v_buf, v_out.at[layer], 4),
                 "o": (rights.at[O_AT:QKV_AT], o_out.at[layer], 5), "a": (lefts.at[0:6], gelu_out.at[layer], 6),
                 "mid": (state, acts.at[2 * layer], 7), "end": (state, acts.at[2 * layer + 1], 8)}
        return [pltpu.make_async_copy(parts[name][0], parts[name][1], save_sem.at[parts[name][2]]) for name in names]

    def save(layer, names):
        @pl.when(layer < last)
        def _():
            for copy in save_copies(layer, names):
                copy.start()

    def saved_all(layer, names):
        @pl.when(layer < last)
        def _():
            for copy in save_copies(layer, names):
                copy.wait()

    def hidden_copies(layer, order):
        slot, part, at = _rem(order, 2), order // 6, _at(_rem(order, 6) * COLS, COLS)
        return [pltpu.make_async_copy(hid_buf.at[slot, half], hid_out.at[layer, part, half, :, at],
                                      hid_sem.at[slot, half]) for half in TWO]

    def compute(chunk):
        layer, index = chunk // PER_HALF, _rem(chunk, PER_HALF)
        pair = pair_copy(chunk)
        pair.wait_send()
        pair.wait_recv()
        keep_copy(chunk).start()

        def weights(role):
            block = wbuf[_rem(chunk, slots)] if role == 0 else peer[_rem(chunk, RING)]
            return block.reshape(third, COLS)

        @pl.when(index == 0)
        def _():
            lefts[NORM_ATTN] = _rms(state[ALL])
            save(layer, ["n0"])

        @pl.when(index < 3)
        def _():
            for role, half in torus.sides:
                q_buf[:, _at(3 * COLS * half + COLS * index, COLS)] = _dot(
                    lefts[NORM_ATTN], weights(role)).astype(jnp.bfloat16)

        @pl.when(index == 3)
        def _():
            for role, half in torus.sides:
                both = _dot(lefts[NORM_ATTN], weights(role)).astype(jnp.bfloat16)
                k_buf[:, _at(HEAD * half, HEAD)] = both[:, :HEAD]
                v_buf[:, _at(HEAD * half, HEAD)] = both[:, HEAD:]

        @pl.when(index == QKV)
        def _():
            acc[ALL] = jnp.zeros_like(acc)
            save(layer, ["q", "k", "v"])

        @pl.when((index >= QKV) & (index < ATTN))
        def _():
            causal = _causal(seq)
            for role, half in torus.sides:
                key, value = k_buf[:, _at(HEAD * half, HEAD)], v_buf[:, _at(HEAD * half, HEAD)]
                outs = []
                for head in TWO:
                    at = _at(3 * COLS * half + COLS * (index - QKV) + HEAD * head, HEAD)
                    prob = _probs(q_buf[:, at], key, causal)
                    outs.append(_dot(prob.astype(jnp.bfloat16), value).astype(jnp.bfloat16))
                block = jnp.concatenate(outs, axis=1)
                rights[O_AT + 3 * half + index - QKV] = block
                acc[ALL] += _dot_rhs_t(block, weights(role))

        @pl.when(index == ATTN - 1)
        def _():
            @pl.when(layer > 0)
            def _():
                saved_all(layer - 1, ["end"])
            middle = (state[ALL].astype(jnp.float32) + acc[ALL]).astype(jnp.bfloat16)
            state[ALL] = middle
            lefts[NORM_MLP] = _rms(middle)
            save(layer, ["n1", "o"])
            mid = save_copies(layer, ["mid"])[0]
            mid.start()

        @pl.when((index > ATTN) & (index <= UP_BLOCKS))
        def _():
            for copy in hidden_copies(layer, index - ATTN - 1):
                copy.wait()

        @pl.when((index >= ATTN) & (index < UP_BLOCKS))
        def _():
            order = index - ATTN
            for role, half in torus.sides:
                hidden = _dot(lefts[NORM_MLP], weights(role))
                hid_buf[_rem(order, 2), half] = hidden
                lefts[3 * half + order // 6, :, _at(COLS * _rem(order, 6), COLS)] = jax.nn.gelu(
                    hidden).astype(jnp.bfloat16)
            for copy in hidden_copies(layer, order):
                copy.start()

        @pl.when(index == UP_BLOCKS)
        def _():
            save(layer, ["a"])
            save_copies(layer, ["mid"])[0].wait()

        @pl.when(index >= UP_BLOCKS)
        def _():
            part, at = (index - UP_BLOCKS) // 6, _at(COLS * _rem(index - UP_BLOCKS, 6), COLS)
            total = sum(_dot(lefts[3 * half + part], weights(role)) for role, half in torus.sides)

            @pl.when(part == 0)
            def _():
                acc[:, at] = total

            @pl.when(part > 0)
            def _():
                acc[:, at] += total

        @pl.when(index == PER_HALF - 1)
        def _():
            saved_all(layer, ["n0", "n1", "q", "k", "v", "o", "a"])
            result = (state[ALL].astype(jnp.float32) + acc[ALL]).astype(jnp.bfloat16)
            state[ALL] = result
            save(layer, ["end"])

            @pl.when(layer == last)
            def _():
                y_ref[ALL] = result

        keep_copy(chunk).wait()

    steps = [(0, assemble), (0, enter)]
    steps += [((part + 1) * LAG, functools.partial(pass_on, part)) for part in range(5)]
    return steps + [(ready, exchange), (ready + 1, compute)]


def backward_steps(torus, n_layers, g_ref, x_ref, dx_ref, saved, out, wbuf, lefts, rights, hid_buf, dact, dnorm, q_buf,
                   k_buf, v_buf, x_mid, x_in, dk_acc, dv_acc, sums, half_bufs, full_bufs, load_sem, own_sem, push_send,
                   push_recv, pair_send, pair_recv, ring_send, ring_recv):
    acts, w_own, hid_in, gelu_in, norm_in, q_in, k_in, v_in, o_in = saved
    place, near = torus.place, torus.near
    seq = g_ref.shape[0]
    third = 64 * ROWS
    last = n_layers - 1

    def mine_slot(chunk):
        return 6 * _rem(chunk, 2)

    def out_slot(chunk):
        return 7 + _rem(chunk, 2)

    def their_slot(chunk):
        return 9 + _rem(chunk, SLOTS)

    def peer_slot(chunk):
        return 12 + _rem(chunk, RING)

    def pair_of(chunk):
        return last - chunk // PER_HALF

    def columns(chunk):
        index = _rem(chunk, PER_HALF)
        block = jnp.where(index < DOWN_DONE, UP_BLOCKS + index,
                          jnp.where(index < UP_DONE, index - 11, jnp.where(index < O_DONE, index - 32, index - 39)))
        return _at(block * COLS, COLS)

    def loads(pair, names):
        def source(name):
            return {"a": (gelu_in.at[pair], lefts.at[0:6], 0), "n_mlp": (norm_in.at[pair, 1], lefts.at[NORM_MLP], 1),
                    "n_attn": (norm_in.at[pair, 0], lefts.at[NORM_ATTN], 2), "o": (o_in.at[pair], rights.at[O_AT:QKV_AT], 3),
                    "q": (q_in.at[pair], q_buf, 4), "k": (k_in.at[pair], k_buf, 5), "v": (v_in.at[pair], v_buf, 6),
                    "x_mid": (acts.at[2 * pair], x_mid, 7), "h0": (hid_in.at[pair, 0], hid_buf, 8),
                    "h1": (hid_in.at[pair, 1], hid_buf, 8), "h2": (hid_in.at[pair, 2], hid_buf, 8)}[name]
        return [pltpu.make_async_copy(source(name)[0], source(name)[1], load_sem.at[source(name)[2]])
                for name in names]

    def start(pair, names):
        for copy in loads(pair, names):
            copy.start()

    def finish(pair, names):
        for copy in loads(pair, names):
            copy.wait()

    def first_input(ref):
        return pltpu.make_async_copy(ref, x_in, load_sem.at[9])

    for block in SIX:
        rights[block] = g_ref[:, COLS * block:COLS * block + COLS]

    def own_copy(chunk):
        return pltpu.make_async_copy(w_own.at[pair_of(chunk), :, :, :, :, columns(chunk)], wbuf.at[mine_slot(chunk)],
                                     own_sem.at[_rem(chunk, 2)])

    def push_copy(chunk):
        slot = _rem(chunk, SLOTS)
        return torus.remote(w_own.at[pair_of(chunk), :, :, :, :, columns(chunk)], wbuf.at[their_slot(chunk)],
                            push_send.at[slot], push_recv.at[slot], torus.sibling)

    def fetch(chunk):
        own_copy(chunk).start()
        push_copy(chunk).start()

    def total_grad():
        return jnp.concatenate([rights[block] for block in SIX], axis=1).astype(jnp.float32)

    def consume(chunk):
        pair, index = pair_of(chunk), _rem(chunk, PER_HALF)
        own_copy(chunk).wait()
        push = push_copy(chunk)
        push.wait_send()
        push.wait_recv()

        def weights(role):
            return wbuf[(mine_slot, their_slot)[role](chunk)].reshape(third, COLS)

        @pl.when(index == 0)
        def _():
            start(pair, ["x_mid", "h0"])

            @pl.when(pair < last)
            def _():
                start(pair, ["n_mlp", "n_attn", "o", "q", "k", "v"])

            @pl.when(pair == 0)
            def _():
                x_in[ALL] = x_ref[ALL]

            @pl.when(pair > 0)
            def _():
                first_input(acts.at[2 * pair - 1]).start()

        for part in (1, 2):
            @pl.when(index == 6 * part)
            def _(part=part):
                start(pair, [f"h{part}"])

        @pl.when((index < DOWN_DONE) & (_rem(index, 6) == 0))
        def _():
            dact[ALL] = jnp.zeros_like(dact)

        @pl.when(index < DOWN_DONE)
        def _():
            for role, half in torus.sides:
                dact[half] += _dot_rhs_t(rights[_rem(index, 6)], weights(role))

        @pl.when((index < DOWN_DONE) & (_rem(index, 6) == 5))
        def _():
            finish(pair, ["h0"])
            for half in TWO:
                for block in SIX:
                    cols = slice(COLS * block, COLS * block + COLS)
                    hidden = hid_buf[half, :, cols]
                    bend = jnp.tanh(0.7978845608028654 * (hidden + 0.044715 * (hidden * hidden * hidden)))
                    slope = 0.5 * (1.0 + bend) + 0.5 * hidden * (1.0 - bend * bend) * (
                        0.7978845608028654 * (1.0 + 0.134145 * (hidden * hidden)))
                    rights[DH_AT + FF * half + index - 5 + block] = (dact[half, :, cols] * slope).astype(jnp.bfloat16)

        @pl.when(index == DOWN_DONE - 1)
        def _():
            @pl.when(pair < last)
            def _():
                finish(pair, ["n_mlp", "n_attn", "o", "q", "k", "v"])

        @pl.when(index == DOWN_DONE)
        def _():
            dnorm[ALL] = jnp.zeros_like(dnorm)

            @pl.when(pair > 0)
            def _():
                start(pair - 1, ["a"])

        @pl.when((index >= DOWN_DONE) & (index < UP_DONE))
        def _():
            dnorm[ALL] += sum(_dot_rhs_t(rights[DH_AT + FF * half + index - DOWN_DONE], weights(role))
                              for role, half in torus.sides)

        @pl.when(index == UP_DONE - 1)
        def _():
            finish(pair, ["x_mid"])
            lefts[GRAD] = (total_grad() + _rms_back(x_mid[ALL], dnorm[ALL])).astype(jnp.bfloat16)

        @pl.when(index == UP_DONE)
        def _():
            dk_acc[ALL] = jnp.zeros_like(dk_acc)
            dv_acc[ALL] = jnp.zeros_like(dv_acc)

        @pl.when((index >= UP_DONE) & (index < O_DONE))
        def _():
            causal = _causal(seq)
            for role, half in torus.sides:
                d_o = _dot(lefts[GRAD], weights(role)).astype(jnp.bfloat16)
                key, value = k_buf[:, _at(HEAD * half, HEAD)], v_buf[:, _at(HEAD * half, HEAD)]
                d_q = []
                for head in TWO:
                    query = q_buf[:, _at(3 * COLS * half + COLS * (index - UP_DONE) + HEAD * head, HEAD)]
                    d_head = d_o[:, HEAD * head:HEAD * head + HEAD]
                    prob = _probs(query, key, causal)
                    d_prob = _dot_rhs_t(d_head, value)
                    dv_acc[half] += _dot_lhs_t(prob.astype(jnp.bfloat16), d_head)
                    d_score = prob * (d_prob - jnp.sum(prob * d_prob, axis=-1, keepdims=True))
                    d_score = (d_score * (HEAD ** -0.5)).astype(jnp.bfloat16)
                    d_q.append(_dot(d_score, key).astype(jnp.bfloat16))
                    dk_acc[half] += _dot_lhs_t(d_score, query)
                rights[QKV_AT + QKV * half + index - UP_DONE] = jnp.concatenate(d_q, axis=1)

        @pl.when(index == O_DONE - 1)
        def _():
            for half in TWO:
                rights[QKV_AT + QKV * half + QKV - 1] = jnp.concatenate([dk_acc[half], dv_acc[half]], axis=1).astype(jnp.bfloat16)

        @pl.when(index == O_DONE)
        def _():
            dnorm[ALL] = jnp.zeros_like(dnorm)

        @pl.when(index >= O_DONE)
        def _():
            dnorm[ALL] += sum(_dot_rhs_t(rights[QKV_AT + QKV * half + index - O_DONE], weights(role))
                              for role, half in torus.sides)

        @pl.when(index == PER_HALF - 1)
        def _():
            @pl.when(pair > 0)
            def _():
                first_input(acts.at[2 * pair - 1]).wait()
                finish(pair - 1, ["a"])
            result = (lefts[GRAD].astype(jnp.float32) + _rms_back(x_in[ALL], dnorm[ALL])).astype(jnp.bfloat16)
            dx_ref[ALL] = result
            for block in SIX:
                rights[block] = result[:, COLS * block:COLS * block + COLS]

    def pair_copy(chunk):
        slot = _rem(chunk, RING)
        return torus.remote(wbuf.at[out_slot(chunk)], wbuf.at[peer_slot(chunk)], pair_send.at[slot], pair_recv.at[slot],
                            torus.sibling)

    def multiply(chunk):
        index = _rem(chunk, PER_HALF)
        lead = _rem(chunk, sums[0].shape[0])
        quarter = third // RING
        for role, half in torus.sides[::-1]:
            left = jnp.where(index < DOWN_DONE, 3 * half + index // 6,
                             jnp.where(index < UP_DONE, NORM_MLP, jnp.where(index < O_DONE, GRAD, NORM_ATTN)))
            right = jnp.where(index < DOWN_DONE, _rem(index, 6),
                              jnp.where(index < UP_DONE, DH_AT + FF * half + index - DOWN_DONE,
                                        jnp.where(index < O_DONE, O_AT + 3 * half + index - UP_DONE,
                                                  QKV_AT + QKV * half + index - O_DONE)))
            for z in range(RING):
                part = _dot_lhs_t(lefts[left, :, quarter * z:quarter * z + quarter], rights[right])
                if role == 0:
                    sums[0][lead, z] = part.reshape(RING, RING, ROWS, COLS)
                else:
                    wbuf[out_slot(chunk), z] = part.astype(jnp.bfloat16).reshape(RING, RING, ROWS, COLS)
        pair_copy(chunk).start()

    def merge_pair(chunk):
        lead = _rem(chunk, sums[0].shape[0])
        pair_copy(chunk).wait_send()
        pair_copy(chunk).wait_recv()
        for z in range(RING):
            for y in range(RING):
                sums[0][lead, z, y] = sums[0][lead, z, y] + wbuf[peer_slot(chunk), z, y].astype(jnp.float32)

    def ring_copy(stage, part, slot, color, way):
        send, recv = (half_bufs, full_bufs)[part][stage]
        dim = ORDERS[color][stage]
        return torus.remote(send.at[slot, color, way], recv.at[slot, color, way],
                            ring_send.at[2 * stage + part, slot], ring_recv.at[2 * stage + part, slot],
                            {dim: near[way][dim]})

    def ring_wait(stage, part, slot):
        send, recv = (half_bufs, full_bufs)[part][stage]
        whole = torus.remote(send.at[slot], recv.at[slot], ring_send.at[2 * stage + part, slot],
                             ring_recv.at[2 * stage + part, slot], torus.sibling)
        whole.wait_send()
        whole.wait_recv()

    def source(stage, chunk, color, position, cols):
        lead = _rem(chunk, sums[stage].shape[0])
        if stage == 0:
            return sums[0][(lead,) + _block(color, 0, position) + (_rows(color), cols)]
        return sums[stage][(lead, color) + _block(color, stage, position) + (EVERY, cols)]

    left_cols, right_cols, every = slice(0, COLS // 2), slice(COLS // 2, COLS), slice(0, COLS)

    def store_halves(stage, chunk):
        slot = _rem(chunk, RING)
        send = half_bufs[stage][0]
        for color in COLORS:
            far = torus.far[ORDERS[color][stage]]
            send[slot, color, 0] = source(stage, chunk, color, far, left_cols).astype(jnp.bfloat16)
            send[slot, color, 1] = source(stage, chunk, color, far, right_cols).astype(jnp.bfloat16)

    def store_fulls(stage, chunk):
        slot = _rem(chunk, RING)
        ring_wait(stage, 0, slot)
        recv = half_bufs[stage][1]
        send = full_bufs[stage][0]
        lead = (EVERY,) * (len(send.shape) - 4)
        for color in COLORS:
            dim = ORDERS[color][stage]
            for way, summed, plain in ((0, left_cols, right_cols), (1, right_cols, left_cols)):
                send[(slot, color, way) + lead + (summed,)] = (
                    source(stage, chunk, color, near[way][dim], summed)
                    + recv[slot, color, way].astype(jnp.float32)).astype(jnp.bfloat16)
                send[(slot, color, way) + lead + (plain,)] = source(
                    stage, chunk, color, near[way][dim], plain).astype(jnp.bfloat16)

    def close_stage(stage, chunk):
        slot = _rem(chunk, RING)
        ring_wait(stage, 1, slot)
        recv = full_bufs[stage][1]
        for color in COLORS:
            dim = ORDERS[color][stage]
            total = (source(stage, chunk, color, place[dim], every)
                     + recv[slot, color, 0].astype(jnp.float32)
                     + recv[slot, color, 1].astype(jnp.float32))
            if stage < 2:
                sums[stage + 1][_rem(chunk, sums[stage + 1].shape[0]), color] = total
            else:
                out[pair_of(chunk), _rows(color), columns(chunk)] = total

    def send_all(stage, part, chunk):
        for color in COLORS:
            for way in TWO:
                ring_copy(stage, part, _rem(chunk, RING), color, way).start()

    def open_first(chunk):
        merge_pair(chunk)
        store_halves(0, chunk)
        send_all(0, 0, chunk)

    def middle(stage, chunk):
        store_fulls(stage, chunk)
        send_all(stage, 1, chunk)

    def open_stage(stage, chunk):
        store_halves(stage, chunk)
        send_all(stage, 0, chunk)

    def turn(stage, chunk):
        close_stage(stage, chunk)
        if stage < 2:
            open_stage(stage + 1, chunk)

    return [(0, fetch), (2 * LAG, functools.partial(middle, 0)), (LAG, open_first),
            (3 * LAG, functools.partial(turn, 0)), (4 * LAG, functools.partial(middle, 1)),
            (5 * LAG, functools.partial(turn, 1)), (6 * LAG, functools.partial(middle, 2)),
            (7 * LAG, functools.partial(turn, 2)), (1, consume), (0, multiply)]


def train_kernel(n_layers, x_ref, g_ref, rows_ref, down_ref, y_ref, dx_ref, rows_out, out, *refs):
    saved, refs = refs[:9], refs[9:]
    (wbuf, peer, shard, twin, state, lefts, rights, q_buf, k_buf, v_buf, hid_out_buf, acc, hid_in_buf, dact, x_mid, x_in,
     dk_acc, dv_acc, away), refs = refs[:19], refs[19:]
    sums, half_bufs, full_bufs, refs = refs[:3], refs[3:9], refs[9:15], refs[15:]
    half_bufs = [half_bufs[2 * stage:2 * stage + 2] for stage in COLORS]
    full_bufs = [full_bufs[2 * stage:2 * stage + 2] for stage in COLORS]
    forward_sems, backward_sems, (swap_sem, credit) = refs[:8], refs[8:16], refs[16:]
    torus = Torus(credit)
    core = torus.core
    n_chunks = n_layers * PER_HALF
    state[ALL] = x_ref[ALL]
    torus.meet()
    forward = forward_steps(torus, n_layers, x_ref, rows_ref, down_ref, y_ref, saved, wbuf, peer, shard, twin, state, lefts,
                            rights, q_buf, k_buf, v_buf, hid_out_buf, acc, *forward_sems)
    backward = backward_steps(torus, n_layers, g_ref, x_ref, dx_ref, saved, out, wbuf, lefts, rights, hid_in_buf, dact, acc,
                              q_buf, k_buf, v_buf, x_mid, x_in, dk_acc, dv_acc, sums, half_bufs, full_bufs,
                              *backward_sems)
    turn_at = n_chunks + 8
    backward = [(lag + turn_at, step) for lag, step in backward]
    n_ticks = turn_at + n_chunks + 7 * LAG
    half_rows = ROWS // 2
    tail = 2

    def hand_over(layer, part):
        cols = _at(part * FIFTH, FIFTH)
        both = out[layer, :, cols]
        low, high = both[:half_rows], both[half_rows:]
        rows_out[core, layer, :, cols] = jnp.where(core == 0, low, high)
        away[layer, :, cols] = jnp.where(core == 0, high, low)
        torus.remote(away.at[layer, :, cols], rows_out.at[core, layer, :, cols], swap_sem.at[0], swap_sem.at[1],
                     torus.sibling).start()

    def hand_on(now):
        for layer in range(1, n_layers):
            begin = turn_at + (n_layers - layer) * PER_HALF + 8 * LAG

            @pl.when((now >= begin) & (now < begin + 5))
            def _(layer=layer, begin=begin):
                hand_over(layer, now - begin)

        @pl.when(now >= n_ticks - 5 + tail)
        def _():
            hand_over(0, now - n_ticks + 5)

    torus.run(backward[:1] + forward + backward[1:], n_chunks, n_ticks, hand_on)
    for part in range(tail):
        hand_over(0, part)
    swap = torus.remote(away, rows_out.at[core], swap_sem.at[0], swap_sem.at[1], torus.sibling)
    swap.wait_send()
    swap.wait_recv()


def train_stack(x_loc, g_loc, rows, down):
    n_layers = down.shape[0]
    seq, width = x_loc.shape
    bf16, f32 = jnp.bfloat16, jnp.float32
    half = COLS // 2
    chunk = CUBE + (ROWS, COLS)
    shape = jax.ShapeDtypeStruct
    hbm = pl.BlockSpec(memory_space=pl.ANY)
    vmem = pl.BlockSpec(memory_space=pltpu.VMEM)
    dma = pltpu.SemaphoreType.DMA
    saved = (shape((2 * n_layers - 1, seq, width), bf16), shape((n_layers,) + CUBE + (ROWS, PER_HALF * COLS), bf16),
             shape((n_layers, 3, 2, seq, width), f32), shape((n_layers, 6, seq, width), bf16),
             shape((n_layers, 2, seq, width), bf16), shape((n_layers, seq, width), bf16),
             shape((n_layers, seq, 2 * HEAD), bf16), shape((n_layers, seq, 2 * HEAD), bf16),
             shape((n_layers, 6, seq, COLS), bf16))
    scratch = [pltpu.VMEM(full, kind) for full, kind in (
        ((6 * LAG + 4,) + chunk, bf16), ((RING,) + chunk, bf16), ((n_layers, ROWS, PER_HALF * COLS), bf16),
        (rows.shape[1:], bf16), ((seq, width), bf16), ((9, seq, width), bf16), ((56, seq, COLS), bf16),
        ((seq, 6 * COLS), bf16), ((seq, 2 * HEAD), bf16), ((seq, 2 * HEAD), bf16), ((2, 2, seq, COLS), f32),
        ((seq, width), f32), ((2, seq, width), f32), ((2, seq, width), f32), ((seq, width), bf16), ((seq, width), bf16),
        ((2, seq, HEAD), f32), ((2, seq, HEAD), f32), ((n_layers, ROWS // 2, UP_END), f32), ((6,) + chunk, f32),
        ((5, 3, RING, RING, TILE, COLS), f32), ((5, 3, RING, TILE, COLS), f32))]
    for cols in (half, COLS):
        for size in ((RING, RING), (RING,), ()):
            scratch += [pltpu.VMEM((RING, 3, 2) + size + (TILE, cols), bf16)] * 2
    scratch += [dma((6, RING)), dma((6, RING)), dma((RING,)), dma((RING,)), dma((RING,)), dma((9,)), dma((2, 2)), dma((2,))]
    scratch += [dma((10,)), dma((2,)), dma((SLOTS,)), dma((SLOTS,)), dma((RING,)), dma((RING,)), dma((6, RING)),
                dma((6, RING)), dma((2,)), pltpu.SemaphoreType.REGULAR((7,))]
    return pl.pallas_call(
        functools.partial(train_kernel, n_layers), name="train_stack",
        out_shape=(shape((seq, width), bf16), shape((seq, width), bf16), shape((2, n_layers, ROWS // 2, UP_END), f32),
                   shape((n_layers, ROWS, PER_HALF * COLS), f32)) + saved,
        in_specs=[vmem] * 4, out_specs=(vmem,) * 4 + (hbm,) * len(saved), scratch_shapes=scratch,
        compiler_params=pltpu.CompilerParams(collective_id=0, has_side_effects=True, vmem_limit_bytes=VMEM_LIMIT),
    )(x_loc, g_loc, rows, down)[:4]


LANES = 128


def _moves(chips, block, packed_first):
    moves = []
    for half in TWO:
        for part in COLORS:
            for chip in range(chips):
                packed = chips * ROWS * (3 * half + part) + ROWS * chip
                plain = block * (2 * chip + half) + ROWS * part
                pair = (packed, plain) if packed_first else (plain, packed)
                moves.append(pair + (min(ROWS, block - ROWS * part),))
    return moves


def _pieces(moves, size):
    tiles = [[] for _ in range(size // LANES)]
    for target, source, length in moves:
        while length:
            step = min(length, LANES - target % LANES, LANES - source % LANES)
            tiles[target // LANES].append((target % LANES, source // LANES, (target - source) % LANES))
            target, source, length = target + step, source + step, length - step
    return [sorted(tile) for tile in tiles]


def _gather_tile(load, tile, lane):
    total = None
    for first, source, shift in tile:
        value = load(source)
        if shift:
            value = pltpu.roll(value, shift, axis=value.ndim - 1)
        total = value if total is None else jnp.where(lane >= first, value, total)
    return total


def _span(index, size):
    return slice(size * index, size * index + size)


def pack_kernel(chips, q_ref, k_ref, v_ref, o_ref, up_ref, down_ref, rows_out, down_out, wide):
    rows, layers, cols = up_ref.shape
    block, _, width = down_ref.shape
    heads = q_ref.shape[1] // 2
    for half in TWO:
        for layer in range(layers):
            for at, ref in ((0, q_ref), (heads + 2, o_ref)):
                for head in range(heads):
                    rows_out[half, layer, :, _span(at + head, LANES)] = ref[
                        :, heads * half + head].astype(jnp.float32)[:, layer].astype(jnp.bfloat16)
            for at, ref in ((heads, k_ref), (heads + 1, v_ref)):
                rows_out[half, layer, :, _span(at, LANES)] = ref[layer].astype(
                    jnp.float32)[:, half].astype(jnp.bfloat16)
    for tile in range(cols // LANES):
        both = up_ref[:, :, _span(tile, LANES)].astype(jnp.float32)
        for layer in range(layers):
            wide[layer, :, _span(tile, LANES)] = both[:, layer]
    lane = lax.broadcasted_iota(jnp.int32, (layers, rows, LANES), 2)
    half_f = 3 * chips * ROWS
    for index, tile in enumerate(_pieces(_moves(chips, block, True), 2 * half_f)):
        value = _gather_tile(lambda source: wide[:, :, _span(source, LANES)], tile, lane)
        half, at = divmod(LANES * index, half_f)
        if at >= 2 * chips * ROWS:
            position = lax.rem(lane + LANES * index % ROWS, ROWS)
            value = jnp.where(position < block - 2 * ROWS, value, 0.0)
        start = ATTN * COLS + at
        rows_out[half, :, :, start:start + LANES] = value.astype(jnp.bfloat16)
    for part in COLORS:
        used = min(ROWS, block - ROWS * part)
        value = down_ref[ROWS * part:ROWS * part + used].astype(jnp.float32)
        for layer in range(layers):
            one = value[:, layer]
            if used < ROWS:
                one = jnp.concatenate([one, jnp.zeros((ROWS - used, width), jnp.float32)], axis=0)
            down_out[layer, :, _span(part, width)] = one.astype(jnp.bfloat16)


def pack_weights(w_q, w_k, w_v, w_o, w_up, w_down, chips):
    layers, rows = w_up.shape[:2]
    width = w_down.shape[2]
    vmem = pl.BlockSpec(memory_space=pltpu.VMEM)
    shape = jax.ShapeDtypeStruct
    return pl.pallas_call(
        functools.partial(pack_kernel, chips), name="pack_weights",
        out_shape=(shape((2, layers, rows, UP_END), jnp.bfloat16), shape((layers, ROWS, 3 * width), jnp.bfloat16)),
        in_specs=[vmem] * 6, out_specs=(vmem,) * 2,
        scratch_shapes=[pltpu.VMEM(w_up.shape, jnp.float32)],
        compiler_params=pltpu.CompilerParams(vmem_limit_bytes=VMEM_LIMIT),
    )(w_q.transpose(1, 2, 0, 3), w_k, w_v, w_o.transpose(1, 2, 0, 3), w_up.transpose(1, 0, 2),
      w_down.transpose(1, 0, 2))


def unpack_kernel(chips, rows_ref, down_ref, y_ref, dx_ref, q_out, k_out, v_out, o_out, up_out, down_out, y_out,
                  dx_out):
    rows, layers, cols = up_out.shape
    block, _, width = down_out.shape
    heads = q_out.shape[1] // 2
    for half in TWO:
        for layer in range(layers):
            for at, ref in ((0, q_out), (heads + 2, o_out)):
                for head in range(heads):
                    ref[:, heads * half + head, layer, :] = rows_ref[half, layer, :, _span(at + head, LANES)]
            for at, ref in ((heads, k_out), (heads + 1, v_out)):
                ref[layer, :, half, :] = rows_ref[half, layer, :, _span(at, LANES)]
    lane = lax.broadcasted_iota(jnp.int32, (layers, rows, LANES), 2)
    half_f = 3 * chips * ROWS

    def load(source):
        half, at = divmod(LANES * source, half_f)
        return rows_ref[half, :, :, ATTN * COLS + at:ATTN * COLS + at + LANES]

    for index, tile in enumerate(_pieces(_moves(chips, block, False), cols)):
        value = _gather_tile(load, tile, lane)
        for layer in range(layers):
            up_out[:, layer, _span(index, LANES)] = value[layer]
    for part in COLORS:
        used = min(ROWS, block - ROWS * part)
        for layer in range(layers):
            down_out[ROWS * part:ROWS * part + used, layer, :] = down_ref[layer, :used, UP_END + width * part:UP_END + width * part + width]
    y_out[ALL] = y_ref[ALL]
    dx_out[ALL] = dx_ref[ALL]


def unpack_grads(row_grad, down_grad, y_loc, grad_x, shapes, chips):
    vmem = pl.BlockSpec(memory_space=pltpu.VMEM)
    q_shape, k_shape, _, _, up_shape, down_shape = shapes
    layers, rows, heads, head_dim = q_shape
    turned = [(rows, heads, layers, head_dim), k_shape, k_shape, (rows, heads, layers, head_dim),
              (rows, layers, up_shape[2]), (down_shape[1], layers, down_shape[2])]
    shape = jax.ShapeDtypeStruct
    outs = pl.pallas_call(
        functools.partial(unpack_kernel, chips), name="unpack_grads",
        out_shape=tuple(shape(full, jnp.float32) for full in turned) + tuple(
            shape(value.shape, value.dtype) for value in (y_loc, grad_x)),
        in_specs=[vmem] * 4, out_specs=(vmem,) * 8,
        compiler_params=pltpu.CompilerParams(vmem_limit_bytes=VMEM_LIMIT),
    )(row_grad, down_grad, y_loc, grad_x)
    d_q, d_k, d_v, d_o, d_up, d_down, y_out, dx_out = outs
    return (y_out[None], dx_out[None], d_q.transpose(2, 0, 1, 3), d_k, d_v, d_o.transpose(2, 0, 1, 3),
            d_up.transpose(1, 0, 2), d_down.transpose(1, 0, 2))


def solution(mesh):
    mesh4 = Mesh(mesh.devices.reshape(CUBE + (2,)), ALL_AXES)
    row_spec = P(ALL_AXES)
    weight_spec = P(None, ALL_AXES)

    def body(x_in, w_q, w_k, w_v, w_o, w_up, w_down, grad_out):
        weights = (w_q, w_k, w_v, w_o, w_up, w_down)
        chips = w_up.shape[2] // w_down.shape[1] // 2
        rows, down = pack_weights(*weights, chips)
        y_loc, grad_x, row_grad, down_grad = train_stack(x_in[0], grad_out[0], rows, down)
        return unpack_grads(row_grad, down_grad, y_loc, grad_x, [weight.shape for weight in weights], chips)

    return jax.shard_map(body, mesh=mesh4, in_specs=(row_spec,) + (weight_spec,) * 6 + (row_spec,),
                         out_specs=(row_spec, row_spec) + (weight_spec,) * 6, check_vma=False)
```

```python
import functools

import jax
import jax.numpy as jnp
from jax import lax
from jax.experimental import pallas as pl
from jax.experimental.pallas import tpu as pltpu
from jax.sharding import Mesh, PartitionSpec as P

MESH = pl.DeviceIdType.MESH
ALL_AXES = ("z", "y", "x", "c")
EPS = 1e-6
MASK_FILL = -1e30
DIMS = ("z", "y", "x")
ORDERS = (("x", "y", "z"), ("y", "z", "x"), ("z", "x", "y"))
COLS = 256
ROWS = 24
LAG = 2
HEAD = 128
PER_HALF = 43
UP_BLOCKS = 25
UP_END = UP_BLOCKS * COLS
RING = 4
CUBE = (RING, RING, RING)
SLOTS = 3
TILE = 8
COLORS = range(3)
TWO = range(2)
SIX = range(6)
ALL = Ellipsis
EVERY = slice(None)
QKV, ATTN, FF = 4, 7, 18
DOWN_DONE, UP_DONE, O_DONE = 18, 36, 39
G_AT, DH_AT, O_AT, QKV_AT = 0, 6, 42, 48
NORM_MLP, GRAD, NORM_ATTN = 6, 7, 8
VMEM_LIMIT = 67043328


FIFTH = UP_END // 5
GATHER_SLOTS = 6 * LAG + 4


def _rows(color):
    return slice(TILE * color, TILE * color + TILE)


def _rem(value, by):
    return lax.rem(value, by)


def _block(color, stage, position):
    dims = tuple(dim for dim in DIMS if dim not in ORDERS[color][:stage])
    return tuple(position if dim == ORDERS[color][stage] else EVERY for dim in dims)


def _dot(left, right):
    return jnp.dot(left, right, preferred_element_type=jnp.float32)


def _dot_rhs_t(left, right):
    return lax.dot_general(left, right, (((1,), (1,)), ((), ())), preferred_element_type=jnp.float32)


def _dot_lhs_t(left, right):
    return lax.dot_general(left, right, (((0,), (0,)), ((), ())), preferred_element_type=jnp.float32)


def _at(start, size):
    return pl.ds(pl.multiple_of(start, size), size)


def _causal(seq):
    return (lax.broadcasted_iota(jnp.int32, (seq, seq), 0) >= lax.broadcasted_iota(jnp.int32, (seq, seq), 1))


def _probs(query, key, causal):
    scores = jnp.where(causal, _dot_rhs_t(query, key) * (HEAD ** -0.5), MASK_FILL)
    weight = jnp.exp(scores - jnp.max(scores, axis=-1, keepdims=True))
    return weight / jnp.sum(weight, axis=-1, keepdims=True)


def _rms(values):
    wide = values.astype(jnp.float32)
    return (wide * lax.rsqrt(jnp.mean(wide * wide, axis=-1, keepdims=True) + EPS)).astype(jnp.bfloat16)


def _rms_back(values, grad):
    wide = values.astype(jnp.float32)
    scale = lax.rsqrt(jnp.mean(wide * wide, axis=-1, keepdims=True) + EPS)
    return scale * grad - wide * (scale * scale * scale) * jnp.mean(wide * grad, axis=-1, keepdims=True)


class Torus:
    def __init__(self, credit):
        self.core = lax.axis_index("c")
        self.place = {dim: lax.axis_index(dim) for dim in DIMS}
        self.near = tuple({dim: _rem(self.place[dim] + step, 4) for dim in DIMS} for step in (1, 3))
        self.far = {dim: _rem(self.place[dim] + 2, 4) for dim in DIMS}
        self.sibling = {"c": 1 - self.core}
        self.sides = ((0, self.core), (1, 1 - self.core))
        self.credit = credit
        self.partners = [({dim: self.near[way][dim]}, 2 * d + 1 - way, 2 * d + way)
                         for d, dim in enumerate(DIMS) for way in TWO]
        self.partners.append((self.sibling, 6, 6))

    def meet(self):
        barrier = pltpu.get_barrier_semaphore()
        for device, _, _ in self.partners:
            pl.semaphore_signal(barrier, inc=1, device_id=device, device_id_type=MESH)
        pl.semaphore_wait(barrier, len(self.partners))

    def remote(self, source, target, send_sem, recv_sem, device):
        return pltpu.make_async_remote_copy(src_ref=source, dst_ref=target, send_sem=send_sem, recv_sem=recv_sem,
                                            device_id=device, device_id_type=MESH)

    def run(self, steps, n_chunks, n_ticks, after):
        def tick(now, carry):
            @pl.when(now >= 2)
            def _():
                for _, _, mine in self.partners:
                    pl.semaphore_wait(self.credit.at[mine], 1)

            for lag, action in steps:
                @pl.when((now >= lag) & (now < lag + n_chunks))
                def _(lag=lag, action=action):
                    action(now - lag)
            after(now)

            @pl.when(now < n_ticks - 2)
            def _():
                for device, theirs, _ in self.partners:
                    pl.semaphore_signal(self.credit.at[theirs], inc=1, device_id=device, device_id_type=MESH)
            return carry

        lax.fori_loop(0, n_ticks, tick, 0)


def forward_steps(torus, n_layers, x_ref, rows_ref, down_ref, y_ref, saved, wbuf, peer, shard, twin, state, lefts, rights,
                  q_buf, k_buf, v_buf, hid_buf, acc, ring_send, ring_recv, pair_send, pair_recv, keep_sem, save_sem,
                  hid_sem, twin_sem):
    acts, w_out, hid_out, gelu_out, norm_out, q_out, k_out, v_out, o_out = saved
    core, place, near = torus.core, torus.place, torus.near
    slots = GATHER_SLOTS
    n_chunks = n_layers * PER_HALF
    ready = 6 * LAG
    seq = state.shape[0]
    third = 64 * ROWS
    last = n_layers - 1
    swap = torus.remote(rows_ref.at[1 - core], twin, twin_sem.at[0], twin_sem.at[1], torus.sibling)
    swap.start()
    swap.wait_send()
    swap.wait_recv()

    def assemble(chunk):
        @pl.when(chunk < 5 * n_layers)
        def _():
            layer, part = chunk // 5, _rem(chunk, 5)
            cols = _at(part * FIFTH, FIFTH)
            mine, other = [ref[layer, :, cols].astype(jnp.float32) for ref in (rows_ref.at[core], twin)]
            shard[layer, :, cols] = jnp.concatenate(
                [jnp.where(core == 0, mine, other), jnp.where(core == 0, other, mine)], axis=0).astype(jnp.bfloat16)

            @pl.when(part == 4)
            def _():
                shard[layer, :, UP_END:] = down_ref[layer]

    def columns(chunk):
        return _at(_rem(chunk, PER_HALF) * COLS, COLS)

    def spot(slot, color, stage, position, cols):
        order = ORDERS[color]
        index = tuple(EVERY if dim in order[:stage] else position if dim == order[stage] else place[dim]
                      for dim in DIMS)
        return wbuf.at[(slot,) + index + (_rows(color), cols)]

    halves = (slice(0, COLS // 2), slice(COLS // 2, COLS))

    def send_own(stage, chunk):
        slot, sem = _rem(chunk, slots), _rem(chunk, RING)
        for color in COLORS:
            dim = ORDERS[color][stage]
            here = spot(slot, color, stage, place[dim], slice(0, COLS))
            source = here
            if stage == 0:
                source = shard.at[chunk // PER_HALF, _rows(color), columns(chunk)]
            for way in TWO:
                torus.remote(source, here, ring_send.at[2 * stage, sem], ring_recv.at[2 * stage, sem],
                             {dim: near[way][dim]}).start()

    def send_far(stage, chunk):
        slot, sem = _rem(chunk, slots), _rem(chunk, RING)
        for color in COLORS:
            dim = ORDERS[color][stage]
            for way in TWO:
                block = spot(slot, color, stage, near[1 - way][dim], halves[way])
                torus.remote(block, block, ring_send.at[2 * stage + 1, sem], ring_recv.at[2 * stage + 1, sem],
                             {dim: near[way][dim]}).start()

    def arrived(part, chunk):
        slot, sem = _rem(chunk, slots), _rem(chunk, RING)
        block = (wbuf.at[slot, 0, 0, 0:2], wbuf.at[slot, 0, 0, 0], wbuf.at[slot, 0, 0:2], wbuf.at[slot, 0, 0],
                 wbuf.at[slot, 0:2], wbuf.at[slot, 0])[part]
        whole = torus.remote(block, block, ring_send.at[part, sem], ring_recv.at[part, sem], torus.sibling)
        whole.wait_send()
        whole.wait_recv()

    def enter(chunk):
        wbuf[_rem(chunk, slots), place["z"], place["y"], place["x"]] = shard[chunk // PER_HALF, :, columns(chunk)]
        send_own(0, chunk)

    def pass_on(part, chunk):
        arrived(part, chunk)
        if part % 2 == 0:
            send_far(part // 2, chunk)
        else:
            send_own(part // 2 + 1, chunk)

    def pair_copy(chunk):
        slot = _rem(chunk, RING)
        return torus.remote(wbuf.at[_rem(chunk, slots)], peer.at[slot], pair_send.at[slot], pair_recv.at[slot],
                            torus.sibling)

    def exchange(chunk):
        arrived(5, chunk)
        pair_copy(chunk).start()

    def keep_copy(chunk):
        return pltpu.make_async_copy(wbuf.at[_rem(chunk, slots)],
                                     w_out.at[chunk // PER_HALF, :, :, :, :, columns(chunk)],
                                     keep_sem.at[_rem(chunk, RING)])

    def save_copies(layer, names):
        parts = {"n0": (lefts.at[NORM_ATTN], norm_out.at[layer, 0], 0), "n1": (lefts.at[NORM_MLP], norm_out.at[layer, 1], 1),
                 "q": (q_buf, q_out.at[layer], 2), "k": (k_buf, k_out.at[layer], 3), "v": (v_buf, v_out.at[layer], 4),
                 "o": (rights.at[O_AT:QKV_AT], o_out.at[layer], 5), "a": (lefts.at[0:6], gelu_out.at[layer], 6),
                 "mid": (state, acts.at[2 * layer], 7), "end": (state, acts.at[2 * layer + 1], 8)}
        return [pltpu.make_async_copy(parts[name][0], parts[name][1], save_sem.at[parts[name][2]]) for name in names]

    def save(layer, names):
        @pl.when(layer < last)
        def _():
            for copy in save_copies(layer, names):
                copy.start()

    def saved_all(layer, names):
        @pl.when(layer < last)
        def _():
            for copy in save_copies(layer, names):
                copy.wait()

    def hidden_copies(layer, order):
        slot, part, at = _rem(order, 2), order // 6, _at(_rem(order, 6) * COLS, COLS)
        return [pltpu.make_async_copy(hid_buf.at[slot, half], hid_out.at[layer, part, half, :, at],
                                      hid_sem.at[slot, half]) for half in TWO]

    def compute(chunk):
        layer, index = chunk // PER_HALF, _rem(chunk, PER_HALF)
        pair = pair_copy(chunk)
        pair.wait_send()
        pair.wait_recv()
        keep_copy(chunk).start()

        def weights(role):
            block = wbuf[_rem(chunk, slots)] if role == 0 else peer[_rem(chunk, RING)]
            return block.reshape(third, COLS)

        @pl.when(index == 0)
        def _():
            lefts[NORM_ATTN] = _rms(state[ALL])
            save(layer, ["n0"])

        @pl.when(index < 3)
        def _():
            for role, half in torus.sides:
                q_buf[:, _at(3 * COLS * half + COLS * index, COLS)] = _dot(
                    lefts[NORM_ATTN], weights(role)).astype(jnp.bfloat16)

        @pl.when(index == 3)
        def _():
            for role, half in torus.sides:
                both = _dot(lefts[NORM_ATTN], weights(role)).astype(jnp.bfloat16)
                k_buf[:, _at(HEAD * half, HEAD)] = both[:, :HEAD]
                v_buf[:, _at(HEAD * half, HEAD)] = both[:, HEAD:]

        @pl.when(index == QKV)
        def _():
            acc[ALL] = jnp.zeros_like(acc)
            save(layer, ["q", "k", "v"])

        @pl.when((index >= QKV) & (index < ATTN))
        def _():
            causal = _causal(seq)
            for role, half in torus.sides:
                key, value = k_buf[:, _at(HEAD * half, HEAD)], v_buf[:, _at(HEAD * half, HEAD)]
                outs = []
                for head in TWO:
                    at = _at(3 * COLS * half + COLS * (index - QKV) + HEAD * head, HEAD)
                    prob = _probs(q_buf[:, at], key, causal)
                    outs.append(_dot(prob.astype(jnp.bfloat16), value).astype(jnp.bfloat16))
                block = jnp.concatenate(outs, axis=1)
                rights[O_AT + 3 * half + index - QKV] = block
                acc[ALL] += _dot_rhs_t(block, weights(role))

        @pl.when(index == ATTN - 1)
        def _():
            @pl.when(layer > 0)
            def _():
                saved_all(layer - 1, ["end"])
            middle = (state[ALL].astype(jnp.float32) + acc[ALL]).astype(jnp.bfloat16)
            state[ALL] = middle
            lefts[NORM_MLP] = _rms(middle)
            save(layer, ["n1", "o"])
            mid = save_copies(layer, ["mid"])[0]
            mid.start()

        @pl.when((index > ATTN) & (index <= UP_BLOCKS))
        def _():
            for copy in hidden_copies(layer, index - ATTN - 1):
                copy.wait()

        @pl.when((index >= ATTN) & (index < UP_BLOCKS))
        def _():
            order = index - ATTN
            for role, half in torus.sides:
                hidden = _dot(lefts[NORM_MLP], weights(role))
                hid_buf[_rem(order, 2), half] = hidden
                lefts[3 * half + order // 6, :, _at(COLS * _rem(order, 6), COLS)] = jax.nn.gelu(
                    hidden).astype(jnp.bfloat16)
            for copy in hidden_copies(layer, order):
                copy.start()

        @pl.when(index == UP_BLOCKS)
        def _():
            save(layer, ["a"])
            save_copies(layer, ["mid"])[0].wait()

        @pl.when(index >= UP_BLOCKS)
        def _():
            part, at = (index - UP_BLOCKS) // 6, _at(COLS * _rem(index - UP_BLOCKS, 6), COLS)
            total = sum(_dot(lefts[3 * half + part], weights(role)) for role, half in torus.sides)

            @pl.when(part == 0)
            def _():
                acc[:, at] = total

            @pl.when(part > 0)
            def _():
                acc[:, at] += total

        @pl.when(index == PER_HALF - 1)
        def _():
            saved_all(layer, ["n0", "n1", "q", "k", "v", "o", "a"])
            result = (state[ALL].astype(jnp.float32) + acc[ALL]).astype(jnp.bfloat16)
            state[ALL] = result
            save(layer, ["end"])

            @pl.when(layer == last)
            def _():
                pltpu.make_async_copy(state, y_ref, save_sem.at[9]).start()

        keep_copy(chunk).wait()

    steps = [(0, assemble), (0, enter)]
    steps += [((part + 1) * LAG, functools.partial(pass_on, part)) for part in range(5)]
    return steps + [(ready, exchange), (ready + 1, compute)]


def backward_steps(torus, n_layers, g_ref, x_ref, dx_ref, saved, out, wbuf, lefts, rights, hid_buf, dact, dnorm, q_buf,
                   k_buf, v_buf, x_buf, dk_acc, dv_acc, sums, half_bufs, full_bufs, load_sem, own_sem, push_send,
                   push_recv, pair_send, pair_recv, ring_send, ring_recv):
    acts, w_own, hid_in, gelu_in, norm_in, q_in, k_in, v_in, o_in = saved
    place, near = torus.place, torus.near
    seq = g_ref.shape[0]
    third = 64 * ROWS
    last = n_layers - 1

    def mine_slot(chunk):
        return GATHER_SLOTS + _rem(chunk, 2)

    def out_slot(chunk):
        return GATHER_SLOTS + 2 + _rem(chunk, 2)

    def their_slot(chunk):
        return 7 + _rem(chunk, SLOTS)

    def peer_slot(chunk):
        order = _rem(chunk, RING)
        return jnp.where(order == 0, 6, jnp.where(order == 3, 10, GATHER_SLOTS + 3 + order))

    def pair_of(chunk):
        return last - chunk // PER_HALF

    def columns(chunk):
        index = _rem(chunk, PER_HALF)
        block = jnp.where(index < DOWN_DONE, UP_BLOCKS + index,
                          jnp.where(index < UP_DONE, index - 11, jnp.where(index < O_DONE, index - 32, index - 39)))
        return _at(block * COLS, COLS)

    def loads(pair, names):
        def source(name):
            return {"a": (gelu_in.at[pair], lefts.at[0:6], 0), "n_mlp": (norm_in.at[pair, 1], lefts.at[NORM_MLP], 1),
                    "n_attn": (norm_in.at[pair, 0], lefts.at[NORM_ATTN], 2), "o": (o_in.at[pair], rights.at[O_AT:QKV_AT], 3),
                    "q": (q_in.at[pair], q_buf, 4), "k": (k_in.at[pair], k_buf, 5), "v": (v_in.at[pair], v_buf, 6),
                    "x_mid": (acts.at[2 * pair], x_buf, 7)}[name]
        return [pltpu.make_async_copy(source(name)[0], source(name)[1], load_sem.at[source(name)[2]])
                for name in names]

    def start(pair, names):
        for copy in loads(pair, names):
            copy.start()

    def finish(pair, names):
        for copy in loads(pair, names):
            copy.wait()

    def first_input(ref):
        return pltpu.make_async_copy(ref, x_buf, load_sem.at[9])

    def hidden_load(pair, part, half):
        return pltpu.make_async_copy(hid_in.at[pair, part, half], hid_buf, load_sem.at[8])

    def own_copy(chunk):
        return pltpu.make_async_copy(w_own.at[pair_of(chunk), :, :, :, :, columns(chunk)], wbuf.at[mine_slot(chunk)],
                                     own_sem.at[_rem(chunk, 2)])

    def push_copy(chunk):
        slot = _rem(chunk, SLOTS)
        return torus.remote(w_own.at[pair_of(chunk), :, :, :, :, columns(chunk)], wbuf.at[their_slot(chunk)],
                            push_send.at[slot], push_recv.at[slot], torus.sibling)

    def fetch(chunk):
        own_copy(chunk).start()
        push_copy(chunk).start()

    def total_grad():
        return jnp.concatenate([rights[block] for block in SIX], axis=1).astype(jnp.float32)

    def consume(chunk):
        pair, index = pair_of(chunk), _rem(chunk, PER_HALF)
        own_copy(chunk).wait()
        push = push_copy(chunk)
        push.wait_send()
        push.wait_recv()

        def weights(role):
            return wbuf[(mine_slot, their_slot)[role](chunk)].reshape(third, COLS)

        @pl.when(index == 0)
        def _():
            start(pair, ["x_mid"])

            @pl.when(pair < last)
            def _():
                start(pair, ["n_mlp", "n_attn", "o", "q", "k", "v"])

        def bend_back(part, half):
            hidden_load(pair, part, half).wait()
            for block in SIX:
                cols = slice(COLS * block, COLS * block + COLS)
                hidden = hid_buf[:, cols]
                bend = jnp.tanh(0.7978845608028654 * (hidden + 0.044715 * (hidden * hidden * hidden)))
                slope = 0.5 * (1.0 + bend) + 0.5 * hidden * (1.0 - bend * bend) * (
                    0.7978845608028654 * (1.0 + 0.134145 * (hidden * hidden)))
                rights[DH_AT + FF * half + 6 * part + block] = (dact[half, :, cols] * slope).astype(jnp.bfloat16)

        @pl.when((index > 0) & (index <= DOWN_DONE) & (_rem(index, 6) == 0))
        def _():
            bend_back(index // 6 - 1, 1)

        @pl.when((index < DOWN_DONE) & (_rem(index, 6) == 0))
        def _():
            dact[ALL] = jnp.zeros_like(dact)
            hidden_load(pair, index // 6, 0).start()

        @pl.when(index < DOWN_DONE)
        def _():
            for role, half in torus.sides:
                dact[half] += _dot_rhs_t(rights[_rem(index, 6)], weights(role))

        @pl.when((index < DOWN_DONE) & (_rem(index, 6) == 5))
        def _():
            bend_back(index // 6, 0)
            hidden_load(pair, index // 6, 1).start()

        @pl.when(index == DOWN_DONE - 1)
        def _():
            @pl.when(pair < last)
            def _():
                finish(pair, ["n_mlp", "n_attn", "o", "q", "k", "v"])

        @pl.when(index == DOWN_DONE)
        def _():
            dnorm[ALL] = jnp.zeros_like(dnorm)

            @pl.when(pair > 0)
            def _():
                start(pair - 1, ["a"])

        @pl.when((index >= DOWN_DONE) & (index < UP_DONE))
        def _():
            dnorm[ALL] += sum(_dot_rhs_t(rights[DH_AT + FF * half + index - DOWN_DONE], weights(role))
                              for role, half in torus.sides)

        @pl.when(index == UP_DONE - 1)
        def _():
            finish(pair, ["x_mid"])
            lefts[GRAD] = (total_grad() + _rms_back(x_buf[ALL], dnorm[ALL])).astype(jnp.bfloat16)

        @pl.when(index == UP_DONE)
        def _():
            @pl.when(pair == 0)
            def _():
                first_input(x_ref).start()

            @pl.when(pair > 0)
            def _():
                first_input(acts.at[2 * pair - 1]).start()
            dk_acc[ALL] = jnp.zeros_like(dk_acc)
            dv_acc[ALL] = jnp.zeros_like(dv_acc)

        @pl.when((index >= UP_DONE) & (index < O_DONE))
        def _():
            causal = _causal(seq)
            for role, half in torus.sides:
                d_o = _dot(lefts[GRAD], weights(role)).astype(jnp.bfloat16)
                key, value = k_buf[:, _at(HEAD * half, HEAD)], v_buf[:, _at(HEAD * half, HEAD)]
                d_q = []
                for head in TWO:
                    query = q_buf[:, _at(3 * COLS * half + COLS * (index - UP_DONE) + HEAD * head, HEAD)]
                    d_head = d_o[:, HEAD * head:HEAD * head + HEAD]
                    prob = _probs(query, key, causal)
                    d_prob = _dot_rhs_t(d_head, value)
                    dv_acc[half] += _dot_lhs_t(prob.astype(jnp.bfloat16), d_head)
                    d_score = prob * (d_prob - jnp.sum(prob * d_prob, axis=-1, keepdims=True))
                    d_score = (d_score * (HEAD ** -0.5)).astype(jnp.bfloat16)
                    d_q.append(_dot(d_score, key).astype(jnp.bfloat16))
                    dk_acc[half] += _dot_lhs_t(d_score, query)
                rights[QKV_AT + QKV * half + index - UP_DONE] = jnp.concatenate(d_q, axis=1)

        @pl.when(index == O_DONE - 1)
        def _():
            for half in TWO:
                rights[QKV_AT + QKV * half + QKV - 1] = jnp.concatenate([dk_acc[half], dv_acc[half]], axis=1).astype(jnp.bfloat16)

        @pl.when(index == O_DONE)
        def _():
            dnorm[ALL] = jnp.zeros_like(dnorm)

        @pl.when(index >= O_DONE)
        def _():
            dnorm[ALL] += sum(_dot_rhs_t(rights[QKV_AT + QKV * half + index - O_DONE], weights(role))
                              for role, half in torus.sides)

        @pl.when(index == PER_HALF - 1)
        def _():
            first_input(x_ref).wait()

            @pl.when(pair > 0)
            def _():
                finish(pair - 1, ["a"])
            result = (lefts[GRAD].astype(jnp.float32) + _rms_back(x_buf[ALL], dnorm[ALL])).astype(jnp.bfloat16)
            dx_ref[ALL] = result
            for block in SIX:
                rights[block] = result[:, COLS * block:COLS * block + COLS]

    def pair_copy(chunk):
        slot = _rem(chunk, RING)
        return torus.remote(wbuf.at[out_slot(chunk)], wbuf.at[peer_slot(chunk)], pair_send.at[slot], pair_recv.at[slot],
                            torus.sibling)

    def multiply(chunk):
        index = _rem(chunk, PER_HALF)
        lead = _rem(chunk, sums[0].shape[0])
        quarter = third // RING
        for role, half in torus.sides[::-1]:
            left = jnp.where(index < DOWN_DONE, 3 * half + index // 6,
                             jnp.where(index < UP_DONE, NORM_MLP, jnp.where(index < O_DONE, GRAD, NORM_ATTN)))
            right = jnp.where(index < DOWN_DONE, _rem(index, 6),
                              jnp.where(index < UP_DONE, DH_AT + FF * half + index - DOWN_DONE,
                                        jnp.where(index < O_DONE, O_AT + 3 * half + index - UP_DONE,
                                                  QKV_AT + QKV * half + index - O_DONE)))
            for z in range(RING):
                part = _dot_lhs_t(lefts[left, :, quarter * z:quarter * z + quarter], rights[right])
                if role == 0:
                    sums[0][lead, z] = part.reshape(RING, RING, ROWS, COLS)
                else:
                    wbuf[out_slot(chunk), z] = part.astype(jnp.bfloat16).reshape(RING, RING, ROWS, COLS)
        pair_copy(chunk).start()

    def merge_pair(chunk):
        lead = _rem(chunk, sums[0].shape[0])
        pair_copy(chunk).wait_send()
        pair_copy(chunk).wait_recv()
        for z in range(RING):
            for y in range(RING):
                sums[0][lead, z, y] = sums[0][lead, z, y] + wbuf[peer_slot(chunk), z, y].astype(jnp.float32)

    def ring_copy(stage, part, slot, color, way):
        send, recv = (half_bufs, full_bufs)[part][stage]
        dim = ORDERS[color][stage]
        return torus.remote(send.at[slot, color, way], recv.at[slot, color, way],
                            ring_send.at[2 * stage + part, slot], ring_recv.at[2 * stage + part, slot],
                            {dim: near[way][dim]})

    def ring_wait(stage, part, slot):
        send, recv = (half_bufs, full_bufs)[part][stage]
        whole = torus.remote(send.at[slot], recv.at[slot], ring_send.at[2 * stage + part, slot],
                             ring_recv.at[2 * stage + part, slot], torus.sibling)
        whole.wait_send()
        whole.wait_recv()

    def source(stage, chunk, color, position, cols):
        lead = _rem(chunk, sums[stage].shape[0])
        if stage == 0:
            return sums[0][(lead,) + _block(color, 0, position) + (_rows(color), cols)]
        return sums[stage][(lead, color) + _block(color, stage, position) + (EVERY, cols)]

    left_cols, right_cols, every = slice(0, COLS // 2), slice(COLS // 2, COLS), slice(0, COLS)

    def store_halves(stage, chunk):
        slot = _rem(chunk, RING)
        send = half_bufs[stage][0]
        for color in COLORS:
            far = torus.far[ORDERS[color][stage]]
            send[slot, color, 0] = source(stage, chunk, color, far, left_cols).astype(jnp.bfloat16)
            send[slot, color, 1] = source(stage, chunk, color, far, right_cols).astype(jnp.bfloat16)

    def store_fulls(stage, chunk):
        slot = _rem(chunk, RING)
        ring_wait(stage, 0, slot)
        recv = half_bufs[stage][1]
        send = full_bufs[stage][0]
        lead = (EVERY,) * (len(send.shape) - 4)
        for color in COLORS:
            dim = ORDERS[color][stage]
            for way, summed, plain in ((0, left_cols, right_cols), (1, right_cols, left_cols)):
                send[(slot, color, way) + lead + (summed,)] = (
                    source(stage, chunk, color, near[way][dim], summed)
                    + recv[slot, color, way].astype(jnp.float32)).astype(jnp.bfloat16)
                send[(slot, color, way) + lead + (plain,)] = source(
                    stage, chunk, color, near[way][dim], plain).astype(jnp.bfloat16)

    def close_stage(stage, chunk):
        slot = _rem(chunk, RING)
        ring_wait(stage, 1, slot)
        recv = full_bufs[stage][1]
        for color in COLORS:
            dim = ORDERS[color][stage]
            total = (source(stage, chunk, color, place[dim], every)
                     + recv[slot, color, 0].astype(jnp.float32)
                     + recv[slot, color, 1].astype(jnp.float32))
            if stage < 2:
                sums[stage + 1][_rem(chunk, sums[stage + 1].shape[0]), color] = total
            else:
                out[pair_of(chunk), _rows(color), columns(chunk)] = total

    def send_all(stage, part, chunk):
        for color in COLORS:
            for way in TWO:
                ring_copy(stage, part, _rem(chunk, RING), color, way).start()

    def open_first(chunk):
        merge_pair(chunk)
        store_halves(0, chunk)
        send_all(0, 0, chunk)

    def middle(stage, chunk):
        store_fulls(stage, chunk)
        send_all(stage, 1, chunk)

    def open_stage(stage, chunk):
        store_halves(stage, chunk)
        send_all(stage, 0, chunk)

    def turn(stage, chunk):
        close_stage(stage, chunk)
        if stage < 2:
            open_stage(stage + 1, chunk)

    return [(0, fetch), (2 * LAG, functools.partial(middle, 0)), (LAG, open_first),
            (3 * LAG, functools.partial(turn, 0)), (4 * LAG, functools.partial(middle, 1)),
            (5 * LAG, functools.partial(turn, 1)), (6 * LAG, functools.partial(middle, 2)),
            (7 * LAG, functools.partial(turn, 2)), (1, consume), (0, multiply)]


def train_kernel(n_layers, x_ref, g_ref, rows_ref, down_ref, y_ref, dx_ref, rows_out, out, *refs):
    saved, refs = refs[:9], refs[9:]
    (wbuf, peer, shard, twin, state, lefts, rights, q_buf, k_buf, v_buf, hid_out_buf, acc, hid_in_buf, dact, x_buf,
     dk_acc, dv_acc, away), refs = refs[:18], refs[18:]
    sums, half_bufs, full_bufs, refs = refs[:3], refs[3:9], refs[9:15], refs[15:]
    half_bufs = [half_bufs[2 * stage:2 * stage + 2] for stage in COLORS]
    full_bufs = [full_bufs[2 * stage:2 * stage + 2] for stage in COLORS]
    forward_sems, backward_sems, (swap_sem, credit) = refs[:8], refs[8:16], refs[16:]
    torus = Torus(credit)
    core = torus.core
    n_chunks = n_layers * PER_HALF
    fill = pltpu.make_async_copy(x_ref, state, forward_sems[5].at[9])
    fill.start()
    for block in SIX:
        pltpu.make_async_copy(g_ref.at[:, COLS * block:COLS * block + COLS], rights.at[block],
                              backward_sems[0].at[3]).start()
    torus.meet()
    fill.wait()
    pltpu.make_async_copy(rights.at[0:6], rights.at[0:6], backward_sems[0].at[3]).wait()
    forward = forward_steps(torus, n_layers, x_ref, rows_ref, down_ref, y_ref, saved, wbuf, peer, shard, twin, state, lefts,
                            rights, q_buf, k_buf, v_buf, hid_out_buf, acc, *forward_sems)
    backward = backward_steps(torus, n_layers, g_ref, x_ref, dx_ref, saved, out, wbuf, lefts, rights, hid_in_buf, dact, acc,
                              q_buf, k_buf, v_buf, x_buf, dk_acc, dv_acc, sums, half_bufs, full_bufs,
                              *backward_sems)
    turn_at = n_chunks
    backward = [(lag + turn_at, step) for lag, step in backward]
    n_ticks = turn_at + n_chunks + 7 * LAG
    half_rows = ROWS // 2
    tail = 2

    def hand_over(layer, part):
        cols = _at(part * FIFTH, FIFTH)
        both = out[layer, :, cols]
        low, high = both[:half_rows], both[half_rows:]
        rows_out[core, layer, :, cols] = jnp.where(core == 0, low, high)
        away[layer, :, cols] = jnp.where(core == 0, high, low)
        torus.remote(away.at[layer, :, cols], rows_out.at[core, layer, :, cols], swap_sem.at[0], swap_sem.at[1],
                     torus.sibling).start()

    def hand_on(now):
        for layer in range(1, n_layers):
            begin = turn_at + (n_layers - layer) * PER_HALF + 8 * LAG

            @pl.when((now >= begin) & (now < begin + 5))
            def _(layer=layer, begin=begin):
                hand_over(layer, now - begin)

        @pl.when(now >= n_ticks - 5 + tail)
        def _():
            hand_over(0, now - n_ticks + 5)

    torus.run(backward[:1] + forward + backward[1:], n_chunks, n_ticks, hand_on)
    for part in range(tail):
        hand_over(0, part)
    swap = torus.remote(away, rows_out.at[core], swap_sem.at[0], swap_sem.at[1], torus.sibling)
    swap.wait_send()
    swap.wait_recv()
    pltpu.make_async_copy(state, y_ref, forward_sems[5].at[9]).wait()


def train_stack(x_loc, g_loc, rows, down):
    n_layers = down.shape[0]
    seq, width = x_loc.shape
    bf16, f32 = jnp.bfloat16, jnp.float32
    half = COLS // 2
    chunk = CUBE + (ROWS, COLS)
    shape = jax.ShapeDtypeStruct
    hbm = pl.BlockSpec(memory_space=pl.ANY)
    vmem = pl.BlockSpec(memory_space=pltpu.VMEM)
    dma = pltpu.SemaphoreType.DMA
    saved = (shape((2 * n_layers - 1, seq, width), bf16), shape((n_layers,) + CUBE + (ROWS, PER_HALF * COLS), bf16),
             shape((n_layers, 3, 2, seq, width), f32), shape((n_layers, 6, seq, width), bf16),
             shape((n_layers, 2, seq, width), bf16), shape((n_layers, seq, width), bf16),
             shape((n_layers, seq, 2 * HEAD), bf16), shape((n_layers, seq, 2 * HEAD), bf16),
             shape((n_layers, 6, seq, COLS), bf16))
    scratch = [pltpu.VMEM(full, kind) for full, kind in (
        ((GATHER_SLOTS + 6,) + chunk, bf16), ((RING,) + chunk, bf16), ((n_layers, ROWS, PER_HALF * COLS), bf16),
        (rows.shape[1:], bf16), ((seq, width), bf16), ((9, seq, width), bf16), ((56, seq, COLS), bf16),
        ((seq, 6 * COLS), bf16), ((seq, 2 * HEAD), bf16), ((seq, 2 * HEAD), bf16), ((2, 2, seq, COLS), f32),
        ((seq, width), f32), ((seq, width), f32), ((2, seq, width), f32), ((seq, width), bf16),
        ((2, seq, HEAD), f32), ((2, seq, HEAD), f32), ((n_layers, ROWS // 2, UP_END), f32), ((6,) + chunk, f32),
        ((5, 3, RING, RING, TILE, COLS), f32), ((5, 3, RING, TILE, COLS), f32))]
    for cols in (half, COLS):
        for size in ((RING, RING), (RING,), ()):
            scratch += [pltpu.VMEM((RING, 3, 2) + size + (TILE, cols), bf16)] * 2
    scratch += [dma((6, RING)), dma((6, RING)), dma((RING,)), dma((RING,)), dma((RING,)), dma((10,)), dma((2, 2)), dma((2,))]
    scratch += [dma((10,)), dma((2,)), dma((SLOTS,)), dma((SLOTS,)), dma((RING,)), dma((RING,)), dma((6, RING)),
                dma((6, RING)), dma((2,)), pltpu.SemaphoreType.REGULAR((7,))]
    return pl.pallas_call(
        functools.partial(train_kernel, n_layers), name="train_stack",
        out_shape=(shape((seq, width), bf16), shape((seq, width), bf16), shape((2, n_layers, ROWS // 2, UP_END), f32),
                   shape((n_layers, ROWS, PER_HALF * COLS), f32)) + saved,
        in_specs=[hbm, hbm, vmem, vmem], out_specs=(hbm,) + (vmem,) * 3 + (hbm,) * len(saved), scratch_shapes=scratch,
        compiler_params=pltpu.CompilerParams(collective_id=0, has_side_effects=True, vmem_limit_bytes=VMEM_LIMIT),
    )(x_loc, g_loc, rows, down)[:4]


LANES = 128


def _moves(chips, block, packed_first):
    moves = []
    for half in TWO:
        for part in COLORS:
            for chip in range(chips):
                packed = chips * ROWS * (3 * half + part) + ROWS * chip
                plain = block * (2 * chip + half) + ROWS * part
                pair = (packed, plain) if packed_first else (plain, packed)
                moves.append(pair + (min(ROWS, block - ROWS * part),))
    return moves


def _pieces(moves, size):
    tiles = [[] for _ in range(size // LANES)]
    for target, source, length in moves:
        while length:
            step = min(length, LANES - target % LANES, LANES - source % LANES)
            tiles[target // LANES].append((target % LANES, source // LANES, (target - source) % LANES))
            target, source, length = target + step, source + step, length - step
    return [sorted(tile) for tile in tiles]


def _gather_tile(load, tile, lane):
    total = None
    for first, source, shift in tile:
        value = load(source)
        if shift:
            value = pltpu.roll(value, shift, axis=value.ndim - 1)
        total = value if total is None else jnp.where(lane >= first, value, total)
    return total


def _span(index, size):
    return slice(size * index, size * index + size)


def pack_kernel(chips, q_ref, k_ref, v_ref, o_ref, up_ref, down_ref, rows_out, down_out, wide):
    rows, layers, cols = up_ref.shape
    block, _, width = down_ref.shape
    heads = q_ref.shape[1] // 2
    for half in TWO:
        for layer in range(layers):
            for at, ref in ((0, q_ref), (heads + 2, o_ref)):
                for head in range(heads):
                    rows_out[half, layer, :, _span(at + head, LANES)] = ref[
                        :, heads * half + head].astype(jnp.float32)[:, layer].astype(jnp.bfloat16)
            for at, ref in ((heads, k_ref), (heads + 1, v_ref)):
                rows_out[half, layer, :, _span(at, LANES)] = ref[layer].astype(
                    jnp.float32)[:, half].astype(jnp.bfloat16)
    for tile in range(cols // LANES):
        both = up_ref[:, :, _span(tile, LANES)].astype(jnp.float32)
        for layer in range(layers):
            wide[layer, :, _span(tile, LANES)] = both[:, layer]
    lane = lax.broadcasted_iota(jnp.int32, (layers, rows, LANES), 2)
    half_f = 3 * chips * ROWS
    for index, tile in enumerate(_pieces(_moves(chips, block, True), 2 * half_f)):
        value = _gather_tile(lambda source: wide[:, :, _span(source, LANES)], tile, lane)
        half, at = divmod(LANES * index, half_f)
        if at >= 2 * chips * ROWS:
            position = lax.rem(lane + LANES * index % ROWS, ROWS)
            value = jnp.where(position < block - 2 * ROWS, value, 0.0)
        start = ATTN * COLS + at
        rows_out[half, :, :, start:start + LANES] = value.astype(jnp.bfloat16)
    for part in COLORS:
        used = min(ROWS, block - ROWS * part)
        value = down_ref[ROWS * part:ROWS * part + used].astype(jnp.float32)
        for layer in range(layers):
            one = value[:, layer]
            if used < ROWS:
                one = jnp.concatenate([one, jnp.zeros((ROWS - used, width), jnp.float32)], axis=0)
            down_out[layer, :, _span(part, width)] = one.astype(jnp.bfloat16)


def pack_weights(w_q, w_k, w_v, w_o, w_up, w_down, chips):
    layers, rows = w_up.shape[:2]
    width = w_down.shape[2]
    vmem = pl.BlockSpec(memory_space=pltpu.VMEM)
    shape = jax.ShapeDtypeStruct
    return pl.pallas_call(
        functools.partial(pack_kernel, chips), name="pack_weights",
        out_shape=(shape((2, layers, rows, UP_END), jnp.bfloat16), shape((layers, ROWS, 3 * width), jnp.bfloat16)),
        in_specs=[vmem] * 6, out_specs=(vmem,) * 2,
        scratch_shapes=[pltpu.VMEM(w_up.shape, jnp.float32)],
        compiler_params=pltpu.CompilerParams(vmem_limit_bytes=VMEM_LIMIT),
    )(w_q.transpose(1, 2, 0, 3), w_k, w_v, w_o.transpose(1, 2, 0, 3), w_up.transpose(1, 0, 2),
      w_down.transpose(1, 0, 2))


def unpack_kernel(chips, rows_ref, down_ref, y_ref, dx_ref, q_out, k_out, v_out, o_out, up_out, down_out, y_out,
                  dx_out):
    rows, layers, cols = up_out.shape
    block, _, width = down_out.shape
    heads = q_out.shape[1] // 2
    for half in TWO:
        for layer in range(layers):
            for at, ref in ((0, q_out), (heads + 2, o_out)):
                for head in range(heads):
                    ref[:, heads * half + head, layer, :] = rows_ref[half, layer, :, _span(at + head, LANES)]
            for at, ref in ((heads, k_out), (heads + 1, v_out)):
                ref[layer, :, half, :] = rows_ref[half, layer, :, _span(at, LANES)]
    lane = lax.broadcasted_iota(jnp.int32, (layers, rows, LANES), 2)
    half_f = 3 * chips * ROWS

    def load(source):
        half, at = divmod(LANES * source, half_f)
        return rows_ref[half, :, :, ATTN * COLS + at:ATTN * COLS + at + LANES]

    for index, tile in enumerate(_pieces(_moves(chips, block, False), cols)):
        value = _gather_tile(load, tile, lane)
        for layer in range(layers):
            up_out[:, layer, _span(index, LANES)] = value[layer]
    for part in COLORS:
        used = min(ROWS, block - ROWS * part)
        for layer in range(layers):
            down_out[ROWS * part:ROWS * part + used, layer, :] = down_ref[layer, :used, UP_END + width * part:UP_END + width * part + width]
    y_out[ALL] = y_ref[ALL]
    dx_out[ALL] = dx_ref[ALL]


def unpack_grads(row_grad, down_grad, y_loc, grad_x, shapes, chips):
    vmem = pl.BlockSpec(memory_space=pltpu.VMEM)
    q_shape, k_shape, _, _, up_shape, down_shape = shapes
    layers, rows, heads, head_dim = q_shape
    turned = [(rows, heads, layers, head_dim), k_shape, k_shape, (rows, heads, layers, head_dim),
              (rows, layers, up_shape[2]), (down_shape[1], layers, down_shape[2])]
    shape = jax.ShapeDtypeStruct
    outs = pl.pallas_call(
        functools.partial(unpack_kernel, chips), name="unpack_grads",
        out_shape=tuple(shape(full, jnp.float32) for full in turned) + tuple(
            shape(value.shape, value.dtype) for value in (y_loc, grad_x)),
        in_specs=[vmem] * 4, out_specs=(vmem,) * 8,
        compiler_params=pltpu.CompilerParams(vmem_limit_bytes=VMEM_LIMIT),
    )(row_grad, down_grad, y_loc, grad_x)
    d_q, d_k, d_v, d_o, d_up, d_down, y_out, dx_out = outs
    return (y_out[None], dx_out[None], d_q.transpose(2, 0, 1, 3), d_k, d_v, d_o.transpose(2, 0, 1, 3),
            d_up.transpose(1, 0, 2), d_down.transpose(1, 0, 2))


def solution(mesh):
    mesh4 = Mesh(mesh.devices.reshape(CUBE + (2,)), ALL_AXES)
    row_spec = P(ALL_AXES)
    weight_spec = P(None, ALL_AXES)

    def body(x_in, w_q, w_k, w_v, w_o, w_up, w_down, grad_out):
        weights = (w_q, w_k, w_v, w_o, w_up, w_down)
        chips = w_up.shape[2] // w_down.shape[1] // 2
        rows, down = pack_weights(*weights, chips)
        y_loc, grad_x, row_grad, down_grad = train_stack(x_in[0], grad_out[0], rows, down)
        return unpack_grads(row_grad, down_grad, y_loc, grad_x, [weight.shape for weight in weights], chips)

    return jax.shard_map(body, mesh=mesh4, in_specs=(row_spec,) + (weight_spec,) * 6 + (row_spec,),
                         out_specs=(row_spec, row_spec) + (weight_spec,) * 6, check_vma=False)
```

```python
import functools

import jax
import jax.numpy as jnp
from jax import lax
from jax.experimental import pallas as pl
from jax.experimental.pallas import tpu as pltpu
from jax.sharding import Mesh, PartitionSpec as P

MESH = pl.DeviceIdType.MESH
ALL_AXES = ("z", "y", "x", "c")
EPS = 1e-6
MASK_FILL = -1e30
DIMS = ("z", "y", "x")
ORDERS = (("x", "y", "z"), ("y", "z", "x"), ("z", "x", "y"))
COLS = 256
ROWS = 24
LAG = 2
WIDE = COLS // 2
HALF_ROWS = ROWS // 2
HEAD = 128
PER_HALF = 43
UP_BLOCKS = 25
UP_END = UP_BLOCKS * COLS
RING = 4
STAGES = 3
FINAL = STAGES - 1
CUBE = (RING, RING, RING)
CHIPS = RING ** STAGES
SLOTS = 3
TILE = 8
COLORS = range(3)
TWO = range(2)
SIX = range(6)
ALL = Ellipsis
EVERY = slice(None)
QKV, ATTN, FF = 4, 7, 18
DOWN_DONE = FF
UP_DONE = DOWN_DONE + FF
O_DONE = UP_DONE + ATTN - QKV
SIXTH = 6
DH_AT = SIXTH
O_AT = DH_AT + UP_DONE
QKV_AT = O_AT + SIXTH
NORM_MLP, GRAD, NORM_ATTN = 6, 7, 8
VMEM_LIMIT = 67043328


FIFTH = UP_END // 5
GATHER_SLOTS = SIXTH * LAG + RING


def _rows(color):
    return slice(TILE * color, TILE * color + TILE)


def _rem(value, by):
    return lax.rem(value, by)


def _block(color, stage, position):
    dims = tuple(dim for dim in DIMS if dim not in ORDERS[color][:stage])
    return tuple(position if dim == ORDERS[color][stage] else EVERY for dim in dims)


def _dot(left, right):
    return jnp.dot(left, right, preferred_element_type=jnp.float32)


def _dot_rhs_t(left, right):
    return lax.dot_general(left, right, (((1,), (1,)), ((), ())), preferred_element_type=jnp.float32)


def _dot_lhs_t(left, right):
    return lax.dot_general(left, right, (((0,), (0,)), ((), ())), preferred_element_type=jnp.float32)


def _at(start, size):
    return pl.ds(pl.multiple_of(start, size), size)


def _causal(seq):
    return (lax.broadcasted_iota(jnp.int32, (seq, seq), 0) >= lax.broadcasted_iota(jnp.int32, (seq, seq), 1))


def _probs(query, key, causal):
    scores = jnp.where(causal, _dot_rhs_t(query, key) * (HEAD ** -0.5), MASK_FILL)
    weight = jnp.exp(scores - jnp.max(scores, axis=-1, keepdims=True))
    return weight / jnp.sum(weight, axis=-1, keepdims=True)


def _rms(values):
    wide = values.astype(jnp.float32)
    return (wide * lax.rsqrt(jnp.mean(wide * wide, axis=-1, keepdims=True) + EPS)).astype(jnp.bfloat16)


def _rms_back(values, grad):
    wide = values.astype(jnp.float32)
    scale = lax.rsqrt(jnp.mean(wide * wide, axis=-1, keepdims=True) + EPS)
    return scale * grad - wide * (scale * scale * scale) * jnp.mean(wide * grad, axis=-1, keepdims=True)


class Torus:
    def __init__(self, credit):
        self.core = lax.axis_index("c")
        self.place = {dim: lax.axis_index(dim) for dim in DIMS}
        self.near = tuple({dim: _rem(self.place[dim] + step, RING) for dim in DIMS} for step in (1, 3))
        self.far = {dim: _rem(self.place[dim] + 2, RING) for dim in DIMS}
        self.sibling = {"c": 1 - self.core}
        self.sides = ((0, self.core), (1, 1 - self.core))
        self.credit = credit
        self.partners = [({dim: self.near[way][dim]}, 2 * d + 1 - way, 2 * d + way)
                         for d, dim in enumerate(DIMS) for way in TWO]
        self.partners.append((self.sibling, 6, 6))

    def meet(self):
        barrier = pltpu.get_barrier_semaphore()
        for device, _, _ in self.partners:
            pl.semaphore_signal(barrier, inc=1, device_id=device, device_id_type=MESH)
        pl.semaphore_wait(barrier, len(self.partners))

    def remote(self, source, target, send_sem, recv_sem, device):
        return pltpu.make_async_remote_copy(src_ref=source, dst_ref=target, send_sem=send_sem, recv_sem=recv_sem,
                                            device_id=device, device_id_type=MESH)

    def run(self, steps, n_chunks, n_ticks, after):
        def tick(now, carry):
            @pl.when(now >= 2)
            def _():
                for _, _, mine in self.partners:
                    pl.semaphore_wait(self.credit.at[mine], 1)

            for lag, action in steps:
                @pl.when((now >= lag) & (now < lag + n_chunks))
                def _(lag=lag, action=action):
                    action(now - lag)
            after(now)

            @pl.when(now < n_ticks - 2)
            def _():
                for device, theirs, _ in self.partners:
                    pl.semaphore_signal(self.credit.at[theirs], inc=1, device_id=device, device_id_type=MESH)
            return carry

        lax.fori_loop(0, n_ticks, tick, 0)


def forward_steps(torus, n_layers, x_ref, rows_ref, down_ref, y_ref, saved, wbuf, peer, shard, twin, state, lefts, rights,
                  q_buf, k_buf, v_buf, hid_buf, acc, ring_send, ring_recv, pair_send, pair_recv, keep_sem, save_sem,
                  hid_sem, twin_sem):
    acts, w_out, hid_out, gelu_out, norm_out, q_out, k_out, v_out, o_out = saved
    core, place, near = torus.core, torus.place, torus.near
    slots = GATHER_SLOTS
    n_chunks = n_layers * PER_HALF
    ready = SIXTH * LAG
    seq = state.shape[0]
    third = CHIPS * ROWS
    last = n_layers - 1
    swap = torus.remote(rows_ref.at[1 - core], twin, twin_sem.at[0], twin_sem.at[1], torus.sibling)
    swap.start()
    swap.wait_send()
    swap.wait_recv()

    def assemble(chunk):
        @pl.when(chunk < 5 * n_layers)
        def _():
            layer, part = chunk // 5, _rem(chunk, 5)
            cols = _at(part * FIFTH, FIFTH)
            mine, other = [ref[layer, :, cols].astype(jnp.float32) for ref in (rows_ref.at[core], twin)]
            shard[layer, :, cols] = jnp.concatenate(
                [jnp.where(core == 0, mine, other), jnp.where(core == 0, other, mine)], axis=0).astype(jnp.bfloat16)

            @pl.when(part == 4)
            def _():
                shard[layer, :, UP_END:] = down_ref[layer]

    def columns(chunk):
        return _at(_rem(chunk, PER_HALF) * COLS, COLS)

    def spot(slot, color, stage, position, cols):
        order = ORDERS[color]
        index = tuple(EVERY if dim in order[:stage] else position if dim == order[stage] else place[dim]
                      for dim in DIMS)
        return wbuf.at[(slot,) + index + (_rows(color), cols)]

    halves = (slice(0, WIDE), slice(WIDE, COLS))

    def send_own(stage, chunk):
        slot, sem = _rem(chunk, slots), _rem(chunk, RING)
        for color in COLORS:
            dim = ORDERS[color][stage]
            here = spot(slot, color, stage, place[dim], slice(0, COLS))
            source = here
            if stage == 0:
                source = shard.at[chunk // PER_HALF, _rows(color), columns(chunk)]
            for way in TWO:
                torus.remote(source, here, ring_send.at[2 * stage, sem], ring_recv.at[2 * stage, sem],
                             {dim: near[way][dim]}).start()

    def send_far(stage, chunk):
        slot, sem = _rem(chunk, slots), _rem(chunk, RING)
        for color in COLORS:
            dim = ORDERS[color][stage]
            for way in TWO:
                block = spot(slot, color, stage, near[1 - way][dim], halves[way])
                torus.remote(block, block, ring_send.at[2 * stage + 1, sem], ring_recv.at[2 * stage + 1, sem],
                             {dim: near[way][dim]}).start()

    def arrived(part, chunk):
        slot, sem = _rem(chunk, slots), _rem(chunk, RING)
        count = slice(0, 2) if part % 2 == 0 else 0
        block = wbuf.at[(slot,) + (0,) * (2 - part // 2) + (count,)]
        whole = torus.remote(block, block, ring_send.at[part, sem], ring_recv.at[part, sem], torus.sibling)
        whole.wait_send()
        whole.wait_recv()

    def enter(chunk):
        wbuf[_rem(chunk, slots), place["z"], place["y"], place["x"]] = shard[chunk // PER_HALF, :, columns(chunk)]
        send_own(0, chunk)

    def pass_on(part, chunk):
        arrived(part, chunk)
        if part % 2 == 0:
            send_far(part // 2, chunk)
        else:
            send_own(part // 2 + 1, chunk)

    def pair_copy(chunk):
        slot = _rem(chunk, RING)
        return torus.remote(wbuf.at[_rem(chunk, slots)], peer.at[slot], pair_send.at[slot], pair_recv.at[slot],
                            torus.sibling)

    def exchange(chunk):
        arrived(5, chunk)
        pair_copy(chunk).start()

    def keep_copy(chunk):
        return pltpu.make_async_copy(wbuf.at[_rem(chunk, slots)],
                                     w_out.at[chunk // PER_HALF, :, :, :, :, columns(chunk)],
                                     keep_sem.at[_rem(chunk, RING)])

    def save_copies(layer, names):
        parts = {"n0": (lefts.at[NORM_ATTN], norm_out.at[layer, 0]), "n1": (lefts.at[NORM_MLP], norm_out.at[layer, 1]),
                 "q": (q_buf, q_out.at[layer]), "k": (k_buf, k_out.at[layer]), "v": (v_buf, v_out.at[layer]),
                 "o": (rights.at[O_AT:QKV_AT], o_out.at[layer]), "a": (lefts.at[:NORM_MLP], gelu_out.at[layer]),
                 "mid": (state, acts.at[2 * layer]), "end": (state, acts.at[2 * layer + 1])}
        places = list(parts)
        return [pltpu.make_async_copy(*parts[name], save_sem.at[places.index(name)]) for name in names]

    def save(layer, names):
        @pl.when(layer < last)
        def _():
            for copy in save_copies(layer, names):
                copy.start()

    def saved_all(layer, names):
        @pl.when(layer < last)
        def _():
            for copy in save_copies(layer, names):
                copy.wait()

    def hidden_copies(layer, order):
        slot, part, at = _rem(order, 2), order // SIXTH, _at(_rem(order, SIXTH) * COLS, COLS)
        return [pltpu.make_async_copy(hid_buf.at[slot, half], hid_out.at[layer, part, half, :, at],
                                      hid_sem.at[slot, half]) for half in TWO]

    def compute(chunk):
        layer, index = chunk // PER_HALF, _rem(chunk, PER_HALF)
        pair = pair_copy(chunk)
        pair.wait_send()
        pair.wait_recv()
        keep_copy(chunk).start()

        def weights(role):
            block = wbuf[_rem(chunk, slots)] if role == 0 else peer[_rem(chunk, RING)]
            return block.reshape(third, COLS)

        @pl.when(index == 0)
        def _():
            lefts[NORM_ATTN] = _rms(state[ALL])
            save(layer, ["n0"])

        @pl.when(index < 3)
        def _():
            for role, half in torus.sides:
                q_buf[:, _at(STAGES * COLS * half + COLS * index, COLS)] = _dot(
                    lefts[NORM_ATTN], weights(role)).astype(jnp.bfloat16)

        @pl.when(index == 3)
        def _():
            for role, half in torus.sides:
                both = _dot(lefts[NORM_ATTN], weights(role)).astype(jnp.bfloat16)
                k_buf[:, _at(HEAD * half, HEAD)] = both[:, :HEAD]
                v_buf[:, _at(HEAD * half, HEAD)] = both[:, HEAD:]

        @pl.when(index == QKV)
        def _():
            acc[ALL] = jnp.zeros_like(acc)
            save(layer, ["q", "k", "v"])

        @pl.when((index >= QKV) & (index < ATTN))
        def _():
            causal = _causal(seq)
            for role, half in torus.sides:
                key, value = k_buf[:, _at(HEAD * half, HEAD)], v_buf[:, _at(HEAD * half, HEAD)]
                outs = []
                for head in TWO:
                    at = _at(STAGES * COLS * half + COLS * (index - QKV) + HEAD * head, HEAD)
                    prob = _probs(q_buf[:, at], key, causal)
                    outs.append(_dot(prob.astype(jnp.bfloat16), value).astype(jnp.bfloat16))
                block = jnp.concatenate(outs, axis=1)
                rights[O_AT + STAGES * half + index - QKV] = block
                acc[ALL] += _dot_rhs_t(block, weights(role))

        @pl.when(index == ATTN - 1)
        def _():
            @pl.when(layer > 0)
            def _():
                saved_all(layer - 1, ["end"])
            middle = (state[ALL].astype(jnp.float32) + acc[ALL]).astype(jnp.bfloat16)
            state[ALL] = middle
            lefts[NORM_MLP] = _rms(middle)
            save(layer, ["n1", "o"])
            mid = save_copies(layer, ["mid"])[0]
            mid.start()

        @pl.when((index > ATTN) & (index <= UP_BLOCKS))
        def _():
            for copy in hidden_copies(layer, index - ATTN - 1):
                copy.wait()

        @pl.when((index >= ATTN) & (index < UP_BLOCKS))
        def _():
            order = index - ATTN
            for role, half in torus.sides:
                hidden = _dot(lefts[NORM_MLP], weights(role))
                hid_buf[_rem(order, 2), half] = hidden
                lefts[STAGES * half + order // SIXTH, :, _at(COLS * _rem(order, SIXTH), COLS)] = jax.nn.gelu(
                    hidden).astype(jnp.bfloat16)
            for copy in hidden_copies(layer, order):
                copy.start()

        @pl.when(index == UP_BLOCKS)
        def _():
            save(layer, ["a"])
            save_copies(layer, ["mid"])[0].wait()

        @pl.when(index >= UP_BLOCKS)
        def _():
            part, at = (index - UP_BLOCKS) // SIXTH, _at(COLS * _rem(index - UP_BLOCKS, SIXTH), COLS)
            total = sum(_dot(lefts[STAGES * half + part], weights(role)) for role, half in torus.sides)

            @pl.when(part == 0)
            def _():
                acc[:, at] = total

            @pl.when(part > 0)
            def _():
                acc[:, at] += total

        @pl.when(index == PER_HALF - 1)
        def _():
            saved_all(layer, ["n0", "n1", "q", "k", "v", "o", "a"])
            result = (state[ALL].astype(jnp.float32) + acc[ALL]).astype(jnp.bfloat16)
            state[ALL] = result
            save(layer, ["end"])

            @pl.when(layer == last)
            def _():
                pltpu.make_async_copy(state, y_ref, save_sem.at[9]).start()

        keep_copy(chunk).wait()

    steps = [(0, assemble), (0, enter)]
    steps += [((part + 1) * LAG, functools.partial(pass_on, part)) for part in range(5)]
    return steps + [(ready, exchange), (ready + 1, compute)]


def backward_steps(torus, n_layers, x_ref, x_out, saved, out, wbuf, lefts, rights, hid_buf, dact, dnorm, q_buf,
                   k_buf, v_buf, x_buf, dk_acc, dv_acc, sums, half_bufs, full_bufs, load_sem, own_sem, push_send,
                   push_recv, pair_send, pair_recv, ring_send, ring_recv):
    acts, w_own, hid_in, gelu_in, norm_in, q_in, k_in, v_in, o_in = saved
    place, near = torus.place, torus.near
    seq = k_buf.shape[0]
    third = CHIPS * ROWS
    last = n_layers - 1

    def mine_slot(chunk):
        return GATHER_SLOTS + _rem(chunk, 2)

    def out_slot(chunk):
        return GATHER_SLOTS + 2 + _rem(chunk, 2)

    def their_slot(chunk):
        return 7 + _rem(chunk, SLOTS)

    def peer_slot(chunk):
        order = _rem(chunk, RING)
        return jnp.where(order == 0, 6, jnp.where(order == 3, 10, GATHER_SLOTS + 3 + order))

    def pair_of(chunk):
        return last - chunk // PER_HALF

    def columns(chunk):
        index = _rem(chunk, PER_HALF)
        block = jnp.where(index < DOWN_DONE, UP_BLOCKS + index,
                          jnp.where(index < UP_DONE, index - 11, jnp.where(index < O_DONE, index - 32, index - 39)))
        return _at(block * COLS, COLS)

    def loads(pair, names):
        parts = {"a": (gelu_in.at[pair], lefts.at[:NORM_MLP]), "n_mlp": (norm_in.at[pair, 1], lefts.at[NORM_MLP]),
                 "n_attn": (norm_in.at[pair, 0], lefts.at[NORM_ATTN]), "o": (o_in.at[pair], rights.at[O_AT:QKV_AT]),
                 "q": (q_in.at[pair], q_buf), "k": (k_in.at[pair], k_buf), "v": (v_in.at[pair], v_buf),
                 "x_mid": (acts.at[2 * pair], x_buf)}
        places = list(parts)
        return [pltpu.make_async_copy(*parts[name], load_sem.at[places.index(name)]) for name in names]

    def start(pair, names):
        for copy in loads(pair, names):
            copy.start()

    def finish(pair, names):
        for copy in loads(pair, names):
            copy.wait()

    def first_input(ref):
        return pltpu.make_async_copy(ref, x_buf, load_sem.at[9])

    def hidden_load(pair, part, half):
        return pltpu.make_async_copy(hid_in.at[pair, part, half], hid_buf, load_sem.at[8])

    def own_copy(chunk):
        return pltpu.make_async_copy(w_own.at[pair_of(chunk), :, :, :, :, columns(chunk)], wbuf.at[mine_slot(chunk)],
                                     own_sem.at[_rem(chunk, 2)])

    def push_copy(chunk):
        slot = _rem(chunk, SLOTS)
        return torus.remote(w_own.at[pair_of(chunk), :, :, :, :, columns(chunk)], wbuf.at[their_slot(chunk)],
                            push_send.at[slot], push_recv.at[slot], torus.sibling)

    def fetch(chunk):
        own_copy(chunk).start()
        push_copy(chunk).start()

    def total_grad():
        return jnp.concatenate([rights[block] for block in SIX], axis=1).astype(jnp.float32)

    def consume(chunk):
        pair, index = pair_of(chunk), _rem(chunk, PER_HALF)
        own_copy(chunk).wait()
        push = push_copy(chunk)
        push.wait_send()
        push.wait_recv()

        def weights(role):
            return wbuf[(mine_slot, their_slot)[role](chunk)].reshape(third, COLS)

        @pl.when(index == 0)
        def _():
            start(pair, ["x_mid"])

            @pl.when(pair < last)
            def _():
                start(pair, ["n_mlp", "n_attn", "o", "q", "k", "v"])

        def bend_back(part, half):
            hidden_load(pair, part, half).wait()
            for block in SIX:
                cols = slice(COLS * block, COLS * block + COLS)
                hidden = hid_buf[:, cols]
                bend = jnp.tanh(0.7978845608028654 * (hidden + 0.044715 * (hidden * hidden * hidden)))
                slope = 0.5 * (1.0 + bend) + 0.5 * hidden * (1.0 - bend * bend) * (
                    0.7978845608028654 * (1.0 + 0.134145 * (hidden * hidden)))
                rights[DH_AT + FF * half + SIXTH * part + block] = (dact[half, :, cols] * slope).astype(jnp.bfloat16)

        @pl.when((index > 0) & (index <= DOWN_DONE) & (_rem(index, SIXTH) == 0))
        def _():
            bend_back(index // SIXTH - 1, 1)

        @pl.when((index < DOWN_DONE) & (_rem(index, SIXTH) == 0))
        def _():
            dact[ALL] = jnp.zeros_like(dact)
            hidden_load(pair, index // SIXTH, 0).start()

        @pl.when(index < DOWN_DONE)
        def _():
            for role, half in torus.sides:
                dact[half] += _dot_rhs_t(rights[_rem(index, SIXTH)], weights(role))

        @pl.when((index < DOWN_DONE) & (_rem(index, SIXTH) == 5))
        def _():
            bend_back(index // SIXTH, 0)
            hidden_load(pair, index // SIXTH, 1).start()

        @pl.when(index == DOWN_DONE - 1)
        def _():
            @pl.when(pair < last)
            def _():
                finish(pair, ["n_mlp", "n_attn", "o", "q", "k", "v"])

        @pl.when(index == DOWN_DONE)
        def _():
            dnorm[ALL] = jnp.zeros_like(dnorm)

            @pl.when(pair > 0)
            def _():
                start(pair - 1, ["a"])

        @pl.when((index >= DOWN_DONE) & (index < UP_DONE))
        def _():
            dnorm[ALL] += sum(_dot_rhs_t(rights[DH_AT + FF * half + index - DOWN_DONE], weights(role))
                              for role, half in torus.sides)

        @pl.when(index == UP_DONE - 1)
        def _():
            finish(pair, ["x_mid"])
            lefts[GRAD] = (total_grad() + _rms_back(x_buf[ALL], dnorm[ALL])).astype(jnp.bfloat16)

        @pl.when(index == UP_DONE)
        def _():
            @pl.when(pair == 0)
            def _():
                first_input(x_ref).start()

            @pl.when(pair > 0)
            def _():
                first_input(acts.at[2 * pair - 1]).start()
            dk_acc[ALL] = jnp.zeros_like(dk_acc)
            dv_acc[ALL] = jnp.zeros_like(dv_acc)

        @pl.when((index >= UP_DONE) & (index < O_DONE))
        def _():
            causal = _causal(seq)
            for role, half in torus.sides:
                d_o = _dot(lefts[GRAD], weights(role)).astype(jnp.bfloat16)
                key, value = k_buf[:, _at(HEAD * half, HEAD)], v_buf[:, _at(HEAD * half, HEAD)]
                d_q = []
                for head in TWO:
                    query = q_buf[:, _at(STAGES * COLS * half + COLS * (index - UP_DONE) + HEAD * head, HEAD)]
                    d_head = d_o[:, HEAD * head:HEAD * head + HEAD]
                    prob = _probs(query, key, causal)
                    d_prob = _dot_rhs_t(d_head, value)
                    dv_acc[half] += _dot_lhs_t(prob.astype(jnp.bfloat16), d_head)
                    d_score = prob * (d_prob - jnp.sum(prob * d_prob, axis=-1, keepdims=True))
                    d_score = (d_score * (HEAD ** -0.5)).astype(jnp.bfloat16)
                    d_q.append(_dot(d_score, key).astype(jnp.bfloat16))
                    dk_acc[half] += _dot_lhs_t(d_score, query)
                rights[QKV_AT + QKV * half + index - UP_DONE] = jnp.concatenate(d_q, axis=1)

        @pl.when(index == O_DONE - 1)
        def _():
            for half in TWO:
                rights[QKV_AT + QKV * half + QKV - 1] = jnp.concatenate([dk_acc[half], dv_acc[half]], axis=1).astype(jnp.bfloat16)

        @pl.when(index == O_DONE)
        def _():
            dnorm[ALL] = jnp.zeros_like(dnorm)

        @pl.when(index >= O_DONE)
        def _():
            dnorm[ALL] += sum(_dot_rhs_t(rights[QKV_AT + QKV * half + index - O_DONE], weights(role))
                              for role, half in torus.sides)

        @pl.when(index == PER_HALF - 1)
        def _():
            first_input(x_ref).wait()

            @pl.when(pair > 0)
            def _():
                finish(pair - 1, ["a"])
            result = (lefts[GRAD].astype(jnp.float32) + _rms_back(x_buf[ALL], dnorm[ALL])).astype(jnp.bfloat16)

            @pl.when(pair == 0)
            def _():
                x_out(result)
            for block in SIX:
                rights[block] = result[:, COLS * block:COLS * block + COLS]

    def pair_copy(chunk):
        slot = _rem(chunk, RING)
        return torus.remote(wbuf.at[out_slot(chunk)], wbuf.at[peer_slot(chunk)], pair_send.at[slot], pair_recv.at[slot],
                            torus.sibling)

    def multiply(chunk):
        index = _rem(chunk, PER_HALF)
        lead = _rem(chunk, sums[0].shape[0])
        quarter = third // RING
        for role, half in torus.sides[::-1]:
            left = jnp.where(index < DOWN_DONE, STAGES * half + index // SIXTH,
                             jnp.where(index < UP_DONE, NORM_MLP, jnp.where(index < O_DONE, GRAD, NORM_ATTN)))
            right = jnp.where(index < DOWN_DONE, _rem(index, SIXTH),
                              jnp.where(index < UP_DONE, DH_AT + FF * half + index - DOWN_DONE,
                                        jnp.where(index < O_DONE, O_AT + STAGES * half + index - UP_DONE,
                                                  QKV_AT + QKV * half + index - O_DONE)))
            for z in range(RING):
                part = _dot_lhs_t(lefts[left, :, quarter * z:quarter * z + quarter], rights[right])
                if role == 0:
                    sums[0][lead, z] = part.reshape(RING, RING, ROWS, COLS)
                else:
                    wbuf[out_slot(chunk), z] = part.astype(jnp.bfloat16).reshape(RING, RING, ROWS, COLS)
        pair_copy(chunk).start()

    def merge_pair(chunk):
        lead = _rem(chunk, sums[0].shape[0])
        pair_copy(chunk).wait_send()
        pair_copy(chunk).wait_recv()
        for z in range(RING):
            for y in range(RING):
                sums[0][lead, z, y] = sums[0][lead, z, y] + wbuf[peer_slot(chunk), z, y].astype(jnp.float32)

    def ring_copy(stage, part, slot, color, way):
        send, recv = (half_bufs, full_bufs)[part][stage]
        dim = ORDERS[color][stage]
        return torus.remote(send.at[slot, color, way], recv.at[slot, color, way],
                            ring_send.at[2 * stage + part, slot], ring_recv.at[2 * stage + part, slot],
                            {dim: near[way][dim]})

    def ring_wait(stage, part, slot):
        send, recv = (half_bufs, full_bufs)[part][stage]
        whole = torus.remote(send.at[slot], recv.at[slot], ring_send.at[2 * stage + part, slot],
                             ring_recv.at[2 * stage + part, slot], torus.sibling)
        whole.wait_send()
        whole.wait_recv()

    def source(stage, chunk, color, position, cols):
        lead = _rem(chunk, sums[stage].shape[0])
        if stage == 0:
            return sums[0][(lead,) + _block(color, 0, position) + (_rows(color), cols)]
        return sums[stage][(lead, color) + _block(color, stage, position) + (EVERY, cols)]

    left_cols, right_cols, every = slice(0, WIDE), slice(WIDE, COLS), slice(0, COLS)

    def store_halves(stage, chunk):
        slot = _rem(chunk, RING)
        send = half_bufs[stage][0]
        for color in COLORS:
            far = torus.far[ORDERS[color][stage]]
            send[slot, color, 0] = source(stage, chunk, color, far, left_cols).astype(jnp.bfloat16)
            send[slot, color, 1] = source(stage, chunk, color, far, right_cols).astype(jnp.bfloat16)

    def store_fulls(stage, chunk):
        slot = _rem(chunk, RING)
        ring_wait(stage, 0, slot)
        recv = half_bufs[stage][1]
        send = full_bufs[stage][0]
        lead = (EVERY,) * (len(send.shape) - 4)
        for color in COLORS:
            dim = ORDERS[color][stage]
            for way, summed, plain in ((0, left_cols, right_cols), (1, right_cols, left_cols)):
                send[(slot, color, way) + lead + (summed,)] = (
                    source(stage, chunk, color, near[way][dim], summed)
                    + recv[slot, color, way].astype(jnp.float32)).astype(jnp.bfloat16)
                send[(slot, color, way) + lead + (plain,)] = source(
                    stage, chunk, color, near[way][dim], plain).astype(jnp.bfloat16)

    def close_stage(stage, chunk):
        slot = _rem(chunk, RING)
        ring_wait(stage, 1, slot)
        recv = full_bufs[stage][1]
        for color in COLORS:
            dim = ORDERS[color][stage]
            total = (source(stage, chunk, color, place[dim], every)
                     + recv[slot, color, 0].astype(jnp.float32)
                     + recv[slot, color, 1].astype(jnp.float32))
            if stage < 2:
                sums[stage + 1][_rem(chunk, sums[stage + 1].shape[0]), color] = total
            else:
                out[pair_of(chunk), _rows(color), columns(chunk)] = total

    def send_all(stage, part, chunk):
        for color in COLORS:
            for way in TWO:
                ring_copy(stage, part, _rem(chunk, RING), color, way).start()

    def open_first(chunk):
        merge_pair(chunk)
        store_halves(0, chunk)
        send_all(0, 0, chunk)

    def middle(stage, chunk):
        store_fulls(stage, chunk)
        send_all(stage, 1, chunk)

    def open_stage(stage, chunk):
        store_halves(stage, chunk)
        send_all(stage, 0, chunk)

    def turn(stage, chunk):
        close_stage(stage, chunk)
        if stage < 2:
            open_stage(stage + 1, chunk)

    return [(0, fetch), (2 * LAG, functools.partial(middle, 0)), (LAG, open_first),
            (3 * LAG, functools.partial(turn, 0)), (4 * LAG, functools.partial(middle, 1)),
            (5 * LAG, functools.partial(turn, 1)), (SIXTH * LAG, functools.partial(middle, 2)),
            (7 * LAG, functools.partial(turn, 2)), (1, consume), (0, multiply)]


def train_kernel(n_layers, x_ref, g_ref, rows_ref, down_ref, y_ref, dx_ref, rows_hbm, down_hbm, *refs):
    saved, refs = refs[:9], refs[9:]
    (rows_out, out), refs = refs[:2], refs[2:]
    (wbuf, peer, shard, twin, state, lefts, rights, q_buf, k_buf, v_buf, hid_out_buf, acc, hid_in_buf, dact, x_buf,
     dk_acc, dv_acc, away), refs = refs[:18], refs[18:]
    sums, half_bufs, full_bufs, refs = refs[:3], refs[3:9], refs[9:15], refs[15:]
    half_bufs = [half_bufs[2 * stage:2 * stage + 2] for stage in COLORS]
    full_bufs = [full_bufs[2 * stage:2 * stage + 2] for stage in COLORS]
    forward_sems, backward_sems, (swap_sem, end_sem, credit) = refs[:8], refs[8:16], refs[16:]
    torus = Torus(credit)
    core = torus.core
    n_chunks = n_layers * PER_HALF
    fill = pltpu.make_async_copy(x_ref, state, forward_sems[5].at[9])
    fill.start()
    for block in SIX:
        pltpu.make_async_copy(g_ref.at[:, COLS * block:COLS * block + COLS], rights.at[block],
                              backward_sems[0].at[3]).start()
    torus.meet()
    fill.wait()
    pltpu.make_async_copy(rights.at[:DH_AT], rights.at[:DH_AT], backward_sems[0].at[3]).wait()
    def y_copy():
        return pltpu.make_async_copy(state, y_ref, forward_sems[5].at[9])

    def x_out(result):
        y_copy().wait()
        state[ALL] = result
        pltpu.make_async_copy(state, dx_ref, forward_sems[5].at[9]).start()

    forward = forward_steps(torus, n_layers, x_ref, rows_ref, down_ref, y_ref, saved, wbuf, peer, shard, twin, state, lefts,
                            rights, q_buf, k_buf, v_buf, hid_out_buf, acc, *forward_sems)
    backward = backward_steps(torus, n_layers, x_ref, x_out, saved, out, wbuf, lefts, rights, hid_in_buf, dact, acc,
                              q_buf, k_buf, v_buf, x_buf, dk_acc, dv_acc, sums, half_bufs, full_bufs,
                              *backward_sems)
    turn_at = n_chunks
    backward = [(lag + turn_at, step) for lag, step in backward]
    n_ticks = turn_at + n_chunks + 7 * LAG
    tail = 2

    def hand_over(layer, part):
        cols = _at(part * FIFTH, FIFTH)
        both = out[layer, :, cols]
        low, high = both[:HALF_ROWS], both[HALF_ROWS:]
        rows_out[core, layer, :, cols] = jnp.where(core == 0, low, high)
        away[layer, :, cols] = jnp.where(core == 0, high, low)
        torus.remote(away.at[layer, :, cols], rows_out.at[core, layer, :, cols], swap_sem.at[0, layer],
                     swap_sem.at[1, layer], torus.sibling).start()

    def down_result(layer):
        return pltpu.make_async_copy(out.at[layer, :, UP_END:], down_hbm.at[layer], end_sem.at[0, layer])

    def rows_result(layer):
        return pltpu.make_async_copy(rows_out.at[:, layer], rows_hbm.at[:, layer], end_sem.at[1, layer])

    def rows_meet(layer):
        swap = torus.remote(away.at[layer], rows_out.at[core, layer], swap_sem.at[0, layer], swap_sem.at[1, layer],
                            torus.sibling)
        swap.wait_send()
        swap.wait_recv()
        rows_result(layer).start()

    def hand_on(now):
        for layer in range(n_layers):
            begin = turn_at + (n_layers - layer) * PER_HALF + 8 * LAG

            @pl.when(now == begin - UP_BLOCKS)
            def _(layer=layer):
                down_result(layer).start()

            if layer > 0:
                @pl.when((now >= begin) & (now < begin + 5))
                def _(layer=layer, begin=begin):
                    hand_over(layer, now - begin)

                @pl.when(now == begin + 8)
                def _(layer=layer):
                    rows_meet(layer)

        @pl.when(now >= n_ticks - 5 + tail)
        def _():
            hand_over(0, now - n_ticks + 5)

    torus.run(backward[:1] + forward + backward[1:], n_chunks, n_ticks, hand_on)
    for part in range(tail):
        hand_over(0, part)
    rows_meet(0)
    for layer in range(n_layers):
        _all_done([down_result(layer), rows_result(layer)])
    pltpu.make_async_copy(state, dx_ref, forward_sems[5].at[9]).wait()


def train_stack(x_loc, g_loc, rows, down):
    n_layers = down.shape[0]
    seq, width = x_loc.shape
    bf16, f32 = jnp.bfloat16, jnp.float32
    half = WIDE
    chunk = CUBE + (ROWS, COLS)
    shape = jax.ShapeDtypeStruct
    hbm = pl.BlockSpec(memory_space=pl.ANY)
    vmem = pl.BlockSpec(memory_space=pltpu.VMEM)
    dma = pltpu.SemaphoreType.DMA
    saved = (shape((2 * n_layers - 1, seq, width), bf16), shape((n_layers,) + CUBE + (ROWS, PER_HALF * COLS), bf16),
             shape((n_layers, 3, 2, seq, width), f32), shape((n_layers, SIXTH, seq, width), bf16),
             shape((n_layers, 2, seq, width), bf16), shape((n_layers, seq, width), bf16),
             shape((n_layers, seq, 2 * HEAD), bf16), shape((n_layers, seq, 2 * HEAD), bf16),
             shape((n_layers, SIXTH, seq, COLS), bf16))
    scratch = [pltpu.VMEM(full, kind) for full, kind in (
        ((2, n_layers, HALF_ROWS, UP_END), f32), ((n_layers, ROWS, PER_HALF * COLS), f32),
        ((GATHER_SLOTS + 6,) + chunk, bf16), ((RING,) + chunk, bf16), ((n_layers, ROWS, PER_HALF * COLS), bf16),
        (rows.shape[1:], bf16), ((seq, width), bf16), ((9, seq, width), bf16), ((56, seq, COLS), bf16),
        ((seq, SIXTH * COLS), bf16), ((seq, 2 * HEAD), bf16), ((seq, 2 * HEAD), bf16), ((2, 2, seq, COLS), f32),
        ((seq, width), f32), ((seq, width), f32), ((2, seq, width), f32), ((seq, width), bf16),
        ((2, seq, HEAD), f32), ((2, seq, HEAD), f32), ((n_layers, HALF_ROWS, UP_END), f32), ((6,) + chunk, f32),
        ((5, 3, RING, RING, TILE, COLS), f32), ((5, 3, RING, TILE, COLS), f32))]
    for cols in (half, COLS):
        for size in ((RING, RING), (RING,), ()):
            scratch += [pltpu.VMEM((RING, 3, 2) + size + (TILE, cols), bf16)] * 2
    scratch += [dma((SIXTH, RING)), dma((SIXTH, RING)), dma((RING,)), dma((RING,)), dma((RING,)), dma((10,)), dma((2, 2)), dma((2,))]
    scratch += [dma((10,)), dma((2,)), dma((SLOTS,)), dma((SLOTS,)), dma((RING,)), dma((RING,)), dma((SIXTH, RING)),
                dma((SIXTH, RING)), dma((2, n_layers)), dma((2, n_layers)), pltpu.SemaphoreType.REGULAR((7,))]
    return pl.pallas_call(
        functools.partial(train_kernel, n_layers), name="train_stack",
        out_shape=(shape((seq, width), bf16), shape((seq, width), bf16), shape((2, n_layers, HALF_ROWS, UP_END), f32),
                   shape(down.shape, f32)) + saved,
        in_specs=[hbm, hbm, vmem, vmem], out_specs=(hbm,) * (4 + len(saved)), scratch_shapes=scratch,
        compiler_params=pltpu.CompilerParams(collective_id=0, has_side_effects=True, vmem_limit_bytes=VMEM_LIMIT),
    )(x_loc, g_loc, rows, down)[:4]


LANES = 128


def _moves(chips, block, packed_first):
    moves = []
    for half in TWO:
        for part in COLORS:
            for chip in range(chips):
                packed = chips * ROWS * (STAGES * half + part) + ROWS * chip
                plain = block * (2 * chip + half) + ROWS * part
                pair = (packed, plain) if packed_first else (plain, packed)
                moves.append(pair + (min(ROWS, block - ROWS * part),))
    return moves


def _pieces(moves, size):
    tiles = [[] for _ in range(size // LANES)]
    for target, source, length in moves:
        while length:
            step = min(length, LANES - target % LANES, LANES - source % LANES)
            tiles[target // LANES].append((target % LANES, source // LANES, (target - source) % LANES))
            target, source, length = target + step, source + step, length - step
    return [sorted(tile) for tile in tiles]


def _gather_tile(load, tile, lane):
    total = None
    for first, source, shift in tile:
        value = load(source)
        if shift:
            value = pltpu.roll(value, shift, axis=value.ndim - 1)
        total = value if total is None else jnp.where(lane >= first, value, total)
    return total


def _span(index, size):
    return slice(size * index, size * index + size)


def _moved(pairs, sems):
    copies = [pltpu.make_async_copy(source, target, sems.at[order]) for order, (source, target) in enumerate(pairs)]
    for copy in copies:
        copy.start()
    return copies


def _all_done(copies):
    for copy in copies:
        copy.wait()


def _head_spots(heads):
    return [[(head, 0, heads * half + head) for head in range(heads)]
            + [(heads + 2 + head, 3, heads * half + head) for head in range(heads)] for half in TWO]


def pack_kernel(chips, *refs):
    sources, (rows_hbm, down_hbm), arrays, refs = refs[:6], refs[6:8], refs[8:14], refs[14:]
    rows_out, down_out, wide, in_sems, out_sems = refs
    k_ref, v_ref, up_ref, down_ref = arrays[1], arrays[2], arrays[4], arrays[5]
    rows, layers, _ = up_ref.shape
    block, _, width = down_ref.shape
    heads = arrays[0].shape[1] // 2
    half_f = STAGES * chips * ROWS
    inward = _moved(zip(sources, arrays), in_sems)
    _all_done(inward[:QKV])
    for half, spots in enumerate(_head_spots(heads)):
        for at, which, head in spots:
            rows_out[half, :, :, _span(at, LANES)] = jnp.swapaxes(
                arrays[which][:, head].astype(jnp.float32), 0, 1).astype(jnp.bfloat16)
        for layer in range(layers):
            for at, ref in ((heads, k_ref), (heads + 1, v_ref)):
                rows_out[half, layer, :, _span(at, LANES)] = ref[layer].astype(
                    jnp.float32)[:, half].astype(jnp.bfloat16)
    inward[QKV].wait()
    wide[ALL] = jnp.swapaxes(up_ref[ALL].astype(jnp.float32), 0, 1)
    lane = lax.broadcasted_iota(jnp.int32, (layers, rows, LANES), 2)
    tiles = _pieces(_moves(chips, block, True), 2 * half_f)
    outward = []
    for half in TWO:
        for index in range(half_f // LANES):
            tile = tiles[half * (half_f // LANES) + index]
            value = _gather_tile(lambda source: wide[:, :, _span(source, LANES)], tile, lane)
            if LANES * index >= 2 * chips * ROWS:
                position = lax.rem(lane + LANES * index % ROWS, ROWS)
                value = jnp.where(position < block - 2 * ROWS, value, 0.0)
            rows_out[half, :, :, _span(2 * ATTN + index, LANES)] = value.astype(jnp.bfloat16)
        outward += _moved([(rows_out.at[half], rows_hbm.at[half])], out_sems.at[half:half + 1])
    inward[5].wait()
    for part in COLORS:
        used = min(ROWS, block - ROWS * part)
        both = jnp.swapaxes(down_ref[ROWS * part:ROWS * part + used].astype(jnp.float32), 0, 1)
        for layer in range(layers):
            one = both[layer]
            if used < ROWS:
                one = jnp.concatenate([one, jnp.zeros((ROWS - used, width), jnp.float32)], axis=0)
            down_out[layer, :, _span(part, width)] = one.astype(jnp.bfloat16)
    _all_done(outward + _moved([(down_out, down_hbm)], out_sems.at[2:3]))


def _bounced(kernel, name, inputs, outs, arrays, n_sems):
    hbm = pl.BlockSpec(memory_space=pl.ANY)
    scratch = [pltpu.VMEM(array.shape, array.dtype) for array in arrays]
    return pl.pallas_call(
        kernel, name=name, out_shape=tuple(outs), in_specs=[hbm] * len(inputs), out_specs=(hbm,) * len(outs),
        scratch_shapes=scratch + [pltpu.SemaphoreType.DMA((size,)) for size in n_sems],
        compiler_params=pltpu.CompilerParams(vmem_limit_bytes=VMEM_LIMIT))(*inputs)


def pack_weights(w_q, w_k, w_v, w_o, w_up, w_down, chips):
    layers, rows = w_up.shape[:2]
    shape = jax.ShapeDtypeStruct
    inputs = [w_q.transpose(1, 2, 0, 3), w_k, w_v, w_o.transpose(1, 2, 0, 3), w_up.transpose(1, 0, 2),
              w_down.transpose(1, 0, 2)]
    outs = [shape((2, layers, rows, UP_END), jnp.bfloat16), shape((layers, ROWS, 3 * w_down.shape[2]), jnp.bfloat16)]
    return _bounced(functools.partial(pack_kernel, chips), "pack_weights", inputs, outs,
                    inputs + outs + [shape(w_up.shape, jnp.float32)], (6, 3))


def unpack_kernel(chips, *refs):
    sources, results, arrays, (in_sems, out_sems) = refs[:4], refs[4:12], refs[12:22], refs[22:]
    rows_ref, down_ref, q_out, k_out, v_out, o_out, up_out, down_out = arrays[:2] + arrays[4:]
    rows, layers, cols = up_out.shape
    block, _, width = down_out.shape
    heads = q_out.shape[1] // 2
    inward = _moved(zip(sources, arrays), in_sems)
    inward[0].wait()
    for half, spots in enumerate(_head_spots(heads)):
        for at, which, head in spots:
            (q_out, o_out)[which // 3][:, head] = jnp.swapaxes(rows_ref[half, :, :, _span(at, LANES)], 0, 1)
        for layer in range(layers):
            for at, ref in ((heads, k_out), (heads + 1, v_out)):
                ref[layer, :, half, :] = rows_ref[half, layer, :, _span(at, LANES)]
    outward = _moved(zip((q_out, k_out, v_out, o_out), results), out_sems)
    lane = lax.broadcasted_iota(jnp.int32, (layers, rows, LANES), 2)
    per_half = STAGES * chips * ROWS // LANES

    def load(source):
        half, tile = divmod(source, per_half)
        return rows_ref[half, :, :, _span(2 * ATTN + tile, LANES)]

    for index, tile in enumerate(_pieces(_moves(chips, block, False), cols)):
        up_out[:, :, _span(index, LANES)] = jnp.swapaxes(_gather_tile(load, tile, lane), 0, 1)
    _all_done(inward[1:])
    outward += _moved(zip((up_out,) + arrays[2:4], results[4:5] + results[6:]), out_sems.at[QKV:])
    for part in COLORS:
        used = min(ROWS, block - ROWS * part)
        for layer in range(layers):
            down_out[ROWS * part:ROWS * part + used, layer, :] = down_ref[layer, :used, _span(part, width)]
    _all_done(outward + _moved([(down_out, results[5])], out_sems.at[ATTN:]))


def unpack_grads(row_grad, down_grad, y_loc, grad_x, shapes, chips):
    q_shape, k_shape, _, _, up_shape, down_shape = shapes
    layers, rows, heads, head_dim = q_shape
    shape = jax.ShapeDtypeStruct
    turned = [(rows, heads, layers, head_dim), k_shape, k_shape, (rows, heads, layers, head_dim),
              (rows, layers, up_shape[2]), (down_shape[1], layers, down_shape[2])]
    turned = [shape(full, jnp.float32) for full in turned]
    inputs = [row_grad, down_grad, y_loc, grad_x]
    outs = _bounced(functools.partial(unpack_kernel, chips), "unpack_grads", inputs,
                    turned + [shape(value.shape, value.dtype) for value in (y_loc, grad_x)], inputs + turned, (4, 8))
    d_q, d_k, d_v, d_o, d_up, d_down, y_out, dx_out = outs
    return (y_out[None], dx_out[None], d_q.transpose(2, 0, 1, 3), d_k, d_v, d_o.transpose(2, 0, 1, 3),
            d_up.transpose(1, 0, 2), d_down.transpose(1, 0, 2))


def solution(mesh):
    mesh4 = Mesh(mesh.devices.reshape(CUBE + (2,)), ALL_AXES)
    row_spec = P(ALL_AXES)
    weight_spec = P(None, ALL_AXES)

    def body(x_in, w_q, w_k, w_v, w_o, w_up, w_down, grad_out):
        weights = (w_q, w_k, w_v, w_o, w_up, w_down)
        chips = w_up.shape[2] // w_down.shape[1] // 2
        rows, down = pack_weights(*weights, chips)
        y_loc, grad_x, row_grad, down_grad = train_stack(x_in[0], grad_out[0], rows, down)
        return unpack_grads(row_grad, down_grad, y_loc, grad_x, [weight.shape for weight in weights], chips)

    return jax.shard_map(body, mesh=mesh4, in_specs=(row_spec,) + (weight_spec,) * 6 + (row_spec,),
                         out_specs=(row_spec, row_spec) + (weight_spec,) * 6, check_vma=False)
```

```python
import functools

import jax
import jax.numpy as jnp
from jax import lax
from jax.experimental import pallas as pl
from jax.experimental.pallas import tpu as pltpu
from jax.sharding import Mesh, PartitionSpec as P

MESH = pl.DeviceIdType.MESH
ALL_AXES = ("z", "y", "x", "c")
EPS = 1e-6
MASK_FILL = -1e30
DIMS = ("z", "y", "x")
ORDERS = (("x", "y", "z"), ("y", "z", "x"), ("z", "x", "y"))
COLS = 256
ROWS = 24
LAG = 2
WIDE = COLS // 2
HALF_ROWS = ROWS // 2
HEAD = 128
PER_HALF = 43
UP_BLOCKS = 25
UP_END = UP_BLOCKS * COLS
RING = 4
STAGES = 3
FINAL = STAGES - 1
CUBE = (RING, RING, RING)
CHIPS = RING ** STAGES
SLOTS = 3
TILE = 8
COLORS = range(3)
TWO = range(2)
SIX = range(6)
ALL = Ellipsis
EVERY = slice(None)
QKV, ATTN, FF = 4, 7, 18
DOWN_DONE = FF
UP_DONE = DOWN_DONE + FF
O_DONE = UP_DONE + ATTN - QKV
SIXTH = 6
DH_AT = SIXTH
O_AT = DH_AT + UP_DONE
QKV_AT = O_AT + SIXTH
NORM_MLP, GRAD, NORM_ATTN = 6, 7, 8
VMEM_LIMIT = 67043328


FIFTH = UP_END // 5
GATHER_SLOTS = SIXTH * LAG + RING


def _rows(color):
    return slice(TILE * color, TILE * color + TILE)


def _rem(value, by):
    return lax.rem(value, by)


def _block(color, stage, position):
    dims = tuple(dim for dim in DIMS if dim not in ORDERS[color][:stage])
    return tuple(position if dim == ORDERS[color][stage] else EVERY for dim in dims)


def _dot(left, right):
    return jnp.dot(left, right, preferred_element_type=jnp.float32)


def _dot_rhs_t(left, right):
    return lax.dot_general(left, right, (((1,), (1,)), ((), ())), preferred_element_type=jnp.float32)


def _dot_lhs_t(left, right):
    return lax.dot_general(left, right, (((0,), (0,)), ((), ())), preferred_element_type=jnp.float32)


def _at(start, size):
    return pl.ds(pl.multiple_of(start, size), size)


def _causal(seq):
    return (lax.rem(lax.broadcasted_iota(jnp.int32, (2 * seq, seq), 0), seq)
            >= lax.broadcasted_iota(jnp.int32, (2 * seq, seq), 1))


def _under(block):
    return jnp.concatenate([block[:, :HEAD], block[:, HEAD:]], axis=0)


def _beside(stacked):
    seq = stacked.shape[0] // 2
    return jnp.concatenate([stacked[:seq], stacked[seq:]], axis=1)


def _probs(query, key, causal):
    scores = jnp.where(causal, _dot_rhs_t(query, key) * (HEAD ** -0.5), MASK_FILL)
    weight = jnp.exp(scores - jnp.max(scores, axis=-1, keepdims=True))
    return weight / jnp.sum(weight, axis=-1, keepdims=True)


def _rms(values):
    wide = values.astype(jnp.float32)
    return (wide * lax.rsqrt(jnp.mean(wide * wide, axis=-1, keepdims=True) + EPS)).astype(jnp.bfloat16)


def _rms_back(values, grad):
    wide = values.astype(jnp.float32)
    scale = lax.rsqrt(jnp.mean(wide * wide, axis=-1, keepdims=True) + EPS)
    return scale * grad - wide * (scale * scale * scale) * jnp.mean(wide * grad, axis=-1, keepdims=True)


class Torus:
    def __init__(self, credit):
        self.core = lax.axis_index("c")
        self.place = {dim: lax.axis_index(dim) for dim in DIMS}
        self.near = tuple({dim: _rem(self.place[dim] + step, RING) for dim in DIMS} for step in (1, 3))
        self.far = {dim: _rem(self.place[dim] + 2, RING) for dim in DIMS}
        self.sibling = {"c": 1 - self.core}
        self.sides = ((0, self.core), (1, 1 - self.core))
        self.credit = credit
        self.partners = [({dim: self.near[way][dim]}, 2 * d + 1 - way, 2 * d + way)
                         for d, dim in enumerate(DIMS) for way in TWO]
        self.partners.append((self.sibling, 6, 6))

    def meet(self):
        barrier = pltpu.get_barrier_semaphore()
        for device, _, _ in self.partners:
            pl.semaphore_signal(barrier, inc=1, device_id=device, device_id_type=MESH)
        pl.semaphore_wait(barrier, len(self.partners))

    def remote(self, source, target, send_sem, recv_sem, device):
        return pltpu.make_async_remote_copy(src_ref=source, dst_ref=target, send_sem=send_sem, recv_sem=recv_sem,
                                            device_id=device, device_id_type=MESH)

    def run(self, steps, n_chunks, n_ticks, after):
        def tick(now, carry):
            @pl.when(now >= 2)
            def _():
                for _, _, mine in self.partners:
                    pl.semaphore_wait(self.credit.at[mine], 1)

            for lag, action in steps:
                @pl.when((now >= lag) & (now < lag + n_chunks))
                def _(lag=lag, action=action):
                    action(now - lag)
            after(now)

            @pl.when(now < n_ticks - 2)
            def _():
                for device, theirs, _ in self.partners:
                    pl.semaphore_signal(self.credit.at[theirs], inc=1, device_id=device, device_id_type=MESH)
            return carry

        lax.fori_loop(0, n_ticks, tick, 0)


def forward_steps(torus, n_layers, x_ref, rows_ref, down_ref, y_ref, saved, wbuf, peer, shard, twin, state, lefts, rights,
                  q_buf, k_buf, v_buf, hid_buf, acc, ring_send, ring_recv, pair_send, pair_recv, keep_sem, save_sem,
                  hid_sem, twin_sem):
    acts, w_out, hid_out, gelu_out, norm_out, q_out, k_out, v_out, o_out = saved
    core, place, near = torus.core, torus.place, torus.near
    slots = GATHER_SLOTS
    n_chunks = n_layers * PER_HALF
    ready = SIXTH * LAG
    seq = state.shape[0]
    third = CHIPS * ROWS
    last = n_layers - 1
    pieces = [(0, EVERY, slice(0, FIFTH)), (0, EVERY, slice(FIFTH, None))] + [
        (layer, EVERY, EVERY) for layer in range(1, n_layers)]
    swaps = [torus.remote(rows_ref.at[(1 - core,) + piece], twin.at[piece], twin_sem.at[0, order], twin_sem.at[1, order],
                          torus.sibling) for order, piece in enumerate(pieces)]
    for swap in swaps:
        swap.start()
    swaps[0].wait_send()
    swaps[0].wait_recv()

    def assemble(chunk):
        @pl.when(chunk == 1)
        def _():
            for swap in swaps[1:]:
                swap.wait_send()
                swap.wait_recv()

        @pl.when(chunk < 5 * n_layers)
        def _():
            layer, part = chunk // 5, _rem(chunk, 5)
            cols = _at(part * FIFTH, FIFTH)
            mine, other = [ref[layer, :, cols].astype(jnp.float32) for ref in (rows_ref.at[core], twin)]
            shard[layer, :, cols] = jnp.concatenate(
                [jnp.where(core == 0, mine, other), jnp.where(core == 0, other, mine)], axis=0).astype(jnp.bfloat16)

            @pl.when(part == 4)
            def _():
                shard[layer, :, UP_END:] = down_ref[layer]

    def columns(chunk):
        return _at(_rem(chunk, PER_HALF) * COLS, COLS)

    def spot(slot, color, stage, position, cols):
        order = ORDERS[color]
        index = tuple(EVERY if dim in order[:stage] else position if dim == order[stage] else place[dim]
                      for dim in DIMS)
        return wbuf.at[(slot,) + index + (_rows(color), cols)]

    halves = (slice(0, WIDE), slice(WIDE, COLS))

    def send_own(stage, chunk):
        slot, sem = _rem(chunk, slots), _rem(chunk, RING)
        for color in COLORS:
            dim = ORDERS[color][stage]
            here = spot(slot, color, stage, place[dim], slice(0, COLS))
            source = here
            if stage == 0:
                source = shard.at[chunk // PER_HALF, _rows(color), columns(chunk)]
            for way in TWO:
                torus.remote(source, here, ring_send.at[2 * stage, sem], ring_recv.at[2 * stage, sem],
                             {dim: near[way][dim]}).start()

    def send_far(stage, chunk):
        slot, sem = _rem(chunk, slots), _rem(chunk, RING)
        for color in COLORS:
            dim = ORDERS[color][stage]
            for way in TWO:
                block = spot(slot, color, stage, near[1 - way][dim], halves[way])
                torus.remote(block, block, ring_send.at[2 * stage + 1, sem], ring_recv.at[2 * stage + 1, sem],
                             {dim: near[way][dim]}).start()

    def arrived(part, chunk):
        slot, sem = _rem(chunk, slots), _rem(chunk, RING)
        count = slice(0, 2) if part % 2 == 0 else 0
        block = wbuf.at[(slot,) + (0,) * (2 - part // 2) + (count,)]
        whole = torus.remote(block, block, ring_send.at[part, sem], ring_recv.at[part, sem], torus.sibling)
        whole.wait_send()
        whole.wait_recv()

    def enter(chunk):
        wbuf[_rem(chunk, slots), place["z"], place["y"], place["x"]] = shard[chunk // PER_HALF, :, columns(chunk)]
        send_own(0, chunk)

    def pass_on(part, chunk):
        arrived(part, chunk)
        if part % 2 == 0:
            send_far(part // 2, chunk)
        else:
            send_own(part // 2 + 1, chunk)

    def pair_copy(chunk):
        slot = _rem(chunk, RING)
        return torus.remote(wbuf.at[_rem(chunk, slots)], peer.at[slot], pair_send.at[slot], pair_recv.at[slot],
                            torus.sibling)

    def exchange(chunk):
        arrived(5, chunk)
        pair_copy(chunk).start()

    def keep_copy(chunk):
        return pltpu.make_async_copy(wbuf.at[_rem(chunk, slots)],
                                     w_out.at[chunk // PER_HALF, :, :, :, :, columns(chunk)],
                                     keep_sem.at[_rem(chunk, RING)])

    def save_copies(layer, names):
        parts = {"n0": (lefts.at[NORM_ATTN], norm_out.at[layer, 0]), "n1": (lefts.at[NORM_MLP], norm_out.at[layer, 1]),
                 "q": (q_buf, q_out.at[layer]), "k": (k_buf, k_out.at[layer]), "v": (v_buf, v_out.at[layer]),
                 "o": (rights.at[O_AT:QKV_AT], o_out.at[layer]), "a": (lefts.at[:NORM_MLP], gelu_out.at[layer]),
                 "mid": (state, acts.at[2 * layer]), "end": (state, acts.at[2 * layer + 1])}
        places = list(parts)
        return [pltpu.make_async_copy(*parts[name], save_sem.at[places.index(name)]) for name in names]

    def save(layer, names):
        @pl.when(layer < last)
        def _():
            for copy in save_copies(layer, names):
                copy.start()

    def saved_all(layer, names):
        @pl.when(layer < last)
        def _():
            for copy in save_copies(layer, names):
                copy.wait()

    def hidden_copies(layer, order):
        slot, part, at = _rem(order, 2), order // SIXTH, _at(_rem(order, SIXTH) * COLS, COLS)
        return [pltpu.make_async_copy(hid_buf.at[slot, half], hid_out.at[layer, part, half, :, at],
                                      hid_sem.at[slot, half]) for half in TWO]

    def compute(chunk):
        layer, index = chunk // PER_HALF, _rem(chunk, PER_HALF)
        pair = pair_copy(chunk)
        pair.wait_send()
        pair.wait_recv()
        keep_copy(chunk).start()

        def weights(role):
            block = wbuf[_rem(chunk, slots)] if role == 0 else peer[_rem(chunk, RING)]
            return block.reshape(third, COLS)

        @pl.when(index == 0)
        def _():
            lefts[NORM_ATTN] = _rms(state[ALL])
            save(layer, ["n0"])

        @pl.when(index < 3)
        def _():
            for role, half in torus.sides:
                q_buf[:, _at(STAGES * COLS * half + COLS * index, COLS)] = _dot(
                    lefts[NORM_ATTN], weights(role)).astype(jnp.bfloat16)

        @pl.when(index == 3)
        def _():
            for role, half in torus.sides:
                both = _dot(lefts[NORM_ATTN], weights(role)).astype(jnp.bfloat16)
                k_buf[:, _at(HEAD * half, HEAD)] = both[:, :HEAD]
                v_buf[:, _at(HEAD * half, HEAD)] = both[:, HEAD:]

        @pl.when(index == QKV)
        def _():
            acc[ALL] = jnp.zeros_like(acc)
            save(layer, ["q", "k", "v"])

        @pl.when((index >= QKV) & (index < ATTN))
        def _():
            causal = _causal(seq)
            for role, half in torus.sides:
                key, value = k_buf[:, _at(HEAD * half, HEAD)], v_buf[:, _at(HEAD * half, HEAD)]
                query = _under(q_buf[:, _at(STAGES * COLS * half + COLS * (index - QKV), COLS)])
                prob = _probs(query, key, causal).astype(jnp.bfloat16)
                block = _beside(_dot(prob, value).astype(jnp.bfloat16))
                rights[O_AT + STAGES * half + index - QKV] = block
                acc[ALL] += _dot_rhs_t(block, weights(role))

        @pl.when(index == ATTN - 1)
        def _():
            @pl.when(layer > 0)
            def _():
                saved_all(layer - 1, ["end"])
            middle = (state[ALL].astype(jnp.float32) + acc[ALL]).astype(jnp.bfloat16)
            state[ALL] = middle
            lefts[NORM_MLP] = _rms(middle)
            save(layer, ["n1", "o"])
            mid = save_copies(layer, ["mid"])[0]
            mid.start()

        @pl.when((index > ATTN) & (index <= UP_BLOCKS))
        def _():
            for copy in hidden_copies(layer, index - ATTN - 1):
                copy.wait()

        @pl.when((index >= ATTN) & (index < UP_BLOCKS))
        def _():
            order = index - ATTN
            for role, half in torus.sides:
                hidden = _dot(lefts[NORM_MLP], weights(role))
                hid_buf[_rem(order, 2), half] = hidden
                lefts[STAGES * half + order // SIXTH, :, _at(COLS * _rem(order, SIXTH), COLS)] = jax.nn.gelu(
                    hidden).astype(jnp.bfloat16)
            for copy in hidden_copies(layer, order):
                copy.start()

        @pl.when(index == UP_BLOCKS)
        def _():
            save(layer, ["a"])
            save_copies(layer, ["mid"])[0].wait()

        @pl.when(index >= UP_BLOCKS)
        def _():
            part, at = (index - UP_BLOCKS) // SIXTH, _at(COLS * _rem(index - UP_BLOCKS, SIXTH), COLS)
            total = sum(_dot(lefts[STAGES * half + part], weights(role)) for role, half in torus.sides)

            @pl.when(part == 0)
            def _():
                acc[:, at] = total

            @pl.when(part > 0)
            def _():
                acc[:, at] += total

        @pl.when(index == PER_HALF - 1)
        def _():
            saved_all(layer, ["n0", "n1", "q", "k", "v", "o", "a"])
            result = (state[ALL].astype(jnp.float32) + acc[ALL]).astype(jnp.bfloat16)
            state[ALL] = result
            save(layer, ["end"])

            @pl.when(layer == last)
            def _():
                pltpu.make_async_copy(state, y_ref, save_sem.at[9]).start()

        keep_copy(chunk).wait()

    steps = [(0, assemble), (0, enter)]
    steps += [((part + 1) * LAG, functools.partial(pass_on, part)) for part in range(5)]
    return steps + [(ready, exchange), (ready + 1, compute)]


def backward_steps(torus, n_layers, x_ref, x_out, saved, out, wbuf, lefts, rights, hid_buf, dact, dnorm, q_buf,
                   k_buf, v_buf, x_buf, dk_acc, dv_acc, sums, half_bufs, full_bufs, load_sem, own_sem, push_send,
                   push_recv, pair_send, pair_recv, ring_send, ring_recv):
    acts, w_own, hid_in, gelu_in, norm_in, q_in, k_in, v_in, o_in = saved
    place, near = torus.place, torus.near
    seq = k_buf.shape[0]
    third = CHIPS * ROWS
    last = n_layers - 1

    def mine_slot(chunk):
        return GATHER_SLOTS + _rem(chunk, 2)

    def out_slot(chunk):
        return GATHER_SLOTS + 2 + _rem(chunk, 2)

    def their_slot(chunk):
        return 7 + _rem(chunk, SLOTS)

    def peer_slot(chunk):
        order = _rem(chunk, RING)
        return jnp.where(order == 0, 6, jnp.where(order == 3, 10, GATHER_SLOTS + 3 + order))

    def pair_of(chunk):
        return last - chunk // PER_HALF

    def columns(chunk):
        index = _rem(chunk, PER_HALF)
        block = jnp.where(index < DOWN_DONE, UP_BLOCKS + index,
                          jnp.where(index < UP_DONE, index - 11, jnp.where(index < O_DONE, index - 32, index - 39)))
        return _at(block * COLS, COLS)

    def loads(pair, names):
        parts = {"a": (gelu_in.at[pair], lefts.at[:NORM_MLP]), "n_mlp": (norm_in.at[pair, 1], lefts.at[NORM_MLP]),
                 "n_attn": (norm_in.at[pair, 0], lefts.at[NORM_ATTN]), "o": (o_in.at[pair], rights.at[O_AT:QKV_AT]),
                 "q": (q_in.at[pair], q_buf), "k": (k_in.at[pair], k_buf), "v": (v_in.at[pair], v_buf),
                 "x_mid": (acts.at[2 * pair], x_buf)}
        places = list(parts)
        return [pltpu.make_async_copy(*parts[name], load_sem.at[places.index(name)]) for name in names]

    def start(pair, names):
        for copy in loads(pair, names):
            copy.start()

    def finish(pair, names):
        for copy in loads(pair, names):
            copy.wait()

    def first_input(ref):
        return pltpu.make_async_copy(ref, x_buf, load_sem.at[9])

    def hidden_load(pair, part, half):
        return pltpu.make_async_copy(hid_in.at[pair, part, half], hid_buf, load_sem.at[8])

    def own_copy(chunk):
        return pltpu.make_async_copy(w_own.at[pair_of(chunk), :, :, :, :, columns(chunk)], wbuf.at[mine_slot(chunk)],
                                     own_sem.at[_rem(chunk, 2)])

    def push_copy(chunk):
        slot = _rem(chunk, SLOTS)
        return torus.remote(w_own.at[pair_of(chunk), :, :, :, :, columns(chunk)], wbuf.at[their_slot(chunk)],
                            push_send.at[slot], push_recv.at[slot], torus.sibling)

    def fetch(chunk):
        own_copy(chunk).start()
        push_copy(chunk).start()

    def total_grad():
        return jnp.concatenate([rights[block] for block in SIX], axis=1).astype(jnp.float32)

    def consume(chunk):
        pair, index = pair_of(chunk), _rem(chunk, PER_HALF)
        own_copy(chunk).wait()
        push = push_copy(chunk)
        push.wait_send()
        push.wait_recv()

        def weights(role):
            return wbuf[(mine_slot, their_slot)[role](chunk)].reshape(third, COLS)

        @pl.when(index == 0)
        def _():
            start(pair, ["x_mid"])

            @pl.when(pair < last)
            def _():
                start(pair, ["n_mlp", "n_attn", "o", "q", "k", "v"])

        def bend_back(part, half):
            hidden_load(pair, part, half).wait()
            for block in SIX:
                cols = slice(COLS * block, COLS * block + COLS)
                hidden = hid_buf[:, cols]
                bend = jnp.tanh(0.7978845608028654 * (hidden + 0.044715 * (hidden * hidden * hidden)))
                slope = 0.5 * (1.0 + bend) + 0.5 * hidden * (1.0 - bend * bend) * (
                    0.7978845608028654 * (1.0 + 0.134145 * (hidden * hidden)))
                rights[DH_AT + FF * half + SIXTH * part + block] = (dact[half, :, cols] * slope).astype(jnp.bfloat16)

        @pl.when((index > 0) & (index <= DOWN_DONE) & (_rem(index, SIXTH) == 0))
        def _():
            bend_back(index // SIXTH - 1, 1)

        @pl.when((index < DOWN_DONE) & (_rem(index, SIXTH) == 0))
        def _():
            dact[ALL] = jnp.zeros_like(dact)
            hidden_load(pair, index // SIXTH, 0).start()

        @pl.when(index < DOWN_DONE)
        def _():
            for role, half in torus.sides:
                dact[half] += _dot_rhs_t(rights[_rem(index, SIXTH)], weights(role))

        @pl.when((index < DOWN_DONE) & (_rem(index, SIXTH) == 5))
        def _():
            bend_back(index // SIXTH, 0)
            hidden_load(pair, index // SIXTH, 1).start()

        @pl.when(index == DOWN_DONE - 1)
        def _():
            @pl.when(pair < last)
            def _():
                finish(pair, ["n_mlp", "n_attn", "o", "q", "k", "v"])

        @pl.when(index == DOWN_DONE)
        def _():
            dnorm[ALL] = jnp.zeros_like(dnorm)

            @pl.when(pair > 0)
            def _():
                start(pair - 1, ["a"])

        @pl.when((index >= DOWN_DONE) & (index < UP_DONE))
        def _():
            dnorm[ALL] += sum(_dot_rhs_t(rights[DH_AT + FF * half + index - DOWN_DONE], weights(role))
                              for role, half in torus.sides)

        @pl.when(index == UP_DONE - 1)
        def _():
            finish(pair, ["x_mid"])
            lefts[GRAD] = (total_grad() + _rms_back(x_buf[ALL], dnorm[ALL])).astype(jnp.bfloat16)

        @pl.when(index == UP_DONE)
        def _():
            @pl.when(pair == 0)
            def _():
                first_input(x_ref).start()

            @pl.when(pair > 0)
            def _():
                first_input(acts.at[2 * pair - 1]).start()
            dk_acc[ALL] = jnp.zeros_like(dk_acc)
            dv_acc[ALL] = jnp.zeros_like(dv_acc)

        @pl.when((index >= UP_DONE) & (index < O_DONE))
        def _():
            causal = _causal(seq)
            for role, half in torus.sides:
                d_o = _dot(lefts[GRAD], weights(role)).astype(jnp.bfloat16)
                key, value = k_buf[:, _at(HEAD * half, HEAD)], v_buf[:, _at(HEAD * half, HEAD)]
                query = _under(q_buf[:, _at(STAGES * COLS * half + COLS * (index - UP_DONE), COLS)])
                d_heads = _under(d_o)
                prob = _probs(query, key, causal)
                d_prob = _dot_rhs_t(d_heads, value)
                dv_acc[half] += _dot_lhs_t(prob.astype(jnp.bfloat16), d_heads)
                d_score = prob * (d_prob - jnp.sum(prob * d_prob, axis=-1, keepdims=True))
                d_score = (d_score * (HEAD ** -0.5)).astype(jnp.bfloat16)
                rights[QKV_AT + QKV * half + index - UP_DONE] = _beside(_dot(d_score, key).astype(jnp.bfloat16))
                dk_acc[half] += _dot_lhs_t(d_score, query)

        @pl.when(index == O_DONE - 1)
        def _():
            for half in TWO:
                rights[QKV_AT + QKV * half + QKV - 1] = jnp.concatenate([dk_acc[half], dv_acc[half]], axis=1).astype(jnp.bfloat16)

        @pl.when(index == O_DONE)
        def _():
            dnorm[ALL] = jnp.zeros_like(dnorm)

        @pl.when(index >= O_DONE)
        def _():
            dnorm[ALL] += sum(_dot_rhs_t(rights[QKV_AT + QKV * half + index - O_DONE], weights(role))
                              for role, half in torus.sides)

        @pl.when(index == PER_HALF - 1)
        def _():
            first_input(x_ref).wait()

            @pl.when(pair > 0)
            def _():
                finish(pair - 1, ["a"])
            result = (lefts[GRAD].astype(jnp.float32) + _rms_back(x_buf[ALL], dnorm[ALL])).astype(jnp.bfloat16)

            @pl.when(pair == 0)
            def _():
                x_out(result)
            for block in SIX:
                rights[block] = result[:, COLS * block:COLS * block + COLS]

    def pair_copy(chunk):
        slot = _rem(chunk, RING)
        return torus.remote(wbuf.at[out_slot(chunk)], wbuf.at[peer_slot(chunk)], pair_send.at[slot], pair_recv.at[slot],
                            torus.sibling)

    def multiply(chunk):
        index = _rem(chunk, PER_HALF)
        lead = _rem(chunk, sums[0].shape[0])
        quarter = third // RING
        for role, half in torus.sides[::-1]:
            left = jnp.where(index < DOWN_DONE, STAGES * half + index // SIXTH,
                             jnp.where(index < UP_DONE, NORM_MLP, jnp.where(index < O_DONE, GRAD, NORM_ATTN)))
            right = jnp.where(index < DOWN_DONE, _rem(index, SIXTH),
                              jnp.where(index < UP_DONE, DH_AT + FF * half + index - DOWN_DONE,
                                        jnp.where(index < O_DONE, O_AT + STAGES * half + index - UP_DONE,
                                                  QKV_AT + QKV * half + index - O_DONE)))
            for z in range(RING):
                part = _dot_lhs_t(lefts[left, :, quarter * z:quarter * z + quarter], rights[right])
                if role == 0:
                    sums[0][lead, z] = part.reshape(RING, RING, ROWS, COLS)
                else:
                    wbuf[out_slot(chunk), z] = part.astype(jnp.bfloat16).reshape(RING, RING, ROWS, COLS)
        pair_copy(chunk).start()

    def merge_pair(chunk):
        lead = _rem(chunk, sums[0].shape[0])
        pair_copy(chunk).wait_send()
        pair_copy(chunk).wait_recv()
        for z in range(RING):
            for y in range(RING):
                sums[0][lead, z, y] = sums[0][lead, z, y] + wbuf[peer_slot(chunk), z, y].astype(jnp.float32)

    def ring_copy(stage, part, slot, color, way):
        send, recv = (half_bufs, full_bufs)[part][stage]
        dim = ORDERS[color][stage]
        return torus.remote(send.at[slot, color, way], recv.at[slot, color, way],
                            ring_send.at[2 * stage + part, slot], ring_recv.at[2 * stage + part, slot],
                            {dim: near[way][dim]})

    def ring_wait(stage, part, slot):
        send, recv = (half_bufs, full_bufs)[part][stage]
        whole = torus.remote(send.at[slot], recv.at[slot], ring_send.at[2 * stage + part, slot],
                             ring_recv.at[2 * stage + part, slot], torus.sibling)
        whole.wait_send()
        whole.wait_recv()

    def source(stage, chunk, color, position, cols):
        lead = _rem(chunk, sums[stage].shape[0])
        if stage == 0:
            return sums[0][(lead,) + _block(color, 0, position) + (_rows(color), cols)]
        return sums[stage][(lead, color) + _block(color, stage, position) + (EVERY, cols)]

    left_cols, right_cols, every = slice(0, WIDE), slice(WIDE, COLS), slice(0, COLS)

    def store_halves(stage, chunk):
        slot = _rem(chunk, RING)
        send = half_bufs[stage][0]
        for color in COLORS:
            far = torus.far[ORDERS[color][stage]]
            send[slot, color, 0] = source(stage, chunk, color, far, left_cols).astype(jnp.bfloat16)
            send[slot, color, 1] = source(stage, chunk, color, far, right_cols).astype(jnp.bfloat16)

    def store_fulls(stage, chunk):
        slot = _rem(chunk, RING)
        ring_wait(stage, 0, slot)
        recv = half_bufs[stage][1]
        send = full_bufs[stage][0]
        lead = (EVERY,) * (len(send.shape) - 4)
        for color in COLORS:
            dim = ORDERS[color][stage]
            for way, summed, plain in ((0, left_cols, right_cols), (1, right_cols, left_cols)):
                send[(slot, color, way) + lead + (summed,)] = (
                    source(stage, chunk, color, near[way][dim], summed)
                    + recv[slot, color, way].astype(jnp.float32)).astype(jnp.bfloat16)
                send[(slot, color, way) + lead + (plain,)] = source(
                    stage, chunk, color, near[way][dim], plain).astype(jnp.bfloat16)

    def close_stage(stage, chunk):
        slot = _rem(chunk, RING)
        ring_wait(stage, 1, slot)
        recv = full_bufs[stage][1]
        for color in COLORS:
            dim = ORDERS[color][stage]
            total = (source(stage, chunk, color, place[dim], every)
                     + recv[slot, color, 0].astype(jnp.float32)
                     + recv[slot, color, 1].astype(jnp.float32))
            if stage < 2:
                sums[stage + 1][_rem(chunk, sums[stage + 1].shape[0]), color] = total
            else:
                out[pair_of(chunk), _rows(color), columns(chunk)] = total

    def send_all(stage, part, chunk):
        for color in COLORS:
            for way in TWO:
                ring_copy(stage, part, _rem(chunk, RING), color, way).start()

    def open_first(chunk):
        merge_pair(chunk)
        store_halves(0, chunk)
        send_all(0, 0, chunk)

    def middle(stage, chunk):
        store_fulls(stage, chunk)
        send_all(stage, 1, chunk)

    def open_stage(stage, chunk):
        store_halves(stage, chunk)
        send_all(stage, 0, chunk)

    def turn(stage, chunk):
        close_stage(stage, chunk)
        if stage < 2:
            open_stage(stage + 1, chunk)

    return [(0, fetch), (2 * LAG, functools.partial(middle, 0)), (LAG, open_first),
            (3 * LAG, functools.partial(turn, 0)), (4 * LAG, functools.partial(middle, 1)),
            (5 * LAG, functools.partial(turn, 1)), (SIXTH * LAG, functools.partial(middle, 2)),
            (7 * LAG, functools.partial(turn, 2)), (1, consume), (0, multiply)]


def train_kernel(n_layers, x_ref, g_ref, rows_ref, down_ref, y_ref, dx_ref, rows_hbm, down_hbm, *refs):
    saved, refs = refs[:9], refs[9:]
    (rows_out, out), refs = refs[:2], refs[2:]
    (wbuf, peer, shard, twin, state, lefts, rights, q_buf, k_buf, v_buf, hid_out_buf, acc, hid_in_buf, dact, x_buf,
     dk_acc, dv_acc, away), refs = refs[:18], refs[18:]
    sums, half_bufs, full_bufs, refs = refs[:3], refs[3:9], refs[9:15], refs[15:]
    half_bufs = [half_bufs[2 * stage:2 * stage + 2] for stage in COLORS]
    full_bufs = [full_bufs[2 * stage:2 * stage + 2] for stage in COLORS]
    forward_sems, backward_sems, (swap_sem, end_sem, credit) = refs[:8], refs[8:16], refs[16:]
    torus = Torus(credit)
    core = torus.core
    n_chunks = n_layers * PER_HALF
    fill = pltpu.make_async_copy(x_ref, state, forward_sems[5].at[9])
    fill.start()
    for block in SIX:
        pltpu.make_async_copy(g_ref.at[:, COLS * block:COLS * block + COLS], rights.at[block],
                              backward_sems[0].at[3]).start()
    torus.meet()
    fill.wait()
    pltpu.make_async_copy(rights.at[:DH_AT], rights.at[:DH_AT], backward_sems[0].at[3]).wait()
    def y_copy():
        return pltpu.make_async_copy(state, y_ref, forward_sems[5].at[9])

    def x_out(result):
        y_copy().wait()
        state[ALL] = result
        pltpu.make_async_copy(state, dx_ref, forward_sems[5].at[9]).start()

    forward = forward_steps(torus, n_layers, x_ref, rows_ref, down_ref, y_ref, saved, wbuf, peer, shard, twin, state, lefts,
                            rights, q_buf, k_buf, v_buf, hid_out_buf, acc, *forward_sems)
    backward = backward_steps(torus, n_layers, x_ref, x_out, saved, out, wbuf, lefts, rights, hid_in_buf, dact, acc,
                              q_buf, k_buf, v_buf, x_buf, dk_acc, dv_acc, sums, half_bufs, full_bufs,
                              *backward_sems)
    turn_at = n_chunks
    backward = [(lag + turn_at, step) for lag, step in backward]
    n_ticks = turn_at + n_chunks + 7 * LAG
    def hand_over(layer, part):
        cols = _at(part * FIFTH, FIFTH)
        both = out[layer, :, cols]
        low, high = both[:HALF_ROWS], both[HALF_ROWS:]
        rows_out[core, layer, :, cols] = jnp.where(core == 0, low, high)
        away[layer, :, cols] = jnp.where(core == 0, high, low)
        torus.remote(away.at[layer, :, cols], rows_out.at[core, layer, :, cols], swap_sem.at[0, layer],
                     swap_sem.at[1, layer], torus.sibling).start()

    def down_result(layer):
        return pltpu.make_async_copy(out.at[layer, :, UP_END:], down_hbm.at[layer], end_sem.at[0, layer])

    def rows_result(layer):
        return pltpu.make_async_copy(rows_out.at[:, layer], rows_hbm.at[:, layer], end_sem.at[1, layer])

    def rows_meet(layer):
        swap = torus.remote(away.at[layer], rows_out.at[core, layer], swap_sem.at[0, layer], swap_sem.at[1, layer],
                            torus.sibling)
        swap.wait_send()
        swap.wait_recv()
        rows_result(layer).start()

    def hand_on(now):
        for layer in range(n_layers):
            begin = turn_at + (n_layers - layer) * PER_HALF + 8 * LAG

            @pl.when(now == begin - UP_BLOCKS)
            def _(layer=layer):
                down_result(layer).start()

            if layer > 0:
                @pl.when((now >= begin) & (now < begin + 5))
                def _(layer=layer, begin=begin):
                    hand_over(layer, now - begin)

                @pl.when(now == begin + 8)
                def _(layer=layer):
                    rows_meet(layer)

        @pl.when((now >= n_ticks - ATTN) & (now < n_ticks - ATTN + QKV))
        def _():
            hand_over(0, n_ticks - STAGES - now)

    torus.run(backward[:1] + forward + backward[1:], n_chunks, n_ticks, hand_on)
    hand_over(0, 0)
    rows_meet(0)
    for layer in range(n_layers):
        _all_done([down_result(layer), rows_result(layer)])
    pltpu.make_async_copy(state, dx_ref, forward_sems[5].at[9]).wait()


def train_stack(x_loc, g_loc, rows, down):
    n_layers = down.shape[0]
    seq, width = x_loc.shape
    bf16, f32 = jnp.bfloat16, jnp.float32
    half = WIDE
    chunk = CUBE + (ROWS, COLS)
    shape = jax.ShapeDtypeStruct
    hbm = pl.BlockSpec(memory_space=pl.ANY)
    vmem = pl.BlockSpec(memory_space=pltpu.VMEM)
    dma = pltpu.SemaphoreType.DMA
    saved = (shape((2 * n_layers - 1, seq, width), bf16), shape((n_layers,) + CUBE + (ROWS, PER_HALF * COLS), bf16),
             shape((n_layers, 3, 2, seq, width), f32), shape((n_layers, SIXTH, seq, width), bf16),
             shape((n_layers, 2, seq, width), bf16), shape((n_layers, seq, width), bf16),
             shape((n_layers, seq, 2 * HEAD), bf16), shape((n_layers, seq, 2 * HEAD), bf16),
             shape((n_layers, SIXTH, seq, COLS), bf16))
    scratch = [pltpu.VMEM(full, kind) for full, kind in (
        ((2, n_layers, HALF_ROWS, UP_END), f32), ((n_layers, ROWS, PER_HALF * COLS), f32),
        ((GATHER_SLOTS + 6,) + chunk, bf16), ((RING,) + chunk, bf16), ((n_layers, ROWS, PER_HALF * COLS), bf16),
        (rows.shape[1:], bf16), ((seq, width), bf16), ((9, seq, width), bf16), ((56, seq, COLS), bf16),
        ((seq, SIXTH * COLS), bf16), ((seq, 2 * HEAD), bf16), ((seq, 2 * HEAD), bf16), ((2, 2, seq, COLS), f32),
        ((seq, width), f32), ((seq, width), f32), ((2, seq, width), f32), ((seq, width), bf16),
        ((2, seq, HEAD), f32), ((2, seq, HEAD), f32), ((n_layers, HALF_ROWS, UP_END), f32), ((6,) + chunk, f32),
        ((5, 3, RING, RING, TILE, COLS), f32), ((5, 3, RING, TILE, COLS), f32))]
    for cols in (half, COLS):
        for size in ((RING, RING), (RING,), ()):
            scratch += [pltpu.VMEM((RING, 3, 2) + size + (TILE, cols), bf16)] * 2
    scratch += [dma((SIXTH, RING)), dma((SIXTH, RING)), dma((RING,)), dma((RING,)), dma((RING,)), dma((10,)), dma((2, 2)), dma((2, n_layers + 1))]
    scratch += [dma((10,)), dma((2,)), dma((SLOTS,)), dma((SLOTS,)), dma((RING,)), dma((RING,)), dma((SIXTH, RING)),
                dma((SIXTH, RING)), dma((2, n_layers)), dma((2, n_layers)), pltpu.SemaphoreType.REGULAR((7,))]
    return pl.pallas_call(
        functools.partial(train_kernel, n_layers), name="train_stack",
        out_shape=(shape((seq, width), bf16), shape((seq, width), bf16), shape((2, n_layers, HALF_ROWS, UP_END), f32),
                   shape(down.shape, f32)) + saved,
        in_specs=[hbm, hbm, vmem, vmem], out_specs=(hbm,) * (4 + len(saved)), scratch_shapes=scratch,
        compiler_params=pltpu.CompilerParams(collective_id=0, has_side_effects=True, vmem_limit_bytes=VMEM_LIMIT),
    )(x_loc, g_loc, rows, down)[:4]


LANES = 128


def _moves(chips, block, packed_first):
    moves = []
    for half in TWO:
        for part in COLORS:
            for chip in range(chips):
                packed = chips * ROWS * (STAGES * half + part) + ROWS * chip
                plain = block * (2 * chip + half) + ROWS * part
                pair = (packed, plain) if packed_first else (plain, packed)
                moves.append(pair + (min(ROWS, block - ROWS * part),))
    return moves


def _pieces(moves, size):
    tiles = [[] for _ in range(size // LANES)]
    for target, source, length in moves:
        while length:
            step = min(length, LANES - target % LANES, LANES - source % LANES)
            tiles[target // LANES].append((target % LANES, source // LANES, (target - source) % LANES))
            target, source, length = target + step, source + step, length - step
    return [sorted(tile) for tile in tiles]


def _gather_tile(load, tile, lane):
    total = None
    for first, source, shift in tile:
        value = load(source)
        if shift:
            value = pltpu.roll(value, shift, axis=value.ndim - 1)
        total = value if total is None else jnp.where(lane >= first, value, total)
    return total


def _span(index, size):
    return slice(size * index, size * index + size)


def _moved(pairs, sems):
    copies = [pltpu.make_async_copy(source, target, sems.at[order]) for order, (source, target) in enumerate(pairs)]
    for copy in copies:
        copy.start()
    return copies


def _all_done(copies):
    for copy in copies:
        copy.wait()


def _head_spots(heads):
    return [[(head, 0, heads * half + head) for head in range(heads)]
            + [(heads + 2 + head, 3, heads * half + head) for head in range(heads)] for half in TWO]


def pack_kernel(chips, *refs):
    sources, (rows_hbm, down_hbm), arrays, refs = refs[:6], refs[6:8], refs[8:14], refs[14:]
    rows_out, down_out, wide, in_sems, out_sems = refs
    k_ref, v_ref, up_ref, down_ref = arrays[1], arrays[2], arrays[4], arrays[5]
    rows, layers, _ = up_ref.shape
    block, _, width = down_ref.shape
    heads = arrays[0].shape[1] // 2
    half_f = STAGES * chips * ROWS
    inward = _moved(zip(sources, arrays), in_sems)
    _all_done(inward[:QKV])
    for half, spots in enumerate(_head_spots(heads)):
        for at, which, head in spots:
            rows_out[half, :, :, _span(at, LANES)] = jnp.swapaxes(
                arrays[which][:, head].astype(jnp.float32), 0, 1).astype(jnp.bfloat16)
        for layer in range(layers):
            for at, ref in ((heads, k_ref), (heads + 1, v_ref)):
                rows_out[half, layer, :, _span(at, LANES)] = ref[layer].astype(
                    jnp.float32)[:, half].astype(jnp.bfloat16)
    inward[QKV].wait()
    wide[ALL] = jnp.swapaxes(up_ref[ALL].astype(jnp.float32), 0, 1)
    lane = lax.broadcasted_iota(jnp.int32, (layers, rows, LANES), 2)
    tiles = _pieces(_moves(chips, block, True), 2 * half_f)
    outward = []
    for half in TWO:
        for index in range(half_f // LANES):
            tile = tiles[half * (half_f // LANES) + index]
            value = _gather_tile(lambda source: wide[:, :, _span(source, LANES)], tile, lane)
            if LANES * index >= 2 * chips * ROWS:
                position = lax.rem(lane + LANES * index % ROWS, ROWS)
                value = jnp.where(position < block - 2 * ROWS, value, 0.0)
            rows_out[half, :, :, _span(2 * ATTN + index, LANES)] = value.astype(jnp.bfloat16)
        outward += _moved([(rows_out.at[half], rows_hbm.at[half])], out_sems.at[half:half + 1])
    inward[5].wait()
    for part in COLORS:
        used = min(ROWS, block - ROWS * part)
        both = jnp.swapaxes(down_ref[ROWS * part:ROWS * part + used].astype(jnp.float32), 0, 1)
        for layer in range(layers):
            one = both[layer]
            if used < ROWS:
                one = jnp.concatenate([one, jnp.zeros((ROWS - used, width), jnp.float32)], axis=0)
            down_out[layer, :, _span(part, width)] = one.astype(jnp.bfloat16)
    _all_done(outward + _moved([(down_out, down_hbm)], out_sems.at[2:3]))


def _bounced(kernel, name, inputs, outs, arrays, n_sems):
    hbm = pl.BlockSpec(memory_space=pl.ANY)
    scratch = [pltpu.VMEM(array.shape, array.dtype) for array in arrays]
    return pl.pallas_call(
        kernel, name=name, out_shape=tuple(outs), in_specs=[hbm] * len(inputs), out_specs=(hbm,) * len(outs),
        scratch_shapes=scratch + [pltpu.SemaphoreType.DMA((size,)) for size in n_sems],
        compiler_params=pltpu.CompilerParams(vmem_limit_bytes=VMEM_LIMIT))(*inputs)


def pack_weights(w_q, w_k, w_v, w_o, w_up, w_down, chips):
    layers, rows = w_up.shape[:2]
    shape = jax.ShapeDtypeStruct
    inputs = [w_q.transpose(1, 2, 0, 3), w_k, w_v, w_o.transpose(1, 2, 0, 3), w_up.transpose(1, 0, 2),
              w_down.transpose(1, 0, 2)]
    outs = [shape((2, layers, rows, UP_END), jnp.bfloat16), shape((layers, ROWS, 3 * w_down.shape[2]), jnp.bfloat16)]
    return _bounced(functools.partial(pack_kernel, chips), "pack_weights", inputs, outs,
                    inputs + outs + [shape(w_up.shape, jnp.float32)], (6, 3))


def unpack_kernel(chips, *refs):
    sources, results, arrays, (in_sems, out_sems) = refs[:4], refs[4:12], refs[12:22], refs[22:]
    rows_ref, down_ref, q_out, k_out, v_out, o_out, up_out, down_out = arrays[:2] + arrays[4:]
    rows, layers, cols = up_out.shape
    block, _, width = down_out.shape
    heads = q_out.shape[1] // 2
    order = (1, 0, 2, 3)
    inward = _moved([(sources[which], arrays[which]) for which in order], in_sems)
    inward[0].wait()
    for part in COLORS:
        used = min(ROWS, block - ROWS * part)
        for layer in range(layers):
            down_out[ROWS * part:ROWS * part + used, layer, :] = down_ref[layer, :used, _span(part, width)]
    inward[1].wait()
    outward = _moved([(down_out, results[5])], out_sems)
    lane = lax.broadcasted_iota(jnp.int32, (layers, rows, LANES), 2)
    per_half = STAGES * chips * ROWS // LANES

    def load(source):
        half, tile = divmod(source, per_half)
        return rows_ref[half, :, :, _span(2 * ATTN + tile, LANES)]

    _all_done(inward[2:])
    outward += _moved(zip(arrays[2:4], results[6:]), out_sems.at[1:])
    for index, tile in enumerate(_pieces(_moves(chips, block, False), cols)):
        up_out[:, :, _span(index, LANES)] = jnp.swapaxes(_gather_tile(load, tile, lane), 0, 1)
    outward += _moved([(up_out, results[4])], out_sems.at[STAGES:])
    for half, spots in enumerate(_head_spots(heads)):
        for at, which, head in spots:
            (q_out, o_out)[which // 3][:, head] = jnp.swapaxes(rows_ref[half, :, :, _span(at, LANES)], 0, 1)
        for layer in range(layers):
            for at, ref in ((heads, k_out), (heads + 1, v_out)):
                ref[layer, :, half, :] = rows_ref[half, layer, :, _span(at, LANES)]
    _all_done(outward + _moved(zip((q_out, k_out, v_out, o_out), results), out_sems.at[QKV:]))


def unpack_grads(row_grad, down_grad, y_loc, grad_x, shapes, chips):
    q_shape, k_shape, _, _, up_shape, down_shape = shapes
    layers, rows, heads, head_dim = q_shape
    shape = jax.ShapeDtypeStruct
    turned = [(rows, heads, layers, head_dim), k_shape, k_shape, (rows, heads, layers, head_dim),
              (rows, layers, up_shape[2]), (down_shape[1], layers, down_shape[2])]
    turned = [shape(full, jnp.float32) for full in turned]
    inputs = [row_grad, down_grad, y_loc, grad_x]
    outs = _bounced(functools.partial(unpack_kernel, chips), "unpack_grads", inputs,
                    turned + [shape(value.shape, value.dtype) for value in (y_loc, grad_x)], inputs + turned, (4, 8))
    d_q, d_k, d_v, d_o, d_up, d_down, y_out, dx_out = outs
    return (y_out[None], dx_out[None], d_q.transpose(2, 0, 1, 3), d_k, d_v, d_o.transpose(2, 0, 1, 3),
            d_up.transpose(1, 0, 2), d_down.transpose(1, 0, 2))


def solution(mesh):
    mesh4 = Mesh(mesh.devices.reshape(CUBE + (2,)), ALL_AXES)
    row_spec = P(ALL_AXES)
    weight_spec = P(None, ALL_AXES)

    def body(x_in, w_q, w_k, w_v, w_o, w_up, w_down, grad_out):
        weights = (w_q, w_k, w_v, w_o, w_up, w_down)
        chips = w_up.shape[2] // w_down.shape[1] // 2
        rows, down = pack_weights(*weights, chips)
        y_loc, grad_x, row_grad, down_grad = train_stack(x_in[0], grad_out[0], rows, down)
        return unpack_grads(row_grad, down_grad, y_loc, grad_x, [weight.shape for weight in weights], chips)

    return jax.shard_map(body, mesh=mesh4, in_specs=(row_spec,) + (weight_spec,) * 6 + (row_spec,),
                         out_specs=(row_spec, row_spec) + (weight_spec,) * 6, check_vma=False)
```

```python
import functools

import jax
import jax.numpy as jnp
from jax import lax
from jax.experimental import pallas as pl
from jax.experimental.pallas import tpu as pltpu
from jax.sharding import Mesh, PartitionSpec as P

MESH = pl.DeviceIdType.MESH
ALL_AXES = ("z", "y", "x", "c")
EPS = 1e-6
MASK_FILL = -1e30
DIMS = ("z", "y", "x")
ORDERS = (("x", "y", "z"), ("y", "z", "x"), ("z", "x", "y"))
COLS = 256
ROWS = 24
LAG = 2
WIDE = COLS // 2
HALF_ROWS = ROWS // 2
HEAD = 128
PER_HALF = 43
UP_BLOCKS = 25
UP_END = UP_BLOCKS * COLS
RING = 4
STAGES = 3
FINAL = STAGES - 1
CUBE = (RING, RING, RING)
CHIPS = RING ** STAGES
SLOTS = 3
TILE = 8
COLORS = range(3)
TWO = range(2)
SIX = range(6)
ALL = Ellipsis
EVERY = slice(None)
QKV, ATTN, FF = 4, 7, 18
DOWN_DONE = FF
UP_DONE = DOWN_DONE + FF
O_DONE = UP_DONE + ATTN - QKV
SIXTH = 6
DH_AT = SIXTH
O_AT = DH_AT + UP_DONE
QKV_AT = O_AT + SIXTH
NORM_MLP, GRAD, NORM_ATTN = 6, 7, 8
VMEM_LIMIT = 67043328


FIFTH = UP_END // 5
GELU_A = 0.7978845608028654
GELU_B = GELU_A * 0.044715
GELU_C = 0.5 * GELU_A
GELU_D = 1.5 * GELU_B
GATHER_SLOTS = SIXTH * LAG + RING


def _rows(color):
    return slice(TILE * color, TILE * color + TILE)


def _rem(value, by):
    return lax.rem(value, by)


def _block(color, stage, position):
    dims = tuple(dim for dim in DIMS if dim not in ORDERS[color][:stage])
    return tuple(position if dim == ORDERS[color][stage] else EVERY for dim in dims)


def _dot(left, right):
    return jnp.dot(left, right, preferred_element_type=jnp.float32)


def _dot_rhs_t(left, right):
    return lax.dot_general(left, right, (((1,), (1,)), ((), ())), preferred_element_type=jnp.float32)


def _dot_lhs_t(left, right):
    return lax.dot_general(left, right, (((0,), (0,)), ((), ())), preferred_element_type=jnp.float32)


def _at(start, size):
    return pl.ds(pl.multiple_of(start, size), size)


def _causal(seq):
    return (lax.rem(lax.broadcasted_iota(jnp.int32, (2 * seq, seq), 0), seq)
            >= lax.broadcasted_iota(jnp.int32, (2 * seq, seq), 1))


def _under(block):
    return jnp.concatenate([block[:, :HEAD], block[:, HEAD:]], axis=0)


def _beside(stacked):
    seq = stacked.shape[0] // 2
    return jnp.concatenate([stacked[:seq], stacked[seq:]], axis=1)


def _probs(query, key, causal):
    scores = jnp.where(causal, _dot_rhs_t(query, key) * (HEAD ** -0.5), MASK_FILL)
    weight = jnp.exp(scores - jnp.max(scores, axis=-1, keepdims=True))
    return weight / jnp.sum(weight, axis=-1, keepdims=True)


def _rms(values):
    wide = values.astype(jnp.float32)
    return (wide * lax.rsqrt(jnp.mean(wide * wide, axis=-1, keepdims=True) + EPS)).astype(jnp.bfloat16)


def _rms_back(values, grad):
    wide = values.astype(jnp.float32)
    scale = lax.rsqrt(jnp.mean(wide * wide, axis=-1, keepdims=True) + EPS)
    return scale * grad - wide * (scale * scale * scale) * jnp.mean(wide * grad, axis=-1, keepdims=True)


class Torus:
    def __init__(self, credit):
        self.core = lax.axis_index("c")
        self.place = {dim: lax.axis_index(dim) for dim in DIMS}
        self.near = tuple({dim: _rem(self.place[dim] + step, RING) for dim in DIMS} for step in (1, 3))
        self.far = {dim: _rem(self.place[dim] + 2, RING) for dim in DIMS}
        self.sibling = {"c": 1 - self.core}
        self.sides = ((0, self.core), (1, 1 - self.core))
        self.credit = credit
        self.partners = [({dim: self.near[way][dim]}, 2 * d + 1 - way, 2 * d + way)
                         for d, dim in enumerate(DIMS) for way in TWO]
        self.partners.append((self.sibling, 6, 6))

    def meet(self):
        barrier = pltpu.get_barrier_semaphore()
        for device, _, _ in self.partners:
            pl.semaphore_signal(barrier, inc=1, device_id=device, device_id_type=MESH)
        pl.semaphore_wait(barrier, len(self.partners))

    def remote(self, source, target, send_sem, recv_sem, device):
        return pltpu.make_async_remote_copy(src_ref=source, dst_ref=target, send_sem=send_sem, recv_sem=recv_sem,
                                            device_id=device, device_id_type=MESH)

    def run(self, steps, n_chunks, n_ticks, after):
        def tick(now, carry):
            @pl.when(now >= 2)
            def _():
                for _, _, mine in self.partners:
                    pl.semaphore_wait(self.credit.at[mine], 1)

            for lag, action in steps:
                @pl.when((now >= lag) & (now < lag + n_chunks))
                def _(lag=lag, action=action):
                    action(now - lag)
            after(now)

            @pl.when(now < n_ticks - 2)
            def _():
                for device, theirs, _ in self.partners:
                    pl.semaphore_signal(self.credit.at[theirs], inc=1, device_id=device, device_id_type=MESH)
            return carry

        lax.fori_loop(0, n_ticks, tick, 0)


def forward_steps(torus, n_layers, x_ref, rows_ref, down_ref, y_ref, saved, wbuf, peer, shard, twin, state, lefts, rights,
                  q_buf, k_buf, v_buf, hid_buf, acc, ring_send, ring_recv, pair_send, pair_recv, keep_sem, save_sem,
                  hid_sem, twin_sem):
    acts, w_out, hid_out, gelu_out, norm_out, q_out, k_out, v_out, o_out = saved
    core, place, near = torus.core, torus.place, torus.near
    slots = GATHER_SLOTS
    n_chunks = n_layers * PER_HALF
    ready = SIXTH * LAG
    seq = state.shape[0]
    third = CHIPS * ROWS
    last = n_layers - 1
    pieces = [(0, EVERY, slice(0, FIFTH)), (0, EVERY, slice(FIFTH, None))] + [
        (layer, EVERY, EVERY) for layer in range(1, n_layers)]
    swaps = [torus.remote(rows_ref.at[(1 - core,) + piece], twin.at[piece], twin_sem.at[0, order], twin_sem.at[1, order],
                          torus.sibling) for order, piece in enumerate(pieces)]
    for swap in swaps:
        swap.start()
    swaps[0].wait_send()
    swaps[0].wait_recv()

    def assemble(chunk):
        @pl.when(chunk == 1)
        def _():
            for swap in swaps[1:]:
                swap.wait_send()
                swap.wait_recv()

        @pl.when(chunk < 5 * n_layers)
        def _():
            layer, part = chunk // 5, _rem(chunk, 5)
            cols = _at(part * FIFTH, FIFTH)
            mine, other = [ref[layer, :, cols].astype(jnp.float32) for ref in (rows_ref.at[core], twin)]
            shard[layer, :, cols] = jnp.concatenate(
                [jnp.where(core == 0, mine, other), jnp.where(core == 0, other, mine)], axis=0).astype(jnp.bfloat16)

            @pl.when(part == 4)
            def _():
                shard[layer, :, UP_END:] = down_ref[layer]

    def columns(chunk):
        return _at(_rem(chunk, PER_HALF) * COLS, COLS)

    def spot(slot, color, stage, position, cols):
        order = ORDERS[color]
        index = tuple(EVERY if dim in order[:stage] else position if dim == order[stage] else place[dim]
                      for dim in DIMS)
        return wbuf.at[(slot,) + index + (_rows(color), cols)]

    halves = (slice(0, WIDE), slice(WIDE, COLS))

    def send_own(stage, chunk):
        slot, sem = _rem(chunk, slots), _rem(chunk, RING)
        for color in COLORS:
            dim = ORDERS[color][stage]
            here = spot(slot, color, stage, place[dim], slice(0, COLS))
            source = here
            if stage == 0:
                source = shard.at[chunk // PER_HALF, _rows(color), columns(chunk)]
            for way in TWO:
                torus.remote(source, here, ring_send.at[2 * stage, sem], ring_recv.at[2 * stage, sem],
                             {dim: near[way][dim]}).start()

    def send_far(stage, chunk):
        slot, sem = _rem(chunk, slots), _rem(chunk, RING)
        for color in COLORS:
            dim = ORDERS[color][stage]
            for way in TWO:
                block = spot(slot, color, stage, near[1 - way][dim], halves[way])
                torus.remote(block, block, ring_send.at[2 * stage + 1, sem], ring_recv.at[2 * stage + 1, sem],
                             {dim: near[way][dim]}).start()

    def arrived(part, chunk):
        slot, sem = _rem(chunk, slots), _rem(chunk, RING)
        count = slice(0, 2) if part % 2 == 0 else 0
        block = wbuf.at[(slot,) + (0,) * (2 - part // 2) + (count,)]
        whole = torus.remote(block, block, ring_send.at[part, sem], ring_recv.at[part, sem], torus.sibling)
        whole.wait_send()
        whole.wait_recv()

    def enter(chunk):
        wbuf[_rem(chunk, slots), place["z"], place["y"], place["x"]] = shard[chunk // PER_HALF, :, columns(chunk)]
        send_own(0, chunk)

    def pass_on(part, chunk):
        arrived(part, chunk)
        if part % 2 == 0:
            send_far(part // 2, chunk)
        else:
            send_own(part // 2 + 1, chunk)

    def pair_copy(chunk):
        slot = _rem(chunk, RING)
        return torus.remote(wbuf.at[_rem(chunk, slots)], peer.at[slot], pair_send.at[slot], pair_recv.at[slot],
                            torus.sibling)

    def exchange(chunk):
        arrived(5, chunk)
        pair_copy(chunk).start()

    def keep_copy(chunk):
        return pltpu.make_async_copy(wbuf.at[_rem(chunk, slots)],
                                     w_out.at[chunk // PER_HALF, :, :, :, :, columns(chunk)],
                                     keep_sem.at[_rem(chunk, RING)])

    def save_copies(layer, names):
        parts = {"n0": (lefts.at[NORM_ATTN], norm_out.at[layer, 0]), "n1": (lefts.at[NORM_MLP], norm_out.at[layer, 1]),
                 "q": (q_buf, q_out.at[layer]), "k": (k_buf, k_out.at[layer]), "v": (v_buf, v_out.at[layer]),
                 "o": (rights.at[O_AT:QKV_AT], o_out.at[layer]), "a": (lefts.at[:NORM_MLP], gelu_out.at[layer]),
                 "mid": (state, acts.at[2 * layer]), "end": (state, acts.at[2 * layer + 1])}
        places = list(parts)
        return [pltpu.make_async_copy(*parts[name], save_sem.at[places.index(name)]) for name in names]

    def save(layer, names):
        @pl.when(layer < last)
        def _():
            for copy in save_copies(layer, names):
                copy.start()

    def saved_all(layer, names):
        @pl.when(layer < last)
        def _():
            for copy in save_copies(layer, names):
                copy.wait()

    def hidden_copies(layer, order):
        slot, part, at = _rem(order, 2), order // SIXTH, _at(_rem(order, SIXTH) * COLS, COLS)
        return [pltpu.make_async_copy(hid_buf.at[slot, half], hid_out.at[layer, part, half, :, at],
                                      hid_sem.at[slot, half]) for half in TWO]

    def compute(chunk):
        layer, index = chunk // PER_HALF, _rem(chunk, PER_HALF)
        pair = pair_copy(chunk)
        pair.wait_send()
        pair.wait_recv()
        keep_copy(chunk).start()

        def weights(role):
            block = wbuf[_rem(chunk, slots)] if role == 0 else peer[_rem(chunk, RING)]
            return block.reshape(third, COLS)

        @pl.when(index == 0)
        def _():
            lefts[NORM_ATTN] = _rms(state[ALL])
            save(layer, ["n0"])

        @pl.when(index < 3)
        def _():
            for role, half in torus.sides:
                q_buf[:, _at(STAGES * COLS * half + COLS * index, COLS)] = _dot(
                    lefts[NORM_ATTN], weights(role)).astype(jnp.bfloat16)

        @pl.when(index == 3)
        def _():
            for role, half in torus.sides:
                both = _dot(lefts[NORM_ATTN], weights(role)).astype(jnp.bfloat16)
                k_buf[:, _at(HEAD * half, HEAD)] = both[:, :HEAD]
                v_buf[:, _at(HEAD * half, HEAD)] = both[:, HEAD:]

        @pl.when(index == QKV)
        def _():
            acc[ALL] = jnp.zeros_like(acc)
            save(layer, ["q", "k", "v"])

        @pl.when((index >= QKV) & (index < ATTN))
        def _():
            causal = _causal(seq)
            queries = [_under(q_buf[:, _at(STAGES * COLS * half + COLS * (index - QKV), COLS)]) for _, half in torus.sides]
            probs = [_probs(queries[role], k_buf[:, _at(HEAD * half, HEAD)], causal).astype(jnp.bfloat16)
                     for role, half in torus.sides]
            blocks = [_beside(_dot(probs[role], v_buf[:, _at(HEAD * half, HEAD)]).astype(jnp.bfloat16))
                      for role, half in torus.sides]
            acc[ALL] += sum(_dot_rhs_t(blocks[role], weights(role)) for role in TWO)
            for role, half in torus.sides:
                rights[O_AT + STAGES * half + index - QKV] = blocks[role]

        @pl.when(index == ATTN - 1)
        def _():
            @pl.when(layer > 0)
            def _():
                saved_all(layer - 1, ["end"])
            middle = (state[ALL].astype(jnp.float32) + acc[ALL]).astype(jnp.bfloat16)
            state[ALL] = middle
            lefts[NORM_MLP] = _rms(middle)
            save(layer, ["n1", "o"])
            mid = save_copies(layer, ["mid"])[0]
            mid.start()

        @pl.when((index > ATTN) & (index <= UP_BLOCKS))
        def _():
            for copy in hidden_copies(layer, index - ATTN - 1):
                copy.wait()

        @pl.when((index >= ATTN) & (index < UP_BLOCKS))
        def _():
            order = index - ATTN
            for role, half in torus.sides:
                hidden = _dot(lefts[NORM_MLP], weights(role))
                hid_buf[_rem(order, 2), half] = hidden
                lefts[STAGES * half + order // SIXTH, :, _at(COLS * _rem(order, SIXTH), COLS)] = jax.nn.gelu(
                    hidden).astype(jnp.bfloat16)
            for copy in hidden_copies(layer, order):
                copy.start()

        @pl.when(index == UP_BLOCKS)
        def _():
            save(layer, ["a"])
            save_copies(layer, ["mid"])[0].wait()

        @pl.when(index >= UP_BLOCKS)
        def _():
            part, at = (index - UP_BLOCKS) // SIXTH, _at(COLS * _rem(index - UP_BLOCKS, SIXTH), COLS)
            total = sum(_dot(lefts[STAGES * half + part], weights(role)) for role, half in torus.sides)

            @pl.when(part == 0)
            def _():
                acc[:, at] = total

            @pl.when(part > 0)
            def _():
                acc[:, at] += total

        @pl.when(index == PER_HALF - 1)
        def _():
            saved_all(layer, ["n0", "n1", "q", "k", "v", "o", "a"])
            result = (state[ALL].astype(jnp.float32) + acc[ALL]).astype(jnp.bfloat16)
            state[ALL] = result
            save(layer, ["end"])

            @pl.when(layer == last)
            def _():
                pltpu.make_async_copy(state, y_ref, save_sem.at[9]).start()

        keep_copy(chunk).wait()

    steps = [(0, assemble), (0, enter)]
    steps += [((part + 1) * LAG, functools.partial(pass_on, part)) for part in range(5)]
    return steps + [(ready, exchange), (ready + 1, compute)]


def backward_steps(torus, n_layers, x_ref, x_out, saved, out, wbuf, lefts, rights, hid_buf, dact, dnorm, q_buf,
                   k_buf, v_buf, x_buf, dk_acc, dv_acc, sums, half_bufs, full_bufs, load_sem, own_sem, push_send,
                   push_recv, pair_send, pair_recv, ring_send, ring_recv):
    acts, w_own, hid_in, gelu_in, norm_in, q_in, k_in, v_in, o_in = saved
    place, near = torus.place, torus.near
    seq = k_buf.shape[0]
    third = CHIPS * ROWS
    last = n_layers - 1

    def mine_slot(chunk):
        return GATHER_SLOTS + _rem(chunk, 2)

    def out_slot(chunk):
        return GATHER_SLOTS + 2 + _rem(chunk, 2)

    def their_slot(chunk):
        return 7 + _rem(chunk, SLOTS)

    def peer_slot(chunk):
        order = _rem(chunk, RING)
        return jnp.where(order == 0, 6, jnp.where(order == 3, 10, GATHER_SLOTS + 3 + order))

    def pair_of(chunk):
        return last - chunk // PER_HALF

    def columns(chunk):
        index = _rem(chunk, PER_HALF)
        block = jnp.where(index < DOWN_DONE, UP_BLOCKS + index,
                          jnp.where(index < UP_DONE, index - 11, jnp.where(index < O_DONE, index - 32, index - 39)))
        return _at(block * COLS, COLS)

    def loads(pair, names):
        parts = {"a": (gelu_in.at[pair], lefts.at[:NORM_MLP]), "n_mlp": (norm_in.at[pair, 1], lefts.at[NORM_MLP]),
                 "n_attn": (norm_in.at[pair, 0], lefts.at[NORM_ATTN]), "o": (o_in.at[pair], rights.at[O_AT:QKV_AT]),
                 "q": (q_in.at[pair], q_buf), "k": (k_in.at[pair], k_buf), "v": (v_in.at[pair], v_buf),
                 "x_mid": (acts.at[2 * pair], x_buf)}
        places = list(parts)
        return [pltpu.make_async_copy(*parts[name], load_sem.at[places.index(name)]) for name in names]

    def start(pair, names):
        for copy in loads(pair, names):
            copy.start()

    def finish(pair, names):
        for copy in loads(pair, names):
            copy.wait()

    def first_input(ref):
        return pltpu.make_async_copy(ref, x_buf, load_sem.at[9])

    def hidden_load(pair, part, half):
        return pltpu.make_async_copy(hid_in.at[pair, part, half], hid_buf, load_sem.at[8])

    def own_copy(chunk):
        return pltpu.make_async_copy(w_own.at[pair_of(chunk), :, :, :, :, columns(chunk)], wbuf.at[mine_slot(chunk)],
                                     own_sem.at[_rem(chunk, 2)])

    def push_copy(chunk):
        slot = _rem(chunk, SLOTS)
        return torus.remote(w_own.at[pair_of(chunk), :, :, :, :, columns(chunk)], wbuf.at[their_slot(chunk)],
                            push_send.at[slot], push_recv.at[slot], torus.sibling)

    def fetch(chunk):
        own_copy(chunk).start()
        push_copy(chunk).start()

    def total_grad():
        return jnp.concatenate([rights[block] for block in SIX], axis=1).astype(jnp.float32)

    def consume(chunk):
        pair, index = pair_of(chunk), _rem(chunk, PER_HALF)
        own_copy(chunk).wait()
        push = push_copy(chunk)
        push.wait_send()
        push.wait_recv()

        def weights(role):
            return wbuf[(mine_slot, their_slot)[role](chunk)].reshape(third, COLS)

        @pl.when(index == 0)
        def _():
            start(pair, ["x_mid"])

            @pl.when(pair < last)
            def _():
                start(pair, ["n_mlp", "n_attn", "o", "q", "k", "v"])

        def bend_back(part, half):
            hidden_load(pair, part, half).wait()
            for block in SIX:
                cols = slice(COLS * block, COLS * block + COLS)
                hidden = hid_buf[:, cols]
                square = hidden * hidden
                bend = jnp.tanh(hidden * (GELU_A + GELU_B * square))
                slope = (0.5 + 0.5 * bend) + (hidden * (1.0 - bend * bend)) * (GELU_C + GELU_D * square)
                rights[DH_AT + FF * half + SIXTH * part + block] = (dact[half, :, cols] * slope).astype(jnp.bfloat16)

        @pl.when((index > 0) & (index <= DOWN_DONE) & (_rem(index, SIXTH) == 0))
        def _():
            bend_back(index // SIXTH - 1, 1)

        @pl.when((index < DOWN_DONE) & (_rem(index, SIXTH) == 0))
        def _():
            dact[ALL] = jnp.zeros_like(dact)
            hidden_load(pair, index // SIXTH, 0).start()

        @pl.when(index < DOWN_DONE)
        def _():
            products = [_dot_rhs_t(rights[_rem(index, SIXTH)], weights(role)) for role in TWO]
            for role, half in torus.sides:
                dact[half] += products[role]

        @pl.when((index < DOWN_DONE) & (_rem(index, SIXTH) == 5))
        def _():
            bend_back(index // SIXTH, 0)
            hidden_load(pair, index // SIXTH, 1).start()

        @pl.when(index == DOWN_DONE - 1)
        def _():
            @pl.when(pair < last)
            def _():
                finish(pair, ["n_mlp", "n_attn", "o", "q", "k", "v"])

        @pl.when(index == DOWN_DONE)
        def _():
            dnorm[ALL] = jnp.zeros_like(dnorm)

            @pl.when(pair > 0)
            def _():
                start(pair - 1, ["a"])

        @pl.when((index >= DOWN_DONE) & (index < UP_DONE))
        def _():
            dnorm[ALL] += sum(_dot_rhs_t(rights[DH_AT + FF * half + index - DOWN_DONE], weights(role))
                              for role, half in torus.sides)

        @pl.when(index == UP_DONE - 1)
        def _():
            finish(pair, ["x_mid"])
            lefts[GRAD] = (total_grad() + _rms_back(x_buf[ALL], dnorm[ALL])).astype(jnp.bfloat16)

        @pl.when(index == UP_DONE)
        def _():
            @pl.when(pair == 0)
            def _():
                first_input(x_ref).start()

            @pl.when(pair > 0)
            def _():
                first_input(acts.at[2 * pair - 1]).start()
            dk_acc[ALL] = jnp.zeros_like(dk_acc)
            dv_acc[ALL] = jnp.zeros_like(dv_acc)

        @pl.when((index >= UP_DONE) & (index < O_DONE))
        def _():
            causal = _causal(seq)
            keys = [k_buf[:, _at(HEAD * half, HEAD)] for _, half in torus.sides]
            values = [v_buf[:, _at(HEAD * half, HEAD)] for _, half in torus.sides]
            queries = [_under(q_buf[:, _at(STAGES * COLS * half + COLS * (index - UP_DONE), COLS)])
                       for _, half in torus.sides]
            probs = [_probs(queries[role], keys[role], causal) for role in TWO]
            d_heads = [_under(_dot(lefts[GRAD], weights(role)).astype(jnp.bfloat16)) for role in TWO]
            d_probs = [_dot_rhs_t(d_heads[role], values[role]) for role in TWO]
            d_scores = [probs[role] * (d_probs[role] - jnp.sum(probs[role] * d_probs[role], axis=-1, keepdims=True))
                        for role in TWO]
            d_scores = [(d_score * (HEAD ** -0.5)).astype(jnp.bfloat16) for d_score in d_scores]
            d_v = [_dot_lhs_t(probs[role].astype(jnp.bfloat16), d_heads[role]) for role in TWO]
            d_k = [_dot_lhs_t(d_scores[role], queries[role]) for role in TWO]
            d_q = [_beside(_dot(d_scores[role], keys[role]).astype(jnp.bfloat16)) for role in TWO]
            for role, half in torus.sides:
                dv_acc[half] += d_v[role]
                dk_acc[half] += d_k[role]
                rights[QKV_AT + QKV * half + index - UP_DONE] = d_q[role]

        @pl.when(index == O_DONE - 1)
        def _():
            for half in TWO:
                rights[QKV_AT + QKV * half + QKV - 1] = jnp.concatenate([dk_acc[half], dv_acc[half]], axis=1).astype(jnp.bfloat16)

        @pl.when(index == O_DONE)
        def _():
            dnorm[ALL] = jnp.zeros_like(dnorm)

        @pl.when(index >= O_DONE)
        def _():
            dnorm[ALL] += sum(_dot_rhs_t(rights[QKV_AT + QKV * half + index - O_DONE], weights(role))
                              for role, half in torus.sides)

        @pl.when(index == PER_HALF - 1)
        def _():
            first_input(x_ref).wait()

            @pl.when(pair > 0)
            def _():
                finish(pair - 1, ["a"])
            result = (lefts[GRAD].astype(jnp.float32) + _rms_back(x_buf[ALL], dnorm[ALL])).astype(jnp.bfloat16)

            @pl.when(pair == 0)
            def _():
                x_out(result)
            for block in SIX:
                rights[block] = result[:, COLS * block:COLS * block + COLS]

    def pair_copy(chunk):
        slot = _rem(chunk, RING)
        return torus.remote(wbuf.at[out_slot(chunk)], wbuf.at[peer_slot(chunk)], pair_send.at[slot], pair_recv.at[slot],
                            torus.sibling)

    def multiply(chunk):
        index = _rem(chunk, PER_HALF)
        lead = _rem(chunk, sums[0].shape[0])
        quarter = third // RING
        for role, half in torus.sides[::-1]:
            left = jnp.where(index < DOWN_DONE, STAGES * half + index // SIXTH,
                             jnp.where(index < UP_DONE, NORM_MLP, jnp.where(index < O_DONE, GRAD, NORM_ATTN)))
            right = jnp.where(index < DOWN_DONE, _rem(index, SIXTH),
                              jnp.where(index < UP_DONE, DH_AT + FF * half + index - DOWN_DONE,
                                        jnp.where(index < O_DONE, O_AT + STAGES * half + index - UP_DONE,
                                                  QKV_AT + QKV * half + index - O_DONE)))
            for z in range(RING):
                part = _dot_lhs_t(lefts[left, :, quarter * z:quarter * z + quarter], rights[right])
                if role == 0:
                    sums[0][lead, z] = part.reshape(RING, RING, ROWS, COLS)
                else:
                    wbuf[out_slot(chunk), z] = part.astype(jnp.bfloat16).reshape(RING, RING, ROWS, COLS)
        pair_copy(chunk).start()

    def merge_pair(chunk):
        lead = _rem(chunk, sums[0].shape[0])
        pair_copy(chunk).wait_send()
        pair_copy(chunk).wait_recv()
        for z in range(RING):
            for y in range(RING):
                sums[0][lead, z, y] = sums[0][lead, z, y] + wbuf[peer_slot(chunk), z, y].astype(jnp.float32)

    def ring_copy(stage, part, slot, color, way):
        send, recv = (half_bufs, full_bufs)[part][stage]
        dim = ORDERS[color][stage]
        return torus.remote(send.at[slot, color, way], recv.at[slot, color, way],
                            ring_send.at[2 * stage + part, slot], ring_recv.at[2 * stage + part, slot],
                            {dim: near[way][dim]})

    def ring_wait(stage, part, slot):
        send, recv = (half_bufs, full_bufs)[part][stage]
        whole = torus.remote(send.at[slot], recv.at[slot], ring_send.at[2 * stage + part, slot],
                             ring_recv.at[2 * stage + part, slot], torus.sibling)
        whole.wait_send()
        whole.wait_recv()

    def source(stage, chunk, color, position, cols):
        lead = _rem(chunk, sums[stage].shape[0])
        if stage == 0:
            return sums[0][(lead,) + _block(color, 0, position) + (_rows(color), cols)]
        return sums[stage][(lead, color) + _block(color, stage, position) + (EVERY, cols)]

    left_cols, right_cols, every = slice(0, WIDE), slice(WIDE, COLS), slice(0, COLS)

    def store_halves(stage, chunk):
        slot = _rem(chunk, RING)
        send = half_bufs[stage][0]
        for color in COLORS:
            far = torus.far[ORDERS[color][stage]]
            send[slot, color, 0] = source(stage, chunk, color, far, left_cols).astype(jnp.bfloat16)
            send[slot, color, 1] = source(stage, chunk, color, far, right_cols).astype(jnp.bfloat16)

    def store_fulls(stage, chunk):
        slot = _rem(chunk, RING)
        ring_wait(stage, 0, slot)
        recv = half_bufs[stage][1]
        send = full_bufs[stage][0]
        lead = (EVERY,) * (len(send.shape) - 4)
        for color in COLORS:
            dim = ORDERS[color][stage]
            for way, summed, plain in ((0, left_cols, right_cols), (1, right_cols, left_cols)):
                send[(slot, color, way) + lead + (summed,)] = (
                    source(stage, chunk, color, near[way][dim], summed)
                    + recv[slot, color, way].astype(jnp.float32)).astype(jnp.bfloat16)
                send[(slot, color, way) + lead + (plain,)] = source(
                    stage, chunk, color, near[way][dim], plain).astype(jnp.bfloat16)

    def close_stage(stage, chunk):
        slot = _rem(chunk, RING)
        ring_wait(stage, 1, slot)
        recv = full_bufs[stage][1]
        for color in COLORS:
            dim = ORDERS[color][stage]
            total = (source(stage, chunk, color, place[dim], every)
                     + recv[slot, color, 0].astype(jnp.float32)
                     + recv[slot, color, 1].astype(jnp.float32))
            if stage < 2:
                sums[stage + 1][_rem(chunk, sums[stage + 1].shape[0]), color] = total
            else:
                out[pair_of(chunk), _rows(color), columns(chunk)] = total

    def send_all(stage, part, chunk):
        for color in COLORS:
            for way in TWO:
                ring_copy(stage, part, _rem(chunk, RING), color, way).start()

    def open_first(chunk):
        merge_pair(chunk)
        store_halves(0, chunk)
        send_all(0, 0, chunk)

    def middle(stage, chunk):
        store_fulls(stage, chunk)
        send_all(stage, 1, chunk)

    def open_stage(stage, chunk):
        store_halves(stage, chunk)
        send_all(stage, 0, chunk)

    def turn(stage, chunk):
        close_stage(stage, chunk)
        if stage < 2:
            open_stage(stage + 1, chunk)

    return [(0, fetch), (2 * LAG, functools.partial(middle, 0)), (LAG, open_first),
            (3 * LAG, functools.partial(turn, 0)), (4 * LAG, functools.partial(middle, 1)),
            (5 * LAG, functools.partial(turn, 1)), (SIXTH * LAG, functools.partial(middle, 2)),
            (7 * LAG, functools.partial(turn, 2)), (1, consume), (0, multiply)]


def train_kernel(n_layers, x_ref, g_ref, rows_ref, down_ref, y_ref, dx_ref, rows_hbm, down_hbm, *refs):
    saved, refs = refs[:9], refs[9:]
    (rows_out, out), refs = refs[:2], refs[2:]
    (wbuf, peer, shard, twin, state, lefts, rights, q_buf, k_buf, v_buf, hid_out_buf, acc, hid_in_buf, dact, x_buf,
     dk_acc, dv_acc, away), refs = refs[:18], refs[18:]
    sums, half_bufs, full_bufs, refs = refs[:3], refs[3:9], refs[9:15], refs[15:]
    half_bufs = [half_bufs[2 * stage:2 * stage + 2] for stage in COLORS]
    full_bufs = [full_bufs[2 * stage:2 * stage + 2] for stage in COLORS]
    forward_sems, backward_sems, (swap_sem, end_sem, credit) = refs[:8], refs[8:16], refs[16:]
    torus = Torus(credit)
    core = torus.core
    n_chunks = n_layers * PER_HALF
    fill = pltpu.make_async_copy(x_ref, state, forward_sems[5].at[9])
    fill.start()
    for block in SIX:
        pltpu.make_async_copy(g_ref.at[:, COLS * block:COLS * block + COLS], rights.at[block],
                              backward_sems[0].at[3]).start()
    torus.meet()
    fill.wait()
    pltpu.make_async_copy(rights.at[:DH_AT], rights.at[:DH_AT], backward_sems[0].at[3]).wait()
    def y_copy():
        return pltpu.make_async_copy(state, y_ref, forward_sems[5].at[9])

    def x_out(result):
        y_copy().wait()
        state[ALL] = result
        pltpu.make_async_copy(state, dx_ref, forward_sems[5].at[9]).start()

    forward = forward_steps(torus, n_layers, x_ref, rows_ref, down_ref, y_ref, saved, wbuf, peer, shard, twin, state, lefts,
                            rights, q_buf, k_buf, v_buf, hid_out_buf, acc, *forward_sems)
    backward = backward_steps(torus, n_layers, x_ref, x_out, saved, out, wbuf, lefts, rights, hid_in_buf, dact, acc,
                              q_buf, k_buf, v_buf, x_buf, dk_acc, dv_acc, sums, half_bufs, full_bufs,
                              *backward_sems)
    turn_at = n_chunks
    backward = [(lag + turn_at, step) for lag, step in backward]
    n_ticks = turn_at + n_chunks + 7 * LAG
    def hand_over(layer, part):
        cols = _at(part * FIFTH, FIFTH)
        both = out[layer, :, cols]
        low, high = both[:HALF_ROWS], both[HALF_ROWS:]
        rows_out[core, layer, :, cols] = jnp.where(core == 0, low, high)
        away[layer, :, cols] = jnp.where(core == 0, high, low)
        torus.remote(away.at[layer, :, cols], rows_out.at[core, layer, :, cols], swap_sem.at[0, layer],
                     swap_sem.at[1, layer], torus.sibling).start()

    def down_result(layer):
        return pltpu.make_async_copy(out.at[layer, :, UP_END:], down_hbm.at[layer], end_sem.at[0, layer])

    def rows_result(layer):
        return pltpu.make_async_copy(rows_out.at[:, layer], rows_hbm.at[:, layer], end_sem.at[1, layer])

    def rows_meet(layer):
        swap = torus.remote(away.at[layer], rows_out.at[core, layer], swap_sem.at[0, layer], swap_sem.at[1, layer],
                            torus.sibling)
        swap.wait_send()
        swap.wait_recv()
        rows_result(layer).start()

    def hand_on(now):
        for layer in range(n_layers):
            begin = turn_at + (n_layers - layer) * PER_HALF + 8 * LAG

            @pl.when(now == begin - UP_BLOCKS)
            def _(layer=layer):
                down_result(layer).start()

            if layer > 0:
                @pl.when((now >= begin) & (now < begin + 5))
                def _(layer=layer, begin=begin):
                    hand_over(layer, now - begin)

                @pl.when(now == begin + 8)
                def _(layer=layer):
                    rows_meet(layer)

        @pl.when((now >= n_ticks - ATTN) & (now < n_ticks - ATTN + QKV))
        def _():
            hand_over(0, n_ticks - STAGES - now)

    torus.run(backward[:1] + forward + backward[1:], n_chunks, n_ticks, hand_on)
    hand_over(0, 0)
    rows_meet(0)
    for layer in range(n_layers):
        _all_done([down_result(layer), rows_result(layer)])
    pltpu.make_async_copy(state, dx_ref, forward_sems[5].at[9]).wait()


def train_stack(x_loc, g_loc, rows, down):
    n_layers = down.shape[0]
    seq, width = x_loc.shape
    bf16, f32 = jnp.bfloat16, jnp.float32
    half = WIDE
    chunk = CUBE + (ROWS, COLS)
    shape = jax.ShapeDtypeStruct
    hbm = pl.BlockSpec(memory_space=pl.ANY)
    vmem = pl.BlockSpec(memory_space=pltpu.VMEM)
    dma = pltpu.SemaphoreType.DMA
    saved = (shape((2 * n_layers - 1, seq, width), bf16), shape((n_layers,) + CUBE + (ROWS, PER_HALF * COLS), bf16),
             shape((n_layers, 3, 2, seq, width), f32), shape((n_layers, SIXTH, seq, width), bf16),
             shape((n_layers, 2, seq, width), bf16), shape((n_layers, seq, width), bf16),
             shape((n_layers, seq, 2 * HEAD), bf16), shape((n_layers, seq, 2 * HEAD), bf16),
             shape((n_layers, SIXTH, seq, COLS), bf16))
    scratch = [pltpu.VMEM(full, kind) for full, kind in (
        ((2, n_layers, HALF_ROWS, UP_END), f32), ((n_layers, ROWS, PER_HALF * COLS), f32),
        ((GATHER_SLOTS + 6,) + chunk, bf16), ((RING,) + chunk, bf16), ((n_layers, ROWS, PER_HALF * COLS), bf16),
        (rows.shape[1:], bf16), ((seq, width), bf16), ((9, seq, width), bf16), ((56, seq, COLS), bf16),
        ((seq, SIXTH * COLS), bf16), ((seq, 2 * HEAD), bf16), ((seq, 2 * HEAD), bf16), ((2, 2, seq, COLS), f32),
        ((seq, width), f32), ((seq, width), f32), ((2, seq, width), f32), ((seq, width), bf16),
        ((2, seq, HEAD), f32), ((2, seq, HEAD), f32), ((n_layers, HALF_ROWS, UP_END), f32), ((6,) + chunk, f32),
        ((5, 3, RING, RING, TILE, COLS), f32), ((5, 3, RING, TILE, COLS), f32))]
    for cols in (half, COLS):
        for size in ((RING, RING), (RING,), ()):
            scratch += [pltpu.VMEM((RING, 3, 2) + size + (TILE, cols), bf16)] * 2
    scratch += [dma((SIXTH, RING)), dma((SIXTH, RING)), dma((RING,)), dma((RING,)), dma((RING,)), dma((10,)), dma((2, 2)), dma((2, n_layers + 1))]
    scratch += [dma((10,)), dma((2,)), dma((SLOTS,)), dma((SLOTS,)), dma((RING,)), dma((RING,)), dma((SIXTH, RING)),
                dma((SIXTH, RING)), dma((2, n_layers)), dma((2, n_layers)), pltpu.SemaphoreType.REGULAR((7,))]
    return pl.pallas_call(
        functools.partial(train_kernel, n_layers), name="train_stack",
        out_shape=(shape((seq, width), bf16), shape((seq, width), bf16), shape((2, n_layers, HALF_ROWS, UP_END), f32),
                   shape(down.shape, f32)) + saved,
        in_specs=[hbm, hbm, vmem, vmem], out_specs=(hbm,) * (4 + len(saved)), scratch_shapes=scratch,
        compiler_params=pltpu.CompilerParams(collective_id=0, has_side_effects=True, vmem_limit_bytes=VMEM_LIMIT),
    )(x_loc, g_loc, rows, down)[:4]


LANES = 128


def _moves(chips, block, packed_first):
    moves = []
    for half in TWO:
        for part in COLORS:
            for chip in range(chips):
                packed = chips * ROWS * (STAGES * half + part) + ROWS * chip
                plain = block * (2 * chip + half) + ROWS * part
                pair = (packed, plain) if packed_first else (plain, packed)
                moves.append(pair + (min(ROWS, block - ROWS * part),))
    return moves


def _pieces(moves, size):
    tiles = [[] for _ in range(size // LANES)]
    for target, source, length in moves:
        while length:
            step = min(length, LANES - target % LANES, LANES - source % LANES)
            tiles[target // LANES].append((target % LANES, source // LANES, (target - source) % LANES))
            target, source, length = target + step, source + step, length - step
    return [sorted(tile) for tile in tiles]


def _gather_tile(load, tile, lane):
    total = None
    for first, source, shift in tile:
        value = load(source)
        if shift:
            value = pltpu.roll(value, shift, axis=value.ndim - 1)
        total = value if total is None else jnp.where(lane >= first, value, total)
    return total


def _span(index, size):
    return slice(size * index, size * index + size)


def _moved(pairs, sems):
    copies = [pltpu.make_async_copy(source, target, sems.at[order]) for order, (source, target) in enumerate(pairs)]
    for copy in copies:
        copy.start()
    return copies


def _all_done(copies):
    for copy in copies:
        copy.wait()


def _head_spots(heads):
    return [[(head, 0, heads * half + head) for head in range(heads)]
            + [(heads + 2 + head, 3, heads * half + head) for head in range(heads)] for half in TWO]


def pack_kernel(chips, *refs):
    sources, (rows_hbm, down_hbm), arrays, refs = refs[:6], refs[6:8], refs[8:14], refs[14:]
    rows_out, down_out, wide, in_sems, out_sems = refs
    k_ref, v_ref, up_ref, down_ref = arrays[1], arrays[2], arrays[4], arrays[5]
    rows, layers, _ = up_ref.shape
    block, _, width = down_ref.shape
    heads = arrays[0].shape[1] // 2
    half_f = STAGES * chips * ROWS
    inward = _moved(zip(sources, arrays), in_sems)
    _all_done(inward[:QKV])
    for half, spots in enumerate(_head_spots(heads)):
        for at, which, head in spots:
            rows_out[half, :, :, _span(at, LANES)] = jnp.swapaxes(
                arrays[which][:, head].astype(jnp.float32), 0, 1).astype(jnp.bfloat16)
        for layer in range(layers):
            for at, ref in ((heads, k_ref), (heads + 1, v_ref)):
                rows_out[half, layer, :, _span(at, LANES)] = ref[layer].astype(
                    jnp.float32)[:, half].astype(jnp.bfloat16)
    inward[QKV].wait()
    wide[ALL] = jnp.swapaxes(up_ref[ALL].astype(jnp.float32), 0, 1)
    lane = lax.broadcasted_iota(jnp.int32, (layers, rows, LANES), 2)
    tiles = _pieces(_moves(chips, block, True), 2 * half_f)
    outward = []
    for half in TWO:
        for index in range(half_f // LANES):
            tile = tiles[half * (half_f // LANES) + index]
            value = _gather_tile(lambda source: wide[:, :, _span(source, LANES)], tile, lane)
            if LANES * index >= 2 * chips * ROWS:
                position = lax.rem(lane + LANES * index % ROWS, ROWS)
                value = jnp.where(position < block - 2 * ROWS, value, 0.0)
            rows_out[half, :, :, _span(2 * ATTN + index, LANES)] = value.astype(jnp.bfloat16)
        outward += _moved([(rows_out.at[half], rows_hbm.at[half])], out_sems.at[half:half + 1])
    inward[5].wait()
    for part in COLORS:
        used = min(ROWS, block - ROWS * part)
        both = jnp.swapaxes(down_ref[ROWS * part:ROWS * part + used].astype(jnp.float32), 0, 1)
        for layer in range(layers):
            one = both[layer]
            if used < ROWS:
                one = jnp.concatenate([one, jnp.zeros((ROWS - used, width), jnp.float32)], axis=0)
            down_out[layer, :, _span(part, width)] = one.astype(jnp.bfloat16)
    _all_done(outward + _moved([(down_out, down_hbm)], out_sems.at[2:3]))


def _bounced(kernel, name, inputs, outs, arrays, n_sems):
    hbm = pl.BlockSpec(memory_space=pl.ANY)
    scratch = [pltpu.VMEM(array.shape, array.dtype) for array in arrays]
    return pl.pallas_call(
        kernel, name=name, out_shape=tuple(outs), in_specs=[hbm] * len(inputs), out_specs=(hbm,) * len(outs),
        scratch_shapes=scratch + [pltpu.SemaphoreType.DMA((size,)) for size in n_sems],
        compiler_params=pltpu.CompilerParams(vmem_limit_bytes=VMEM_LIMIT))(*inputs)


def pack_weights(w_q, w_k, w_v, w_o, w_up, w_down, chips):
    layers, rows = w_up.shape[:2]
    shape = jax.ShapeDtypeStruct
    inputs = [w_q.transpose(1, 2, 0, 3), w_k, w_v, w_o.transpose(1, 2, 0, 3), w_up.transpose(1, 0, 2),
              w_down.transpose(1, 0, 2)]
    outs = [shape((2, layers, rows, UP_END), jnp.bfloat16), shape((layers, ROWS, 3 * w_down.shape[2]), jnp.bfloat16)]
    return _bounced(functools.partial(pack_kernel, chips), "pack_weights", inputs, outs,
                    inputs + outs + [shape(w_up.shape, jnp.float32)], (6, 3))


def unpack_kernel(chips, *refs):
    sources, results, arrays, (in_sems, out_sems) = refs[:4], refs[4:12], refs[12:22], refs[22:]
    rows_ref, down_ref, q_out, k_out, v_out, o_out, up_out, down_out = arrays[:2] + arrays[4:]
    rows, layers, cols = up_out.shape
    block, _, width = down_out.shape
    heads = q_out.shape[1] // 2
    order = (1, 0, 2, 3)
    inward = _moved([(sources[which], arrays[which]) for which in order], in_sems)
    inward[0].wait()
    for part in COLORS:
        used = min(ROWS, block - ROWS * part)
        for layer in range(layers):
            down_out[ROWS * part:ROWS * part + used, layer, :] = down_ref[layer, :used, _span(part, width)]
    inward[1].wait()
    outward = _moved([(down_out, results[5])], out_sems)
    lane = lax.broadcasted_iota(jnp.int32, (layers, rows, LANES), 2)
    per_half = STAGES * chips * ROWS // LANES

    def load(source):
        half, tile = divmod(source, per_half)
        return rows_ref[half, :, :, _span(2 * ATTN + tile, LANES)]

    _all_done(inward[2:])
    outward += _moved(zip(arrays[2:4], results[6:]), out_sems.at[1:])
    for index, tile in enumerate(_pieces(_moves(chips, block, False), cols)):
        up_out[:, :, _span(index, LANES)] = jnp.swapaxes(_gather_tile(load, tile, lane), 0, 1)
    outward += _moved([(up_out, results[4])], out_sems.at[STAGES:])
    for half, spots in enumerate(_head_spots(heads)):
        for at, which, head in spots:
            (q_out, o_out)[which // 3][:, head] = jnp.swapaxes(rows_ref[half, :, :, _span(at, LANES)], 0, 1)
        for layer in range(layers):
            for at, ref in ((heads, k_out), (heads + 1, v_out)):
                ref[layer, :, half, :] = rows_ref[half, layer, :, _span(at, LANES)]
    _all_done(outward + _moved(zip((q_out, k_out, v_out, o_out), results), out_sems.at[QKV:]))


def unpack_grads(row_grad, down_grad, y_loc, grad_x, shapes, chips):
    q_shape, k_shape, _, _, up_shape, down_shape = shapes
    layers, rows, heads, head_dim = q_shape
    shape = jax.ShapeDtypeStruct
    turned = [(rows, heads, layers, head_dim), k_shape, k_shape, (rows, heads, layers, head_dim),
              (rows, layers, up_shape[2]), (down_shape[1], layers, down_shape[2])]
    turned = [shape(full, jnp.float32) for full in turned]
    inputs = [row_grad, down_grad, y_loc, grad_x]
    outs = _bounced(functools.partial(unpack_kernel, chips), "unpack_grads", inputs,
                    turned + [shape(value.shape, value.dtype) for value in (y_loc, grad_x)], inputs + turned, (4, 8))
    d_q, d_k, d_v, d_o, d_up, d_down, y_out, dx_out = outs
    return (y_out[None], dx_out[None], d_q.transpose(2, 0, 1, 3), d_k, d_v, d_o.transpose(2, 0, 1, 3),
            d_up.transpose(1, 0, 2), d_down.transpose(1, 0, 2))


def solution(mesh):
    mesh4 = Mesh(mesh.devices.reshape(CUBE + (2,)), ALL_AXES)
    row_spec = P(ALL_AXES)
    weight_spec = P(None, ALL_AXES)

    def body(x_in, w_q, w_k, w_v, w_o, w_up, w_down, grad_out):
        weights = (w_q, w_k, w_v, w_o, w_up, w_down)
        chips = w_up.shape[2] // w_down.shape[1] // 2
        rows, down = pack_weights(*weights, chips)
        y_loc, grad_x, row_grad, down_grad = train_stack(x_in[0], grad_out[0], rows, down)
        return unpack_grads(row_grad, down_grad, y_loc, grad_x, [weight.shape for weight in weights], chips)

    return jax.shard_map(body, mesh=mesh4, in_specs=(row_spec,) + (weight_spec,) * 6 + (row_spec,),
                         out_specs=(row_spec, row_spec) + (weight_spec,) * 6, check_vma=False)
```

```python
import functools

import jax
import jax.numpy as jnp
from jax import lax
from jax.experimental import pallas as pl
from jax.experimental.pallas import tpu as pltpu
from jax.sharding import Mesh, PartitionSpec as P

MESH = pl.DeviceIdType.MESH
ALL_AXES = ("z", "y", "x", "c")
EPS = 1e-6
MASK_FILL = -1e30
DIMS = ("z", "y", "x")
ORDERS = (("x", "y", "z"), ("y", "z", "x"), ("z", "x", "y"))
COLS = 256
ROWS = 24
LAG = 2
WIDE = COLS // 2
HALF_ROWS = ROWS // 2
HEAD = 128
PER_HALF = 43
UP_BLOCKS = 25
UP_END = UP_BLOCKS * COLS
RING = 4
STAGES = 3
FINAL = STAGES - 1
CUBE = (RING, RING, RING)
CHIPS = RING ** STAGES
SLOTS = 3
TILE = 8
COLORS = range(3)
TWO = range(2)
SIX = range(6)
ALL = Ellipsis
EVERY = slice(None)
QKV, ATTN, FF = 4, 7, 18
DOWN_DONE = FF
UP_DONE = DOWN_DONE + FF
O_DONE = UP_DONE + ATTN - QKV
SIXTH = 6
DH_AT = SIXTH
O_AT = DH_AT + UP_DONE
QKV_AT = O_AT + SIXTH
NORM_MLP, GRAD, NORM_ATTN = 6, 7, 8
VMEM_LIMIT = 67043328


FIFTH = UP_END // 5
GELU_A = 0.7978845608028654
GELU_B = GELU_A * 0.044715
GELU_C = 0.5 * GELU_A
GELU_D = 1.5 * GELU_B
AHEAD = 7
GATHER_SLOTS = 22
MANY = 16


def _rows(color):
    return slice(TILE * color, TILE * color + TILE)


def _rem(value, by):
    return lax.rem(value, by)


def _block(color, stage, position):
    dims = tuple(dim for dim in DIMS if dim not in ORDERS[color][:stage])
    return tuple(position if dim == ORDERS[color][stage] else EVERY for dim in dims)


def _dot(left, right):
    return jnp.dot(left, right, preferred_element_type=jnp.float32)


def _dot_rhs_t(left, right):
    return lax.dot_general(left, right, (((1,), (1,)), ((), ())), preferred_element_type=jnp.float32)


def _dot_lhs_t(left, right):
    return lax.dot_general(left, right, (((0,), (0,)), ((), ())), preferred_element_type=jnp.float32)


def _at(start, size):
    return pl.ds(pl.multiple_of(start, size), size)


def _causal(seq):
    return (lax.rem(lax.broadcasted_iota(jnp.int32, (2 * seq, seq), 0), seq)
            >= lax.broadcasted_iota(jnp.int32, (2 * seq, seq), 1))


def _under(block):
    return jnp.concatenate([block[:, :HEAD], block[:, HEAD:]], axis=0)


def _beside(stacked):
    seq = stacked.shape[0] // 2
    return jnp.concatenate([stacked[:seq], stacked[seq:]], axis=1)


def _probs(query, key, causal):
    scores = jnp.where(causal, _dot_rhs_t(query, key) * (HEAD ** -0.5), MASK_FILL)
    weight = jnp.exp(scores - jnp.max(scores, axis=-1, keepdims=True))
    return weight / jnp.sum(weight, axis=-1, keepdims=True)


def _rms(values):
    wide = values.astype(jnp.float32)
    return (wide * lax.rsqrt(jnp.mean(wide * wide, axis=-1, keepdims=True) + EPS)).astype(jnp.bfloat16)


def _rms_back(values, grad):
    wide = values.astype(jnp.float32)
    scale = lax.rsqrt(jnp.mean(wide * wide, axis=-1, keepdims=True) + EPS)
    return scale * grad - wide * (scale * scale * scale) * jnp.mean(wide * grad, axis=-1, keepdims=True)


class Torus:
    def __init__(self, credit):
        self.core = lax.axis_index("c")
        self.place = {dim: lax.axis_index(dim) for dim in DIMS}
        self.near = tuple({dim: _rem(self.place[dim] + step, RING) for dim in DIMS} for step in (1, 3))
        self.far = {dim: _rem(self.place[dim] + 2, RING) for dim in DIMS}
        self.sibling = {"c": 1 - self.core}
        self.sides = ((0, self.core), (1, 1 - self.core))
        self.credit = credit
        self.partners = [({dim: self.near[way][dim]}, 2 * d + 1 - way, 2 * d + way)
                         for d, dim in enumerate(DIMS) for way in TWO]
        self.partners.append((self.sibling, 6, 6))

    def meet(self):
        barrier = pltpu.get_barrier_semaphore()
        for device, _, _ in self.partners:
            pl.semaphore_signal(barrier, inc=1, device_id=device, device_id_type=MESH)
        pl.semaphore_wait(barrier, len(self.partners))

    def remote(self, source, target, send_sem, recv_sem, device):
        return pltpu.make_async_remote_copy(src_ref=source, dst_ref=target, send_sem=send_sem, recv_sem=recv_sem,
                                            device_id=device, device_id_type=MESH)

    def run(self, steps, n_chunks, n_ticks, after):
        def tick(now, carry):
            @pl.when(now >= 2)
            def _():
                for _, _, mine in self.partners:
                    pl.semaphore_wait(self.credit.at[mine], 1)

            for lag, action, early in steps:
                beat = now - lag
                if not early:
                    @pl.when((beat >= 0) & (beat < n_chunks))
                    def _(beat=beat, action=action):
                        action(beat)
                    continue
                double = beat < AHEAD

                @pl.when((beat >= 0) & (beat < n_chunks - AHEAD))
                def _(beat=beat, double=double, action=action):
                    first = jnp.where(double, 2 * beat, beat + AHEAD)

                    def one(order, inner):
                        action(first + order)
                        return inner
                    lax.fori_loop(0, jnp.where(double, 2, 1), one, 0)
            after(now)

            @pl.when(now < n_ticks - 2)
            def _():
                for device, theirs, _ in self.partners:
                    pl.semaphore_signal(self.credit.at[theirs], inc=1, device_id=device, device_id_type=MESH)
            return carry

        lax.fori_loop(0, n_ticks, tick, 0)


def forward_steps(torus, n_layers, x_ref, rows_ref, down_ref, y_ref, saved, wbuf, peer, shard, twin, state, lefts, rights,
                  q_buf, k_buf, v_buf, hid_buf, acc, ring_send, ring_recv, pair_send, pair_recv, keep_sem, save_sem,
                  hid_sem, twin_sem):
    acts, w_out, hid_out, gelu_out, norm_out, q_out, k_out, v_out, o_out = saved
    core, place, near = torus.core, torus.place, torus.near
    slots = GATHER_SLOTS
    n_chunks = n_layers * PER_HALF
    ready = SIXTH * LAG
    seq = state.shape[0]
    third = CHIPS * ROWS
    last = n_layers - 1
    pieces = [(0, EVERY, slice(0, FIFTH)), (0, EVERY, slice(FIFTH, None))] + [
        (layer, EVERY, EVERY) for layer in range(1, n_layers)]
    swaps = [torus.remote(rows_ref.at[(1 - core,) + piece], twin.at[piece], twin_sem.at[0, order], twin_sem.at[1, order],
                          torus.sibling) for order, piece in enumerate(pieces)]
    for swap in swaps:
        swap.start()
    swaps[0].wait_send()
    swaps[0].wait_recv()

    def assemble(chunk):
        @pl.when(chunk == 1)
        def _():
            for swap in swaps[1:]:
                swap.wait_send()
                swap.wait_recv()

        @pl.when(chunk < 5 * n_layers)
        def _():
            layer, part = chunk // 5, _rem(chunk, 5)
            cols = _at(part * FIFTH, FIFTH)
            mine, other = [ref[layer, :, cols].astype(jnp.float32) for ref in (rows_ref.at[core], twin)]
            shard[layer, :, cols] = jnp.concatenate(
                [jnp.where(core == 0, mine, other), jnp.where(core == 0, other, mine)], axis=0).astype(jnp.bfloat16)

            @pl.when(part == 4)
            def _():
                shard[layer, :, UP_END:] = down_ref[layer]

    def columns(chunk):
        return _at(_rem(chunk, PER_HALF) * COLS, COLS)

    def spot(slot, color, stage, position, cols):
        order = ORDERS[color]
        index = tuple(EVERY if dim in order[:stage] else position if dim == order[stage] else place[dim]
                      for dim in DIMS)
        return wbuf.at[(slot,) + index + (_rows(color), cols)]

    halves = (slice(0, WIDE), slice(WIDE, COLS))

    def send_own(stage, chunk):
        slot, sem = _rem(chunk, slots), _rem(chunk, MANY)
        for color in COLORS:
            dim = ORDERS[color][stage]
            here = spot(slot, color, stage, place[dim], slice(0, COLS))
            source = here
            if stage == 0:
                source = shard.at[chunk // PER_HALF, _rows(color), columns(chunk)]
            for way in TWO:
                torus.remote(source, here, ring_send.at[2 * stage, sem], ring_recv.at[2 * stage, sem],
                             {dim: near[way][dim]}).start()

    def send_far(stage, chunk):
        slot, sem = _rem(chunk, slots), _rem(chunk, MANY)
        for color in COLORS:
            dim = ORDERS[color][stage]
            for way in TWO:
                block = spot(slot, color, stage, near[1 - way][dim], halves[way])
                torus.remote(block, block, ring_send.at[2 * stage + 1, sem], ring_recv.at[2 * stage + 1, sem],
                             {dim: near[way][dim]}).start()

    def arrived(part, chunk):
        slot, sem = _rem(chunk, slots), _rem(chunk, MANY)
        count = slice(0, 2) if part % 2 == 0 else 0
        block = wbuf.at[(slot,) + (0,) * (2 - part // 2) + (count,)]
        whole = torus.remote(block, block, ring_send.at[part, sem], ring_recv.at[part, sem], torus.sibling)
        whole.wait_send()
        whole.wait_recv()

    def enter(chunk):
        wbuf[_rem(chunk, slots), place["z"], place["y"], place["x"]] = shard[chunk // PER_HALF, :, columns(chunk)]
        send_own(0, chunk)

    def pass_on(part, chunk):
        arrived(part, chunk)
        if part % 2 == 0:
            send_far(part // 2, chunk)
        else:
            send_own(part // 2 + 1, chunk)

    def pair_copy(chunk):
        slot = _rem(chunk, RING)
        return torus.remote(wbuf.at[_rem(chunk, slots)], peer.at[slot], pair_send.at[slot], pair_recv.at[slot],
                            torus.sibling)

    def exchange(chunk):
        arrived(5, chunk)
        pair_copy(chunk).start()

    def keep_copy(chunk):
        return pltpu.make_async_copy(wbuf.at[_rem(chunk, slots)],
                                     w_out.at[chunk // PER_HALF, :, :, :, :, columns(chunk)],
                                     keep_sem.at[_rem(chunk, RING)])

    def save_copies(layer, names):
        parts = {"n0": (lefts.at[NORM_ATTN], norm_out.at[layer, 0]), "n1": (lefts.at[NORM_MLP], norm_out.at[layer, 1]),
                 "q": (q_buf, q_out.at[layer]), "k": (k_buf, k_out.at[layer]), "v": (v_buf, v_out.at[layer]),
                 "o": (rights.at[O_AT:QKV_AT], o_out.at[layer]), "a": (lefts.at[:NORM_MLP], gelu_out.at[layer]),
                 "mid": (state, acts.at[2 * layer]), "end": (state, acts.at[2 * layer + 1])}
        places = list(parts)
        return [pltpu.make_async_copy(*parts[name], save_sem.at[places.index(name)]) for name in names]

    def save(layer, names):
        @pl.when(layer < last)
        def _():
            for copy in save_copies(layer, names):
                copy.start()

    def saved_all(layer, names):
        @pl.when(layer < last)
        def _():
            for copy in save_copies(layer, names):
                copy.wait()

    def hidden_copies(layer, order):
        slot, part, at = _rem(order, 2), order // SIXTH, _at(_rem(order, SIXTH) * COLS, COLS)
        return [pltpu.make_async_copy(hid_buf.at[slot, half], hid_out.at[layer, part, half, :, at],
                                      hid_sem.at[slot, half]) for half in TWO]

    def compute(chunk):
        layer, index = chunk // PER_HALF, _rem(chunk, PER_HALF)
        pair = pair_copy(chunk)
        pair.wait_send()
        pair.wait_recv()
        keep_copy(chunk).start()

        def weights(role):
            block = wbuf[_rem(chunk, slots)] if role == 0 else peer[_rem(chunk, RING)]
            return block.reshape(third, COLS)

        @pl.when(index == 0)
        def _():
            lefts[NORM_ATTN] = _rms(state[ALL])
            save(layer, ["n0"])

        @pl.when(index < 3)
        def _():
            for role, half in torus.sides:
                q_buf[:, _at(STAGES * COLS * half + COLS * index, COLS)] = _dot(
                    lefts[NORM_ATTN], weights(role)).astype(jnp.bfloat16)

        @pl.when(index == 3)
        def _():
            for role, half in torus.sides:
                both = _dot(lefts[NORM_ATTN], weights(role)).astype(jnp.bfloat16)
                k_buf[:, _at(HEAD * half, HEAD)] = both[:, :HEAD]
                v_buf[:, _at(HEAD * half, HEAD)] = both[:, HEAD:]

        @pl.when(index == QKV)
        def _():
            acc[ALL] = jnp.zeros_like(acc)
            save(layer, ["q", "k", "v"])

        @pl.when((index >= QKV) & (index < ATTN))
        def _():
            causal = _causal(seq)
            queries = [_under(q_buf[:, _at(STAGES * COLS * half + COLS * (index - QKV), COLS)]) for _, half in torus.sides]
            probs = [_probs(queries[role], k_buf[:, _at(HEAD * half, HEAD)], causal).astype(jnp.bfloat16)
                     for role, half in torus.sides]
            blocks = [_beside(_dot(probs[role], v_buf[:, _at(HEAD * half, HEAD)]).astype(jnp.bfloat16))
                      for role, half in torus.sides]
            acc[ALL] += sum(_dot_rhs_t(blocks[role], weights(role)) for role in TWO)
            for role, half in torus.sides:
                rights[O_AT + STAGES * half + index - QKV] = blocks[role]

        @pl.when(index == ATTN - 1)
        def _():
            @pl.when(layer > 0)
            def _():
                saved_all(layer - 1, ["end"])
            middle = (state[ALL].astype(jnp.float32) + acc[ALL]).astype(jnp.bfloat16)
            state[ALL] = middle
            lefts[NORM_MLP] = _rms(middle)
            save(layer, ["n1", "o"])
            mid = save_copies(layer, ["mid"])[0]
            mid.start()

        @pl.when((index > ATTN) & (index <= UP_BLOCKS))
        def _():
            for copy in hidden_copies(layer, index - ATTN - 1):
                copy.wait()

        @pl.when((index >= ATTN) & (index < UP_BLOCKS))
        def _():
            order = index - ATTN
            for role, half in torus.sides:
                hidden = _dot(lefts[NORM_MLP], weights(role))
                hid_buf[_rem(order, 2), half] = hidden
                lefts[STAGES * half + order // SIXTH, :, _at(COLS * _rem(order, SIXTH), COLS)] = jax.nn.gelu(
                    hidden).astype(jnp.bfloat16)
            for copy in hidden_copies(layer, order):
                copy.start()

        @pl.when(index == UP_BLOCKS)
        def _():
            save(layer, ["a"])
            save_copies(layer, ["mid"])[0].wait()

        @pl.when(index >= UP_BLOCKS)
        def _():
            part, at = (index - UP_BLOCKS) // SIXTH, _at(COLS * _rem(index - UP_BLOCKS, SIXTH), COLS)
            total = sum(_dot(lefts[STAGES * half + part], weights(role)) for role, half in torus.sides)

            @pl.when(part == 0)
            def _():
                acc[:, at] = total

            @pl.when(part > 0)
            def _():
                acc[:, at] += total

        @pl.when(index == PER_HALF - 1)
        def _():
            saved_all(layer, ["n0", "n1", "q", "k", "v", "o", "a"])
            result = (state[ALL].astype(jnp.float32) + acc[ALL]).astype(jnp.bfloat16)
            state[ALL] = result
            save(layer, ["end"])

            @pl.when(layer == last)
            def _():
                pltpu.make_async_copy(state, y_ref, save_sem.at[9]).start()

        keep_copy(chunk).wait()

    steps = [(0, assemble, False), (0, enter, True)]
    steps += [((part + 1) * LAG, functools.partial(pass_on, part), part < STAGES) for part in range(5)]
    return steps + [(ready, exchange, False), (ready + 1, compute, False)]


def backward_steps(torus, n_layers, x_ref, x_out, saved, out, wbuf, lefts, rights, hid_buf, dact, dnorm, q_buf,
                   k_buf, v_buf, x_buf, dk_acc, dv_acc, sums, half_bufs, full_bufs, load_sem, own_sem, push_send,
                   push_recv, pair_send, pair_recv, ring_send, ring_recv):
    acts, w_own, hid_in, gelu_in, norm_in, q_in, k_in, v_in, o_in = saved
    place, near = torus.place, torus.near
    seq = k_buf.shape[0]
    third = CHIPS * ROWS
    last = n_layers - 1

    def mine_slot(chunk):
        return GATHER_SLOTS - 2 + _rem(chunk, 2)

    def out_slot(chunk):
        return _rem(chunk, 2)

    def their_slot(chunk):
        return 5 + _rem(chunk, SLOTS)

    def peer_slot(chunk):
        order = _rem(chunk, RING)
        return jnp.where(order == 3, 8, 2 + order)

    def pair_of(chunk):
        return last - chunk // PER_HALF

    def columns(chunk):
        index = _rem(chunk, PER_HALF)
        block = jnp.where(index < DOWN_DONE, UP_BLOCKS + index,
                          jnp.where(index < UP_DONE, index - 11, jnp.where(index < O_DONE, index - 32, index - 39)))
        return _at(block * COLS, COLS)

    def loads(pair, names):
        parts = {"a": (gelu_in.at[pair], lefts.at[:NORM_MLP]), "n_mlp": (norm_in.at[pair, 1], lefts.at[NORM_MLP]),
                 "n_attn": (norm_in.at[pair, 0], lefts.at[NORM_ATTN]), "o": (o_in.at[pair], rights.at[O_AT:QKV_AT]),
                 "q": (q_in.at[pair], q_buf), "k": (k_in.at[pair], k_buf), "v": (v_in.at[pair], v_buf),
                 "x_mid": (acts.at[2 * pair], x_buf)}
        places = list(parts)
        return [pltpu.make_async_copy(*parts[name], load_sem.at[places.index(name)]) for name in names]

    def start(pair, names):
        for copy in loads(pair, names):
            copy.start()

    def finish(pair, names):
        for copy in loads(pair, names):
            copy.wait()

    def first_input(ref):
        return pltpu.make_async_copy(ref, x_buf, load_sem.at[9])

    def hidden_load(pair, part, half):
        return pltpu.make_async_copy(hid_in.at[pair, part, half], hid_buf, load_sem.at[8])

    def own_copy(chunk):
        return pltpu.make_async_copy(w_own.at[pair_of(chunk), :, :, :, :, columns(chunk)], wbuf.at[mine_slot(chunk)],
                                     own_sem.at[_rem(chunk, 2)])

    def push_copy(chunk):
        slot = _rem(chunk, SLOTS)
        return torus.remote(w_own.at[pair_of(chunk), :, :, :, :, columns(chunk)], wbuf.at[their_slot(chunk)],
                            push_send.at[slot], push_recv.at[slot], torus.sibling)

    def fetch(chunk):
        own_copy(chunk).start()
        push_copy(chunk).start()

    def total_grad():
        return jnp.concatenate([rights[block] for block in SIX], axis=1).astype(jnp.float32)

    def consume(chunk):
        pair, index = pair_of(chunk), _rem(chunk, PER_HALF)
        own_copy(chunk).wait()
        push = push_copy(chunk)
        push.wait_send()
        push.wait_recv()

        def weights(role):
            return wbuf[(mine_slot, their_slot)[role](chunk)].reshape(third, COLS)

        @pl.when(index == 0)
        def _():
            start(pair, ["x_mid"])

            @pl.when(pair < last)
            def _():
                start(pair, ["n_mlp", "n_attn", "o", "q", "k", "v"])

        def bend_back(part, half):
            hidden_load(pair, part, half).wait()
            for block in SIX:
                cols = slice(COLS * block, COLS * block + COLS)
                hidden = hid_buf[:, cols]
                square = hidden * hidden
                bend = jnp.tanh(hidden * (GELU_A + GELU_B * square))
                slope = (0.5 + 0.5 * bend) + (hidden * (1.0 - bend * bend)) * (GELU_C + GELU_D * square)
                rights[DH_AT + FF * half + SIXTH * part + block] = (dact[half, :, cols] * slope).astype(jnp.bfloat16)

        @pl.when((index > 0) & (index <= DOWN_DONE) & (_rem(index, SIXTH) == 0))
        def _():
            bend_back(index // SIXTH - 1, 1)

        @pl.when((index < DOWN_DONE) & (_rem(index, SIXTH) == 0))
        def _():
            dact[ALL] = jnp.zeros_like(dact)
            hidden_load(pair, index // SIXTH, 0).start()

        @pl.when(index < DOWN_DONE)
        def _():
            products = [_dot_rhs_t(rights[_rem(index, SIXTH)], weights(role)) for role in TWO]
            for role, half in torus.sides:
                dact[half] += products[role]

        @pl.when((index < DOWN_DONE) & (_rem(index, SIXTH) == 5))
        def _():
            bend_back(index // SIXTH, 0)
            hidden_load(pair, index // SIXTH, 1).start()

        @pl.when(index == DOWN_DONE - 1)
        def _():
            @pl.when(pair < last)
            def _():
                finish(pair, ["n_mlp", "n_attn", "o", "q", "k", "v"])

        @pl.when(index == DOWN_DONE)
        def _():
            dnorm[ALL] = jnp.zeros_like(dnorm)

            @pl.when(pair > 0)
            def _():
                start(pair - 1, ["a"])

        @pl.when((index >= DOWN_DONE) & (index < UP_DONE))
        def _():
            dnorm[ALL] += sum(_dot_rhs_t(rights[DH_AT + FF * half + index - DOWN_DONE], weights(role))
                              for role, half in torus.sides)

        @pl.when(index == UP_DONE - 1)
        def _():
            finish(pair, ["x_mid"])
            lefts[GRAD] = (total_grad() + _rms_back(x_buf[ALL], dnorm[ALL])).astype(jnp.bfloat16)

        @pl.when(index == UP_DONE)
        def _():
            @pl.when(pair == 0)
            def _():
                first_input(x_ref).start()

            @pl.when(pair > 0)
            def _():
                first_input(acts.at[2 * pair - 1]).start()
            dk_acc[ALL] = jnp.zeros_like(dk_acc)
            dv_acc[ALL] = jnp.zeros_like(dv_acc)

        @pl.when((index >= UP_DONE) & (index < O_DONE))
        def _():
            causal = _causal(seq)
            keys = [k_buf[:, _at(HEAD * half, HEAD)] for _, half in torus.sides]
            values = [v_buf[:, _at(HEAD * half, HEAD)] for _, half in torus.sides]
            queries = [_under(q_buf[:, _at(STAGES * COLS * half + COLS * (index - UP_DONE), COLS)])
                       for _, half in torus.sides]
            probs = [_probs(queries[role], keys[role], causal) for role in TWO]
            d_heads = [_under(_dot(lefts[GRAD], weights(role)).astype(jnp.bfloat16)) for role in TWO]
            d_probs = [_dot_rhs_t(d_heads[role], values[role]) for role in TWO]
            d_scores = [probs[role] * (d_probs[role] - jnp.sum(probs[role] * d_probs[role], axis=-1, keepdims=True))
                        for role in TWO]
            d_scores = [(d_score * (HEAD ** -0.5)).astype(jnp.bfloat16) for d_score in d_scores]
            d_v = [_dot_lhs_t(probs[role].astype(jnp.bfloat16), d_heads[role]) for role in TWO]
            d_k = [_dot_lhs_t(d_scores[role], queries[role]) for role in TWO]
            d_q = [_beside(_dot(d_scores[role], keys[role]).astype(jnp.bfloat16)) for role in TWO]
            for role, half in torus.sides:
                dv_acc[half] += d_v[role]
                dk_acc[half] += d_k[role]
                rights[QKV_AT + QKV * half + index - UP_DONE] = d_q[role]

        @pl.when(index == O_DONE - 1)
        def _():
            for half in TWO:
                rights[QKV_AT + QKV * half + QKV - 1] = jnp.concatenate([dk_acc[half], dv_acc[half]], axis=1).astype(jnp.bfloat16)

        @pl.when(index == O_DONE)
        def _():
            dnorm[ALL] = jnp.zeros_like(dnorm)

        @pl.when(index >= O_DONE)
        def _():
            dnorm[ALL] += sum(_dot_rhs_t(rights[QKV_AT + QKV * half + index - O_DONE], weights(role))
                              for role, half in torus.sides)

        @pl.when(index == PER_HALF - 1)
        def _():
            first_input(x_ref).wait()

            @pl.when(pair > 0)
            def _():
                finish(pair - 1, ["a"])
            result = (lefts[GRAD].astype(jnp.float32) + _rms_back(x_buf[ALL], dnorm[ALL])).astype(jnp.bfloat16)

            @pl.when(pair == 0)
            def _():
                x_out(result)
            for block in SIX:
                rights[block] = result[:, COLS * block:COLS * block + COLS]

    def pair_copy(chunk):
        slot = _rem(chunk, RING)
        return torus.remote(wbuf.at[out_slot(chunk)], wbuf.at[peer_slot(chunk)], pair_send.at[slot], pair_recv.at[slot],
                            torus.sibling)

    def multiply(chunk):
        index = _rem(chunk, PER_HALF)
        lead = _rem(chunk, sums[0].shape[0])
        quarter = third // RING
        for role, half in torus.sides[::-1]:
            left = jnp.where(index < DOWN_DONE, STAGES * half + index // SIXTH,
                             jnp.where(index < UP_DONE, NORM_MLP, jnp.where(index < O_DONE, GRAD, NORM_ATTN)))
            right = jnp.where(index < DOWN_DONE, _rem(index, SIXTH),
                              jnp.where(index < UP_DONE, DH_AT + FF * half + index - DOWN_DONE,
                                        jnp.where(index < O_DONE, O_AT + STAGES * half + index - UP_DONE,
                                                  QKV_AT + QKV * half + index - O_DONE)))
            for z in range(RING):
                part = _dot_lhs_t(lefts[left, :, quarter * z:quarter * z + quarter], rights[right])
                if role == 0:
                    sums[0][lead, z] = part.reshape(RING, RING, ROWS, COLS)
                else:
                    wbuf[out_slot(chunk), z] = part.astype(jnp.bfloat16).reshape(RING, RING, ROWS, COLS)
        pair_copy(chunk).start()

    def merge_pair(chunk):
        lead = _rem(chunk, sums[0].shape[0])
        pair_copy(chunk).wait_send()
        pair_copy(chunk).wait_recv()
        for z in range(RING):
            for y in range(RING):
                sums[0][lead, z, y] = sums[0][lead, z, y] + wbuf[peer_slot(chunk), z, y].astype(jnp.float32)

    def ring_copy(stage, part, slot, color, way):
        send, recv = (half_bufs, full_bufs)[part][stage]
        dim = ORDERS[color][stage]
        return torus.remote(send.at[slot, color, way], recv.at[slot, color, way],
                            ring_send.at[2 * stage + part, slot], ring_recv.at[2 * stage + part, slot],
                            {dim: near[way][dim]})

    def ring_wait(stage, part, slot):
        send, recv = (half_bufs, full_bufs)[part][stage]
        whole = torus.remote(send.at[slot], recv.at[slot], ring_send.at[2 * stage + part, slot],
                             ring_recv.at[2 * stage + part, slot], torus.sibling)
        whole.wait_send()
        whole.wait_recv()

    def source(stage, chunk, color, position, cols):
        lead = _rem(chunk, sums[stage].shape[0])
        if stage == 0:
            return sums[0][(lead,) + _block(color, 0, position) + (_rows(color), cols)]
        return sums[stage][(lead, color) + _block(color, stage, position) + (EVERY, cols)]

    left_cols, right_cols, every = slice(0, WIDE), slice(WIDE, COLS), slice(0, COLS)

    def store_halves(stage, chunk):
        slot = _rem(chunk, RING)
        send = half_bufs[stage][0]
        for color in COLORS:
            far = torus.far[ORDERS[color][stage]]
            send[slot, color, 0] = source(stage, chunk, color, far, left_cols).astype(jnp.bfloat16)
            send[slot, color, 1] = source(stage, chunk, color, far, right_cols).astype(jnp.bfloat16)

    def store_fulls(stage, chunk):
        slot = _rem(chunk, RING)
        ring_wait(stage, 0, slot)
        recv = half_bufs[stage][1]
        send = full_bufs[stage][0]
        lead = (EVERY,) * (len(send.shape) - 4)
        for color in COLORS:
            dim = ORDERS[color][stage]
            for way, summed, plain in ((0, left_cols, right_cols), (1, right_cols, left_cols)):
                send[(slot, color, way) + lead + (summed,)] = (
                    source(stage, chunk, color, near[way][dim], summed)
                    + recv[slot, color, way].astype(jnp.float32)).astype(jnp.bfloat16)
                send[(slot, color, way) + lead + (plain,)] = source(
                    stage, chunk, color, near[way][dim], plain).astype(jnp.bfloat16)

    def close_stage(stage, chunk):
        slot = _rem(chunk, RING)
        ring_wait(stage, 1, slot)
        recv = full_bufs[stage][1]
        for color in COLORS:
            dim = ORDERS[color][stage]
            total = (source(stage, chunk, color, place[dim], every)
                     + recv[slot, color, 0].astype(jnp.float32)
                     + recv[slot, color, 1].astype(jnp.float32))
            if stage < 2:
                sums[stage + 1][_rem(chunk, sums[stage + 1].shape[0]), color] = total
            else:
                out[pair_of(chunk), _rows(color), columns(chunk)] = total

    def send_all(stage, part, chunk):
        for color in COLORS:
            for way in TWO:
                ring_copy(stage, part, _rem(chunk, RING), color, way).start()

    def open_first(chunk):
        merge_pair(chunk)
        store_halves(0, chunk)
        send_all(0, 0, chunk)

    def middle(stage, chunk):
        store_fulls(stage, chunk)
        send_all(stage, 1, chunk)

    def open_stage(stage, chunk):
        store_halves(stage, chunk)
        send_all(stage, 0, chunk)

    def turn(stage, chunk):
        close_stage(stage, chunk)
        if stage < 2:
            open_stage(stage + 1, chunk)

    return [(0, fetch), (2 * LAG, functools.partial(middle, 0)), (LAG, open_first),
            (3 * LAG, functools.partial(turn, 0)), (4 * LAG, functools.partial(middle, 1)),
            (5 * LAG, functools.partial(turn, 1)), (SIXTH * LAG, functools.partial(middle, 2)),
            (7 * LAG, functools.partial(turn, 2)), (1, consume), (0, multiply)]


def train_kernel(n_layers, x_ref, g_ref, rows_ref, down_ref, y_ref, dx_ref, rows_hbm, down_hbm, *refs):
    saved, refs = refs[:9], refs[9:]
    (rows_out, out), refs = refs[:2], refs[2:]
    (wbuf, peer, shard, twin, state, lefts, rights, q_buf, k_buf, v_buf, hid_out_buf, acc, hid_in_buf, dact, x_buf,
     dk_acc, dv_acc, away), refs = refs[:18], refs[18:]
    sums, half_bufs, full_bufs, refs = refs[:3], refs[3:9], refs[9:15], refs[15:]
    half_bufs = [half_bufs[2 * stage:2 * stage + 2] for stage in COLORS]
    full_bufs = [full_bufs[2 * stage:2 * stage + 2] for stage in COLORS]
    forward_sems, backward_sems, (swap_sem, end_sem, credit) = refs[:8], refs[8:16], refs[16:]
    torus = Torus(credit)
    core = torus.core
    n_chunks = n_layers * PER_HALF
    fill = pltpu.make_async_copy(x_ref, state, forward_sems[5].at[9])
    fill.start()
    for block in SIX:
        pltpu.make_async_copy(g_ref.at[:, COLS * block:COLS * block + COLS], rights.at[block],
                              backward_sems[0].at[3]).start()
    torus.meet()
    fill.wait()
    pltpu.make_async_copy(rights.at[:DH_AT], rights.at[:DH_AT], backward_sems[0].at[3]).wait()
    def y_copy():
        return pltpu.make_async_copy(state, y_ref, forward_sems[5].at[9])

    def x_out(result):
        y_copy().wait()
        state[ALL] = result
        pltpu.make_async_copy(state, dx_ref, forward_sems[5].at[9]).start()

    forward = forward_steps(torus, n_layers, x_ref, rows_ref, down_ref, y_ref, saved, wbuf, peer, shard, twin, state, lefts,
                            rights, q_buf, k_buf, v_buf, hid_out_buf, acc, *forward_sems)
    backward = backward_steps(torus, n_layers, x_ref, x_out, saved, out, wbuf, lefts, rights, hid_in_buf, dact, acc,
                              q_buf, k_buf, v_buf, x_buf, dk_acc, dv_acc, sums, half_bufs, full_bufs,
                              *backward_sems)
    turn_at = n_chunks
    backward = [(lag + turn_at, step, False) for lag, step in backward]
    n_ticks = turn_at + n_chunks + 7 * LAG
    def hand_over(layer, part):
        cols = _at(part * FIFTH, FIFTH)
        both = out[layer, :, cols]
        low, high = both[:HALF_ROWS], both[HALF_ROWS:]
        rows_out[core, layer, :, cols] = jnp.where(core == 0, low, high)
        away[layer, :, cols] = jnp.where(core == 0, high, low)
        torus.remote(away.at[layer, :, cols], rows_out.at[core, layer, :, cols], swap_sem.at[0, layer],
                     swap_sem.at[1, layer], torus.sibling).start()

    def down_result(layer):
        return pltpu.make_async_copy(out.at[layer, :, UP_END:], down_hbm.at[layer], end_sem.at[0, layer])

    def rows_result(layer):
        return pltpu.make_async_copy(rows_out.at[:, layer], rows_hbm.at[:, layer], end_sem.at[1, layer])

    def rows_meet(layer):
        swap = torus.remote(away.at[layer], rows_out.at[core, layer], swap_sem.at[0, layer], swap_sem.at[1, layer],
                            torus.sibling)
        swap.wait_send()
        swap.wait_recv()
        rows_result(layer).start()

    def hand_on(now):
        for layer in range(n_layers):
            begin = turn_at + (n_layers - layer) * PER_HALF + 8 * LAG

            @pl.when(now == begin - UP_BLOCKS)
            def _(layer=layer):
                down_result(layer).start()

            if layer > 0:
                @pl.when((now >= begin) & (now < begin + 5))
                def _(layer=layer, begin=begin):
                    hand_over(layer, now - begin)

                @pl.when(now == begin + 8)
                def _(layer=layer):
                    rows_meet(layer)

        @pl.when((now >= n_ticks - ATTN) & (now < n_ticks - ATTN + QKV))
        def _():
            hand_over(0, n_ticks - STAGES - now)

    torus.run(backward[:1] + forward + backward[1:], n_chunks, n_ticks, hand_on)
    hand_over(0, 0)
    rows_meet(0)
    for layer in range(n_layers):
        _all_done([down_result(layer), rows_result(layer)])
    pltpu.make_async_copy(state, dx_ref, forward_sems[5].at[9]).wait()


def train_stack(x_loc, g_loc, rows, down):
    n_layers = down.shape[0]
    seq, width = x_loc.shape
    bf16, f32 = jnp.bfloat16, jnp.float32
    half = WIDE
    chunk = CUBE + (ROWS, COLS)
    shape = jax.ShapeDtypeStruct
    hbm = pl.BlockSpec(memory_space=pl.ANY)
    vmem = pl.BlockSpec(memory_space=pltpu.VMEM)
    dma = pltpu.SemaphoreType.DMA
    saved = (shape((2 * n_layers - 1, seq, width), bf16), shape((n_layers,) + CUBE + (ROWS, PER_HALF * COLS), bf16),
             shape((n_layers, 3, 2, seq, width), f32), shape((n_layers, SIXTH, seq, width), bf16),
             shape((n_layers, 2, seq, width), bf16), shape((n_layers, seq, width), bf16),
             shape((n_layers, seq, 2 * HEAD), bf16), shape((n_layers, seq, 2 * HEAD), bf16),
             shape((n_layers, SIXTH, seq, COLS), bf16))
    scratch = [pltpu.VMEM(full, kind) for full, kind in (
        ((2, n_layers, HALF_ROWS, UP_END), f32), ((n_layers, ROWS, PER_HALF * COLS), f32),
        ((GATHER_SLOTS,) + chunk, bf16), ((RING,) + chunk, bf16), ((n_layers, ROWS, PER_HALF * COLS), bf16),
        (rows.shape[1:], bf16), ((seq, width), bf16), ((9, seq, width), bf16), ((56, seq, COLS), bf16),
        ((seq, SIXTH * COLS), bf16), ((seq, 2 * HEAD), bf16), ((seq, 2 * HEAD), bf16), ((2, 2, seq, COLS), f32),
        ((seq, width), f32), ((seq, width), f32), ((2, seq, width), f32), ((seq, width), bf16),
        ((2, seq, HEAD), f32), ((2, seq, HEAD), f32), ((n_layers, HALF_ROWS, UP_END), f32), ((6,) + chunk, f32),
        ((5, 3, RING, RING, TILE, COLS), f32), ((5, 3, RING, TILE, COLS), f32))]
    for cols in (half, COLS):
        for size in ((RING, RING), (RING,), ()):
            scratch += [pltpu.VMEM((RING, 3, 2) + size + (TILE, cols), bf16)] * 2
    scratch += [dma((SIXTH, MANY)), dma((SIXTH, MANY)), dma((RING,)), dma((RING,)), dma((RING,)), dma((10,)), dma((2, 2)), dma((2, n_layers + 1))]
    scratch += [dma((10,)), dma((2,)), dma((SLOTS,)), dma((SLOTS,)), dma((RING,)), dma((RING,)), dma((SIXTH, RING)),
                dma((SIXTH, RING)), dma((2, n_layers)), dma((2, n_layers)), pltpu.SemaphoreType.REGULAR((7,))]
    return pl.pallas_call(
        functools.partial(train_kernel, n_layers), name="train_stack",
        out_shape=(shape((seq, width), bf16), shape((seq, width), bf16), shape((2, n_layers, HALF_ROWS, UP_END), f32),
                   shape(down.shape, f32)) + saved,
        in_specs=[hbm, hbm, vmem, vmem], out_specs=(hbm,) * (4 + len(saved)), scratch_shapes=scratch,
        compiler_params=pltpu.CompilerParams(collective_id=0, has_side_effects=True, vmem_limit_bytes=VMEM_LIMIT),
    )(x_loc, g_loc, rows, down)[:4]


LANES = 128


def _moves(chips, block, packed_first):
    moves = []
    for half in TWO:
        for part in COLORS:
            for chip in range(chips):
                packed = chips * ROWS * (STAGES * half + part) + ROWS * chip
                plain = block * (2 * chip + half) + ROWS * part
                pair = (packed, plain) if packed_first else (plain, packed)
                moves.append(pair + (min(ROWS, block - ROWS * part),))
    return moves


def _pieces(moves, size):
    tiles = [[] for _ in range(size // LANES)]
    for target, source, length in moves:
        while length:
            step = min(length, LANES - target % LANES, LANES - source % LANES)
            tiles[target // LANES].append((target % LANES, source // LANES, (target - source) % LANES))
            target, source, length = target + step, source + step, length - step
    return [sorted(tile) for tile in tiles]


def _gather_tile(load, tile, lane):
    total = None
    for first, source, shift in tile:
        value = load(source)
        if shift:
            value = pltpu.roll(value, shift, axis=value.ndim - 1)
        total = value if total is None else jnp.where(lane >= first, value, total)
    return total


def _span(index, size):
    return slice(size * index, size * index + size)


def _moved(pairs, sems):
    copies = [pltpu.make_async_copy(source, target, sems.at[order]) for order, (source, target) in enumerate(pairs)]
    for copy in copies:
        copy.start()
    return copies


def _all_done(copies):
    for copy in copies:
        copy.wait()


def _head_spots(heads):
    return [[(head, 0, heads * half + head) for head in range(heads)]
            + [(heads + 2 + head, 3, heads * half + head) for head in range(heads)] for half in TWO]


def pack_kernel(chips, *refs):
    sources, (rows_hbm, down_hbm), arrays, refs = refs[:6], refs[6:8], refs[8:14], refs[14:]
    rows_out, down_out, wide, in_sems, out_sems = refs
    k_ref, v_ref, up_ref, down_ref = arrays[1], arrays[2], arrays[4], arrays[5]
    rows, layers, _ = up_ref.shape
    block, _, width = down_ref.shape
    heads = arrays[0].shape[1] // 2
    half_f = STAGES * chips * ROWS
    inward = _moved(zip(sources, arrays), in_sems)
    _all_done(inward[:QKV])
    for half, spots in enumerate(_head_spots(heads)):
        for at, which, head in spots:
            rows_out[half, :, :, _span(at, LANES)] = jnp.swapaxes(
                arrays[which][:, head].astype(jnp.float32), 0, 1).astype(jnp.bfloat16)
        for layer in range(layers):
            for at, ref in ((heads, k_ref), (heads + 1, v_ref)):
                rows_out[half, layer, :, _span(at, LANES)] = ref[layer].astype(
                    jnp.float32)[:, half].astype(jnp.bfloat16)
    inward[QKV].wait()
    wide[ALL] = jnp.swapaxes(up_ref[ALL].astype(jnp.float32), 0, 1)
    lane = lax.broadcasted_iota(jnp.int32, (layers, rows, LANES), 2)
    tiles = _pieces(_moves(chips, block, True), 2 * half_f)
    outward = []
    for half in TWO:
        for index in range(half_f // LANES):
            tile = tiles[half * (half_f // LANES) + index]
            value = _gather_tile(lambda source: wide[:, :, _span(source, LANES)], tile, lane)
            if LANES * index >= 2 * chips * ROWS:
                position = lax.rem(lane + LANES * index % ROWS, ROWS)
                value = jnp.where(position < block - 2 * ROWS, value, 0.0)
            rows_out[half, :, :, _span(2 * ATTN + index, LANES)] = value.astype(jnp.bfloat16)
        outward += _moved([(rows_out.at[half], rows_hbm.at[half])], out_sems.at[half:half + 1])
    inward[5].wait()
    for part in COLORS:
        used = min(ROWS, block - ROWS * part)
        both = jnp.swapaxes(down_ref[ROWS * part:ROWS * part + used].astype(jnp.float32), 0, 1)
        for layer in range(layers):
            one = both[layer]
            if used < ROWS:
                one = jnp.concatenate([one, jnp.zeros((ROWS - used, width), jnp.float32)], axis=0)
            down_out[layer, :, _span(part, width)] = one.astype(jnp.bfloat16)
    _all_done(outward + _moved([(down_out, down_hbm)], out_sems.at[2:3]))


def _bounced(kernel, name, inputs, outs, arrays, n_sems):
    hbm = pl.BlockSpec(memory_space=pl.ANY)
    scratch = [pltpu.VMEM(array.shape, array.dtype) for array in arrays]
    return pl.pallas_call(
        kernel, name=name, out_shape=tuple(outs), in_specs=[hbm] * len(inputs), out_specs=(hbm,) * len(outs),
        scratch_shapes=scratch + [pltpu.SemaphoreType.DMA((size,)) for size in n_sems],
        compiler_params=pltpu.CompilerParams(vmem_limit_bytes=VMEM_LIMIT))(*inputs)


def pack_weights(w_q, w_k, w_v, w_o, w_up, w_down, chips):
    layers, rows = w_up.shape[:2]
    shape = jax.ShapeDtypeStruct
    inputs = [w_q.transpose(1, 2, 0, 3), w_k, w_v, w_o.transpose(1, 2, 0, 3), w_up.transpose(1, 0, 2),
              w_down.transpose(1, 0, 2)]
    outs = [shape((2, layers, rows, UP_END), jnp.bfloat16), shape((layers, ROWS, 3 * w_down.shape[2]), jnp.bfloat16)]
    return _bounced(functools.partial(pack_kernel, chips), "pack_weights", inputs, outs,
                    inputs + outs + [shape(w_up.shape, jnp.float32)], (6, 3))


def unpack_kernel(chips, *refs):
    sources, results, arrays, (in_sems, out_sems, down_sems) = refs[:4], refs[4:12], refs[12:23], refs[23:]
    rows_ref, down_ref, q_out, k_out, v_out, o_out, up_out, down_out = arrays[:2] + arrays[4:10]
    short = arrays[10]
    rows, layers, cols = up_out.shape
    block, _, width = down_out.shape
    heads = q_out.shape[1] // 2
    order = (1, 0, 2, 3)
    inward = _moved([(sources[which], arrays[which]) for which in order], in_sems)
    inward[0].wait()
    pairs = []
    for part in COLORS:
        used = min(ROWS, block - ROWS * part)
        for layer in range(layers):
            source = down_ref.at[layer, :, _span(part, width)]
            if used < ROWS:
                short[layer] = down_ref[layer, :used, _span(part, width)]
                source = short.at[layer]
            pairs.append((source,
                          results[5].at[ROWS * part:ROWS * part + used, layer, :]))
    outward = _moved(pairs, down_sems)
    inward[1].wait()
    lane = lax.broadcasted_iota(jnp.int32, (layers, rows, LANES), 2)
    per_half = STAGES * chips * ROWS // LANES

    def load(source):
        half, tile = divmod(source, per_half)
        return rows_ref[half, :, :, _span(2 * ATTN + tile, LANES)]

    _all_done(inward[2:])
    outward += _moved(zip(arrays[2:4], results[6:]), out_sems.at[1:])
    for index, tile in enumerate(_pieces(_moves(chips, block, False), cols)):
        up_out[:, :, _span(index, LANES)] = jnp.swapaxes(_gather_tile(load, tile, lane), 0, 1)
    outward += _moved([(up_out, results[4])], out_sems.at[STAGES:])
    for half, spots in enumerate(_head_spots(heads)):
        for at, which, head in spots:
            (q_out, o_out)[which // 3][:, head] = jnp.swapaxes(rows_ref[half, :, :, _span(at, LANES)], 0, 1)
        for layer in range(layers):
            for at, ref in ((heads, k_out), (heads + 1, v_out)):
                ref[layer, :, half, :] = rows_ref[half, layer, :, _span(at, LANES)]
    _all_done(outward + _moved(zip((q_out, k_out, v_out, o_out), results), out_sems.at[QKV:]))


def unpack_grads(row_grad, down_grad, y_loc, grad_x, shapes, chips):
    q_shape, k_shape, _, _, up_shape, down_shape = shapes
    layers, rows, heads, head_dim = q_shape
    shape = jax.ShapeDtypeStruct
    turned = [(rows, heads, layers, head_dim), k_shape, k_shape, (rows, heads, layers, head_dim),
              (rows, layers, up_shape[2]), (down_shape[1], layers, down_shape[2])]
    turned = [shape(full, jnp.float32) for full in turned]
    inputs = [row_grad, down_grad, y_loc, grad_x]
    outs = _bounced(functools.partial(unpack_kernel, chips), "unpack_grads", inputs,
                    turned + [shape(value.shape, value.dtype) for value in (y_loc, grad_x)], inputs + turned + [shape((layers, down_shape[1] - 2 * ROWS, down_shape[2]), jnp.float32)], (4, 8, 6))
    d_q, d_k, d_v, d_o, d_up, d_down, y_out, dx_out = outs
    return (y_out[None], dx_out[None], d_q.transpose(2, 0, 1, 3), d_k, d_v, d_o.transpose(2, 0, 1, 3),
            d_up.transpose(1, 0, 2), d_down.transpose(1, 0, 2))


def solution(mesh):
    mesh4 = Mesh(mesh.devices.reshape(CUBE + (2,)), ALL_AXES)
    row_spec = P(ALL_AXES)
    weight_spec = P(None, ALL_AXES)

    def body(x_in, w_q, w_k, w_v, w_o, w_up, w_down, grad_out):
        weights = (w_q, w_k, w_v, w_o, w_up, w_down)
        chips = w_up.shape[2] // w_down.shape[1] // 2
        rows, down = pack_weights(*weights, chips)
        y_loc, grad_x, row_grad, down_grad = train_stack(x_in[0], grad_out[0], rows, down)
        return unpack_grads(row_grad, down_grad, y_loc, grad_x, [weight.shape for weight in weights], chips)

    return jax.shard_map(body, mesh=mesh4, in_specs=(row_spec,) + (weight_spec,) * 6 + (row_spec,),
                         out_specs=(row_spec, row_spec) + (weight_spec,) * 6, check_vma=False)
```

```python
import functools

import jax
import jax.numpy as jnp
from jax import lax
from jax.experimental import pallas as pl
from jax.experimental.pallas import tpu as pltpu
from jax.sharding import Mesh, PartitionSpec as P

MESH = pl.DeviceIdType.MESH
ALL_AXES = ("z", "y", "x", "c")
EPS = 1e-6
MASK_FILL = -1e30
DIMS = ("z", "y", "x")
ORDERS = (("x", "y", "z"), ("y", "z", "x"), ("z", "x", "y"))
COLS = 256
ROWS = 24
LAG = 2
WIDE = COLS // 2
HALF_ROWS = ROWS // 2
HEAD = 128
PER_HALF = 43
UP_BLOCKS = 25
UP_END = UP_BLOCKS * COLS
RING = 4
STAGES = 3
FINAL = STAGES - 1
CUBE = (RING, RING, RING)
CHIPS = RING ** STAGES
SLOTS = 3
TILE = 8
COLORS = range(3)
TWO = range(2)
SIX = range(6)
ALL = Ellipsis
EVERY = slice(None)
QKV, ATTN, FF = 4, 7, 18
DOWN_DONE = FF
UP_DONE = DOWN_DONE + FF
O_DONE = UP_DONE + ATTN - QKV
SIXTH = 6
DH_AT = SIXTH
O_AT = DH_AT + UP_DONE
QKV_AT = O_AT + SIXTH
NORM_MLP, GRAD, NORM_ATTN = 6, 7, 8
VMEM_LIMIT = 67043328


FIFTH = UP_END // 5
GELU_A = 0.7978845608028654
GELU_B = GELU_A * 0.044715
GELU_C = 0.5 * GELU_A
GELU_D = 1.5 * GELU_B
GATHER_SLOTS = SIXTH * LAG + RING


def _rows(color):
    return slice(TILE * color, TILE * color + TILE)


def _rem(value, by):
    return lax.rem(value, by)


def _block(color, stage, position):
    dims = tuple(dim for dim in DIMS if dim not in ORDERS[color][:stage])
    return tuple(position if dim == ORDERS[color][stage] else EVERY for dim in dims)


def _dot(left, right):
    return jnp.dot(left, right, preferred_element_type=jnp.float32)


def _dot_rhs_t(left, right):
    return lax.dot_general(left, right, (((1,), (1,)), ((), ())), preferred_element_type=jnp.float32)


def _dot_lhs_t(left, right):
    return lax.dot_general(left, right, (((0,), (0,)), ((), ())), preferred_element_type=jnp.float32)


def _at(start, size):
    return pl.ds(pl.multiple_of(start, size), size)


def _causal(seq):
    return (lax.rem(lax.broadcasted_iota(jnp.int32, (2 * seq, seq), 0), seq)
            >= lax.broadcasted_iota(jnp.int32, (2 * seq, seq), 1))


def _under(block):
    return jnp.concatenate([block[:, :HEAD], block[:, HEAD:]], axis=0)


def _beside(stacked):
    seq = stacked.shape[0] // 2
    return jnp.concatenate([stacked[:seq], stacked[seq:]], axis=1)


def _probs(query, key, causal):
    scores = jnp.where(causal, _dot_rhs_t(query, key) * (HEAD ** -0.5), MASK_FILL)
    weight = jnp.exp(scores - jnp.max(scores, axis=-1, keepdims=True))
    return weight / jnp.sum(weight, axis=-1, keepdims=True)


def _rms(values):
    wide = values.astype(jnp.float32)
    return (wide * lax.rsqrt(jnp.mean(wide * wide, axis=-1, keepdims=True) + EPS)).astype(jnp.bfloat16)


def _rms_back(values, grad):
    wide = values.astype(jnp.float32)
    scale = lax.rsqrt(jnp.mean(wide * wide, axis=-1, keepdims=True) + EPS)
    return scale * grad - wide * (scale * scale * scale) * jnp.mean(wide * grad, axis=-1, keepdims=True)


class Torus:
    def __init__(self, credit):
        self.core = lax.axis_index("c")
        self.place = {dim: lax.axis_index(dim) for dim in DIMS}
        self.near = tuple({dim: _rem(self.place[dim] + step, RING) for dim in DIMS} for step in (1, 3))
        self.far = {dim: _rem(self.place[dim] + 2, RING) for dim in DIMS}
        self.sibling = {"c": 1 - self.core}
        self.sides = ((0, self.core), (1, 1 - self.core))
        self.credit = credit
        self.partners = [({dim: self.near[way][dim]}, 2 * d + 1 - way, 2 * d + way)
                         for d, dim in enumerate(DIMS) for way in TWO]
        self.partners.append((self.sibling, 6, 6))

    def meet(self):
        barrier = pltpu.get_barrier_semaphore()
        for device, _, _ in self.partners:
            pl.semaphore_signal(barrier, inc=1, device_id=device, device_id_type=MESH)
        pl.semaphore_wait(barrier, len(self.partners))

    def remote(self, source, target, send_sem, recv_sem, device):
        return pltpu.make_async_remote_copy(src_ref=source, dst_ref=target, send_sem=send_sem, recv_sem=recv_sem,
                                            device_id=device, device_id_type=MESH)

    def run(self, steps, n_chunks, n_ticks, after):
        def tick(now, carry):
            @pl.when(now >= 2)
            def _():
                for _, _, mine in self.partners:
                    pl.semaphore_wait(self.credit.at[mine], 1)

            for lag, action in steps:
                @pl.when((now >= lag) & (now < lag + n_chunks))
                def _(lag=lag, action=action):
                    action(now - lag)
            after(now)

            @pl.when(now < n_ticks - 2)
            def _():
                for device, theirs, _ in self.partners:
                    pl.semaphore_signal(self.credit.at[theirs], inc=1, device_id=device, device_id_type=MESH)
            return carry

        lax.fori_loop(0, n_ticks, tick, 0)


def forward_steps(torus, n_layers, x_ref, rows_ref, down_ref, y_ref, saved, wbuf, peer, shard, twin, state, lefts, rights,
                  q_buf, k_buf, v_buf, hid_buf, acc, ring_send, ring_recv, pair_send, pair_recv, keep_sem, save_sem,
                  hid_sem, twin_sem):
    acts, w_out, hid_out, gelu_out, norm_out, q_out, k_out, v_out, o_out = saved
    core, place, near = torus.core, torus.place, torus.near
    slots = GATHER_SLOTS
    n_chunks = n_layers * PER_HALF
    ready = SIXTH * LAG
    seq = state.shape[0]
    third = CHIPS * ROWS
    last = n_layers - 1
    pieces = [(0, EVERY, slice(0, FIFTH)), (0, EVERY, slice(FIFTH, None))] + [
        (layer, EVERY, EVERY) for layer in range(1, n_layers)]
    swaps = [torus.remote(rows_ref.at[(1 - core,) + piece], twin.at[piece], twin_sem.at[0, order], twin_sem.at[1, order],
                          torus.sibling) for order, piece in enumerate(pieces)]
    for swap in swaps:
        swap.start()
    swaps[0].wait_send()
    swaps[0].wait_recv()

    def assemble(chunk):
        @pl.when(chunk == 1)
        def _():
            for swap in swaps[1:]:
                swap.wait_send()
                swap.wait_recv()

        @pl.when(chunk < 5 * n_layers)
        def _():
            layer, part = chunk // 5, _rem(chunk, 5)
            cols = _at(part * FIFTH, FIFTH)
            mine, other = [ref[layer, :, cols].astype(jnp.float32) for ref in (rows_ref.at[core], twin)]
            shard[layer, :, cols] = jnp.concatenate(
                [jnp.where(core == 0, mine, other), jnp.where(core == 0, other, mine)], axis=0).astype(jnp.bfloat16)

            @pl.when(part == 4)
            def _():
                shard[layer, :, UP_END:] = down_ref[layer]

    def columns(chunk):
        return _at(_rem(chunk, PER_HALF) * COLS, COLS)

    def spot(slot, color, stage, position, cols):
        order = ORDERS[color]
        index = tuple(EVERY if dim in order[:stage] else position if dim == order[stage] else place[dim]
                      for dim in DIMS)
        return wbuf.at[(slot,) + index + (_rows(color), cols)]

    halves = (slice(0, WIDE), slice(WIDE, COLS))

    def send_own(stage, chunk):
        slot, sem = _rem(chunk, slots), _rem(chunk, RING)
        for color in COLORS:
            dim = ORDERS[color][stage]
            here = spot(slot, color, stage, place[dim], slice(0, COLS))
            source = here
            if stage == 0:
                source = shard.at[chunk // PER_HALF, _rows(color), columns(chunk)]
            for way in TWO:
                torus.remote(source, here, ring_send.at[2 * stage, sem], ring_recv.at[2 * stage, sem],
                             {dim: near[way][dim]}).start()

    def send_far(stage, chunk):
        slot, sem = _rem(chunk, slots), _rem(chunk, RING)
        for color in COLORS:
            dim = ORDERS[color][stage]
            for way in TWO:
                block = spot(slot, color, stage, near[1 - way][dim], halves[way])
                torus.remote(block, block, ring_send.at[2 * stage + 1, sem], ring_recv.at[2 * stage + 1, sem],
                             {dim: near[way][dim]}).start()

    def arrived(part, chunk):
        slot, sem = _rem(chunk, slots), _rem(chunk, RING)
        count = slice(0, 2) if part % 2 == 0 else 0
        block = wbuf.at[(slot,) + (0,) * (2 - part // 2) + (count,)]
        whole = torus.remote(block, block, ring_send.at[part, sem], ring_recv.at[part, sem], torus.sibling)
        whole.wait_send()
        whole.wait_recv()

    def enter(chunk):
        wbuf[_rem(chunk, slots), place["z"], place["y"], place["x"]] = shard[chunk // PER_HALF, :, columns(chunk)]
        send_own(0, chunk)

    def pass_on(part, chunk):
        arrived(part, chunk)
        if part % 2 == 0:
            send_far(part // 2, chunk)
        else:
            send_own(part // 2 + 1, chunk)

    def pair_copy(chunk):
        slot = _rem(chunk, RING)
        return torus.remote(wbuf.at[_rem(chunk, slots)], peer.at[slot], pair_send.at[slot], pair_recv.at[slot],
                            torus.sibling)

    def exchange(chunk):
        arrived(5, chunk)
        pair_copy(chunk).start()

    def keep_copy(chunk):
        return pltpu.make_async_copy(wbuf.at[_rem(chunk, slots)],
                                     w_out.at[chunk // PER_HALF, :, :, :, :, columns(chunk)],
                                     keep_sem.at[_rem(chunk, RING)])

    def save_copies(layer, names):
        parts = {"n0": (lefts.at[NORM_ATTN], norm_out.at[layer, 0]), "n1": (lefts.at[NORM_MLP], norm_out.at[layer, 1]),
                 "q": (q_buf, q_out.at[layer]), "k": (k_buf, k_out.at[layer]), "v": (v_buf, v_out.at[layer]),
                 "o": (rights.at[O_AT:QKV_AT], o_out.at[layer]), "a": (lefts.at[:NORM_MLP], gelu_out.at[layer]),
                 "mid": (state, acts.at[2 * layer]), "end": (state, acts.at[2 * layer + 1])}
        places = list(parts)
        return [pltpu.make_async_copy(*parts[name], save_sem.at[places.index(name)]) for name in names]

    def save(layer, names):
        @pl.when(layer < last)
        def _():
            for copy in save_copies(layer, names):
                copy.start()

    def saved_all(layer, names):
        @pl.when(layer < last)
        def _():
            for copy in save_copies(layer, names):
                copy.wait()

    def hidden_copies(layer, order):
        slot, part, at = _rem(order, 2), order // SIXTH, _at(_rem(order, SIXTH) * COLS, COLS)
        return [pltpu.make_async_copy(hid_buf.at[slot, half], hid_out.at[layer, part, half, :, at],
                                      hid_sem.at[slot, half]) for half in TWO]

    def compute(chunk):
        layer, index = chunk // PER_HALF, _rem(chunk, PER_HALF)
        pair = pair_copy(chunk)
        pair.wait_send()
        pair.wait_recv()
        keep_copy(chunk).start()

        def weights(role):
            block = wbuf[_rem(chunk, slots)] if role == 0 else peer[_rem(chunk, RING)]
            return block.reshape(third, COLS)

        @pl.when(index == 0)
        def _():
            lefts[NORM_ATTN] = _rms(state[ALL])
            save(layer, ["n0"])

        @pl.when(index < 3)
        def _():
            for role, half in torus.sides:
                q_buf[:, _at(STAGES * COLS * half + COLS * index, COLS)] = _dot(
                    lefts[NORM_ATTN], weights(role)).astype(jnp.bfloat16)

        @pl.when(index == 3)
        def _():
            for role, half in torus.sides:
                both = _dot(lefts[NORM_ATTN], weights(role)).astype(jnp.bfloat16)
                k_buf[:, _at(HEAD * half, HEAD)] = both[:, :HEAD]
                v_buf[:, _at(HEAD * half, HEAD)] = both[:, HEAD:]

        @pl.when(index == QKV)
        def _():
            acc[ALL] = jnp.zeros_like(acc)
            save(layer, ["q", "k", "v"])

        @pl.when((index >= QKV) & (index < ATTN))
        def _():
            causal = _causal(seq)
            queries = [_under(q_buf[:, _at(STAGES * COLS * half + COLS * (index - QKV), COLS)]) for _, half in torus.sides]
            probs = [_probs(queries[role], k_buf[:, _at(HEAD * half, HEAD)], causal).astype(jnp.bfloat16)
                     for role, half in torus.sides]
            blocks = [_beside(_dot(probs[role], v_buf[:, _at(HEAD * half, HEAD)]).astype(jnp.bfloat16))
                      for role, half in torus.sides]
            acc[ALL] += sum(_dot_rhs_t(blocks[role], weights(role)) for role in TWO)
            for role, half in torus.sides:
                rights[O_AT + STAGES * half + index - QKV] = blocks[role]

        @pl.when(index == ATTN - 1)
        def _():
            @pl.when(layer > 0)
            def _():
                saved_all(layer - 1, ["end"])
            middle = (state[ALL].astype(jnp.float32) + acc[ALL]).astype(jnp.bfloat16)
            state[ALL] = middle
            lefts[NORM_MLP] = _rms(middle)
            save(layer, ["n1", "o"])
            mid = save_copies(layer, ["mid"])[0]
            mid.start()

        @pl.when((index > ATTN) & (index <= UP_BLOCKS))
        def _():
            for copy in hidden_copies(layer, index - ATTN - 1):
                copy.wait()

        @pl.when((index >= ATTN) & (index < UP_BLOCKS))
        def _():
            order = index - ATTN
            for role, half in torus.sides:
                hidden = _dot(lefts[NORM_MLP], weights(role))
                hid_buf[_rem(order, 2), half] = hidden
                lefts[STAGES * half + order // SIXTH, :, _at(COLS * _rem(order, SIXTH), COLS)] = jax.nn.gelu(
                    hidden).astype(jnp.bfloat16)
            for copy in hidden_copies(layer, order):
                copy.start()

        @pl.when(index == UP_BLOCKS)
        def _():
            save(layer, ["a"])
            save_copies(layer, ["mid"])[0].wait()

        @pl.when(index >= UP_BLOCKS)
        def _():
            part, at = (index - UP_BLOCKS) // SIXTH, _at(COLS * _rem(index - UP_BLOCKS, SIXTH), COLS)
            total = sum(_dot(lefts[STAGES * half + part], weights(role)) for role, half in torus.sides)

            @pl.when(part == 0)
            def _():
                acc[:, at] = total

            @pl.when(part > 0)
            def _():
                acc[:, at] += total

        @pl.when(index == PER_HALF - 1)
        def _():
            saved_all(layer, ["n0", "n1", "q", "k", "v", "o", "a"])
            result = (state[ALL].astype(jnp.float32) + acc[ALL]).astype(jnp.bfloat16)
            state[ALL] = result
            save(layer, ["end"])

            @pl.when(layer == last)
            def _():
                pltpu.make_async_copy(state, y_ref, save_sem.at[9]).start()

        keep_copy(chunk).wait()

    steps = [(0, assemble), (0, enter)]
    steps += [((part + 1) * LAG, functools.partial(pass_on, part)) for part in range(5)]
    return steps + [(ready, exchange), (ready + 1, compute)]


def backward_steps(torus, n_layers, x_ref, x_out, saved, out, wbuf, lefts, rights, hid_buf, dact, dnorm, q_buf,
                   k_buf, v_buf, x_buf, dk_acc, dv_acc, sums, half_bufs, full_bufs, load_sem, own_sem, push_send,
                   push_recv, pair_send, pair_recv, ring_send, ring_recv):
    acts, w_own, hid_in, gelu_in, norm_in, q_in, k_in, v_in, o_in = saved
    place, near = torus.place, torus.near
    seq = k_buf.shape[0]
    third = CHIPS * ROWS
    last = n_layers - 1

    def mine_slot(chunk):
        return GATHER_SLOTS + _rem(chunk, 2)

    def out_slot(chunk):
        return GATHER_SLOTS + 2 + _rem(chunk, 2)

    def their_slot(chunk):
        return 7 + _rem(chunk, SLOTS)

    def peer_slot(chunk):
        order = _rem(chunk, RING)
        return jnp.where(order == 0, 6, jnp.where(order == 3, 10, GATHER_SLOTS + 3 + order))

    def pair_of(chunk):
        return last - chunk // PER_HALF

    def columns(chunk):
        index = _rem(chunk, PER_HALF)
        block = jnp.where(index < DOWN_DONE, UP_BLOCKS + index,
                          jnp.where(index < UP_DONE, index - 11, jnp.where(index < O_DONE, index - 32, index - 39)))
        return _at(block * COLS, COLS)

    def loads(pair, names):
        parts = {"a": (gelu_in.at[pair], lefts.at[:NORM_MLP]), "n_mlp": (norm_in.at[pair, 1], lefts.at[NORM_MLP]),
                 "n_attn": (norm_in.at[pair, 0], lefts.at[NORM_ATTN]), "o": (o_in.at[pair], rights.at[O_AT:QKV_AT]),
                 "q": (q_in.at[pair], q_buf), "k": (k_in.at[pair], k_buf), "v": (v_in.at[pair], v_buf),
                 "x_mid": (acts.at[2 * pair], x_buf)}
        places = list(parts)
        return [pltpu.make_async_copy(*parts[name], load_sem.at[places.index(name)]) for name in names]

    def start(pair, names):
        for copy in loads(pair, names):
            copy.start()

    def finish(pair, names):
        for copy in loads(pair, names):
            copy.wait()

    def first_input(ref):
        return pltpu.make_async_copy(ref, x_buf, load_sem.at[9])

    def hidden_load(pair, part, half):
        return pltpu.make_async_copy(hid_in.at[pair, part, half], hid_buf, load_sem.at[8])

    def own_copy(chunk):
        return pltpu.make_async_copy(w_own.at[pair_of(chunk), :, :, :, :, columns(chunk)], wbuf.at[mine_slot(chunk)],
                                     own_sem.at[_rem(chunk, 2)])

    def push_copy(chunk):
        slot = _rem(chunk, SLOTS)
        return torus.remote(w_own.at[pair_of(chunk), :, :, :, :, columns(chunk)], wbuf.at[their_slot(chunk)],
                            push_send.at[slot], push_recv.at[slot], torus.sibling)

    def fetch(chunk):
        own_copy(chunk).start()
        push_copy(chunk).start()

    def total_grad():
        return jnp.concatenate([rights[block] for block in SIX], axis=1).astype(jnp.float32)

    def consume(chunk):
        pair, index = pair_of(chunk), _rem(chunk, PER_HALF)
        own_copy(chunk).wait()
        push = push_copy(chunk)
        push.wait_send()
        push.wait_recv()

        def weights(role):
            return wbuf[(mine_slot, their_slot)[role](chunk)].reshape(third, COLS)

        @pl.when(index == 0)
        def _():
            start(pair, ["x_mid"])

            @pl.when(pair < last)
            def _():
                start(pair, ["n_mlp", "n_attn", "o", "q", "k", "v"])

        def bend_back(part, half):
            hidden_load(pair, part, half).wait()
            for block in SIX:
                cols = slice(COLS * block, COLS * block + COLS)
                hidden = hid_buf[:, cols]
                square = hidden * hidden
                bend = jnp.tanh(hidden * (GELU_A + GELU_B * square))
                slope = (0.5 + 0.5 * bend) + (hidden * (1.0 - bend * bend)) * (GELU_C + GELU_D * square)
                rights[DH_AT + FF * half + SIXTH * part + block] = (dact[half, :, cols] * slope).astype(jnp.bfloat16)

        @pl.when((index > 0) & (index <= DOWN_DONE) & (_rem(index, SIXTH) == 0))
        def _():
            bend_back(index // SIXTH - 1, 1)

        @pl.when((index < DOWN_DONE) & (_rem(index, SIXTH) == 0))
        def _():
            dact[ALL] = jnp.zeros_like(dact)
            hidden_load(pair, index // SIXTH, 0).start()

        @pl.when(index < DOWN_DONE)
        def _():
            products = [_dot_rhs_t(rights[_rem(index, SIXTH)], weights(role)) for role in TWO]
            for role, half in torus.sides:
                dact[half] += products[role]

        @pl.when((index < DOWN_DONE) & (_rem(index, SIXTH) == 5))
        def _():
            bend_back(index // SIXTH, 0)
            hidden_load(pair, index // SIXTH, 1).start()

        @pl.when(index == DOWN_DONE - 1)
        def _():
            @pl.when(pair < last)
            def _():
                finish(pair, ["n_mlp", "n_attn", "o", "q", "k", "v"])

        @pl.when(index == DOWN_DONE)
        def _():
            dnorm[ALL] = jnp.zeros_like(dnorm)

            @pl.when(pair > 0)
            def _():
                start(pair - 1, ["a"])

        @pl.when((index >= DOWN_DONE) & (index < UP_DONE))
        def _():
            dnorm[ALL] += sum(_dot_rhs_t(rights[DH_AT + FF * half + index - DOWN_DONE], weights(role))
                              for role, half in torus.sides)

        @pl.when(index == UP_DONE - 1)
        def _():
            finish(pair, ["x_mid"])
            lefts[GRAD] = (total_grad() + _rms_back(x_buf[ALL], dnorm[ALL])).astype(jnp.bfloat16)

        @pl.when(index == UP_DONE)
        def _():
            @pl.when(pair == 0)
            def _():
                first_input(x_ref).start()

            @pl.when(pair > 0)
            def _():
                first_input(acts.at[2 * pair - 1]).start()
            dk_acc[ALL] = jnp.zeros_like(dk_acc)
            dv_acc[ALL] = jnp.zeros_like(dv_acc)

        @pl.when((index >= UP_DONE) & (index < O_DONE))
        def _():
            causal = _causal(seq)
            keys = [k_buf[:, _at(HEAD * half, HEAD)] for _, half in torus.sides]
            values = [v_buf[:, _at(HEAD * half, HEAD)] for _, half in torus.sides]
            queries = [_under(q_buf[:, _at(STAGES * COLS * half + COLS * (index - UP_DONE), COLS)])
                       for _, half in torus.sides]
            probs = [_probs(queries[role], keys[role], causal) for role in TWO]
            d_heads = [_under(_dot(lefts[GRAD], weights(role)).astype(jnp.bfloat16)) for role in TWO]
            d_probs = [_dot_rhs_t(d_heads[role], values[role]) for role in TWO]
            d_scores = [probs[role] * (d_probs[role] - jnp.sum(probs[role] * d_probs[role], axis=-1, keepdims=True))
                        for role in TWO]
            d_scores = [(d_score * (HEAD ** -0.5)).astype(jnp.bfloat16) for d_score in d_scores]
            d_v = [_dot_lhs_t(probs[role].astype(jnp.bfloat16), d_heads[role]) for role in TWO]
            d_k = [_dot_lhs_t(d_scores[role], queries[role]) for role in TWO]
            d_q = [_beside(_dot(d_scores[role], keys[role]).astype(jnp.bfloat16)) for role in TWO]
            for role, half in torus.sides:
                dv_acc[half] += d_v[role]
                dk_acc[half] += d_k[role]
                rights[QKV_AT + QKV * half + index - UP_DONE] = d_q[role]

        @pl.when(index == O_DONE - 1)
        def _():
            for half in TWO:
                rights[QKV_AT + QKV * half + QKV - 1] = jnp.concatenate([dk_acc[half], dv_acc[half]], axis=1).astype(jnp.bfloat16)

        @pl.when(index == O_DONE)
        def _():
            dnorm[ALL] = jnp.zeros_like(dnorm)

        @pl.when(index >= O_DONE)
        def _():
            dnorm[ALL] += sum(_dot_rhs_t(rights[QKV_AT + QKV * half + index - O_DONE], weights(role))
                              for role, half in torus.sides)

        @pl.when(index == PER_HALF - 1)
        def _():
            first_input(x_ref).wait()

            @pl.when(pair > 0)
            def _():
                finish(pair - 1, ["a"])
            result = (lefts[GRAD].astype(jnp.float32) + _rms_back(x_buf[ALL], dnorm[ALL])).astype(jnp.bfloat16)

            @pl.when(pair == 0)
            def _():
                x_out(result)
            for block in SIX:
                rights[block] = result[:, COLS * block:COLS * block + COLS]

    def pair_copy(chunk):
        slot = _rem(chunk, RING)
        return torus.remote(wbuf.at[out_slot(chunk)], wbuf.at[peer_slot(chunk)], pair_send.at[slot], pair_recv.at[slot],
                            torus.sibling)

    def multiply(chunk):
        index = _rem(chunk, PER_HALF)
        lead = _rem(chunk, sums[0].shape[0])
        quarter = third // RING
        for role, half in torus.sides[::-1]:
            left = jnp.where(index < DOWN_DONE, STAGES * half + index // SIXTH,
                             jnp.where(index < UP_DONE, NORM_MLP, jnp.where(index < O_DONE, GRAD, NORM_ATTN)))
            right = jnp.where(index < DOWN_DONE, _rem(index, SIXTH),
                              jnp.where(index < UP_DONE, DH_AT + FF * half + index - DOWN_DONE,
                                        jnp.where(index < O_DONE, O_AT + STAGES * half + index - UP_DONE,
                                                  QKV_AT + QKV * half + index - O_DONE)))
            for z in range(RING):
                part = _dot_lhs_t(lefts[left, :, quarter * z:quarter * z + quarter], rights[right])
                if role == 0:
                    sums[0][lead, z] = part.reshape(RING, RING, ROWS, COLS)
                else:
                    wbuf[out_slot(chunk), z] = part.astype(jnp.bfloat16).reshape(RING, RING, ROWS, COLS)
        pair_copy(chunk).start()

    def merge_pair(chunk):
        lead = _rem(chunk, sums[0].shape[0])
        pair_copy(chunk).wait_send()
        pair_copy(chunk).wait_recv()
        for z in range(RING):
            for y in range(RING):
                sums[0][lead, z, y] = sums[0][lead, z, y] + wbuf[peer_slot(chunk), z, y].astype(jnp.float32)

    def ring_copy(stage, part, slot, color, way):
        send, recv = (half_bufs, full_bufs)[part][stage]
        dim = ORDERS[color][stage]
        return torus.remote(send.at[slot, color, way], recv.at[slot, color, way],
                            ring_send.at[2 * stage + part, slot], ring_recv.at[2 * stage + part, slot],
                            {dim: near[way][dim]})

    def ring_wait(stage, part, slot):
        send, recv = (half_bufs, full_bufs)[part][stage]
        whole = torus.remote(send.at[slot], recv.at[slot], ring_send.at[2 * stage + part, slot],
                             ring_recv.at[2 * stage + part, slot], torus.sibling)
        whole.wait_send()
        whole.wait_recv()

    def source(stage, chunk, color, position, cols):
        lead = _rem(chunk, sums[stage].shape[0])
        if stage == 0:
            return sums[0][(lead,) + _block(color, 0, position) + (_rows(color), cols)]
        return sums[stage][(lead, color) + _block(color, stage, position) + (EVERY, cols)]

    left_cols, right_cols, every = slice(0, WIDE), slice(WIDE, COLS), slice(0, COLS)

    def store_halves(stage, chunk):
        slot = _rem(chunk, RING)
        send = half_bufs[stage][0]
        for color in COLORS:
            far = torus.far[ORDERS[color][stage]]
            send[slot, color, 0] = source(stage, chunk, color, far, left_cols).astype(jnp.bfloat16)
            send[slot, color, 1] = source(stage, chunk, color, far, right_cols).astype(jnp.bfloat16)

    def store_fulls(stage, chunk):
        slot = _rem(chunk, RING)
        ring_wait(stage, 0, slot)
        recv = half_bufs[stage][1]
        send = full_bufs[stage][0]
        lead = (EVERY,) * (len(send.shape) - 4)
        for color in COLORS:
            dim = ORDERS[color][stage]
            for way, summed, plain in ((0, left_cols, right_cols), (1, right_cols, left_cols)):
                send[(slot, color, way) + lead + (summed,)] = (
                    source(stage, chunk, color, near[way][dim], summed)
                    + recv[slot, color, way].astype(jnp.float32)).astype(jnp.bfloat16)
                send[(slot, color, way) + lead + (plain,)] = source(
                    stage, chunk, color, near[way][dim], plain).astype(jnp.bfloat16)

    def close_stage(stage, chunk):
        slot = _rem(chunk, RING)
        ring_wait(stage, 1, slot)
        recv = full_bufs[stage][1]
        for color in COLORS:
            dim = ORDERS[color][stage]
            total = (source(stage, chunk, color, place[dim], every)
                     + recv[slot, color, 0].astype(jnp.float32)
                     + recv[slot, color, 1].astype(jnp.float32))
            if stage < 2:
                sums[stage + 1][_rem(chunk, sums[stage + 1].shape[0]), color] = total
            else:
                out[pair_of(chunk), _rows(color), columns(chunk)] = total

    def send_all(stage, part, chunk):
        for color in COLORS:
            for way in TWO:
                ring_copy(stage, part, _rem(chunk, RING), color, way).start()

    def open_first(chunk):
        merge_pair(chunk)
        store_halves(0, chunk)
        send_all(0, 0, chunk)

    def middle(stage, chunk):
        store_fulls(stage, chunk)
        send_all(stage, 1, chunk)

    def open_stage(stage, chunk):
        store_halves(stage, chunk)
        send_all(stage, 0, chunk)

    def turn(stage, chunk):
        close_stage(stage, chunk)
        if stage < 2:
            open_stage(stage + 1, chunk)

    return [(0, fetch), (2 * LAG, functools.partial(middle, 0)), (LAG, open_first),
            (3 * LAG, functools.partial(turn, 0)), (4 * LAG, functools.partial(middle, 1)),
            (5 * LAG, functools.partial(turn, 1)), (SIXTH * LAG, functools.partial(middle, 2)),
            (7 * LAG, functools.partial(turn, 2)), (1, consume), (0, multiply)]


def train_kernel(n_layers, x_ref, g_ref, rows_in, down_in, y_ref, dx_ref, rows_hbm, down_hbm, *refs):
    saved, refs = refs[:9], refs[9:]
    (rows_ref, down_ref, rows_out, out), refs = refs[:4], refs[4:]
    (wbuf, peer, shard, twin, state, lefts, rights, q_buf, k_buf, v_buf, hid_out_buf, acc, hid_in_buf, dact, x_buf,
     dk_acc, dv_acc, away), refs = refs[:18], refs[18:]
    sums, half_bufs, full_bufs, refs = refs[:3], refs[3:9], refs[9:15], refs[15:]
    half_bufs = [half_bufs[2 * stage:2 * stage + 2] for stage in COLORS]
    full_bufs = [full_bufs[2 * stage:2 * stage + 2] for stage in COLORS]
    forward_sems, backward_sems, (swap_sem, end_sem, credit) = refs[:8], refs[8:16], refs[16:]
    torus = Torus(credit)
    core = torus.core
    n_chunks = n_layers * PER_HALF
    inward = _moved([(rows_in, rows_ref), (down_in, down_ref)], backward_sems[0])
    fill = pltpu.make_async_copy(x_ref, state, forward_sems[5].at[9])
    fill.start()
    for block in SIX:
        pltpu.make_async_copy(g_ref.at[:, COLS * block:COLS * block + COLS], rights.at[block],
                              backward_sems[0].at[3]).start()
    torus.meet()
    _all_done(inward)
    fill.wait()
    pltpu.make_async_copy(rights.at[:DH_AT], rights.at[:DH_AT], backward_sems[0].at[3]).wait()
    def y_copy():
        return pltpu.make_async_copy(state, y_ref, forward_sems[5].at[9])

    def x_out(result):
        y_copy().wait()
        state[ALL] = result
        pltpu.make_async_copy(state, dx_ref, forward_sems[5].at[9]).start()

    forward = forward_steps(torus, n_layers, x_ref, rows_ref, down_ref, y_ref, saved, wbuf, peer, shard, twin, state, lefts,
                            rights, q_buf, k_buf, v_buf, hid_out_buf, acc, *forward_sems)
    backward = backward_steps(torus, n_layers, x_ref, x_out, saved, out, wbuf, lefts, rights, hid_in_buf, dact, acc,
                              q_buf, k_buf, v_buf, x_buf, dk_acc, dv_acc, sums, half_bufs, full_bufs,
                              *backward_sems)
    turn_at = n_chunks
    backward = [(lag + turn_at, step) for lag, step in backward]
    n_ticks = turn_at + n_chunks + 7 * LAG
    def hand_over(layer, part):
        cols = _at(part * FIFTH, FIFTH)
        both = out[layer, :, cols]
        low, high = both[:HALF_ROWS], both[HALF_ROWS:]
        rows_out[core, layer, :, cols] = jnp.where(core == 0, low, high)
        away[layer, :, cols] = jnp.where(core == 0, high, low)
        torus.remote(away.at[layer, :, cols], rows_out.at[core, layer, :, cols], swap_sem.at[0, layer],
                     swap_sem.at[1, layer], torus.sibling).start()

    def down_result(layer):
        return pltpu.make_async_copy(out.at[layer, :, UP_END:], down_hbm.at[layer], end_sem.at[0, layer])

    def rows_result(layer):
        return pltpu.make_async_copy(rows_out.at[:, layer], rows_hbm.at[:, layer], end_sem.at[1, layer])

    def rows_meet(layer):
        swap = torus.remote(away.at[layer], rows_out.at[core, layer], swap_sem.at[0, layer], swap_sem.at[1, layer],
                            torus.sibling)
        swap.wait_send()
        swap.wait_recv()
        rows_result(layer).start()

    def hand_on(now):
        for layer in range(n_layers):
            begin = turn_at + (n_layers - layer) * PER_HALF + 8 * LAG

            @pl.when(now == begin - UP_BLOCKS)
            def _(layer=layer):
                down_result(layer).start()

            if layer > 0:
                @pl.when((now >= begin) & (now < begin + 5))
                def _(layer=layer, begin=begin):
                    hand_over(layer, now - begin)

                @pl.when(now == begin + 8)
                def _(layer=layer):
                    rows_meet(layer)

        @pl.when((now >= n_ticks - ATTN) & (now < n_ticks - ATTN + QKV))
        def _():
            hand_over(0, n_ticks - STAGES - now)

    torus.run(backward[:1] + forward + backward[1:], n_chunks, n_ticks, hand_on)
    hand_over(0, 0)
    rows_meet(0)
    for layer in range(n_layers):
        _all_done([down_result(layer), rows_result(layer)])
    pltpu.make_async_copy(state, dx_ref, forward_sems[5].at[9]).wait()


def train_stack(x_loc, g_loc, rows, down):
    n_layers = down.shape[0]
    seq, width = x_loc.shape
    bf16, f32 = jnp.bfloat16, jnp.float32
    half = WIDE
    chunk = CUBE + (ROWS, COLS)
    shape = jax.ShapeDtypeStruct
    hbm = pl.BlockSpec(memory_space=pl.ANY)
    vmem = pl.BlockSpec(memory_space=pltpu.VMEM)
    dma = pltpu.SemaphoreType.DMA
    saved = (shape((2 * n_layers - 1, seq, width), bf16), shape((n_layers,) + CUBE + (ROWS, PER_HALF * COLS), bf16),
             shape((n_layers, 3, 2, seq, width), f32), shape((n_layers, SIXTH, seq, width), bf16),
             shape((n_layers, 2, seq, width), bf16), shape((n_layers, seq, width), bf16),
             shape((n_layers, seq, 2 * HEAD), bf16), shape((n_layers, seq, 2 * HEAD), bf16),
             shape((n_layers, SIXTH, seq, COLS), bf16))
    scratch = [pltpu.VMEM(full, kind) for full, kind in (
        (rows.shape, bf16), (down.shape, bf16),
        ((2, n_layers, HALF_ROWS, UP_END), f32), ((n_layers, ROWS, PER_HALF * COLS), f32),
        ((GATHER_SLOTS + 6,) + chunk, bf16), ((RING,) + chunk, bf16), ((n_layers, ROWS, PER_HALF * COLS), bf16),
        (rows.shape[1:], bf16), ((seq, width), bf16), ((9, seq, width), bf16), ((56, seq, COLS), bf16),
        ((seq, SIXTH * COLS), bf16), ((seq, 2 * HEAD), bf16), ((seq, 2 * HEAD), bf16), ((2, 2, seq, COLS), f32),
        ((seq, width), f32), ((seq, width), f32), ((2, seq, width), f32), ((seq, width), bf16),
        ((2, seq, HEAD), f32), ((2, seq, HEAD), f32), ((n_layers, HALF_ROWS, UP_END), f32), ((6,) + chunk, f32),
        ((5, 3, RING, RING, TILE, COLS), f32), ((5, 3, RING, TILE, COLS), f32))]
    for cols in (half, COLS):
        for size in ((RING, RING), (RING,), ()):
            scratch += [pltpu.VMEM((RING, 3, 2) + size + (TILE, cols), bf16)] * 2
    scratch += [dma((SIXTH, RING)), dma((SIXTH, RING)), dma((RING,)), dma((RING,)), dma((RING,)), dma((10,)), dma((2, 2)), dma((2, n_layers + 1))]
    scratch += [dma((10,)), dma((2,)), dma((SLOTS,)), dma((SLOTS,)), dma((RING,)), dma((RING,)), dma((SIXTH, RING)),
                dma((SIXTH, RING)), dma((2, n_layers)), dma((2, n_layers)), pltpu.SemaphoreType.REGULAR((7,))]
    return pl.pallas_call(
        functools.partial(train_kernel, n_layers), name="train_stack",
        out_shape=(shape((seq, width), bf16), shape((seq, width), bf16), shape((2, n_layers, HALF_ROWS, UP_END), f32),
                   shape(down.shape, f32)) + saved,
        in_specs=[hbm] * 4, out_specs=(hbm,) * (4 + len(saved)), scratch_shapes=scratch,
        compiler_params=pltpu.CompilerParams(collective_id=0, has_side_effects=True, vmem_limit_bytes=VMEM_LIMIT),
    )(x_loc, g_loc, rows, down)[:4]


LANES = 128


def _moves(chips, block, packed_first):
    moves = []
    for half in TWO:
        for part in COLORS:
            for chip in range(chips):
                packed = chips * ROWS * (STAGES * half + part) + ROWS * chip
                plain = block * (2 * chip + half) + ROWS * part
                pair = (packed, plain) if packed_first else (plain, packed)
                moves.append(pair + (min(ROWS, block - ROWS * part),))
    return moves


def _pieces(moves, size):
    tiles = [[] for _ in range(size // LANES)]
    for target, source, length in moves:
        while length:
            step = min(length, LANES - target % LANES, LANES - source % LANES)
            tiles[target // LANES].append((target % LANES, source // LANES, (target - source) % LANES))
            target, source, length = target + step, source + step, length - step
    return [sorted(tile) for tile in tiles]


def _gather_tile(load, tile, lane):
    total = None
    for first, source, shift in tile:
        value = load(source)
        if shift:
            value = pltpu.roll(value, shift, axis=value.ndim - 1)
        total = value if total is None else jnp.where(lane >= first, value, total)
    return total


def _span(index, size):
    return slice(size * index, size * index + size)


def _moved(pairs, sems):
    copies = [pltpu.make_async_copy(source, target, sems.at[order]) for order, (source, target) in enumerate(pairs)]
    for copy in copies:
        copy.start()
    return copies


def _all_done(copies):
    for copy in copies:
        copy.wait()


def _head_spots(heads):
    return [[(head, 0, heads * half + head) for head in range(heads)]
            + [(heads + 2 + head, 3, heads * half + head) for head in range(heads)] for half in TWO]


def pack_kernel(chips, *refs):
    sources, (rows_hbm, down_hbm), arrays, refs = refs[:6], refs[6:8], refs[8:14], refs[14:]
    rows_out, down_out, wide, in_sems, out_sems = refs
    k_ref, v_ref, up_ref, down_ref = arrays[1], arrays[2], arrays[4], arrays[5]
    rows, layers, _ = up_ref.shape
    block, _, width = down_ref.shape
    heads = arrays[0].shape[1] // 2
    half_f = STAGES * chips * ROWS
    inward = _moved(zip(sources, arrays), in_sems)
    _all_done(inward[:QKV])
    for half, spots in enumerate(_head_spots(heads)):
        for at, which, head in spots:
            rows_out[half, :, :, _span(at, LANES)] = jnp.swapaxes(
                arrays[which][:, head].astype(jnp.float32), 0, 1).astype(jnp.bfloat16)
        for layer in range(layers):
            for at, ref in ((heads, k_ref), (heads + 1, v_ref)):
                rows_out[half, layer, :, _span(at, LANES)] = ref[layer].astype(
                    jnp.float32)[:, half].astype(jnp.bfloat16)
    inward[QKV].wait()
    wide[ALL] = jnp.swapaxes(up_ref[ALL].astype(jnp.float32), 0, 1)
    lane = lax.broadcasted_iota(jnp.int32, (layers, rows, LANES), 2)
    tiles = _pieces(_moves(chips, block, True), 2 * half_f)
    outward = []
    for half in TWO:
        for index in range(half_f // LANES):
            tile = tiles[half * (half_f // LANES) + index]
            value = _gather_tile(lambda source: wide[:, :, _span(source, LANES)], tile, lane)
            if LANES * index >= 2 * chips * ROWS:
                position = lax.rem(lane + LANES * index % ROWS, ROWS)
                value = jnp.where(position < block - 2 * ROWS, value, 0.0)
            rows_out[half, :, :, _span(2 * ATTN + index, LANES)] = value.astype(jnp.bfloat16)
        outward += _moved([(rows_out.at[half], rows_hbm.at[half])], out_sems.at[half:half + 1])
    inward[5].wait()
    for part in COLORS:
        used = min(ROWS, block - ROWS * part)
        both = jnp.swapaxes(down_ref[ROWS * part:ROWS * part + used].astype(jnp.float32), 0, 1)
        for layer in range(layers):
            one = both[layer]
            if used < ROWS:
                one = jnp.concatenate([one, jnp.zeros((ROWS - used, width), jnp.float32)], axis=0)
            down_out[layer, :, _span(part, width)] = one.astype(jnp.bfloat16)
    _all_done(outward + _moved([(down_out, down_hbm)], out_sems.at[2:3]))


def _bounced(kernel, name, inputs, outs, arrays, n_sems):
    hbm = pl.BlockSpec(memory_space=pl.ANY)
    scratch = [pltpu.VMEM(array.shape, array.dtype) for array in arrays]
    return pl.pallas_call(
        kernel, name=name, out_shape=tuple(outs), in_specs=[hbm] * len(inputs), out_specs=(hbm,) * len(outs),
        scratch_shapes=scratch + [pltpu.SemaphoreType.DMA((size,)) for size in n_sems],
        compiler_params=pltpu.CompilerParams(vmem_limit_bytes=VMEM_LIMIT))(*inputs)


def pack_weights(w_q, w_k, w_v, w_o, w_up, w_down, chips):
    layers, rows = w_up.shape[:2]
    shape = jax.ShapeDtypeStruct
    inputs = [w_q.transpose(1, 2, 0, 3), w_k, w_v, w_o.transpose(1, 2, 0, 3), w_up.transpose(1, 0, 2),
              w_down.transpose(1, 0, 2)]
    outs = [shape((2, layers, rows, UP_END), jnp.bfloat16), shape((layers, ROWS, 3 * w_down.shape[2]), jnp.bfloat16)]
    return _bounced(functools.partial(pack_kernel, chips), "pack_weights", inputs, outs,
                    inputs + outs + [shape(w_up.shape, jnp.float32)], (6, 3))


def unpack_kernel(chips, *refs):
    sources, results, arrays, (in_sems, out_sems) = refs[:4], refs[4:12], refs[12:22], refs[22:]
    rows_ref, down_ref, q_out, k_out, v_out, o_out, up_out, down_out = arrays[:2] + arrays[4:]
    rows, layers, cols = up_out.shape
    block, _, width = down_out.shape
    heads = q_out.shape[1] // 2
    inward = _moved([(sources[which], arrays[which]) for which in (1, 0)], in_sems)
    inward[0].wait()
    for part in COLORS:
        used = min(ROWS, block - ROWS * part)
        for layer in range(layers):
            down_out[ROWS * part:ROWS * part + used, layer, :] = down_ref[layer, :used, _span(part, width)]
    inward[1].wait()
    outward = _moved([(down_out, results[5])], out_sems)
    lane = lax.broadcasted_iota(jnp.int32, (layers, rows, LANES), 2)
    per_half = STAGES * chips * ROWS // LANES

    def load(source):
        half, tile = divmod(source, per_half)
        return rows_ref[half, :, :, _span(2 * ATTN + tile, LANES)]

    through = _moved(zip(sources[2:], arrays[2:4]), in_sems.at[2:])
    for index, tile in enumerate(_pieces(_moves(chips, block, False), cols)):
        up_out[:, :, _span(index, LANES)] = jnp.swapaxes(_gather_tile(load, tile, lane), 0, 1)
    _all_done(through)
    outward += _moved(zip(arrays[2:4] + (up_out,), results[6:] + results[4:5]), out_sems.at[1:])
    for half, spots in enumerate(_head_spots(heads)):
        for at, which, head in spots:
            (q_out, o_out)[which // 3][:, head] = jnp.swapaxes(rows_ref[half, :, :, _span(at, LANES)], 0, 1)
        for layer in range(layers):
            for at, ref in ((heads, k_out), (heads + 1, v_out)):
                ref[layer, :, half, :] = rows_ref[half, layer, :, _span(at, LANES)]
    _all_done(outward + _moved(zip((q_out, k_out, v_out, o_out), results), out_sems.at[QKV:]))


def unpack_grads(row_grad, down_grad, y_loc, grad_x, shapes, chips):
    q_shape, k_shape, _, _, up_shape, down_shape = shapes
    layers, rows, heads, head_dim = q_shape
    shape = jax.ShapeDtypeStruct
    turned = [(rows, heads, layers, head_dim), k_shape, k_shape, (rows, heads, layers, head_dim),
              (rows, layers, up_shape[2]), (down_shape[1], layers, down_shape[2])]
    turned = [shape(full, jnp.float32) for full in turned]
    inputs = [row_grad, down_grad, y_loc, grad_x]
    outs = _bounced(functools.partial(unpack_kernel, chips), "unpack_grads", inputs,
                    turned + [shape(value.shape, value.dtype) for value in (y_loc, grad_x)], inputs + turned, (4, 8))
    d_q, d_k, d_v, d_o, d_up, d_down, y_out, dx_out = outs
    return (y_out[None], dx_out[None], d_q.transpose(2, 0, 1, 3), d_k, d_v, d_o.transpose(2, 0, 1, 3),
            d_up.transpose(1, 0, 2), d_down.transpose(1, 0, 2))


def solution(mesh):
    mesh4 = Mesh(mesh.devices.reshape(CUBE + (2,)), ALL_AXES)
    row_spec = P(ALL_AXES)
    weight_spec = P(None, ALL_AXES)

    def body(x_in, w_q, w_k, w_v, w_o, w_up, w_down, grad_out):
        weights = (w_q, w_k, w_v, w_o, w_up, w_down)
        chips = w_up.shape[2] // w_down.shape[1] // 2
        rows, down = pack_weights(*weights, chips)
        y_loc, grad_x, row_grad, down_grad = train_stack(x_in[0], grad_out[0], rows, down)
        return unpack_grads(row_grad, down_grad, y_loc, grad_x, [weight.shape for weight in weights], chips)

    return jax.shard_map(body, mesh=mesh4, in_specs=(row_spec,) + (weight_spec,) * 6 + (row_spec,),
                         out_specs=(row_spec, row_spec) + (weight_spec,) * 6, check_vma=False)
```

```python
import functools

import jax
import jax.numpy as jnp
from jax import lax
from jax.experimental import pallas as pl
from jax.experimental.pallas import tpu as pltpu
from jax.sharding import Mesh, PartitionSpec as P

MESH = pl.DeviceIdType.MESH
ALL_AXES = ("z", "y", "x", "c")
EPS = 1e-6
MASK_FILL = -1e30
DIMS = ("z", "y", "x")
ORDERS = (("x", "y", "z"), ("y", "z", "x"), ("z", "x", "y"))
COLS = 256
ROWS = 24
LAG = 2
WIDE = COLS // 2
HALF_ROWS = ROWS // 2
HEAD = 128
PER_HALF = 43
UP_BLOCKS = 25
UP_END = UP_BLOCKS * COLS
RING = 4
STAGES = 3
FINAL = STAGES - 1
CUBE = (RING, RING, RING)
CHIPS = RING ** STAGES
SLOTS = 3
TILE = 8
COLORS = range(3)
TWO = range(2)
SIX = range(6)
ALL = Ellipsis
EVERY = slice(None)
QKV, ATTN, FF = 4, 7, 18
DOWN_DONE = FF
UP_DONE = DOWN_DONE + FF
O_DONE = UP_DONE + ATTN - QKV
SIXTH = 6
DH_AT = SIXTH
O_AT = DH_AT + UP_DONE
QKV_AT = O_AT + SIXTH
NORM_MLP, GRAD, NORM_ATTN = 6, 7, 8
VMEM_LIMIT = 67043328


FIFTH = UP_END // 5
GELU_A = 0.7978845608028654
GELU_B = GELU_A * 0.044715
GELU_C = 0.5 * GELU_A
GELU_D = 1.5 * GELU_B
GATHER_SLOTS = SIXTH * LAG + RING


def _rows(color):
    return slice(TILE * color, TILE * color + TILE)


def _rem(value, by):
    return lax.rem(value, by)


def _block(color, stage, position):
    dims = tuple(dim for dim in DIMS if dim not in ORDERS[color][:stage])
    return tuple(position if dim == ORDERS[color][stage] else EVERY for dim in dims)


def _dot(left, right):
    return jnp.dot(left, right, preferred_element_type=jnp.float32)


def _dot_rhs_t(left, right):
    return lax.dot_general(left, right, (((1,), (1,)), ((), ())), preferred_element_type=jnp.float32)


def _dot_lhs_t(left, right):
    return lax.dot_general(left, right, (((0,), (0,)), ((), ())), preferred_element_type=jnp.float32)


def _at(start, size):
    return pl.ds(pl.multiple_of(start, size), size)


def _causal(seq):
    return (lax.rem(lax.broadcasted_iota(jnp.int32, (2 * seq, seq), 0), seq)
            >= lax.broadcasted_iota(jnp.int32, (2 * seq, seq), 1))


def _under(block):
    return jnp.concatenate([block[:, :HEAD], block[:, HEAD:]], axis=0)


def _beside(stacked):
    seq = stacked.shape[0] // 2
    return jnp.concatenate([stacked[:seq], stacked[seq:]], axis=1)


def _probs(query, key, causal):
    scores = jnp.where(causal, _dot_rhs_t(query, key) * (HEAD ** -0.5), MASK_FILL)
    weight = jnp.exp(scores - jnp.max(scores, axis=-1, keepdims=True))
    return weight / jnp.sum(weight, axis=-1, keepdims=True)


def _rms(values):
    wide = values.astype(jnp.float32)
    return (wide * lax.rsqrt(jnp.mean(wide * wide, axis=-1, keepdims=True) + EPS)).astype(jnp.bfloat16)


def _rms_back(values, grad):
    wide = values.astype(jnp.float32)
    scale = lax.rsqrt(jnp.mean(wide * wide, axis=-1, keepdims=True) + EPS)
    return scale * grad - wide * (scale * scale * scale) * jnp.mean(wide * grad, axis=-1, keepdims=True)


class Torus:
    def __init__(self, credit):
        self.core = lax.axis_index("c")
        self.place = {dim: lax.axis_index(dim) for dim in DIMS}
        self.near = tuple({dim: _rem(self.place[dim] + step, RING) for dim in DIMS} for step in (1, 3))
        self.far = {dim: _rem(self.place[dim] + 2, RING) for dim in DIMS}
        self.sibling = {"c": 1 - self.core}
        self.sides = ((0, self.core), (1, 1 - self.core))
        self.credit = credit
        self.partners = [({dim: self.near[way][dim]}, 2 * d + 1 - way, 2 * d + way)
                         for d, dim in enumerate(DIMS) for way in TWO]
        self.partners.append((self.sibling, 6, 6))

    def meet(self):
        barrier = pltpu.get_barrier_semaphore()
        for device, _, _ in self.partners:
            pl.semaphore_signal(barrier, inc=1, device_id=device, device_id_type=MESH)
        pl.semaphore_wait(barrier, len(self.partners))

    def remote(self, source, target, send_sem, recv_sem, device):
        return pltpu.make_async_remote_copy(src_ref=source, dst_ref=target, send_sem=send_sem, recv_sem=recv_sem,
                                            device_id=device, device_id_type=MESH)

    def run(self, steps, n_chunks, n_ticks, after):
        def tick(now, carry):
            @pl.when(now >= 2)
            def _():
                for _, _, mine in self.partners:
                    pl.semaphore_wait(self.credit.at[mine], 1)

            for lag, action in steps:
                @pl.when((now >= lag) & (now < lag + n_chunks))
                def _(lag=lag, action=action):
                    action(now - lag)
            after(now)

            @pl.when(now < n_ticks - 2)
            def _():
                for device, theirs, _ in self.partners:
                    pl.semaphore_signal(self.credit.at[theirs], inc=1, device_id=device, device_id_type=MESH)
            return carry

        lax.fori_loop(0, n_ticks, tick, 0)


def forward_steps(torus, n_layers, x_ref, rows_ref, down_ref, y_ref, saved, wbuf, peer, shard, twin, state, lefts, rights,
                  q_buf, k_buf, v_buf, hid_buf, acc, ring_send, ring_recv, pair_send, pair_recv, keep_sem, save_sem,
                  hid_sem, twin_sem):
    acts, w_out, hid_out, gelu_out, norm_out, q_out, k_out, v_out, o_out = saved
    core, place, near = torus.core, torus.place, torus.near
    slots = GATHER_SLOTS
    n_chunks = n_layers * PER_HALF
    ready = SIXTH * LAG
    seq = state.shape[0]
    third = CHIPS * ROWS
    last = n_layers - 1
    pieces = [(0, EVERY, slice(0, FIFTH)), (0, EVERY, slice(FIFTH, None))] + [
        (layer, EVERY, EVERY) for layer in range(1, n_layers)]
    swaps = [torus.remote(rows_ref.at[(1 - core,) + piece], twin.at[piece], twin_sem.at[0, order], twin_sem.at[1, order],
                          torus.sibling) for order, piece in enumerate(pieces)]
    for swap in swaps:
        swap.start()
    swaps[0].wait_send()
    swaps[0].wait_recv()

    def assemble(chunk):
        @pl.when(chunk == 1)
        def _():
            for swap in swaps[1:]:
                swap.wait_send()
                swap.wait_recv()

        @pl.when(chunk < 5 * n_layers)
        def _():
            layer, part = chunk // 5, _rem(chunk, 5)
            cols = _at(part * FIFTH, FIFTH)
            mine, other = [ref[layer, :, cols].astype(jnp.float32) for ref in (rows_ref.at[core], twin)]
            shard[layer, :, cols] = jnp.concatenate(
                [jnp.where(core == 0, mine, other), jnp.where(core == 0, other, mine)], axis=0).astype(jnp.bfloat16)

            @pl.when(part == 4)
            def _():
                shard[layer, :, UP_END:] = down_ref[layer]

    def columns(chunk):
        return _at(_rem(chunk, PER_HALF) * COLS, COLS)

    def spot(slot, color, stage, position, cols):
        order = ORDERS[color]
        index = tuple(EVERY if dim in order[:stage] else position if dim == order[stage] else place[dim]
                      for dim in DIMS)
        return wbuf.at[(slot,) + index + (_rows(color), cols)]

    halves = (slice(0, WIDE), slice(WIDE, COLS))

    def send_own(stage, chunk):
        slot, sem = _rem(chunk, slots), _rem(chunk, RING)
        for color in COLORS:
            dim = ORDERS[color][stage]
            here = spot(slot, color, stage, place[dim], slice(0, COLS))
            source = here
            if stage == 0:
                source = shard.at[chunk // PER_HALF, _rows(color), columns(chunk)]
            for way in TWO:
                torus.remote(source, here, ring_send.at[2 * stage, sem], ring_recv.at[2 * stage, sem],
                             {dim: near[way][dim]}).start()

    def send_far(stage, chunk):
        slot, sem = _rem(chunk, slots), _rem(chunk, RING)
        for color in COLORS:
            dim = ORDERS[color][stage]
            for way in TWO:
                block = spot(slot, color, stage, near[1 - way][dim], halves[way])
                torus.remote(block, block, ring_send.at[2 * stage + 1, sem], ring_recv.at[2 * stage + 1, sem],
                             {dim: near[way][dim]}).start()

    def arrived(part, chunk):
        slot, sem = _rem(chunk, slots), _rem(chunk, RING)
        count = slice(0, 2) if part % 2 == 0 else 0
        block = wbuf.at[(slot,) + (0,) * (2 - part // 2) + (count,)]
        whole = torus.remote(block, block, ring_send.at[part, sem], ring_recv.at[part, sem], torus.sibling)
        whole.wait_send()
        whole.wait_recv()

    def enter(chunk):
        wbuf[_rem(chunk, slots), place["z"], place["y"], place["x"]] = shard[chunk // PER_HALF, :, columns(chunk)]
        send_own(0, chunk)

    def pass_on(part, chunk):
        arrived(part, chunk)
        if part % 2 == 0:
            send_far(part // 2, chunk)
        else:
            send_own(part // 2 + 1, chunk)

    def pair_copy(chunk):
        slot = _rem(chunk, RING)
        return torus.remote(wbuf.at[_rem(chunk, slots)], peer.at[slot], pair_send.at[slot], pair_recv.at[slot],
                            torus.sibling)

    def exchange(chunk):
        arrived(5, chunk)
        pair_copy(chunk).start()

    def keep_copy(chunk):
        return pltpu.make_async_copy(wbuf.at[_rem(chunk, slots)],
                                     w_out.at[chunk // PER_HALF, :, :, :, :, columns(chunk)],
                                     keep_sem.at[_rem(chunk, RING)])

    def save_copies(layer, names):
        parts = {"n0": (lefts.at[NORM_ATTN], norm_out.at[layer, 0]), "n1": (lefts.at[NORM_MLP], norm_out.at[layer, 1]),
                 "q": (q_buf, q_out.at[layer]), "k": (k_buf, k_out.at[layer]), "v": (v_buf, v_out.at[layer]),
                 "o": (rights.at[O_AT:QKV_AT], o_out.at[layer]), "a": (lefts.at[:NORM_MLP], gelu_out.at[layer]),
                 "mid": (state, acts.at[2 * layer]), "end": (state, acts.at[2 * layer + 1])}
        places = list(parts)
        return [pltpu.make_async_copy(*parts[name], save_sem.at[places.index(name)]) for name in names]

    def save(layer, names):
        @pl.when(layer < last)
        def _():
            for copy in save_copies(layer, names):
                copy.start()

    def saved_all(layer, names):
        @pl.when(layer < last)
        def _():
            for copy in save_copies(layer, names):
                copy.wait()

    def hidden_copies(layer, order):
        slot, part, at = _rem(order, 2), order // SIXTH, _at(_rem(order, SIXTH) * COLS, COLS)
        return [pltpu.make_async_copy(hid_buf.at[slot, half], hid_out.at[layer, part, half, :, at],
                                      hid_sem.at[slot, half]) for half in TWO]

    def compute(chunk):
        layer, index = chunk // PER_HALF, _rem(chunk, PER_HALF)
        pair = pair_copy(chunk)
        pair.wait_send()
        pair.wait_recv()
        keep_copy(chunk).start()

        def weights(role):
            block = wbuf[_rem(chunk, slots)] if role == 0 else peer[_rem(chunk, RING)]
            return block.reshape(third, COLS)

        @pl.when(index == 0)
        def _():
            lefts[NORM_ATTN] = _rms(state[ALL])
            save(layer, ["n0"])

        @pl.when(index < 3)
        def _():
            for role, half in torus.sides:
                q_buf[:, _at(STAGES * COLS * half + COLS * index, COLS)] = _dot(
                    lefts[NORM_ATTN], weights(role)).astype(jnp.bfloat16)

        @pl.when(index == 3)
        def _():
            for role, half in torus.sides:
                both = _dot(lefts[NORM_ATTN], weights(role)).astype(jnp.bfloat16)
                k_buf[:, _at(HEAD * half, HEAD)] = both[:, :HEAD]
                v_buf[:, _at(HEAD * half, HEAD)] = both[:, HEAD:]

        @pl.when(index == QKV)
        def _():
            acc[ALL] = jnp.zeros_like(acc)
            save(layer, ["q", "k", "v"])

        @pl.when((index >= QKV) & (index < ATTN))
        def _():
            causal = _causal(seq)
            queries = [_under(q_buf[:, _at(STAGES * COLS * half + COLS * (index - QKV), COLS)]) for _, half in torus.sides]
            probs = [_probs(queries[role], k_buf[:, _at(HEAD * half, HEAD)], causal).astype(jnp.bfloat16)
                     for role, half in torus.sides]
            blocks = [_beside(_dot(probs[role], v_buf[:, _at(HEAD * half, HEAD)]).astype(jnp.bfloat16))
                      for role, half in torus.sides]
            acc[ALL] += sum(_dot_rhs_t(blocks[role], weights(role)) for role in TWO)
            for role, half in torus.sides:
                rights[O_AT + STAGES * half + index - QKV] = blocks[role]

        @pl.when(index == ATTN - 1)
        def _():
            @pl.when(layer > 0)
            def _():
                saved_all(layer - 1, ["end"])
            middle = (state[ALL].astype(jnp.float32) + acc[ALL]).astype(jnp.bfloat16)
            state[ALL] = middle
            lefts[NORM_MLP] = _rms(middle)
            save(layer, ["n1", "o"])
            mid = save_copies(layer, ["mid"])[0]
            mid.start()

        @pl.when((index > ATTN) & (index <= UP_BLOCKS))
        def _():
            for copy in hidden_copies(layer, index - ATTN - 1):
                copy.wait()

        @pl.when((index >= ATTN) & (index < UP_BLOCKS))
        def _():
            order = index - ATTN
            for role, half in torus.sides:
                hidden = _dot(lefts[NORM_MLP], weights(role))
                hid_buf[_rem(order, 2), half] = hidden
                lefts[STAGES * half + order // SIXTH, :, _at(COLS * _rem(order, SIXTH), COLS)] = jax.nn.gelu(
                    hidden).astype(jnp.bfloat16)
            for copy in hidden_copies(layer, order):
                copy.start()

        @pl.when(index == UP_BLOCKS)
        def _():
            save(layer, ["a"])
            save_copies(layer, ["mid"])[0].wait()

        @pl.when(index >= UP_BLOCKS)
        def _():
            part, at = (index - UP_BLOCKS) // SIXTH, _at(COLS * _rem(index - UP_BLOCKS, SIXTH), COLS)
            total = sum(_dot(lefts[STAGES * half + part], weights(role)) for role, half in torus.sides)

            @pl.when(part == 0)
            def _():
                acc[:, at] = total

            @pl.when(part > 0)
            def _():
                acc[:, at] += total

        @pl.when(index == PER_HALF - 1)
        def _():
            saved_all(layer, ["n0", "n1", "q", "k", "v", "o", "a"])
            result = (state[ALL].astype(jnp.float32) + acc[ALL]).astype(jnp.bfloat16)
            state[ALL] = result
            save(layer, ["end"])

            @pl.when(layer == last)
            def _():
                pltpu.make_async_copy(state, y_ref, save_sem.at[9]).start()

        keep_copy(chunk).wait()

    steps = [(0, assemble), (0, enter)]
    steps += [((part + 1) * LAG, functools.partial(pass_on, part)) for part in range(5)]
    return steps + [(ready, exchange), (ready + 1, compute)]


def backward_steps(torus, n_layers, x_ref, x_out, saved, out, wbuf, lefts, rights, hid_buf, dact, dnorm, q_buf,
                   k_buf, v_buf, x_buf, dk_acc, dv_acc, sums, half_bufs, full_bufs, load_sem, own_sem, push_send,
                   push_recv, pair_send, pair_recv, ring_send, ring_recv):
    acts, w_own, hid_in, gelu_in, norm_in, q_in, k_in, v_in, o_in = saved
    place, near = torus.place, torus.near
    seq = k_buf.shape[0]
    third = CHIPS * ROWS
    last = n_layers - 1

    def mine_slot(chunk):
        return GATHER_SLOTS + _rem(chunk, 2)

    def out_slot(chunk):
        return GATHER_SLOTS + 2 + _rem(chunk, 2)

    def their_slot(chunk):
        return 7 + _rem(chunk, SLOTS)

    def peer_slot(chunk):
        order = _rem(chunk, RING)
        return jnp.where(order == 0, 6, jnp.where(order == 3, 10, GATHER_SLOTS + 3 + order))

    def pair_of(chunk):
        return last - chunk // PER_HALF

    def columns(chunk):
        index = _rem(chunk, PER_HALF)
        block = jnp.where(index < DOWN_DONE, UP_BLOCKS + index,
                          jnp.where(index < UP_DONE, index - 11, jnp.where(index < O_DONE, index - 32, index - 39)))
        return _at(block * COLS, COLS)

    def loads(pair, names):
        parts = {"a": (gelu_in.at[pair], lefts.at[:NORM_MLP]), "n_mlp": (norm_in.at[pair, 1], lefts.at[NORM_MLP]),
                 "n_attn": (norm_in.at[pair, 0], lefts.at[NORM_ATTN]), "o": (o_in.at[pair], rights.at[O_AT:QKV_AT]),
                 "q": (q_in.at[pair], q_buf), "k": (k_in.at[pair], k_buf), "v": (v_in.at[pair], v_buf),
                 "x_mid": (acts.at[2 * pair], x_buf)}
        places = list(parts)
        return [pltpu.make_async_copy(*parts[name], load_sem.at[places.index(name)]) for name in names]

    def start(pair, names):
        for copy in loads(pair, names):
            copy.start()

    def finish(pair, names):
        for copy in loads(pair, names):
            copy.wait()

    def first_input(ref):
        return pltpu.make_async_copy(ref, x_buf, load_sem.at[9])

    def hidden_load(pair, part, half):
        return pltpu.make_async_copy(hid_in.at[pair, part, half], hid_buf, load_sem.at[8])

    def own_copy(chunk):
        return pltpu.make_async_copy(w_own.at[pair_of(chunk), :, :, :, :, columns(chunk)], wbuf.at[mine_slot(chunk)],
                                     own_sem.at[_rem(chunk, 2)])

    def push_copy(chunk):
        slot = _rem(chunk, SLOTS)
        return torus.remote(w_own.at[pair_of(chunk), :, :, :, :, columns(chunk)], wbuf.at[their_slot(chunk)],
                            push_send.at[slot], push_recv.at[slot], torus.sibling)

    def fetch(chunk):
        own_copy(chunk).start()
        push_copy(chunk).start()

    def total_grad():
        return jnp.concatenate([rights[block] for block in SIX], axis=1).astype(jnp.float32)

    def consume(chunk):
        pair, index = pair_of(chunk), _rem(chunk, PER_HALF)
        own_copy(chunk).wait()
        push = push_copy(chunk)
        push.wait_send()
        push.wait_recv()

        def weights(role):
            return wbuf[(mine_slot, their_slot)[role](chunk)].reshape(third, COLS)

        @pl.when(index == 0)
        def _():
            start(pair, ["x_mid"])

            @pl.when(pair < last)
            def _():
                start(pair, ["n_mlp", "n_attn", "o", "q", "k", "v"])

        def bend_back(part, half):
            hidden_load(pair, part, half).wait()
            for block in SIX:
                cols = slice(COLS * block, COLS * block + COLS)
                hidden = hid_buf[:, cols]
                square = hidden * hidden
                bend = jnp.tanh(hidden * (GELU_A + GELU_B * square))
                slope = (0.5 + 0.5 * bend) + (hidden * (1.0 - bend * bend)) * (GELU_C + GELU_D * square)
                rights[DH_AT + FF * half + SIXTH * part + block] = (dact[half, :, cols] * slope).astype(jnp.bfloat16)

        @pl.when((index > 0) & (index <= DOWN_DONE) & (_rem(index, SIXTH) == 0))
        def _():
            bend_back(index // SIXTH - 1, 1)

        @pl.when((index < DOWN_DONE) & (_rem(index, SIXTH) == 0))
        def _():
            dact[ALL] = jnp.zeros_like(dact)
            hidden_load(pair, index // SIXTH, 0).start()

        @pl.when(index < DOWN_DONE)
        def _():
            products = [_dot_rhs_t(rights[_rem(index, SIXTH)], weights(role)) for role in TWO]
            for role, half in torus.sides:
                dact[half] += products[role]

        @pl.when((index < DOWN_DONE) & (_rem(index, SIXTH) == 5))
        def _():
            bend_back(index // SIXTH, 0)
            hidden_load(pair, index // SIXTH, 1).start()

        @pl.when(index == DOWN_DONE - 1)
        def _():
            @pl.when(pair < last)
            def _():
                finish(pair, ["n_mlp", "n_attn", "o", "q", "k", "v"])

        @pl.when(index == DOWN_DONE)
        def _():
            dnorm[ALL] = jnp.zeros_like(dnorm)

            @pl.when(pair > 0)
            def _():
                start(pair - 1, ["a"])

        @pl.when((index >= DOWN_DONE) & (index < UP_DONE))
        def _():
            dnorm[ALL] += sum(_dot_rhs_t(rights[DH_AT + FF * half + index - DOWN_DONE], weights(role))
                              for role, half in torus.sides)

        @pl.when(index == UP_DONE - 1)
        def _():
            finish(pair, ["x_mid"])
            lefts[GRAD] = (total_grad() + _rms_back(x_buf[ALL], dnorm[ALL])).astype(jnp.bfloat16)

        @pl.when(index == UP_DONE)
        def _():
            @pl.when(pair == 0)
            def _():
                first_input(x_ref).start()

            @pl.when(pair > 0)
            def _():
                first_input(acts.at[2 * pair - 1]).start()
            dk_acc[ALL] = jnp.zeros_like(dk_acc)
            dv_acc[ALL] = jnp.zeros_like(dv_acc)

        @pl.when((index >= UP_DONE) & (index < O_DONE))
        def _():
            causal = _causal(seq)
            keys = [k_buf[:, _at(HEAD * half, HEAD)] for _, half in torus.sides]
            values = [v_buf[:, _at(HEAD * half, HEAD)] for _, half in torus.sides]
            queries = [_under(q_buf[:, _at(STAGES * COLS * half + COLS * (index - UP_DONE), COLS)])
                       for _, half in torus.sides]
            probs = [_probs(queries[role], keys[role], causal) for role in TWO]
            d_heads = [_under(_dot(lefts[GRAD], weights(role)).astype(jnp.bfloat16)) for role in TWO]
            d_probs = [_dot_rhs_t(d_heads[role], values[role]) for role in TWO]
            d_scores = [probs[role] * (d_probs[role] - jnp.sum(probs[role] * d_probs[role], axis=-1, keepdims=True))
                        for role in TWO]
            d_scores = [(d_score * (HEAD ** -0.5)).astype(jnp.bfloat16) for d_score in d_scores]
            d_v = [_dot_lhs_t(probs[role].astype(jnp.bfloat16), d_heads[role]) for role in TWO]
            d_k = [_dot_lhs_t(d_scores[role], queries[role]) for role in TWO]
            d_q = [_beside(_dot(d_scores[role], keys[role]).astype(jnp.bfloat16)) for role in TWO]
            for role, half in torus.sides:
                dv_acc[half] += d_v[role]
                dk_acc[half] += d_k[role]
                rights[QKV_AT + QKV * half + index - UP_DONE] = d_q[role]

        @pl.when(index == O_DONE - 1)
        def _():
            for half in TWO:
                rights[QKV_AT + QKV * half + QKV - 1] = jnp.concatenate([dk_acc[half], dv_acc[half]], axis=1).astype(jnp.bfloat16)

        @pl.when(index == O_DONE)
        def _():
            dnorm[ALL] = jnp.zeros_like(dnorm)

        @pl.when(index >= O_DONE)
        def _():
            dnorm[ALL] += sum(_dot_rhs_t(rights[QKV_AT + QKV * half + index - O_DONE], weights(role))
                              for role, half in torus.sides)

        @pl.when(index == PER_HALF - 1)
        def _():
            first_input(x_ref).wait()

            @pl.when(pair > 0)
            def _():
                finish(pair - 1, ["a"])
            result = (lefts[GRAD].astype(jnp.float32) + _rms_back(x_buf[ALL], dnorm[ALL])).astype(jnp.bfloat16)

            @pl.when(pair == 0)
            def _():
                x_out(result)
            for block in SIX:
                rights[block] = result[:, COLS * block:COLS * block + COLS]

    def pair_copy(chunk):
        slot = _rem(chunk, RING)
        return torus.remote(wbuf.at[out_slot(chunk)], wbuf.at[peer_slot(chunk)], pair_send.at[slot], pair_recv.at[slot],
                            torus.sibling)

    def multiply(chunk):
        index = _rem(chunk, PER_HALF)
        lead = _rem(chunk, sums[0].shape[0])
        quarter = third // RING
        for role, half in torus.sides[::-1]:
            left = jnp.where(index < DOWN_DONE, STAGES * half + index // SIXTH,
                             jnp.where(index < UP_DONE, NORM_MLP, jnp.where(index < O_DONE, GRAD, NORM_ATTN)))
            right = jnp.where(index < DOWN_DONE, _rem(index, SIXTH),
                              jnp.where(index < UP_DONE, DH_AT + FF * half + index - DOWN_DONE,
                                        jnp.where(index < O_DONE, O_AT + STAGES * half + index - UP_DONE,
                                                  QKV_AT + QKV * half + index - O_DONE)))
            for z in range(RING):
                part = _dot_lhs_t(lefts[left, :, quarter * z:quarter * z + quarter], rights[right])
                if role == 0:
                    sums[0][lead, z] = part.reshape(RING, RING, ROWS, COLS)
                else:
                    wbuf[out_slot(chunk), z] = part.astype(jnp.bfloat16).reshape(RING, RING, ROWS, COLS)
        pair_copy(chunk).start()

    def merge_pair(chunk):
        lead = _rem(chunk, sums[0].shape[0])
        pair_copy(chunk).wait_send()
        pair_copy(chunk).wait_recv()
        for z in range(RING):
            for y in range(RING):
                sums[0][lead, z, y] = sums[0][lead, z, y] + wbuf[peer_slot(chunk), z, y].astype(jnp.float32)

    def ring_copy(stage, part, slot, color, way):
        send, recv = (half_bufs, full_bufs)[part][stage]
        dim = ORDERS[color][stage]
        return torus.remote(send.at[slot, color, way], recv.at[slot, color, way],
                            ring_send.at[2 * stage + part, slot], ring_recv.at[2 * stage + part, slot],
                            {dim: near[way][dim]})

    def ring_wait(stage, part, slot):
        send, recv = (half_bufs, full_bufs)[part][stage]
        whole = torus.remote(send.at[slot], recv.at[slot], ring_send.at[2 * stage + part, slot],
                             ring_recv.at[2 * stage + part, slot], torus.sibling)
        whole.wait_send()
        whole.wait_recv()

    def source(stage, chunk, color, position, cols):
        lead = _rem(chunk, sums[stage].shape[0])
        if stage == 0:
            return sums[0][(lead,) + _block(color, 0, position) + (_rows(color), cols)]
        return sums[stage][(lead, color) + _block(color, stage, position) + (EVERY, cols)]

    left_cols, right_cols, every = slice(0, WIDE), slice(WIDE, COLS), slice(0, COLS)

    def store_halves(stage, chunk):
        slot = _rem(chunk, RING)
        send = half_bufs[stage][0]
        for color in COLORS:
            far = torus.far[ORDERS[color][stage]]
            send[slot, color, 0] = source(stage, chunk, color, far, left_cols).astype(jnp.bfloat16)
            send[slot, color, 1] = source(stage, chunk, color, far, right_cols).astype(jnp.bfloat16)

    def store_fulls(stage, chunk):
        slot = _rem(chunk, RING)
        ring_wait(stage, 0, slot)
        recv = half_bufs[stage][1]
        send = full_bufs[stage][0]
        lead = (EVERY,) * (len(send.shape) - 4)
        for color in COLORS:
            dim = ORDERS[color][stage]
            for way, summed, plain in ((0, left_cols, right_cols), (1, right_cols, left_cols)):
                send[(slot, color, way) + lead + (summed,)] = (
                    source(stage, chunk, color, near[way][dim], summed)
                    + recv[slot, color, way].astype(jnp.float32)).astype(jnp.bfloat16)
                send[(slot, color, way) + lead + (plain,)] = source(
                    stage, chunk, color, near[way][dim], plain).astype(jnp.bfloat16)

    def close_stage(stage, chunk):
        slot = _rem(chunk, RING)
        ring_wait(stage, 1, slot)
        recv = full_bufs[stage][1]
        for color in COLORS:
            dim = ORDERS[color][stage]
            total = (source(stage, chunk, color, place[dim], every)
                     + recv[slot, color, 0].astype(jnp.float32)
                     + recv[slot, color, 1].astype(jnp.float32))
            if stage < 2:
                sums[stage + 1][_rem(chunk, sums[stage + 1].shape[0]), color] = total
            else:
                out[pair_of(chunk), _rows(color), columns(chunk)] = total

    def send_all(stage, part, chunk):
        for color in COLORS:
            for way in TWO:
                ring_copy(stage, part, _rem(chunk, RING), color, way).start()

    def open_first(chunk):
        merge_pair(chunk)
        store_halves(0, chunk)
        send_all(0, 0, chunk)

    def middle(stage, chunk):
        store_fulls(stage, chunk)
        send_all(stage, 1, chunk)

    def open_stage(stage, chunk):
        store_halves(stage, chunk)
        send_all(stage, 0, chunk)

    def turn(stage, chunk):
        close_stage(stage, chunk)
        if stage < 2:
            open_stage(stage + 1, chunk)

    return [(0, fetch), (2 * LAG, functools.partial(middle, 0)), (LAG, open_first),
            (3 * LAG, functools.partial(turn, 0)), (4 * LAG, functools.partial(middle, 1)),
            (5 * LAG, functools.partial(turn, 1)), (SIXTH * LAG, functools.partial(middle, 2)),
            (7 * LAG, functools.partial(turn, 2)), (1, consume), (0, multiply)]


def train_kernel(n_layers, x_ref, g_ref, rows_in, down_in, y_ref, dx_ref, rows_hbm, down_hbm, *refs):
    saved, refs = refs[:9], refs[9:]
    (rows_ref, down_ref, rows_out, out), refs = refs[:4], refs[4:]
    (wbuf, peer, shard, twin, state, lefts, rights, q_buf, k_buf, v_buf, hid_out_buf, acc, hid_in_buf, dact, x_buf,
     dk_acc, dv_acc, away), refs = refs[:18], refs[18:]
    sums, half_bufs, full_bufs, refs = refs[:3], refs[3:9], refs[9:15], refs[15:]
    half_bufs = [half_bufs[2 * stage:2 * stage + 2] for stage in COLORS]
    full_bufs = [full_bufs[2 * stage:2 * stage + 2] for stage in COLORS]
    forward_sems, backward_sems, (swap_sem, end_sem, credit) = refs[:8], refs[8:16], refs[16:]
    torus = Torus(credit)
    core = torus.core
    n_chunks = n_layers * PER_HALF
    inward = _moved([(rows_in, rows_ref), (down_in, down_ref)], backward_sems[0])
    fill = pltpu.make_async_copy(x_ref, state, forward_sems[5].at[9])
    fill.start()
    for block in SIX:
        pltpu.make_async_copy(g_ref.at[:, COLS * block:COLS * block + COLS], rights.at[block],
                              backward_sems[0].at[3]).start()
    torus.meet()
    _all_done(inward)
    fill.wait()
    pltpu.make_async_copy(rights.at[:DH_AT], rights.at[:DH_AT], backward_sems[0].at[3]).wait()
    def y_copy():
        return pltpu.make_async_copy(state, y_ref, forward_sems[5].at[9])

    def x_out(result):
        y_copy().wait()
        state[ALL] = result
        pltpu.make_async_copy(state, dx_ref, forward_sems[5].at[9]).start()

    forward = forward_steps(torus, n_layers, x_ref, rows_ref, down_ref, y_ref, saved, wbuf, peer, shard, twin, state, lefts,
                            rights, q_buf, k_buf, v_buf, hid_out_buf, acc, *forward_sems)
    backward = backward_steps(torus, n_layers, x_ref, x_out, saved, out, wbuf, lefts, rights, hid_in_buf, dact, acc,
                              q_buf, k_buf, v_buf, x_buf, dk_acc, dv_acc, sums, half_bufs, full_bufs,
                              *backward_sems)
    turn_at = n_chunks
    backward = [(lag + turn_at, step) for lag, step in backward]
    n_ticks = turn_at + n_chunks + 7 * LAG
    def hand_over(layer, part):
        cols = _at(part * FIFTH, FIFTH)
        both = out[layer, :, cols]
        low, high = both[:HALF_ROWS], both[HALF_ROWS:]
        rows_out[core, layer, :, cols] = jnp.where(core == 0, low, high)
        away[layer, :, cols] = jnp.where(core == 0, high, low)
        torus.remote(away.at[layer, :, cols], rows_out.at[core, layer, :, cols], swap_sem.at[0, layer],
                     swap_sem.at[1, layer], torus.sibling).start()

    def down_result(layer):
        return pltpu.make_async_copy(out.at[layer, :, UP_END:], down_hbm.at[layer], end_sem.at[0, layer])

    def rows_result(layer):
        return pltpu.make_async_copy(rows_out.at[:, layer], rows_hbm.at[:, layer], end_sem.at[1, layer])

    def rows_meet(layer):
        swap = torus.remote(away.at[layer], rows_out.at[core, layer], swap_sem.at[0, layer], swap_sem.at[1, layer],
                            torus.sibling)
        swap.wait_send()
        swap.wait_recv()
        rows_result(layer).start()

    def hand_on(now):
        for layer in range(n_layers):
            begin = turn_at + (n_layers - layer) * PER_HALF + 8 * LAG

            @pl.when(now == begin - UP_BLOCKS)
            def _(layer=layer):
                down_result(layer).start()

            if layer > 0:
                @pl.when((now >= begin) & (now < begin + 5))
                def _(layer=layer, begin=begin):
                    hand_over(layer, now - begin)

                @pl.when(now == begin + 8)
                def _(layer=layer):
                    rows_meet(layer)

        @pl.when((now >= n_ticks - ATTN) & (now < n_ticks - ATTN + QKV))
        def _():
            hand_over(0, n_ticks - STAGES - now)

    torus.run(backward[:1] + forward + backward[1:], n_chunks, n_ticks, hand_on)
    hand_over(0, 0)
    rows_meet(0)
    for layer in range(n_layers):
        _all_done([down_result(layer), rows_result(layer)])
    pltpu.make_async_copy(state, dx_ref, forward_sems[5].at[9]).wait()


def train_stack(x_loc, g_loc, rows, down):
    n_layers = down.shape[0]
    seq, width = x_loc.shape
    bf16, f32 = jnp.bfloat16, jnp.float32
    half = WIDE
    chunk = CUBE + (ROWS, COLS)
    shape = jax.ShapeDtypeStruct
    hbm = pl.BlockSpec(memory_space=pl.ANY)
    vmem = pl.BlockSpec(memory_space=pltpu.VMEM)
    dma = pltpu.SemaphoreType.DMA
    saved = (shape((2 * n_layers - 1, seq, width), bf16), shape((n_layers,) + CUBE + (ROWS, PER_HALF * COLS), bf16),
             shape((n_layers, 3, 2, seq, width), f32), shape((n_layers, SIXTH, seq, width), bf16),
             shape((n_layers, 2, seq, width), bf16), shape((n_layers, seq, width), bf16),
             shape((n_layers, seq, 2 * HEAD), bf16), shape((n_layers, seq, 2 * HEAD), bf16),
             shape((n_layers, SIXTH, seq, COLS), bf16))
    scratch = [pltpu.VMEM(full, kind) for full, kind in (
        (rows.shape, bf16), (down.shape, bf16),
        ((2, n_layers, HALF_ROWS, UP_END), f32), ((n_layers, ROWS, PER_HALF * COLS), f32),
        ((GATHER_SLOTS + 6,) + chunk, bf16), ((RING,) + chunk, bf16), ((n_layers, ROWS, PER_HALF * COLS), bf16),
        (rows.shape[1:], bf16), ((seq, width), bf16), ((9, seq, width), bf16), ((56, seq, COLS), bf16),
        ((seq, SIXTH * COLS), bf16), ((seq, 2 * HEAD), bf16), ((seq, 2 * HEAD), bf16), ((2, 2, seq, COLS), f32),
        ((seq, width), f32), ((seq, width), f32), ((2, seq, width), f32), ((seq, width), bf16),
        ((2, seq, HEAD), f32), ((2, seq, HEAD), f32), ((n_layers, HALF_ROWS, UP_END), f32), ((6,) + chunk, f32),
        ((5, 3, RING, RING, TILE, COLS), f32), ((5, 3, RING, TILE, COLS), f32))]
    for cols in (half, COLS):
        for size in ((RING, RING), (RING,), ()):
            scratch += [pltpu.VMEM((RING, 3, 2) + size + (TILE, cols), bf16)] * 2
    scratch += [dma((SIXTH, RING)), dma((SIXTH, RING)), dma((RING,)), dma((RING,)), dma((RING,)), dma((10,)), dma((2, 2)), dma((2, n_layers + 1))]
    scratch += [dma((10,)), dma((2,)), dma((SLOTS,)), dma((SLOTS,)), dma((RING,)), dma((RING,)), dma((SIXTH, RING)),
                dma((SIXTH, RING)), dma((2, n_layers)), dma((2, n_layers)), pltpu.SemaphoreType.REGULAR((7,))]
    return pl.pallas_call(
        functools.partial(train_kernel, n_layers), name="train_stack",
        out_shape=(shape((seq, width), bf16), shape((seq, width), bf16), shape((2, n_layers, HALF_ROWS, UP_END), f32),
                   shape(down.shape, f32)) + saved,
        in_specs=[hbm] * 4, out_specs=(hbm,) * (4 + len(saved)), scratch_shapes=scratch,
        compiler_params=pltpu.CompilerParams(collective_id=0, has_side_effects=True, vmem_limit_bytes=VMEM_LIMIT),
    )(x_loc, g_loc, rows, down)[:4]


LANES = 128


def _moves(chips, block, packed_first):
    moves = []
    for half in TWO:
        for part in COLORS:
            for chip in range(chips):
                packed = chips * ROWS * (STAGES * half + part) + ROWS * chip
                plain = block * (2 * chip + half) + ROWS * part
                pair = (packed, plain) if packed_first else (plain, packed)
                moves.append(pair + (min(ROWS, block - ROWS * part),))
    return moves


def _pieces(moves, size):
    tiles = [[] for _ in range(size // LANES)]
    for target, source, length in moves:
        while length:
            step = min(length, LANES - target % LANES, LANES - source % LANES)
            tiles[target // LANES].append((target % LANES, source // LANES, (target - source) % LANES))
            target, source, length = target + step, source + step, length - step
    return [sorted(tile) for tile in tiles]


def _gather_tile(load, tile, lane):
    total = None
    for first, source, shift in tile:
        value = load(source)
        if shift:
            value = pltpu.roll(value, shift, axis=value.ndim - 1)
        total = value if total is None else jnp.where(lane >= first, value, total)
    return total


def _span(index, size):
    return slice(size * index, size * index + size)


def _moved(pairs, sems):
    copies = [pltpu.make_async_copy(source, target, sems.at[order]) for order, (source, target) in enumerate(pairs)]
    for copy in copies:
        copy.start()
    return copies


def _all_done(copies):
    for copy in copies:
        copy.wait()


def _head_spots(heads):
    return [[(head, 0, heads * half + head) for head in range(heads)]
            + [(heads + 2 + head, 3, heads * half + head) for head in range(heads)] for half in TWO]


def pack_kernel(chips, *refs):
    sources, (rows_hbm, down_hbm), arrays, refs = refs[:6], refs[6:8], refs[8:14], refs[14:]
    rows_out, down_out, wide, in_sems, out_sems = refs
    k_ref, v_ref, up_ref, down_ref = arrays[1], arrays[2], arrays[4], arrays[5]
    rows, layers, _ = up_ref.shape
    block, _, width = down_ref.shape
    heads = arrays[0].shape[1] // 2
    half_f = STAGES * chips * ROWS
    inward = _moved(zip(sources, arrays), in_sems)
    _all_done(inward[:QKV])
    for half, spots in enumerate(_head_spots(heads)):
        for at, which, head in spots:
            rows_out[half, :, :, _span(at, LANES)] = jnp.swapaxes(
                arrays[which][:, head].astype(jnp.float32), 0, 1).astype(jnp.bfloat16)
        for layer in range(layers):
            for at, ref in ((heads, k_ref), (heads + 1, v_ref)):
                rows_out[half, layer, :, _span(at, LANES)] = ref[layer].astype(
                    jnp.float32)[:, half].astype(jnp.bfloat16)
    inward[QKV].wait()
    wide[ALL] = jnp.swapaxes(up_ref[ALL].astype(jnp.float32), 0, 1)
    lane = lax.broadcasted_iota(jnp.int32, (layers, rows, LANES), 2)
    tiles = _pieces(_moves(chips, block, True), 2 * half_f)
    outward = []
    for half in TWO:
        for index in range(half_f // LANES):
            tile = tiles[half * (half_f // LANES) + index]
            value = _gather_tile(lambda source: wide[:, :, _span(source, LANES)], tile, lane)
            if LANES * index >= 2 * chips * ROWS:
                position = lax.rem(lane + LANES * index % ROWS, ROWS)
                value = jnp.where(position < block - 2 * ROWS, value, 0.0)
            rows_out[half, :, :, _span(2 * ATTN + index, LANES)] = value.astype(jnp.bfloat16)
        outward += _moved([(rows_out.at[half], rows_hbm.at[half])], out_sems.at[half:half + 1])
    inward[5].wait()
    for part in COLORS:
        used = min(ROWS, block - ROWS * part)
        both = jnp.swapaxes(down_ref[ROWS * part:ROWS * part + used].astype(jnp.float32), 0, 1)
        for layer in range(layers):
            one = both[layer]
            if used < ROWS:
                one = jnp.concatenate([one, jnp.zeros((ROWS - used, width), jnp.float32)], axis=0)
            down_out[layer, :, _span(part, width)] = one.astype(jnp.bfloat16)
    _all_done(outward + _moved([(down_out, down_hbm)], out_sems.at[2:3]))


def _bounced(kernel, name, inputs, outs, arrays, n_sems):
    hbm = pl.BlockSpec(memory_space=pl.ANY)
    scratch = [pltpu.VMEM(array.shape, array.dtype) for array in arrays]
    return pl.pallas_call(
        kernel, name=name, out_shape=tuple(outs), in_specs=[hbm] * len(inputs), out_specs=(hbm,) * len(outs),
        scratch_shapes=scratch + [pltpu.SemaphoreType.DMA((size,)) for size in n_sems],
        compiler_params=pltpu.CompilerParams(vmem_limit_bytes=VMEM_LIMIT))(*inputs)


def pack_weights(w_q, w_k, w_v, w_o, w_up, w_down, chips):
    layers, rows = w_up.shape[:2]
    shape = jax.ShapeDtypeStruct
    inputs = [w_q.transpose(1, 2, 0, 3), w_k, w_v, w_o.transpose(1, 2, 0, 3), w_up.transpose(1, 0, 2),
              w_down.transpose(1, 0, 2)]
    outs = [shape((2, layers, rows, UP_END), jnp.bfloat16), shape((layers, ROWS, 3 * w_down.shape[2]), jnp.bfloat16)]
    return _bounced(functools.partial(pack_kernel, chips), "pack_weights", inputs, outs,
                    inputs + outs + [shape(w_up.shape, jnp.float32)], (6, 3))


def unpack_kernel(chips, *refs):
    sources, results, arrays, (in_sems, out_sems) = refs[:4], refs[4:12], refs[12:22], refs[22:]
    rows_ref, down_ref, q_out, k_out, v_out, o_out, up_out, down_out = arrays[:2] + arrays[4:]
    rows, layers, cols = up_out.shape
    block, _, width = down_out.shape
    heads = q_out.shape[1] // 2
    order = (1, 0, 2, 3)
    inward = _moved([(sources[which], arrays[which]) for which in order], in_sems)
    inward[0].wait()
    for part in COLORS:
        used = min(ROWS, block - ROWS * part)
        for layer in range(layers):
            down_out[ROWS * part:ROWS * part + used, layer, :] = down_ref[layer, :used, _span(part, width)]
    inward[1].wait()
    outward = _moved([(down_out, results[5])], out_sems)
    lane = lax.broadcasted_iota(jnp.int32, (layers, rows, LANES), 2)
    per_half = STAGES * chips * ROWS // LANES

    def load(source):
        half, tile = divmod(source, per_half)
        return rows_ref[half, :, :, _span(2 * ATTN + tile, LANES)]

    _all_done(inward[2:])
    outward += _moved(zip(arrays[2:4], results[6:]), out_sems.at[1:])
    for index, tile in enumerate(_pieces(_moves(chips, block, False), cols)):
        up_out[:, :, _span(index, LANES)] = jnp.swapaxes(_gather_tile(load, tile, lane), 0, 1)
    outward += _moved([(up_out, results[4])], out_sems.at[STAGES:])
    for half, spots in enumerate(_head_spots(heads)):
        for at, which, head in spots:
            (q_out, o_out)[which // 3][:, head] = jnp.swapaxes(rows_ref[half, :, :, _span(at, LANES)], 0, 1)
        for layer in range(layers):
            for at, ref in ((heads, k_out), (heads + 1, v_out)):
                ref[layer, :, half, :] = rows_ref[half, layer, :, _span(at, LANES)]
    _all_done(outward + _moved(zip((q_out, k_out, v_out, o_out), results), out_sems.at[QKV:]))


def unpack_grads(row_grad, down_grad, y_loc, grad_x, shapes, chips):
    q_shape, k_shape, _, _, up_shape, down_shape = shapes
    layers, rows, heads, head_dim = q_shape
    shape = jax.ShapeDtypeStruct
    turned = [(rows, heads, layers, head_dim), k_shape, k_shape, (rows, heads, layers, head_dim),
              (rows, layers, up_shape[2]), (down_shape[1], layers, down_shape[2])]
    turned = [shape(full, jnp.float32) for full in turned]
    inputs = [row_grad, down_grad, y_loc, grad_x]
    outs = _bounced(functools.partial(unpack_kernel, chips), "unpack_grads", inputs,
                    turned + [shape(value.shape, value.dtype) for value in (y_loc, grad_x)], inputs + turned, (4, 8))
    d_q, d_k, d_v, d_o, d_up, d_down, y_out, dx_out = outs
    return (y_out[None], dx_out[None], d_q.transpose(2, 0, 1, 3), d_k, d_v, d_o.transpose(2, 0, 1, 3),
            d_up.transpose(1, 0, 2), d_down.transpose(1, 0, 2))


def solution(mesh):
    mesh4 = Mesh(mesh.devices.reshape(CUBE + (2,)), ALL_AXES)
    row_spec = P(ALL_AXES)
    weight_spec = P(None, ALL_AXES)

    def body(x_in, w_q, w_k, w_v, w_o, w_up, w_down, grad_out):
        weights = (w_q, w_k, w_v, w_o, w_up, w_down)
        chips = w_up.shape[2] // w_down.shape[1] // 2
        rows, down = pack_weights(*weights, chips)
        y_loc, grad_x, row_grad, down_grad = train_stack(x_in[0], grad_out[0], rows, down)
        return unpack_grads(row_grad, down_grad, y_loc, grad_x, [weight.shape for weight in weights], chips)

    return jax.shard_map(body, mesh=mesh4, in_specs=(row_spec,) + (weight_spec,) * 6 + (row_spec,),
                         out_specs=(row_spec, row_spec) + (weight_spec,) * 6, check_vma=False)
```
